8 devices in a mesh: sp: 8 (over z, y, x, core).
Axes of the slice: x: 2, y: 2, z: 1, core: 2. Of those that a mesh axis runs over, the one named last changes fastest.
Arguments:
- x_in: bfloat16 [2048, 2048], P('sp')
- positions: int32 [2048], P('sp')
- d_out: bfloat16 [2048, 2048], P('sp')
- norm1_gain: bfloat16 [2048], P('sp')
- norm2_gain: bfloat16 [2048], P('sp')
- w_q: bfloat16 [2048, 32, 64], P('sp')
- w_k: bfloat16 [2048, 8, 64], P('sp')
- w_v: bfloat16 [2048, 8, 64], P('sp')
- w_o: bfloat16 [32, 64, 2048], P('sp')
- w_gate: bfloat16 [2048, 8192], P('sp')
- w_up: bfloat16 [2048, 8192], P('sp')
- w_down: bfloat16 [8192, 2048], P('sp')
Outputs:
- output 1: bfloat16 [2048, 2048], P('sp')
- output 2: bfloat16 [2048, 2048], P('sp')
- output 3: float32 [2048], P('sp')
- output 4: float32 [2048], P('sp')
- output 5: float32 [2048, 32, 64], P('sp')
- output 6: float32 [2048, 8, 64], P('sp')
- output 7: float32 [2048, 8, 64], P('sp')
- output 8: float32 [32, 64, 2048], P('sp')
- output 9: float32 [2048, 8192], P('sp')
- output 10: float32 [2048, 8192], P('sp')
- output 11: float32 [8192, 2048], P('sp')
All inputs are finite; a program needn't handle non-finite values.
Results may differ from the reference program's by a relative error of at most 0.0179383.
Values are sent between devices in bfloat16 or wider.
A program may use at most 1 GiB of HBM per device.

```python
import math
import jax
import jax.numpy as jnp
from jax import lax

MODEL_DIM = 2048
FFN_DIM = 8192
Q_HEADS = 32
KV_HEADS = 8
HEAD_DIM = 64
SEQ_LEN = 2048

ROPE_BASE = 10000.0
NORM_EPS = 1e-5
NEG_LARGE = -1e30
GROUP_SIZE = Q_HEADS // KV_HEADS
HALF_DIM = HEAD_DIM // 2


def setup_inputs(seed: int = 0) -> dict:
    key_list = jax.random.split(jax.random.key(seed), 12)
    qk_gain = math.log(SEQ_LEN / 4.0) ** 0.25

    def normal_draw(key_one, shape, scale_by):
        return (jax.random.normal(key_one, shape, jnp.float32) * scale_by).astype(jnp.bfloat16)

    def gain_draw(key_one):
        return (0.6 + 0.8 * jax.random.uniform(key_one, (MODEL_DIM,), jnp.float32)).astype(jnp.bfloat16)

    pos_gaps = jax.random.randint(key_list[1], (SEQ_LEN,), 1, 4, jnp.int32)
    positions = (jnp.cumsum(pos_gaps) - pos_gaps[0]).astype(jnp.int32)
    return {
        'x_in': normal_draw(key_list[0], (SEQ_LEN, MODEL_DIM), 1.0),
        'positions': positions,
        'd_out': normal_draw(key_list[2], (SEQ_LEN, MODEL_DIM), 1.0),
        'norm1_gain': gain_draw(key_list[3]),
        'norm2_gain': gain_draw(key_list[4]),
        'w_q': normal_draw(key_list[5], (MODEL_DIM, Q_HEADS, HEAD_DIM), qk_gain * MODEL_DIM ** -0.5),
        'w_k': normal_draw(key_list[6], (MODEL_DIM, KV_HEADS, HEAD_DIM), qk_gain * MODEL_DIM ** -0.5),
        'w_v': normal_draw(key_list[7], (MODEL_DIM, KV_HEADS, HEAD_DIM), MODEL_DIM ** -0.5),
        'w_o': normal_draw(key_list[8], (Q_HEADS, HEAD_DIM, MODEL_DIM), (Q_HEADS * HEAD_DIM) ** -0.5),
        'w_gate': normal_draw(key_list[9], (MODEL_DIM, FFN_DIM), MODEL_DIM ** -0.5),
        'w_up': normal_draw(key_list[10], (MODEL_DIM, FFN_DIM), MODEL_DIM ** -0.5),
        'w_down': normal_draw(key_list[11], (FFN_DIM, MODEL_DIM), FFN_DIM ** -0.5),
    }


def keep_bf16(values_in):
    return values_in.astype(jnp.bfloat16).astype(jnp.float32)


def rms_norm(hidden, gain_vec):
    inv_rms = lax.rsqrt(jnp.mean(hidden * hidden, axis=-1, keepdims=True) + NORM_EPS)
    return keep_bf16(hidden * inv_rms * gain_vec)


def apply_rope(values_in, cos_tab, sin_tab):
    first_half = values_in[..., :HALF_DIM]
    second_half = values_in[..., HALF_DIM:]
    return jnp.concatenate([first_half * cos_tab - second_half * sin_tab, second_half * cos_tab + first_half * sin_tab], axis=-1)


def head_attention(operands):
    q_head, k_head, v_head = operands
    scores = jnp.dot(q_head, k_head.T, preferred_element_type=jnp.float32) * HEAD_DIM ** -0.5
    causal = jnp.arange(SEQ_LEN)[:, None] >= jnp.arange(SEQ_LEN)[None, :]
    attn_probs = jax.nn.softmax(jnp.where(causal, scores, NEG_LARGE), axis=-1)
    return keep_bf16(jnp.dot(keep_bf16(attn_probs), v_head, preferred_element_type=jnp.float32))


def layer_forward(x_f32, cos_tab, sin_tab, gain_first, gain_second, wq_f32, wk_f32, wv_f32, wo_f32, gate_f32, up_f32, down_f32):
    normed = rms_norm(x_f32, gain_first)
    q_lin = keep_bf16(jnp.einsum('td,dhe->the', normed, wq_f32))
    k_lin = keep_bf16(jnp.einsum('td,dhe->the', normed, wk_f32))
    v_lin = keep_bf16(jnp.einsum('td,dhe->the', normed, wv_f32))
    queries = keep_bf16(apply_rope(q_lin, cos_tab, sin_tab))
    keys_rot = keep_bf16(apply_rope(k_lin, cos_tab, sin_tab))
    keys_full = jnp.repeat(keys_rot, GROUP_SIZE, axis=1)
    values_full = jnp.repeat(v_lin, GROUP_SIZE, axis=1)
    attn_heads = lax.map(jax.checkpoint(head_attention), (queries.transpose(1, 0, 2), keys_full.transpose(1, 0, 2), values_full.transpose(1, 0, 2)))
    attn_proj = jnp.einsum('hte,hed->td', attn_heads, wo_f32)
    hidden = keep_bf16(x_f32 + attn_proj)
    mlp_in = rms_norm(hidden, gain_second)
    gate_act = keep_bf16(jnp.dot(mlp_in, gate_f32, preferred_element_type=jnp.float32))
    up_act = keep_bf16(jnp.dot(mlp_in, up_f32, preferred_element_type=jnp.float32))
    glu_out = keep_bf16(jax.nn.silu(gate_act) * up_act)
    return keep_bf16(hidden + jnp.dot(glu_out, down_f32, preferred_element_type=jnp.float32))


def reference(x_in, positions, d_out, norm1_gain, norm2_gain, w_q, w_k, w_v, w_o, w_gate, w_up, w_down):
    inv_freq = 1.0 / (ROPE_BASE ** (jnp.arange(HALF_DIM, dtype=jnp.float32) * (2.0 / HEAD_DIM)))
    angles = positions.astype(jnp.float32)[:, None] * inv_freq[None, :]
    cos_tab = jnp.cos(angles)[:, None, :]
    sin_tab = jnp.sin(angles)[:, None, :]

    def forward_fn(x_f32, gain_first, gain_second, wq_f32, wk_f32, wv_f32, wo_f32, gate_f32, up_f32, down_f32):
        return layer_forward(x_f32, cos_tab, sin_tab, gain_first, gain_second, wq_f32, wk_f32, wv_f32, wo_f32, gate_f32, up_f32, down_f32)

    to_f32 = [tensor.astype(jnp.float32) for tensor in (x_in, norm1_gain, norm2_gain, w_q, w_k, w_v, w_o, w_gate, w_up, w_down)]
    y_f32, pullback = jax.vjp(forward_fn, to_f32[0], to_f32[1], to_f32[2], to_f32[3], to_f32[4], to_f32[5], to_f32[6], to_f32[7], to_f32[8], to_f32[9])
    grad_list = pullback(d_out.astype(jnp.float32))
    return (y_f32.astype(jnp.bfloat16), grad_list[0].astype(jnp.bfloat16), grad_list[1], grad_list[2], grad_list[3], grad_list[4], grad_list[5], grad_list[6], grad_list[7], grad_list[8], grad_list[9])
```

```python
import functools
import jax
import jax.numpy as jnp
from jax import lax
from jax.experimental import pallas as pl
from jax.experimental.pallas import tpu as pltpu
from jax.sharding import PartitionSpec as P

ROPE_BASE = 10000.0
NORM_EPS = 1e-5
NEG_LARGE = -1e30
F32 = jnp.float32
BF16 = jnp.bfloat16
BLK = 256


def dot(lhs, rhs, lhs_dim, rhs_dim):
    return lax.dot_general(lhs, rhs, (((lhs_dim,), (rhs_dim,)), ((), ())), preferred_element_type=F32)


def norm_forward(hidden, gain_vec):
    inv_rms = lax.rsqrt(jnp.mean(hidden * hidden, axis=-1, keepdims=True) + NORM_EPS)
    return hidden * inv_rms * gain_vec


def rope_tables(positions, head_dim):
    half_dim = head_dim // 2
    inv_freq = 1.0 / (ROPE_BASE ** (jnp.arange(half_dim, dtype=F32) * (2.0 / head_dim)))
    angles = positions.astype(F32)[:, None] * inv_freq[None, :]
    return jnp.cos(angles)[:, None, :], jnp.sin(angles)[:, None, :]


def rotate(values_in, cos_tab, sin_tab):
    half_dim = values_in.shape[-1] // 2
    first_half = values_in[..., :half_dim].astype(F32)
    second_half = values_in[..., half_dim:].astype(F32)
    return jnp.concatenate([first_half * cos_tab - second_half * sin_tab, second_half * cos_tab + first_half * sin_tab], axis=-1)


def probs_transposed(k_rows, q_blk, start):
    scores = dot(k_rows, q_blk, 1, 1)
    rows = lax.broadcasted_iota(jnp.int32, (BLK, BLK), 0)
    cols = lax.broadcasted_iota(jnp.int32, (BLK, BLK), 1)
    tail = jnp.where(rows <= cols, scores[start:], NEG_LARGE)
    scores = jnp.concatenate([scores[:start], tail], axis=0) if start else tail
    top = jnp.max(scores, axis=0, keepdims=True)
    weights = jnp.exp((scores - top) * (q_blk.shape[1] ** -0.5))
    return weights * (1.0 / jnp.sum(weights, axis=0, keepdims=True))


def attention_fwd_kernel(q_ref, k_ref, v_ref, o_ref):
    seq_len = k_ref.shape[0]
    for start in range(0, seq_len, BLK):
        keys = pl.ds(0, start + BLK)
        probs = probs_transposed(k_ref[keys, :], q_ref[0, pl.ds(start, BLK), :], start)
        o_ref[0, pl.ds(start, BLK), :] = dot(probs.astype(BF16), v_ref[keys, :], 0, 0).astype(BF16)


def attention_bwd_kernel(q_ref, k_ref, v_ref, do_ref, dq_ref, dk_ref, dv_ref, dk_acc, dv_acc):
    seq_len, head_dim = k_ref.shape

    @pl.when(pl.program_id(0) == 0)
    def _():
        dk_acc[...] = jnp.zeros_like(dk_acc)
        dv_acc[...] = jnp.zeros_like(dv_acc)

    for start in range(0, seq_len, BLK):
        keys = pl.ds(0, start + BLK)
        rows = pl.ds(start, BLK)
        q_blk, do_blk = q_ref[0, rows, :], do_ref[0, rows, :]
        probs = probs_transposed(k_ref[keys, :], q_blk, start)
        d_probs = dot(v_ref[keys, :], do_blk, 1, 1).astype(BF16).astype(F32)
        row_dot = jnp.sum(d_probs * probs, axis=0, keepdims=True)
        d_scores = (probs * (d_probs - row_dot) * (head_dim ** -0.5)).astype(BF16)
        dq_ref[0, rows, :] = dot(d_scores, k_ref[keys, :], 0, 0).astype(BF16)
        dk_acc[keys, :] += dot(d_scores, q_blk, 1, 0)
        dv_acc[keys, :] += dot(probs.astype(BF16), do_blk, 1, 0)

    @pl.when(pl.program_id(0) == pl.num_programs(0) - 1)
    def _():
        dk_ref[...] = dk_acc[...].astype(BF16)
        dv_ref[...] = dv_acc[...].astype(BF16)


def head_spec(seq_len, head_dim):
    return pl.BlockSpec((1, seq_len, head_dim), lambda h: (h, 0, 0))


def full_spec(seq_len, head_dim):
    return pl.BlockSpec((seq_len, head_dim), lambda h: (0, 0))


def attention_forward(q_heads, keys, values):
    heads, seq_len, head_dim = q_heads.shape
    hs, fs = head_spec(seq_len, head_dim), full_spec(seq_len, head_dim)
    flops = 4 * heads * seq_len * seq_len * head_dim
    return pl.pallas_call(
        attention_fwd_kernel, grid=(heads,), in_specs=[hs, fs, fs], out_specs=hs,
        out_shape=jax.ShapeDtypeStruct(q_heads.shape, BF16), name='attn_fwd',
        cost_estimate=pl.CostEstimate(flops=flops, bytes_accessed=8 * heads * seq_len * head_dim, transcendentals=heads * seq_len * seq_len // 2),
    )(q_heads, keys, values)


def attention_backward(q_heads, keys, values, d_attn):
    heads, seq_len, head_dim = q_heads.shape
    hs, fs = head_spec(seq_len, head_dim), full_spec(seq_len, head_dim)
    flops = 10 * heads * seq_len * seq_len * head_dim
    kv_shape = jax.ShapeDtypeStruct(keys.shape, BF16)
    return pl.pallas_call(
        attention_bwd_kernel, grid=(heads,), in_specs=[hs, fs, fs, hs], out_specs=[hs, fs, fs],
        out_shape=[jax.ShapeDtypeStruct(q_heads.shape, BF16), kv_shape, kv_shape], name='attn_bwd',
        scratch_shapes=[pltpu.VMEM((seq_len, head_dim), F32), pltpu.VMEM((seq_len, head_dim), F32)],
        cost_estimate=pl.CostEstimate(flops=flops, bytes_accessed=8 * heads * seq_len * head_dim, transcendentals=heads * seq_len * seq_len // 2),
    )(q_heads, keys, values, d_attn)


def solution(mesh):
    n_dev = mesh.shape['sp']
    gather_rows = functools.partial(lax.all_gather, axis_name='sp', axis=0, tiled=True)
    scatter_rows = functools.partial(lax.psum_scatter, axis_name='sp', scatter_dimension=0, tiled=True)
    a2a = functools.partial(lax.all_to_all, axis_name='sp', tiled=True)

    def layer_step(x_in, positions, d_out, norm1_gain, norm2_gain, w_q, w_k, w_v, w_o, w_gate, w_up, w_down):
        tokens, model = x_in.shape
        seq_len = tokens * n_dev
        head_dim = w_q.shape[2]
        heads = w_q.shape[1] // n_dev
        rows_own = w_q.shape[0]
        gains = gather_rows(jnp.stack([norm1_gain, norm2_gain], axis=1))
        g1_full, g2_full = gains[:, 0].astype(F32), gains[:, 1].astype(F32)
        pos_all = gather_rows(positions)
        cos_tab, sin_tab = rope_tables(pos_all, head_dim)
        x_all = gather_rows(x_in)
        wo_all = gather_rows(w_o.reshape(-1, model))
        dout_all = gather_rows(d_out)
        to_cols = lambda w: w.transpose(1, 2, 0).reshape(n_dev, -1, rows_own)
        qkv_rows = jnp.concatenate([to_cols(w_q), to_cols(w_k), to_cols(w_v)], axis=1)
        qkv_w = a2a(qkv_rows, split_axis=0, concat_axis=2)[0]
        w13 = jnp.stack([w_gate, w_up])
        w13 = a2a(w13, split_axis=2, concat_axis=1)
        w1, w3 = w13[0], w13[1]

        normed = norm_forward(x_all.astype(F32), g1_full).astype(BF16)
        qkv = dot(normed, qkv_w, 1, 1).astype(BF16)
        split_q, split_k = heads * head_dim, (heads + 1) * head_dim
        q_rot = rotate(qkv[:, :split_q].reshape(seq_len, heads, head_dim), cos_tab, sin_tab).astype(BF16).transpose(1, 0, 2)
        k_rot = rotate(qkv[:, split_q:split_k][:, None, :], cos_tab, sin_tab).astype(BF16)[:, 0]
        v_lin = qkv[:, split_k:]
        o_heads = attention_forward(q_rot, k_rot, v_lin)
        o_cols = o_heads.transpose(1, 0, 2).reshape(seq_len, heads * head_dim)
        o_tok = a2a(o_cols, split_axis=0, concat_axis=1)
        hidden = (x_in.astype(F32) + dot(o_tok, wo_all, 1, 0)).astype(BF16)
        hidden_f32 = hidden.astype(F32)
        mlp_pre, norm2_pull = jax.vjp(norm_forward, hidden_f32, g2_full)
        mlp_in = gather_rows(mlp_pre.astype(BF16))
        gate_act = dot(mlp_in, w1, 1, 0).astype(BF16)
        up_act = dot(mlp_in, w3, 1, 0).astype(BF16)
        glu_pre, glu_pull = jax.vjp(lambda g, u: jax.nn.silu(g) * u, gate_act.astype(F32), up_act.astype(F32))
        glu_out = glu_pre.astype(BF16)
        y_out = (hidden_f32 + scatter_rows(dot(glu_out, w_down, 1, 0))).astype(BF16)

        d_down = dot(glu_out, dout_all, 0, 0)
        d_glu = dot(dout_all, w_down, 1, 1).astype(BF16)
        d_gate_f, d_up_f = glu_pull(d_glu.astype(F32))
        d_gate_act, d_up_act = d_gate_f.astype(BF16), d_up_f.astype(BF16)
        d_w13 = jnp.stack([dot(mlp_in, d_gate_act, 0, 0), dot(mlp_in, d_up_act, 0, 0)])
        d_w13 = a2a(d_w13, split_axis=1, concat_axis=2)
        d_mlp = scatter_rows(dot(d_gate_act, w1, 1, 1) + dot(d_up_act, w3, 1, 1)).astype(BF16)
        d_hidden_norm, d_g2 = norm2_pull(d_mlp.astype(F32))
        d_hidden = (d_out.astype(F32) + d_hidden_norm).astype(BF16)
        dh_all = gather_rows(d_hidden)
        wo_own = w_o.reshape(-1, model)
        d_wo = dot(o_cols, dh_all, 0, 0).reshape(w_o.shape)
        d_attn = dot(dh_all, wo_own, 1, 1).astype(BF16).reshape(seq_len, heads, head_dim).transpose(1, 0, 2)
        d_q_rot, d_k_rot, d_v = attention_backward(q_rot, k_rot, v_lin, d_attn)
        d_q = rotate(d_q_rot.transpose(1, 0, 2), cos_tab, -sin_tab).astype(BF16).reshape(seq_len, -1)
        d_k = rotate(d_k_rot[:, None, :], cos_tab, -sin_tab).astype(BF16)[:, 0]
        d_qkv = jnp.concatenate([d_q, d_k, d_v], axis=1)
        d_qkv_all = gather_rows(d_qkv.T)
        normed_own = a2a(norm_forward(x_in.astype(F32), g1_full).astype(BF16), split_axis=1, concat_axis=0)
        w_own = jnp.concatenate([to_cols(w_q), to_cols(w_k), to_cols(w_v)], axis=1).reshape(-1, rows_own)
        d_w_own = dot(d_qkv_all, normed_own, 1, 0).reshape(n_dev, -1, rows_own)
        from_cols = lambda d, w: d.reshape(w.shape[1], w.shape[2], rows_own).transpose(2, 0, 1)
        d_wq = from_cols(d_w_own[:, :split_q], w_q)
        d_wk = from_cols(d_w_own[:, split_q:split_k], w_k)
        d_wv = from_cols(d_w_own[:, split_k:], w_v)
        d_normed = a2a(dot(d_qkv_all, w_own, 0, 0).astype(BF16), split_axis=0, concat_axis=1)
        _, norm1_pull = jax.vjp(norm_forward, x_in.astype(F32), g1_full)
        d_x_norm, d_g1 = norm1_pull(d_normed.astype(F32))
        d_x = (d_hidden.astype(F32) + d_x_norm).astype(BF16)
        d_gains = scatter_rows(jnp.stack([d_g1, d_g2], axis=1))
        return (y_out, d_x, d_gains[:, 0], d_gains[:, 1], d_wq, d_wk, d_wv, d_wo, d_w13[0], d_w13[1], d_down)

    all_rows = P('sp')
    return jax.shard_map(layer_step, mesh=mesh, in_specs=(all_rows,) * 12, out_specs=(all_rows,) * 11, check_vma=False)
```

```python
import functools
import jax
import jax.numpy as jnp
from jax import lax
from jax.experimental import pallas as pl
from jax.experimental.pallas import tpu as pltpu
from jax.sharding import PartitionSpec as P

ROPE_BASE = 10000.0
NORM_EPS = 1e-5
NEG_LARGE = -1e30
F32 = jnp.float32
BF16 = jnp.bfloat16
BLK = 256


def dot(lhs, rhs, lhs_dim, rhs_dim):
    return lax.dot_general(lhs, rhs, (((lhs_dim,), (rhs_dim,)), ((), ())), preferred_element_type=F32)


def norm_forward(hidden, gain_vec):
    inv_rms = lax.rsqrt(jnp.mean(hidden * hidden, axis=-1, keepdims=True) + NORM_EPS)
    return hidden * inv_rms * gain_vec


def rope_tables(positions, head_dim):
    half_dim = head_dim // 2
    inv_freq = 1.0 / (ROPE_BASE ** (jnp.arange(half_dim, dtype=F32) * (2.0 / head_dim)))
    angles = positions.astype(F32)[:, None] * inv_freq[None, :]
    return jnp.cos(angles)[:, None, :], jnp.sin(angles)[:, None, :]


def rotate(values_in, cos_tab, sin_tab):
    half_dim = values_in.shape[-1] // 2
    first_half = values_in[..., :half_dim].astype(F32)
    second_half = values_in[..., half_dim:].astype(F32)
    return jnp.concatenate([first_half * cos_tab - second_half * sin_tab, second_half * cos_tab + first_half * sin_tab], axis=-1)


def probs_transposed(k_rows, q_blk, start):
    scores = dot(k_rows, q_blk, 1, 1)
    rows = lax.broadcasted_iota(jnp.int32, (BLK, BLK), 0)
    cols = lax.broadcasted_iota(jnp.int32, (BLK, BLK), 1)
    tail = jnp.where(rows <= cols, scores[start:], NEG_LARGE)
    scores = jnp.concatenate([scores[:start], tail], axis=0) if start else tail
    top = jnp.max(scores, axis=0, keepdims=True)
    weights = jnp.exp((scores - top) * (q_blk.shape[1] ** -0.5))
    return weights * (1.0 / jnp.sum(weights, axis=0, keepdims=True))


def attention_fwd_kernel(q_ref, k_ref, v_ref, o_ref):
    seq_len = k_ref.shape[0]
    for start in range(0, seq_len, BLK):
        keys = pl.ds(0, start + BLK)
        probs = probs_transposed(k_ref[keys, :], q_ref[0, pl.ds(start, BLK), :], start)
        o_ref[0, pl.ds(start, BLK), :] = dot(probs.astype(BF16), v_ref[keys, :], 0, 0).astype(BF16)


def attention_bwd_kernel(q_ref, k_ref, v_ref, do_ref, dq_ref, dk_ref, dv_ref, dk_acc, dv_acc):
    seq_len, head_dim = k_ref.shape

    @pl.when(pl.program_id(0) == 0)
    def _():
        dk_acc[...] = jnp.zeros_like(dk_acc)
        dv_acc[...] = jnp.zeros_like(dv_acc)

    for start in range(0, seq_len, BLK):
        keys = pl.ds(0, start + BLK)
        rows = pl.ds(start, BLK)
        q_blk, do_blk = q_ref[0, rows, :], do_ref[0, rows, :]
        probs = probs_transposed(k_ref[keys, :], q_blk, start)
        d_probs = dot(v_ref[keys, :], do_blk, 1, 1).astype(BF16).astype(F32)
        row_dot = jnp.sum(d_probs * probs, axis=0, keepdims=True)
        d_scores = (probs * (d_probs - row_dot) * (head_dim ** -0.5)).astype(BF16)
        dq_ref[0, rows, :] = dot(d_scores, k_ref[keys, :], 0, 0).astype(BF16)
        dk_acc[keys, :] += dot(d_scores, q_blk, 1, 0)
        dv_acc[keys, :] += dot(probs.astype(BF16), do_blk, 1, 0)

    @pl.when(pl.program_id(0) == pl.num_programs(0) - 1)
    def _():
        dk_ref[...] = dk_acc[...].astype(BF16)
        dv_ref[...] = dv_acc[...].astype(BF16)


def head_spec(seq_len, head_dim):
    return pl.BlockSpec((1, seq_len, head_dim), lambda h: (h, 0, 0))


def full_spec(seq_len, head_dim):
    return pl.BlockSpec((seq_len, head_dim), lambda h: (0, 0))


def attention_forward(q_heads, keys, values):
    heads, seq_len, head_dim = q_heads.shape
    hs, fs = head_spec(seq_len, head_dim), full_spec(seq_len, head_dim)
    flops = 4 * heads * seq_len * seq_len * head_dim
    return pl.pallas_call(
        attention_fwd_kernel, grid=(heads,), in_specs=[hs, fs, fs], out_specs=hs,
        out_shape=jax.ShapeDtypeStruct(q_heads.shape, BF16), name='attn_fwd',
        cost_estimate=pl.CostEstimate(flops=flops, bytes_accessed=8 * heads * seq_len * head_dim, transcendentals=heads * seq_len * seq_len // 2),
    )(q_heads, keys, values)


def attention_backward(q_heads, keys, values, d_attn):
    heads, seq_len, head_dim = q_heads.shape
    hs, fs = head_spec(seq_len, head_dim), full_spec(seq_len, head_dim)
    flops = 10 * heads * seq_len * seq_len * head_dim
    kv_shape = jax.ShapeDtypeStruct(keys.shape, BF16)
    return pl.pallas_call(
        attention_bwd_kernel, grid=(heads,), in_specs=[hs, fs, fs, hs], out_specs=[hs, fs, fs],
        out_shape=[jax.ShapeDtypeStruct(q_heads.shape, BF16), kv_shape, kv_shape], name='attn_bwd',
        scratch_shapes=[pltpu.VMEM((seq_len, head_dim), F32), pltpu.VMEM((seq_len, head_dim), F32)],
        cost_estimate=pl.CostEstimate(flops=flops, bytes_accessed=8 * heads * seq_len * head_dim, transcendentals=heads * seq_len * seq_len // 2),
    )(q_heads, keys, values, d_attn)


MESH = pl.DeviceIdType.MESH


def place(axis):
    me = lax.axis_index(axis)
    core = lax.rem(me, 2)
    col = lax.rem(lax.div(me, 2), 2)
    row = lax.div(me, 4)

    def other(flip_core, flip_col, flip_row):
        pick = lambda v, f: 1 - v if f else v
        return pick(row, flip_row) * 4 + pick(col, flip_col) * 2 + pick(core, flip_core)

    nbr_x, nbr_y = other(0, 1, 0), other(0, 0, 1)
    first = nbr_x * (1 - core) + nbr_y * core
    second = nbr_y * (1 - core) + nbr_x * core
    return me, other, first, second


def greet(other):
    barrier = pltpu.get_barrier_semaphore()
    for r in range(1, 8):
        pl.semaphore_signal(barrier, inc=1, device_id=(other(r & 1, (r >> 1) & 1, r >> 2),), device_id_type=MESH)
    pl.semaphore_wait(barrier, 7)


class Gather:
    def __init__(self, slot, send_sem, recv_sem, where, own=None):
        me, other, first, second = where
        partner, diag = other(1, 0, 0), other(0, 1, 1)
        own = slot(me) if own is None else own
        self.copies = []
        plan = [(own, me, first), (own, me, second), (own, me, partner), (slot(first), first, second),
                (slot(first), first, partner), (slot(second), second, partner), (slot(diag), diag, partner)]
        for i, (src, what, dest) in enumerate(plan):
            self.copies.append(pltpu.make_async_remote_copy(
                src_ref=src, dst_ref=slot(what), send_sem=send_sem.at[i], recv_sem=recv_sem.at[i],
                device_id=(dest,), device_id_type=MESH))

    def start(self):
        for i in range(3):
            self.copies[i].start()

    def got_first(self):
        self.copies[0].wait_recv()
        self.copies[3].start()
        self.copies[4].start()

    def got_second(self):
        self.copies[1].wait_recv()
        self.copies[5].start()

    def got_diag(self):
        self.copies[3].wait_recv()
        self.copies[6].start()

    def got_partner(self, i):
        self.copies[(2, 4, 5, 6)[i]].wait_recv()

    def drain(self):
        for copy in self.copies:
            copy.wait_send()


def turn_halves(values, cos_blk, sin_blk):
    width = values.shape[1]
    lanes = lax.broadcasted_iota(jnp.int32, values.shape, 1)
    partner = jnp.where(lax.rem(lanes, 64) < 32, pltpu.roll(values, width - 32, 1), pltpu.roll(values, 32, 1))
    return values * cos_blk + partner * sin_blk


def norm_backward(hidden, gain, d_out):
    inv = lax.rsqrt(jnp.mean(hidden * hidden, axis=-1, keepdims=True) + NORM_EPS)
    d_scaled = d_out * gain
    d_hidden = d_scaled * inv - hidden * (inv * inv * inv * jnp.mean(d_scaled * hidden, axis=-1, keepdims=True))
    return d_hidden, jnp.sum(d_out * (hidden * inv), axis=0, keepdims=True)


def attn_bwd_comm_kernel(axis, heads, dh_ref, wo_ref, ot_ref, q_ref, k_ref, v_ref, cos_ref, sin_ref, cosk_ref, sink_ref,
                         dw1_ref, dw3_ref, wown_ref, ut_ref, x_ref, g1_ref,
                         dwo_ref, dwq_ref, dwk_ref, dwv_ref, out1_ref, out3_ref, dx_ref, dg1_ref,
                         slots, do_scr, dk_acc, dv_acc, du_acc, du_scr, du_recv, stage,
                         bulk_send, bulk_recv, gat_send, gat_recv, du_send, du_rsem, loc_sem):
    where = place(axis)
    me, other, first, second = where
    greet(other)
    seq_len, head_dim = k_ref.shape
    rows_own, hid = stage.shape[1], stage.shape[2]
    tokens = x_ref.shape[0]
    qw = heads * head_dim

    rows_of = lambda d: pl.ds(pl.multiple_of(d * rows_own, rows_own), rows_own)
    hid_of = lambda d: pl.ds(pl.multiple_of(d * hid, hid), hid)
    bulk = []
    for n, r in enumerate((2, 4, 6, 3, 5, 7, 1)):
        dest = other(r & 1, (r >> 1) & 1, r >> 2)
        for i, (src, dst) in enumerate(((dw1_ref, out1_ref), (dw3_ref, out3_ref))):
            bulk.append(pltpu.make_async_remote_copy(
                src_ref=src.at[rows_of(dest), :], dst_ref=dst.at[:, hid_of(me)], send_sem=bulk_send.at[2 * n + i],
                recv_sem=bulk_recv.at[2 * n + i], device_id=(dest,), device_id_type=MESH))
            bulk[-1].start()
    for i, src in enumerate((dw1_ref, dw3_ref)):
        pltpu.make_async_copy(src.at[rows_of(me), :], stage.at[i], loc_sem.at[i]).start()

    for start in range(0, seq_len, BLK):
        rows = pl.ds(start, BLK)
        do_blk = dot(dh_ref[rows, :], wo_ref[...], 1, 1).astype(BF16)
        for h in range(heads):
            do_scr[h, rows, :] = do_blk[:, h * head_dim:(h + 1) * head_dim]
    for start in range(0, dwo_ref.shape[1], 512):
        cols = pl.ds(start, 512)
        dwo_ref[:, cols] = dot(ot_ref[...], dh_ref[:, cols], 1, 0)

    for i, (src, dst) in enumerate(((dw1_ref, out1_ref), (dw3_ref, out3_ref))):
        pltpu.make_async_copy(src.at[rows_of(me), :], stage.at[i], loc_sem.at[i]).wait()
        pltpu.make_async_copy(stage.at[i], dst.at[:, hid_of(me)], loc_sem.at[2 + i]).start()

    dk_acc[...] = jnp.zeros_like(dk_acc)
    dv_acc[...] = jnp.zeros_like(dv_acc)
    mine = slots.at[me]
    for h in range(heads):
        def one_block(start):
            keys = pl.ds(0, start + BLK)
            rows = pl.ds(start, BLK)
            q_blk, do_blk = q_ref[h, rows, :], do_scr[h, rows, :]
            probs = probs_transposed(k_ref[keys, :], q_blk, start)
            d_probs = dot(v_ref[keys, :], do_blk, 1, 1).astype(BF16).astype(F32)
            row_dot = jnp.sum(d_probs * probs, axis=0, keepdims=True)
            d_scores = (probs * (d_probs - row_dot) * (head_dim ** -0.5)).astype(BF16)
            mine[rows, h * head_dim:(h + 1) * head_dim] = dot(d_scores, k_ref[keys, :], 0, 0).astype(BF16)
            dk_acc[keys, :] += dot(d_scores, q_blk, 1, 0)
            dv_acc[keys, :] += dot(probs.astype(BF16), do_blk, 1, 0)
        for start in range(0, seq_len, BLK):
            one_block(start)
    mine[:, qw:qw + head_dim] = dk_acc[...].astype(BF16)
    mine[:, qw + head_dim:] = dv_acc[...].astype(BF16)
    for start in range(0, seq_len, BLK):
        rows = pl.ds(start, BLK)
        for h in range(0, qw, 128):
            cols = pl.ds(h, 128)
            mine[rows, cols] = turn_halves(mine[rows, cols].astype(F32), cos_ref[rows, :], -sin_ref[rows, :]).astype(BF16)
        cols = pl.ds(qw, 128)
        mine[rows, cols] = turn_halves(mine[rows, cols].astype(F32), cosk_ref[rows, :], -sink_ref[rows, :]).astype(BF16)

    gather = Gather(lambda d: slots.at[d], gat_send, gat_recv, where)
    gather.start()
    du_acc[...] = jnp.zeros_like(du_acc)

    def use(d):
        kv_rows = pl.ds(pl.multiple_of(d * head_dim, head_dim), head_dim)
        w_rows = pl.ds(pl.multiple_of(d * 384, 384), 384)
        for start in range(0, seq_len, 512):
            rows = pl.ds(start, 512)
            du_acc[rows, :] += dot(slots[d, rows, :], wown_ref[w_rows, :], 1, 0)
        d_w = dot(ut_ref[...], slots[d], 1, 0).T
        dwq_ref[pl.ds(pl.multiple_of(d * qw, qw), qw), :] = d_w[:qw]
        dwk_ref[kv_rows, :] = d_w[qw:qw + head_dim]
        dwv_ref[kv_rows, :] = d_w[qw + head_dim:]

    partner = other(1, 0, 0)
    use(me)
    gather.got_first()
    gather.got_second()
    use(first)
    use(second)
    gather.got_partner(0)
    use(partner)
    gather.got_diag()
    use(other(0, 1, 1))
    gather.got_partner(1)
    gather.got_partner(2)
    use(other(1, 1, 0))
    use(other(1, 0, 1))
    gather.got_partner(3)
    use(other(1, 1, 1))
    du_scr[...] = du_acc[...].astype(BF16)

    tok_of = lambda d: pl.ds(pl.multiple_of(d * tokens, tokens), tokens)
    sends = []
    for n, r in enumerate((6, 7, 2, 4, 3, 5, 1)):
        dest = other(r & 1, (r >> 1) & 1, r >> 2)
        sends.append(pltpu.make_async_remote_copy(
            src_ref=du_scr.at[tok_of(dest), :], dst_ref=du_recv.at[:, rows_of(me)], send_sem=du_send.at[n],
            recv_sem=du_rsem.at[n], device_id=(dest,), device_id_type=MESH))
        sends[-1].start()
    du_recv[:, rows_of(me)] = du_scr[tok_of(me), :]
    for copy in sends:
        copy.wait_recv()
    d_norm, d_gain = norm_backward(x_ref[...].astype(F32), g1_ref[...], du_recv[...].astype(F32))
    dx_ref[...] = (dh_ref[tok_of(me), :].astype(F32) + d_norm).astype(BF16)
    dg1_ref[...] = d_gain
    for copy in sends:
        copy.wait_send()
    gather.drain()
    for copy in bulk:
        copy.wait()
    for i, dst in enumerate((out1_ref, out3_ref)):
        pltpu.make_async_copy(stage.at[i], dst.at[:, hid_of(me)], loc_sem.at[2 + i]).wait()


def attention_backward_step(heads, dh_all, wo_own, o_t, q_rot, k_rot, v_lin, tables, d_w1, d_w3, w_own, u_t, x_in, g1):
    seq_len, model = dh_all.shape
    head_dim = k_rot.shape[1]
    tokens = x_in.shape[0]
    rows_own, hid = model // 8, d_w1.shape[1]
    shape = jax.ShapeDtypeStruct
    vmem, hbm = pl.BlockSpec(memory_space=pltpu.VMEM), pl.BlockSpec(memory_space=pl.ANY)
    dma = pltpu.SemaphoreType.DMA
    return pl.pallas_call(
        functools.partial(attn_bwd_comm_kernel, 'sp', heads), name='attn_bwd_comm',
        in_specs=[vmem] * 10 + [hbm] * 2 + [vmem] * 4,
        out_specs=[vmem] * 4 + [hbm] * 2 + [vmem] * 2,
        out_shape=[shape(wo_own.shape, F32), shape((8 * heads * head_dim, rows_own), F32), shape((8 * head_dim, rows_own), F32),
                   shape((8 * head_dim, rows_own), F32), shape((rows_own, 8 * hid), F32), shape((rows_own, 8 * hid), F32),
                   shape(x_in.shape, BF16), shape((1, model), F32)],
        scratch_shapes=[pltpu.VMEM((8, seq_len, 384), BF16), pltpu.VMEM((heads, seq_len, head_dim), BF16),
                        pltpu.VMEM((seq_len, head_dim), F32), pltpu.VMEM((seq_len, head_dim), F32),
                        pltpu.VMEM((seq_len, rows_own), F32), pltpu.VMEM((seq_len, rows_own), BF16),
                        pltpu.VMEM((tokens, model), BF16), pltpu.VMEM((2, rows_own, hid), F32),
                        dma((14,)), dma((14,)), dma((7,)), dma((7,)), dma((7,)), dma((7,)), dma((4,))],
        compiler_params=pltpu.CompilerParams(collective_id=2, has_side_effects=True, vmem_limit_bytes=63 * 1024 * 1024),
    )(dh_all, wo_own, o_t, q_rot, k_rot, v_lin, *tables, d_w1, d_w3, w_own, u_t, x_in, g1)


def solution(mesh):
    n_dev = mesh.shape['sp']
    gather_rows = functools.partial(lax.all_gather, axis_name='sp', axis=0, tiled=True)
    scatter_rows = functools.partial(lax.psum_scatter, axis_name='sp', scatter_dimension=0, tiled=True)
    a2a = functools.partial(lax.all_to_all, axis_name='sp', tiled=True)

    def layer_step(x_in, positions, d_out, norm1_gain, norm2_gain, w_q, w_k, w_v, w_o, w_gate, w_up, w_down):
        tokens, model = x_in.shape
        seq_len = tokens * n_dev
        head_dim = w_q.shape[2]
        heads = w_q.shape[1] // n_dev
        rows_own = w_q.shape[0]
        gains = gather_rows(jnp.stack([norm1_gain, norm2_gain], axis=1))
        g1_full, g2_full = gains[:, 0].astype(F32), gains[:, 1].astype(F32)
        pos_all = gather_rows(positions)
        cos_tab, sin_tab = rope_tables(pos_all, head_dim)
        x_all = gather_rows(x_in)
        wo_all = gather_rows(w_o.reshape(-1, model))
        dout_all = gather_rows(d_out)
        to_cols = lambda w: w.transpose(1, 2, 0).reshape(n_dev, -1, rows_own)
        qkv_rows = jnp.concatenate([to_cols(w_q), to_cols(w_k), to_cols(w_v)], axis=1)
        qkv_w = a2a(qkv_rows, split_axis=0, concat_axis=2)[0]
        w13 = jnp.stack([w_gate, w_up])
        w13 = a2a(w13, split_axis=2, concat_axis=1)
        w1, w3 = w13[0], w13[1]

        normed = norm_forward(x_all.astype(F32), g1_full).astype(BF16)
        qkv = dot(normed, qkv_w, 1, 1).astype(BF16)
        split_q, split_k = heads * head_dim, (heads + 1) * head_dim
        q_rot = rotate(qkv[:, :split_q].reshape(seq_len, heads, head_dim), cos_tab, sin_tab).astype(BF16).transpose(1, 0, 2)
        k_rot = rotate(qkv[:, split_q:split_k][:, None, :], cos_tab, sin_tab).astype(BF16)[:, 0]
        v_lin = qkv[:, split_k:]
        o_heads = attention_forward(q_rot, k_rot, v_lin)
        o_cols = o_heads.transpose(1, 0, 2).reshape(seq_len, heads * head_dim)
        o_tok = a2a(o_cols, split_axis=0, concat_axis=1)
        hidden = (x_in.astype(F32) + dot(o_tok, wo_all, 1, 0)).astype(BF16)
        hidden_f32 = hidden.astype(F32)
        mlp_pre, norm2_pull = jax.vjp(norm_forward, hidden_f32, g2_full)
        mlp_in = gather_rows(mlp_pre.astype(BF16))
        gate_act = dot(mlp_in, w1, 1, 0).astype(BF16)
        up_act = dot(mlp_in, w3, 1, 0).astype(BF16)
        glu_pre, glu_pull = jax.vjp(lambda g, u: jax.nn.silu(g) * u, gate_act.astype(F32), up_act.astype(F32))
        glu_out = glu_pre.astype(BF16)
        y_out = (hidden_f32 + scatter_rows(dot(glu_out, w_down, 1, 0))).astype(BF16)

        d_down = dot(glu_out, dout_all, 0, 0)
        d_glu = dot(dout_all, w_down, 1, 1).astype(BF16)
        d_gate_f, d_up_f = glu_pull(d_glu.astype(F32))
        d_gate_act, d_up_act = d_gate_f.astype(BF16), d_up_f.astype(BF16)
        d_w1s, d_w3s = dot(mlp_in, d_gate_act, 0, 0), dot(mlp_in, d_up_act, 0, 0)
        d_mlp = scatter_rows(dot(d_gate_act, w1, 1, 1) + dot(d_up_act, w3, 1, 1)).astype(BF16)
        d_hidden_norm, d_g2 = norm2_pull(d_mlp.astype(F32))
        d_hidden = (d_out.astype(F32) + d_hidden_norm).astype(BF16)
        dh_all = gather_rows(d_hidden)
        normed_own = a2a(norm_forward(x_in.astype(F32), g1_full).astype(BF16), split_axis=1, concat_axis=0)
        w_own = qkv_rows.reshape(-1, rows_own)
        cos2, sin2 = cos_tab[:, 0], sin_tab[:, 0]
        cos_lanes = jnp.concatenate([cos2] * 4, axis=1)
        sin_lanes = jnp.concatenate([-sin2, sin2] * 2, axis=1)
        cosk = jnp.concatenate([cos2, cos2, jnp.ones_like(cos2), jnp.ones_like(cos2)], axis=1)
        sink = jnp.concatenate([-sin2, sin2, jnp.zeros_like(cos2), jnp.zeros_like(cos2)], axis=1)
        d_wo, d_wq_t, d_wk_t, d_wv_t, d_w1, d_w3, d_x, d_g1 = attention_backward_step(
            heads, dh_all, w_o.reshape(-1, model), o_cols.T, q_rot, k_rot, v_lin, (cos_lanes, sin_lanes, cosk, sink),
            d_w1s, d_w3s, w_own, normed_own.T, x_in, g1_full[None])
        from_cols = lambda d, w: d.reshape(w.shape[1], w.shape[2], rows_own).transpose(2, 0, 1)
        d_gains = scatter_rows(jnp.stack([d_g1[0], d_g2], axis=1))
        return (y_out, d_x, d_gains[:, 0], d_gains[:, 1], from_cols(d_wq_t, w_q), from_cols(d_wk_t, w_k), from_cols(d_wv_t, w_v),
                d_wo.reshape(w_o.shape), d_w1, d_w3, d_down)

    all_rows = P('sp')
    return jax.shard_map(layer_step, mesh=mesh, in_specs=(all_rows,) * 12, out_specs=(all_rows,) * 11, check_vma=False)
```

```python
import functools
import jax
import jax.numpy as jnp
from jax import lax
from jax.experimental import pallas as pl
from jax.experimental.pallas import tpu as pltpu
from jax.sharding import PartitionSpec as P

ROPE_BASE = 10000.0
NORM_EPS = 1e-5
NEG_LARGE = -1e30
F32 = jnp.float32
BF16 = jnp.bfloat16
BLK = 256


def dot(lhs, rhs, lhs_dim, rhs_dim):
    return lax.dot_general(lhs, rhs, (((lhs_dim,), (rhs_dim,)), ((), ())), preferred_element_type=F32)


def norm_forward(hidden, gain_vec):
    inv_rms = lax.rsqrt(jnp.mean(hidden * hidden, axis=-1, keepdims=True) + NORM_EPS)
    return hidden * inv_rms * gain_vec


def rope_tables(positions, head_dim):
    half_dim = head_dim // 2
    inv_freq = 1.0 / (ROPE_BASE ** (jnp.arange(half_dim, dtype=F32) * (2.0 / head_dim)))
    angles = positions.astype(F32)[:, None] * inv_freq[None, :]
    return jnp.cos(angles)[:, None, :], jnp.sin(angles)[:, None, :]


def rotate(values_in, cos_tab, sin_tab):
    half_dim = values_in.shape[-1] // 2
    first_half = values_in[..., :half_dim].astype(F32)
    second_half = values_in[..., half_dim:].astype(F32)
    return jnp.concatenate([first_half * cos_tab - second_half * sin_tab, second_half * cos_tab + first_half * sin_tab], axis=-1)


def probs_transposed(k_rows, q_blk, start):
    scores = dot(k_rows, q_blk, 1, 1)
    rows = lax.broadcasted_iota(jnp.int32, (BLK, BLK), 0)
    cols = lax.broadcasted_iota(jnp.int32, (BLK, BLK), 1)
    tail = jnp.where(rows <= cols, scores[start:], NEG_LARGE)
    scores = jnp.concatenate([scores[:start], tail], axis=0) if start else tail
    top = jnp.max(scores, axis=0, keepdims=True)
    weights = jnp.exp((scores - top) * (q_blk.shape[1] ** -0.5))
    return weights * (1.0 / jnp.sum(weights, axis=0, keepdims=True))


def attention_fwd_kernel(q_ref, k_ref, v_ref, o_ref):
    seq_len = k_ref.shape[0]
    for start in range(0, seq_len, BLK):
        keys = pl.ds(0, start + BLK)
        probs = probs_transposed(k_ref[keys, :], q_ref[0, pl.ds(start, BLK), :], start)
        o_ref[0, pl.ds(start, BLK), :] = dot(probs.astype(BF16), v_ref[keys, :], 0, 0).astype(BF16)


def attention_bwd_kernel(q_ref, k_ref, v_ref, do_ref, dq_ref, dk_ref, dv_ref, dk_acc, dv_acc):
    seq_len, head_dim = k_ref.shape

    @pl.when(pl.program_id(0) == 0)
    def _():
        dk_acc[...] = jnp.zeros_like(dk_acc)
        dv_acc[...] = jnp.zeros_like(dv_acc)

    for start in range(0, seq_len, BLK):
        keys = pl.ds(0, start + BLK)
        rows = pl.ds(start, BLK)
        q_blk, do_blk = q_ref[0, rows, :], do_ref[0, rows, :]
        probs = probs_transposed(k_ref[keys, :], q_blk, start)
        d_probs = dot(v_ref[keys, :], do_blk, 1, 1).astype(BF16).astype(F32)
        row_dot = jnp.sum(d_probs * probs, axis=0, keepdims=True)
        d_scores = (probs * (d_probs - row_dot) * (head_dim ** -0.5)).astype(BF16)
        dq_ref[0, rows, :] = dot(d_scores, k_ref[keys, :], 0, 0).astype(BF16)
        dk_acc[keys, :] += dot(d_scores, q_blk, 1, 0)
        dv_acc[keys, :] += dot(probs.astype(BF16), do_blk, 1, 0)

    @pl.when(pl.program_id(0) == pl.num_programs(0) - 1)
    def _():
        dk_ref[...] = dk_acc[...].astype(BF16)
        dv_ref[...] = dv_acc[...].astype(BF16)


def head_spec(seq_len, head_dim):
    return pl.BlockSpec((1, seq_len, head_dim), lambda h: (h, 0, 0))


def full_spec(seq_len, head_dim):
    return pl.BlockSpec((seq_len, head_dim), lambda h: (0, 0))


def attention_forward(q_heads, keys, values):
    heads, seq_len, head_dim = q_heads.shape
    hs, fs = head_spec(seq_len, head_dim), full_spec(seq_len, head_dim)
    flops = 4 * heads * seq_len * seq_len * head_dim
    return pl.pallas_call(
        attention_fwd_kernel, grid=(heads,), in_specs=[hs, fs, fs], out_specs=hs,
        out_shape=jax.ShapeDtypeStruct(q_heads.shape, BF16), name='attn_fwd',
        cost_estimate=pl.CostEstimate(flops=flops, bytes_accessed=8 * heads * seq_len * head_dim, transcendentals=heads * seq_len * seq_len // 2),
    )(q_heads, keys, values)


def attention_backward(q_heads, keys, values, d_attn):
    heads, seq_len, head_dim = q_heads.shape
    hs, fs = head_spec(seq_len, head_dim), full_spec(seq_len, head_dim)
    flops = 10 * heads * seq_len * seq_len * head_dim
    kv_shape = jax.ShapeDtypeStruct(keys.shape, BF16)
    return pl.pallas_call(
        attention_bwd_kernel, grid=(heads,), in_specs=[hs, fs, fs, hs], out_specs=[hs, fs, fs],
        out_shape=[jax.ShapeDtypeStruct(q_heads.shape, BF16), kv_shape, kv_shape], name='attn_bwd',
        scratch_shapes=[pltpu.VMEM((seq_len, head_dim), F32), pltpu.VMEM((seq_len, head_dim), F32)],
        cost_estimate=pl.CostEstimate(flops=flops, bytes_accessed=8 * heads * seq_len * head_dim, transcendentals=heads * seq_len * seq_len // 2),
    )(q_heads, keys, values, d_attn)


MESH = pl.DeviceIdType.MESH


def place(axis):
    me = lax.axis_index(axis)
    core = lax.rem(me, 2)
    col = lax.rem(lax.div(me, 2), 2)
    row = lax.div(me, 4)

    def other(flip_core, flip_col, flip_row):
        pick = lambda v, f: 1 - v if f else v
        return pick(row, flip_row) * 4 + pick(col, flip_col) * 2 + pick(core, flip_core)

    nbr_x, nbr_y = other(0, 1, 0), other(0, 0, 1)
    first = nbr_x * (1 - core) + nbr_y * core
    second = nbr_y * (1 - core) + nbr_x * core
    return me, other, first, second


def greet(other):
    barrier = pltpu.get_barrier_semaphore()
    for r in range(1, 8):
        pl.semaphore_signal(barrier, inc=1, device_id=(other(r & 1, (r >> 1) & 1, r >> 2),), device_id_type=MESH)
    pl.semaphore_wait(barrier, 7)


class Gather:
    def __init__(self, slot, send_sem, recv_sem, where, own=None):
        me, other, first, second = where
        partner, diag = other(1, 0, 0), other(0, 1, 1)
        own = slot(me) if own is None else own
        self.copies = []
        plan = [(own, me, first), (own, me, second), (own, me, partner), (slot(first), first, second),
                (slot(first), first, partner), (slot(second), second, partner), (slot(diag), diag, partner)]
        for i, (src, what, dest) in enumerate(plan):
            self.copies.append(pltpu.make_async_remote_copy(
                src_ref=src, dst_ref=slot(what), send_sem=send_sem.at[i], recv_sem=recv_sem.at[i],
                device_id=(dest,), device_id_type=MESH))

    def start(self):
        for i in range(3):
            self.copies[i].start()

    def got_first(self):
        self.copies[0].wait_recv()
        self.copies[3].start()
        self.copies[4].start()

    def got_second(self):
        self.copies[1].wait_recv()
        self.copies[5].start()

    def got_diag(self):
        self.copies[3].wait_recv()
        self.copies[6].start()

    def got_partner(self, i):
        self.copies[(2, 4, 5, 6)[i]].wait_recv()

    def drain(self):
        for copy in self.copies:
            copy.wait_send()


def turn_halves(values, cos_blk, sin_blk):
    width = values.shape[1]
    lanes = lax.broadcasted_iota(jnp.int32, values.shape, 1)
    partner = jnp.where(lax.rem(lanes, 64) < 32, pltpu.roll(values, width - 32, 1), pltpu.roll(values, 32, 1))
    return values * cos_blk + partner * sin_blk


def norm_backward(hidden, gain, d_out):
    inv = lax.rsqrt(jnp.mean(hidden * hidden, axis=-1, keepdims=True) + NORM_EPS)
    d_scaled = d_out * gain
    d_hidden = d_scaled * inv - hidden * (inv * inv * inv * jnp.mean(d_scaled * hidden, axis=-1, keepdims=True))
    return d_hidden, jnp.sum(d_out * (hidden * inv), axis=0, keepdims=True)


def attn_bwd_comm_kernel(axis, heads, dh_ref, wo_ref, ot_ref, q_ref, k_ref, v_ref, cos_ref, sin_ref, cosk_ref, sink_ref,
                         dw1_ref, dw3_ref, wown_ref, ut_ref, x_ref, g1_ref,
                         dwo_ref, dwq_ref, dwk_ref, dwv_ref, out1_ref, out3_ref, dx_ref, dg1_ref,
                         slots, do_scr, dk_acc, dv_acc, du_acc, du_scr, du_recv, stage,
                         bulk_send, bulk_recv, gat_send, gat_recv, du_send, du_rsem, loc_sem):
    where = place(axis)
    me, other, first, second = where
    greet(other)
    seq_len, head_dim = k_ref.shape
    rows_own, hid = stage.shape[1], stage.shape[2]
    tokens = x_ref.shape[0]
    qw = heads * head_dim

    rows_of = lambda d: pl.ds(pl.multiple_of(d * rows_own, rows_own), rows_own)
    hid_of = lambda d: pl.ds(pl.multiple_of(d * hid, hid), hid)
    bulk = []
    for n, r in enumerate((2, 4, 6, 3, 5, 7, 1)):
        dest = other(r & 1, (r >> 1) & 1, r >> 2)
        for i, (src, dst) in enumerate(((dw1_ref, out1_ref), (dw3_ref, out3_ref))):
            bulk.append(pltpu.make_async_remote_copy(
                src_ref=src.at[rows_of(dest), :], dst_ref=dst.at[:, hid_of(me)], send_sem=bulk_send.at[2 * n + i],
                recv_sem=bulk_recv.at[2 * n + i], device_id=(dest,), device_id_type=MESH))
            bulk[-1].start()
    for i, src in enumerate((dw1_ref, dw3_ref)):
        pltpu.make_async_copy(src.at[rows_of(me), :], stage.at[i], loc_sem.at[i]).start()

    for start in range(0, seq_len, BLK):
        rows = pl.ds(start, BLK)
        do_blk = dot(dh_ref[rows, :], wo_ref[...], 1, 1).astype(BF16)
        for h in range(heads):
            do_scr[h, rows, :] = do_blk[:, h * head_dim:(h + 1) * head_dim]
    for start in range(0, dwo_ref.shape[1], 512):
        cols = pl.ds(start, 512)
        dwo_ref[:, cols] = dot(ot_ref[...], dh_ref[:, cols], 1, 0)

    for i, (src, dst) in enumerate(((dw1_ref, out1_ref), (dw3_ref, out3_ref))):
        pltpu.make_async_copy(src.at[rows_of(me), :], stage.at[i], loc_sem.at[i]).wait()
        pltpu.make_async_copy(stage.at[i], dst.at[:, hid_of(me)], loc_sem.at[2 + i]).start()

    dk_acc[...] = jnp.zeros_like(dk_acc)
    dv_acc[...] = jnp.zeros_like(dv_acc)
    mine = slots.at[me]
    for h in range(heads):
        def one_block(start):
            keys = pl.ds(0, start + BLK)
            rows = pl.ds(start, BLK)
            q_blk, do_blk = q_ref[h, rows, :], do_scr[h, rows, :]
            probs = probs_transposed(k_ref[keys, :], q_blk, start)
            d_probs = dot(v_ref[keys, :], do_blk, 1, 1).astype(BF16).astype(F32)
            row_dot = jnp.sum(d_probs * probs, axis=0, keepdims=True)
            d_scores = (probs * (d_probs - row_dot) * (head_dim ** -0.5)).astype(BF16)
            mine[rows, h * head_dim:(h + 1) * head_dim] = dot(d_scores, k_ref[keys, :], 0, 0).astype(BF16)
            dk_acc[keys, :] += dot(d_scores, q_blk, 1, 0)
            dv_acc[keys, :] += dot(probs.astype(BF16), do_blk, 1, 0)
        for start in range(0, seq_len, BLK):
            one_block(start)
    mine[:, qw:qw + head_dim] = dk_acc[...].astype(BF16)
    mine[:, qw + head_dim:] = dv_acc[...].astype(BF16)
    for start in range(0, seq_len, BLK):
        rows = pl.ds(start, BLK)
        for h in range(0, qw, 128):
            cols = pl.ds(h, 128)
            mine[rows, cols] = turn_halves(mine[rows, cols].astype(F32), cos_ref[rows, :], -sin_ref[rows, :]).astype(BF16)
        cols = pl.ds(qw, 128)
        mine[rows, cols] = turn_halves(mine[rows, cols].astype(F32), cosk_ref[rows, :], -sink_ref[rows, :]).astype(BF16)

    gather = Gather(lambda d: slots.at[d], gat_send, gat_recv, where)
    gather.start()
    du_acc[...] = jnp.zeros_like(du_acc)

    def use(d):
        kv_rows = pl.ds(pl.multiple_of(d * head_dim, head_dim), head_dim)
        w_rows = pl.ds(pl.multiple_of(d * 384, 384), 384)
        for start in range(0, seq_len, 512):
            rows = pl.ds(start, 512)
            du_acc[rows, :] += dot(slots[d, rows, :], wown_ref[w_rows, :], 1, 0)
        d_w = dot(ut_ref[...], slots[d], 1, 0).T
        dwq_ref[pl.ds(pl.multiple_of(d * qw, qw), qw), :] = d_w[:qw]
        dwk_ref[kv_rows, :] = d_w[qw:qw + head_dim]
        dwv_ref[kv_rows, :] = d_w[qw + head_dim:]

    partner = other(1, 0, 0)
    use(me)
    gather.got_first()
    gather.got_second()
    use(first)
    use(second)
    gather.got_partner(0)
    use(partner)
    gather.got_diag()
    use(other(0, 1, 1))
    gather.got_partner(1)
    gather.got_partner(2)
    use(other(1, 1, 0))
    use(other(1, 0, 1))
    gather.got_partner(3)
    use(other(1, 1, 1))
    du_scr[...] = du_acc[...].astype(BF16)

    tok_of = lambda d: pl.ds(pl.multiple_of(d * tokens, tokens), tokens)
    sends = []
    for n, r in enumerate((6, 7, 2, 4, 3, 5, 1)):
        dest = other(r & 1, (r >> 1) & 1, r >> 2)
        sends.append(pltpu.make_async_remote_copy(
            src_ref=du_scr.at[tok_of(dest), :], dst_ref=du_recv.at[:, rows_of(me)], send_sem=du_send.at[n],
            recv_sem=du_rsem.at[n], device_id=(dest,), device_id_type=MESH))
        sends[-1].start()
    du_recv[:, rows_of(me)] = du_scr[tok_of(me), :]
    for copy in sends:
        copy.wait_recv()
    dg1_ref[...] = jnp.zeros_like(dg1_ref)

    def input_grad(k, _):
        part = pl.ds(pl.multiple_of(k * 16, 16), 16)
        d_norm, d_gain = norm_backward(x_ref[part, :].astype(F32), g1_ref[...], du_recv[part, :].astype(F32))
        dh_part = dh_ref[pl.ds(pl.multiple_of(me * tokens + k * 16, 16), 16), :]
        dx_ref[part, :] = (dh_part.astype(F32) + d_norm).astype(BF16)
        dg1_ref[...] += d_gain
        return 0
    lax.fori_loop(0, tokens // 16, input_grad, 0)
    for copy in sends:
        copy.wait_send()
    gather.drain()
    for copy in bulk:
        copy.wait()
    for i, dst in enumerate((out1_ref, out3_ref)):
        pltpu.make_async_copy(stage.at[i], dst.at[:, hid_of(me)], loc_sem.at[2 + i]).wait()


def attention_backward_step(heads, dh_all, wo_own, o_t, q_rot, k_rot, v_lin, tables, d_w1, d_w3, w_own, u_t, x_in, g1):
    seq_len, model = dh_all.shape
    head_dim = k_rot.shape[1]
    tokens = x_in.shape[0]
    rows_own, hid = model // 8, d_w1.shape[1]
    shape = jax.ShapeDtypeStruct
    vmem, hbm = pl.BlockSpec(memory_space=pltpu.VMEM), pl.BlockSpec(memory_space=pl.ANY)
    dma = pltpu.SemaphoreType.DMA
    return pl.pallas_call(
        functools.partial(attn_bwd_comm_kernel, 'sp', heads), name='attn_bwd_comm',
        in_specs=[vmem] * 10 + [hbm] * 2 + [vmem] * 4,
        out_specs=[vmem] * 4 + [hbm] * 2 + [vmem] * 2,
        out_shape=[shape(wo_own.shape, F32), shape((8 * heads * head_dim, rows_own), F32), shape((8 * head_dim, rows_own), F32),
                   shape((8 * head_dim, rows_own), F32), shape((rows_own, 8 * hid), F32), shape((rows_own, 8 * hid), F32),
                   shape(x_in.shape, BF16), shape((1, model), F32)],
        scratch_shapes=[pltpu.VMEM((8, seq_len, 384), BF16), pltpu.VMEM((heads, seq_len, head_dim), BF16),
                        pltpu.VMEM((seq_len, head_dim), F32), pltpu.VMEM((seq_len, head_dim), F32),
                        pltpu.VMEM((seq_len, rows_own), F32), pltpu.VMEM((seq_len, rows_own), BF16),
                        pltpu.VMEM((tokens, model), BF16), pltpu.VMEM((2, rows_own, hid), F32),
                        dma((14,)), dma((14,)), dma((7,)), dma((7,)), dma((7,)), dma((7,)), dma((4,))],
        compiler_params=pltpu.CompilerParams(collective_id=2, has_side_effects=True, vmem_limit_bytes=63 * 1024 * 1024),
    )(dh_all, wo_own, o_t, q_rot, k_rot, v_lin, *tables, d_w1, d_w3, w_own, u_t, x_in, g1)


def mlp_comm_kernel(axis, m_ref, dout_ref, w1_ref, w3_ref, w2_ref, h_ref, g2_ref,
                    dw1_ref, dw3_ref, dw2_ref, y_ref, dh_ref, dg2_ref,
                    glu, d_gate, d_up, outbox, chip_sum, inbox, m_blk, do_blk, m_col, do_col, mt_scr, dot_scr, st1, st3, st2, dh_own,
                    part_send, part_recv, mail_send, mail_recv, gat_send, gat_recv, in_sem, col_sem, out_sem, own_sem):
    where = place(axis)
    me, other, first, second = where
    core = lax.rem(me, 2)
    partner = other(1, 0, 0)
    greet(other)
    tokens, model = h_ref.shape
    hid = w1_ref.shape[1]
    tok_of = lambda d: pl.ds(pl.multiple_of(d * tokens, tokens), tokens)
    off_first, off_second = 1 + core, 2 - core

    def block_of(off, flip):
        d_col, d_row = lax.rem(off, 2), lax.div(off, 2)
        col, row = lax.rem(lax.div(me, 2), 2), lax.div(me, 4)
        mix = lambda v, f: v + f - 2 * v * f
        return mix(row, d_row) * 4 + mix(col, d_col) * 2 + mix(core, flip)

    def step_off(step, flip):
        mid_a = off_second * (1 - flip) + off_first * flip
        mid_b = off_first * (1 - flip) + off_second * flip
        return jnp.where(step == 0, 3, jnp.where(step == 1, mid_a, jnp.where(step == 2, mid_b, 0)))

    def fetch(step):
        off = step_off(lax.div(step, 2), 1 - lax.rem(step, 2))
        rows = tok_of(block_of(off, 1 - lax.rem(step, 2)))
        slot = lax.rem(step, 2)
        return (pltpu.make_async_copy(m_ref.at[rows, :], m_blk.at[slot], in_sem.at[0, slot]),
                pltpu.make_async_copy(dout_ref.at[rows, :], do_blk.at[slot], in_sem.at[1, slot]))

    def fetch_cols(j):
        cols = pl.ds(pl.multiple_of(j * 256, 256), 256)
        return (pltpu.make_async_copy(m_ref.at[:, cols], m_col, col_sem.at[0]),
                pltpu.make_async_copy(dout_ref.at[:, cols], do_col, col_sem.at[1]))

    def activations(slot, rows):
        def chunk(j, _):
            cols = pl.ds(pl.multiple_of(j * 256, 256), 256)
            gate = dot(m_blk[slot], w1_ref[:, cols], 1, 0).astype(BF16).astype(F32)
            up = dot(m_blk[slot], w3_ref[:, cols], 1, 0).astype(BF16).astype(F32)
            d_act = dot(do_blk[slot], w2_ref[cols, :], 1, 1).astype(BF16).astype(F32)
            sig = 1.0 / (1.0 + jnp.exp(-gate))
            silu = gate * sig
            glu[rows, cols] = (silu * up).astype(BF16)
            d_up[rows, cols] = (d_act * silu).astype(BF16)
            d_gate[rows, cols] = (d_act * up * (sig + silu * (1.0 - sig))).astype(BF16)
            return 0
        lax.fori_loop(0, hid // 256, chunk, 0)

    def add_mlp_grad(rows, put):
        def chunk(j, _):
            cols = pl.ds(pl.multiple_of(j * 256, 256), 256)
            put(cols, dot(d_gate[rows, :], w1_ref[cols, :], 1, 1) + dot(d_up[rows, :], w3_ref[cols, :], 1, 1))
            return 0
        lax.fori_loop(0, model // 256, chunk, 0)

    def add_mlp_out(rows, put):
        def chunk(j, _):
            cols = pl.ds(pl.multiple_of(j * 256, 256), 256)
            put(cols, dot(glu[rows, :], w2_ref[:, cols], 1, 0))
            return 0
        lax.fori_loop(0, model // 256, chunk, 0)

    def to_partner(step):
        off = step_off(step, 1)
        return pltpu.make_async_remote_copy(
            src_ref=outbox.at[lax.rem(step, 2)], dst_ref=chip_sum.at[off], send_sem=part_send.at[step],
            recv_sem=part_recv.at[off], device_id=(partner,), device_id_type=MESH)

    def from_partner(off):
        return pltpu.make_async_remote_copy(
            src_ref=outbox.at[0], dst_ref=chip_sum.at[off], send_sem=part_send.at[0],
            recv_sem=part_recv.at[off], device_id=(partner,), device_id_type=MESH)

    def mail(kind):
        off = (3, off_first, off_second)[kind]
        dest = (first, first, second)[kind]
        return pltpu.make_async_remote_copy(
            src_ref=chip_sum.at[off], dst_ref=inbox.at[kind], send_sem=mail_send.at[kind],
            recv_sem=mail_recv.at[kind], device_id=(dest,), device_id_type=MESH)

    def scatter_round(prepare, partial):
        def step_body(step, _):
            @pl.when(step >= 2)
            def _():
                to_partner(step - 2).wait_send()

            prepare(2 * step)
            slot = lax.rem(step, 2)

            def put_out(cols, value):
                outbox[slot, :, cols] = value
            partial(tok_of(block_of(step_off(step, 1), 1)), put_out)
            to_partner(step).start()
            prepare(2 * step + 1)
            off = step_off(step, 0)
            from_partner(off).wait_recv()

            def put_sum(cols, value):
                chip_sum[off, :, cols] += value
            partial(tok_of(block_of(off, 0)), put_sum)

            @pl.when(step == 0)
            def _():
                mail(0).start()

            @pl.when(step == 2)
            def _():
                mail(1).start()
                mail(0).wait_recv()

                def add_mail(k, _):
                    part = pl.ds(pl.multiple_of(k * 16, 16), 16)
                    chip_sum[off_second, part, :] += inbox[0, part, :]
                    return 0
                lax.fori_loop(0, tokens // 16, add_mail, 0)
                mail(2).start()
            return 0
        lax.fori_loop(0, 4, step_body, 0)

    def scatter_end():
        mail(1).wait_recv()
        mail(2).wait_recv()

    def scatter_drain():
        to_partner(2).wait_send()
        to_partner(3).wait_send()
        for kind in range(3):
            mail(kind).wait_send()

    for copy in fetch(0):
        copy.start()

    def prepare_grad(half):
        @pl.when(half < 7)
        def _():
            for copy in fetch(half + 1):
                copy.start()
        for copy in fetch(half):
            copy.wait()
        flip = 1 - lax.rem(half, 2)
        activations(lax.rem(half, 2), tok_of(block_of(step_off(lax.div(half, 2), flip), flip)))

    def weight_grads(begin, end):
        for copy in fetch_cols(begin):
            copy.start()

        def body(j, _):
            for copy in fetch_cols(j):
                copy.wait()

            def turn(k, _):
                part = pl.ds(pl.multiple_of(k * 256, 256), 256)
                mt_scr[:, part] = m_col[part, :].T
                dot_scr[:, part] = do_col[part, :].T
                return 0
            lax.fori_loop(0, m_col.shape[0] // 256, turn, 0)

            @pl.when(j + 1 < end)
            def _():
                for copy in fetch_cols(j + 1):
                    copy.start()
            rows = pl.ds(pl.multiple_of(j * 256, 256), 256)
            out = (pltpu.make_async_copy(st1, dw1_ref.at[rows, :], out_sem.at[0]),
                   pltpu.make_async_copy(st3, dw3_ref.at[rows, :], out_sem.at[1]),
                   pltpu.make_async_copy(st2, dw2_ref.at[:, rows], out_sem.at[2]))

            @pl.when(j > begin)
            def _():
                for copy in out:
                    copy.wait()

            def chunk(k, _):
                cols = pl.ds(pl.multiple_of(k * 256, 256), 256)
                st1[:, cols] = dot(mt_scr[...], d_gate[:, cols], 1, 0)
                st3[:, cols] = dot(mt_scr[...], d_up[:, cols], 1, 0)
                st2[cols, :] = dot(dot_scr[...], glu[:, cols], 1, 0).T
                return 0
            lax.fori_loop(0, hid // 256, chunk, 0)
            for copy in out:
                copy.start()
            return 0
        lax.fori_loop(begin, end, body, 0)
        rows = pl.ds((end - 1) * 256, 256)
        for copy in (pltpu.make_async_copy(st1, dw1_ref.at[rows, :], out_sem.at[0]),
                     pltpu.make_async_copy(st3, dw3_ref.at[rows, :], out_sem.at[1]),
                     pltpu.make_async_copy(st2, dw2_ref.at[:, rows], out_sem.at[2])):
            copy.wait()

    scatter_round(prepare_grad, add_mlp_grad)
    own_do = pltpu.make_async_copy(dout_ref.at[tok_of(me), :], dh_own, own_sem.at[0])
    own_do.start()
    weight_grads(0, 4)
    own_do.wait()
    scatter_end()
    dg2_ref[...] = jnp.zeros_like(dg2_ref)

    def hidden_grad(k, _):
        part = pl.ds(pl.multiple_of(k * 16, 16), 16)
        d_mlp = (chip_sum[0, part, :] + inbox[1, part, :] + inbox[2, part, :]).astype(BF16).astype(F32)
        d_norm, d_gain = norm_backward(h_ref[part, :].astype(F32), g2_ref[...], d_mlp)
        dh_own[part, :] = (dh_own[part, :].astype(F32) + d_norm).astype(BF16)
        dg2_ref[...] += d_gain
        return 0
    lax.fori_loop(0, tokens // 16, hidden_grad, 0)
    scatter_drain()
    gather = Gather(lambda d: dh_ref.at[tok_of(d), :], gat_send, gat_recv, where, own=dh_own)
    gather.start()
    own_out = pltpu.make_async_copy(dh_own, dh_ref.at[tok_of(me), :], own_sem.at[1])
    own_out.start()
    weight_grads(4, 8)
    gather.got_first()
    gather.got_second()
    gather.got_partner(0)
    scatter_round(lambda half: None, add_mlp_out)
    gather.got_diag()
    for i in range(1, 4):
        gather.got_partner(i)
    scatter_end()

    def layer_out(k, _):
        part = pl.ds(pl.multiple_of(k * 16, 16), 16)
        y_ref[part, :] = (h_ref[part, :].astype(F32) + (chip_sum[0, part, :] + inbox[1, part, :] + inbox[2, part, :])).astype(BF16)
        return 0
    lax.fori_loop(0, tokens // 16, layer_out, 0)
    scatter_drain()
    gather.drain()
    own_out.wait()


def mlp_step(m_all, dout_all, w1, w3, w2, hidden, g2):
    seq_len, model = m_all.shape
    hid, tokens = w1.shape[1], hidden.shape[0]
    shape = jax.ShapeDtypeStruct
    vmem, hbm = pl.BlockSpec(memory_space=pltpu.VMEM), pl.BlockSpec(memory_space=pl.ANY)
    dma = pltpu.SemaphoreType.DMA
    return pl.pallas_call(
        functools.partial(mlp_comm_kernel, 'sp'), name='mlp_comm',
        in_specs=[hbm] * 2 + [vmem] * 5,
        out_specs=[hbm] * 3 + [vmem, hbm, vmem],
        out_shape=[shape((model, hid), F32), shape((model, hid), F32), shape((hid, model), F32),
                   shape(hidden.shape, BF16), shape((seq_len, model), BF16), shape((1, model), F32)],
        scratch_shapes=[pltpu.VMEM((seq_len, hid), BF16), pltpu.VMEM((seq_len, hid), BF16), pltpu.VMEM((seq_len, hid), BF16),
                        pltpu.VMEM((2, tokens, model), F32), pltpu.VMEM((4, tokens, model), F32), pltpu.VMEM((3, tokens, model), F32),
                        pltpu.VMEM((2, tokens, model), BF16), pltpu.VMEM((2, tokens, model), BF16),
                        pltpu.VMEM((seq_len, 256), BF16), pltpu.VMEM((seq_len, 256), BF16), pltpu.VMEM((256, seq_len), BF16), pltpu.VMEM((256, seq_len), BF16),
                        pltpu.VMEM((256, hid), F32), pltpu.VMEM((256, hid), F32), pltpu.VMEM((hid, 256), F32),
                        pltpu.VMEM((tokens, model), BF16),
                        dma((4,)), dma((4,)), dma((3,)), dma((3,)), dma((7,)), dma((7,)), dma((2, 2)), dma((2,)), dma((3,)), dma((2,))],
        compiler_params=pltpu.CompilerParams(collective_id=1, has_side_effects=True, vmem_limit_bytes=63 * 1024 * 1024),
    )(m_all, dout_all, w1, w3, w2, hidden, g2)


def solution(mesh):
    n_dev = mesh.shape['sp']
    gather_rows = functools.partial(lax.all_gather, axis_name='sp', axis=0, tiled=True)
    scatter_rows = functools.partial(lax.psum_scatter, axis_name='sp', scatter_dimension=0, tiled=True)
    a2a = functools.partial(lax.all_to_all, axis_name='sp', tiled=True)

    def layer_step(x_in, positions, d_out, norm1_gain, norm2_gain, w_q, w_k, w_v, w_o, w_gate, w_up, w_down):
        tokens, model = x_in.shape
        seq_len = tokens * n_dev
        head_dim = w_q.shape[2]
        heads = w_q.shape[1] // n_dev
        rows_own = w_q.shape[0]
        gains = gather_rows(jnp.stack([norm1_gain, norm2_gain], axis=1))
        g1_full, g2_full = gains[:, 0].astype(F32), gains[:, 1].astype(F32)
        pos_all = gather_rows(positions)
        cos_tab, sin_tab = rope_tables(pos_all, head_dim)
        x_all = gather_rows(x_in)
        wo_all = gather_rows(w_o.reshape(-1, model))
        dout_all = gather_rows(d_out)
        to_cols = lambda w: w.transpose(1, 2, 0).reshape(n_dev, -1, rows_own)
        qkv_rows = jnp.concatenate([to_cols(w_q), to_cols(w_k), to_cols(w_v)], axis=1)
        qkv_w = a2a(qkv_rows, split_axis=0, concat_axis=2)[0]
        w13 = jnp.stack([w_gate, w_up])
        w13 = a2a(w13, split_axis=2, concat_axis=1)
        w1, w3 = w13[0], w13[1]

        normed = norm_forward(x_all.astype(F32), g1_full).astype(BF16)
        qkv = dot(normed, qkv_w, 1, 1).astype(BF16)
        split_q, split_k = heads * head_dim, (heads + 1) * head_dim
        q_rot = rotate(qkv[:, :split_q].reshape(seq_len, heads, head_dim), cos_tab, sin_tab).astype(BF16).transpose(1, 0, 2)
        k_rot = rotate(qkv[:, split_q:split_k][:, None, :], cos_tab, sin_tab).astype(BF16)[:, 0]
        v_lin = qkv[:, split_k:]
        o_heads = attention_forward(q_rot, k_rot, v_lin)
        o_cols = o_heads.transpose(1, 0, 2).reshape(seq_len, heads * head_dim)
        o_tok = a2a(o_cols, split_axis=0, concat_axis=1)
        hidden = (x_in.astype(F32) + dot(o_tok, wo_all, 1, 0)).astype(BF16)
        hidden_f32 = hidden.astype(F32)
        mlp_in = gather_rows(norm_forward(hidden.astype(F32), g2_full).astype(BF16))
        d_w1s, d_w3s, d_down, y_out, dh_all, d_g2 = mlp_step(mlp_in, dout_all, w1, w3, w_down, hidden, g2_full[None])
        normed_own = a2a(norm_forward(x_in.astype(F32), g1_full).astype(BF16), split_axis=1, concat_axis=0)
        w_own = qkv_rows.reshape(-1, rows_own)
        cos2, sin2 = cos_tab[:, 0], sin_tab[:, 0]
        cos_lanes = jnp.concatenate([cos2] * 4, axis=1)
        sin_lanes = jnp.concatenate([-sin2, sin2] * 2, axis=1)
        cosk = jnp.concatenate([cos2, cos2, jnp.ones_like(cos2), jnp.ones_like(cos2)], axis=1)
        sink = jnp.concatenate([-sin2, sin2, jnp.zeros_like(cos2), jnp.zeros_like(cos2)], axis=1)
        d_wo, d_wq_t, d_wk_t, d_wv_t, d_w1, d_w3, d_x, d_g1 = attention_backward_step(
            heads, dh_all, w_o.reshape(-1, model), o_cols.T, q_rot, k_rot, v_lin, (cos_lanes, sin_lanes, cosk, sink),
            d_w1s, d_w3s, w_own, normed_own.T, x_in, g1_full[None])
        from_cols = lambda d, w: d.reshape(w.shape[1], w.shape[2], rows_own).transpose(2, 0, 1)
        d_gains = scatter_rows(jnp.stack([d_g1[0], d_g2[0]], axis=1))
        return (y_out, d_x, d_gains[:, 0], d_gains[:, 1], from_cols(d_wq_t, w_q), from_cols(d_wk_t, w_k), from_cols(d_wv_t, w_v),
                d_wo.reshape(w_o.shape), d_w1, d_w3, d_down)

    all_rows = P('sp')
    return jax.shard_map(layer_step, mesh=mesh, in_specs=(all_rows,) * 12, out_specs=(all_rows,) * 11, check_vma=False)
```

```python
import functools
import jax
import jax.numpy as jnp
from jax import lax
from jax.experimental import pallas as pl
from jax.experimental.pallas import tpu as pltpu
from jax.sharding import PartitionSpec as P

ROPE_BASE = 10000.0
NORM_EPS = 1e-5
NEG_LARGE = -1e30
F32 = jnp.float32
BF16 = jnp.bfloat16
BLK = 256


def dot(lhs, rhs, lhs_dim, rhs_dim):
    return lax.dot_general(lhs, rhs, (((lhs_dim,), (rhs_dim,)), ((), ())), preferred_element_type=F32)


def norm_forward(hidden, gain_vec):
    inv_rms = lax.rsqrt(jnp.mean(hidden * hidden, axis=-1, keepdims=True) + NORM_EPS)
    return hidden * inv_rms * gain_vec


def probs_transposed(k_rows, q_blk, start):
    scores = dot(k_rows, q_blk, 1, 1)
    rows = lax.broadcasted_iota(jnp.int32, (BLK, BLK), 0)
    cols = lax.broadcasted_iota(jnp.int32, (BLK, BLK), 1)
    tail = jnp.where(rows <= cols, scores[start:], NEG_LARGE)
    scores = jnp.concatenate([scores[:start], tail], axis=0) if start else tail
    top = jnp.max(scores, axis=0, keepdims=True)
    weights = jnp.exp((scores - top) * (q_blk.shape[1] ** -0.5))
    return weights * (1.0 / jnp.sum(weights, axis=0, keepdims=True))


MESH = pl.DeviceIdType.MESH


def place(axis):
    me = lax.axis_index(axis)
    core = lax.rem(me, 2)
    col = lax.rem(lax.div(me, 2), 2)
    row = lax.div(me, 4)

    def other(flip_core, flip_col, flip_row):
        pick = lambda v, f: 1 - v if f else v
        return pick(row, flip_row) * 4 + pick(col, flip_col) * 2 + pick(core, flip_core)

    nbr_x, nbr_y = other(0, 1, 0), other(0, 0, 1)
    first = nbr_x * (1 - core) + nbr_y * core
    second = nbr_y * (1 - core) + nbr_x * core
    return me, other, first, second


def greet(other):
    barrier = pltpu.get_barrier_semaphore()
    for r in range(1, 8):
        pl.semaphore_signal(barrier, inc=1, device_id=(other(r & 1, (r >> 1) & 1, r >> 2),), device_id_type=MESH)
    pl.semaphore_wait(barrier, 7)


class Gather:
    def __init__(self, slot, send_sem, recv_sem, where, own=None):
        me, other, first, second = where
        partner, diag = other(1, 0, 0), other(0, 1, 1)
        own = slot(me) if own is None else own
        self.copies = []
        plan = [(own, me, first), (own, me, second), (own, me, partner), (slot(first), first, second),
                (slot(first), first, partner), (slot(second), second, partner), (slot(diag), diag, partner)]
        for i, (src, what, dest) in enumerate(plan):
            self.copies.append(pltpu.make_async_remote_copy(
                src_ref=src, dst_ref=slot(what), send_sem=send_sem.at[i], recv_sem=recv_sem.at[i],
                device_id=(dest,), device_id_type=MESH))

    def start(self):
        for i in range(3):
            self.copies[i].start()

    def got_first(self):
        self.copies[0].wait_recv()
        self.copies[3].start()
        self.copies[4].start()

    def got_second(self):
        self.copies[1].wait_recv()
        self.copies[5].start()

    def got_diag(self):
        self.copies[3].wait_recv()
        self.copies[6].start()

    def got_partner(self, i):
        self.copies[(2, 4, 5, 6)[i]].wait_recv()

    def drain(self):
        for copy in self.copies:
            copy.wait_send()


def turn_halves(values, cos_blk, sin_blk):
    width = values.shape[1]
    lanes = lax.broadcasted_iota(jnp.int32, values.shape, 1)
    partner = jnp.where(lax.rem(lanes, 64) < 32, pltpu.roll(values, width - 32, 1), pltpu.roll(values, 32, 1))
    return values * cos_blk + partner * sin_blk


def norm_backward(hidden, gain, d_out):
    inv = lax.rsqrt(jnp.mean(hidden * hidden, axis=-1, keepdims=True) + NORM_EPS)
    d_scaled = d_out * gain
    d_hidden = d_scaled * inv - hidden * (inv * inv * inv * jnp.mean(d_scaled * hidden, axis=-1, keepdims=True))
    return d_hidden, jnp.sum(d_out * (hidden * inv), axis=0, keepdims=True)


def attn_bwd_comm_kernel(axis, heads, dh_ref, wo_ref, ot_ref, q_ref, k_ref, v_ref, cos_ref, sin_ref,
                         dw1_ref, dw3_ref, wown_ref, ut_ref, x_ref, g_ref, dg2_ref,
                         dwo_ref, dwq_ref, dwk_ref, dwv_ref, out1_ref, out3_ref, dx_ref, dg_ref,
                         slots, do_scr, dq_scr, dg_own, dg_all, dk_acc, dv_acc, du_acc, du_scr, du_recv, stage,
                         bulk_send, bulk_recv, gat_send, gat_recv, du_send, du_rsem, dg_send, dg_recv, loc_sem):
    where = place(axis)
    me, other, first, second = where
    greet(other)
    seq_len, head_dim = k_ref.shape
    rows_own, hid = stage.shape[1], stage.shape[2]
    tokens = x_ref.shape[0]
    qw = heads * head_dim

    rows_of = lambda d: pl.ds(pl.multiple_of(d * rows_own, rows_own), rows_own)
    hid_of = lambda d: pl.ds(pl.multiple_of(d * hid, hid), hid)
    bulk = []
    for n, r in enumerate((2, 4, 6, 3, 5, 7, 1)):
        dest = other(r & 1, (r >> 1) & 1, r >> 2)
        for i, (src, dst) in enumerate(((dw1_ref, out1_ref), (dw3_ref, out3_ref))):
            bulk.append(pltpu.make_async_remote_copy(
                src_ref=src.at[rows_of(dest), :], dst_ref=dst.at[:, hid_of(me)], send_sem=bulk_send.at[2 * n + i],
                recv_sem=bulk_recv.at[2 * n + i], device_id=(dest,), device_id_type=MESH))
            bulk[-1].start()
    for i, src in enumerate((dw1_ref, dw3_ref)):
        pltpu.make_async_copy(src.at[rows_of(me), :], stage.at[i], loc_sem.at[i]).start()

    for start in range(0, seq_len, BLK):
        rows = pl.ds(start, BLK)
        do_blk = dot(dh_ref[rows, :], wo_ref[...], 1, 1).astype(BF16)
        for h in range(heads):
            do_scr[h, rows, :] = do_blk[:, h * head_dim:(h + 1) * head_dim]
    for start in range(0, dwo_ref.shape[1], 512):
        cols = pl.ds(start, 512)
        dwo_ref[:, cols] = dot(ot_ref[...], dh_ref[:, cols], 1, 0)

    for i, (src, dst) in enumerate(((dw1_ref, out1_ref), (dw3_ref, out3_ref))):
        pltpu.make_async_copy(src.at[rows_of(me), :], stage.at[i], loc_sem.at[i]).wait()
        pltpu.make_async_copy(stage.at[i], dst.at[:, hid_of(me)], loc_sem.at[2 + i]).start()

    dk_acc[...] = jnp.zeros_like(dk_acc)
    dv_acc[...] = jnp.zeros_like(dv_acc)
    mine = slots.at[me]
    def one_head(h, _):
        def one_block(start):
            keys = pl.ds(0, start + BLK)
            rows = pl.ds(start, BLK)
            q_blk, do_blk = q_ref[h, rows, :], do_scr[h, rows, :]
            probs = probs_transposed(k_ref[keys, :], q_blk, start)
            d_probs = dot(v_ref[keys, :], do_blk, 1, 1).astype(BF16).astype(F32)
            row_dot = jnp.sum(d_probs * probs, axis=0, keepdims=True)
            d_scores = (probs * (d_probs - row_dot) * (head_dim ** -0.5)).astype(BF16)
            dq_scr[h, rows, :] = dot(d_scores, k_ref[keys, :], 0, 0).astype(BF16)
            dk_acc[keys, :] += dot(d_scores, q_blk, 1, 0)
            dv_acc[keys, :] += dot(probs.astype(BF16), do_blk, 1, 0)
        for start in range(0, seq_len, BLK):
            one_block(start)
        return 0
    lax.fori_loop(0, heads, one_head, 0)
    mine[:, qw:qw + head_dim] = dk_acc[...].astype(BF16)
    mine[:, qw + head_dim:] = dv_acc[...].astype(BF16)
    low = lax.broadcasted_iota(jnp.int32, (BLK, 128), 1) < head_dim

    def turn_back(k, _):
        rows = pl.ds(pl.multiple_of(k * BLK, BLK), BLK)
        cos_blk, sin_blk = cos_ref[rows, :], -sin_ref[rows, :]
        for pair in range(heads // 2):
            both = jnp.concatenate([dq_scr[2 * pair, rows, :], dq_scr[2 * pair + 1, rows, :]], axis=1)
            mine[rows, pair * 128:(pair + 1) * 128] = turn_halves(both.astype(F32), cos_blk, sin_blk).astype(BF16)
        kv = mine[rows, qw:].astype(F32)
        mine[rows, qw:] = jnp.where(low, turn_halves(kv, cos_blk, sin_blk), kv).astype(BF16)
        return 0
    lax.fori_loop(0, seq_len // BLK, turn_back, 0)

    gather = Gather(lambda d: slots.at[d], gat_send, gat_recv, where)
    gather.start()
    du_acc[...] = jnp.zeros_like(du_acc)

    def use(d):
        kv_rows = pl.ds(pl.multiple_of(d * head_dim, head_dim), head_dim)
        w_rows = pl.ds(pl.multiple_of(d * 384, 384), 384)
        for start in range(0, seq_len, 512):
            rows = pl.ds(start, 512)
            du_acc[rows, :] += dot(slots[d, rows, :], wown_ref[w_rows, :], 1, 0)
        d_w = dot(ut_ref[...], slots[d], 1, 0).T
        dwq_ref[pl.ds(pl.multiple_of(d * qw, qw), qw), :] = d_w[:qw]
        dwk_ref[kv_rows, :] = d_w[qw:qw + head_dim]
        dwv_ref[kv_rows, :] = d_w[qw + head_dim:]

    partner = other(1, 0, 0)
    use(me)
    gather.got_first()
    gather.got_second()
    use(first)
    use(second)
    gather.got_partner(0)
    use(partner)
    gather.got_diag()
    use(other(0, 1, 1))
    gather.got_partner(1)
    gather.got_partner(2)
    use(other(1, 1, 0))
    use(other(1, 0, 1))
    gather.got_partner(3)
    use(other(1, 1, 1))
    du_scr[...] = du_acc[...].astype(BF16)

    tok_of = lambda d: pl.ds(pl.multiple_of(d * tokens, tokens), tokens)
    sends = []
    for n, r in enumerate((6, 7, 2, 4, 3, 5, 1)):
        dest = other(r & 1, (r >> 1) & 1, r >> 2)
        sends.append(pltpu.make_async_remote_copy(
            src_ref=du_scr.at[tok_of(dest), :], dst_ref=du_recv.at[:, rows_of(me)], send_sem=du_send.at[n],
            recv_sem=du_rsem.at[n], device_id=(dest,), device_id_type=MESH))
        sends[-1].start()
    du_recv[:, rows_of(me)] = du_scr[tok_of(me), :]
    for copy in sends:
        copy.wait_recv()
    dg_own[...] = jnp.zeros_like(dg_own)
    dg_own[1:2, :] = dg2_ref[...]

    def input_grad(k, _):
        part = pl.ds(pl.multiple_of(k * 16, 16), 16)
        d_norm, d_gain = norm_backward(x_ref[part, :].astype(F32), g_ref[0:1, :], du_recv[part, :].astype(F32))
        dh_part = dh_ref[pl.ds(pl.multiple_of(me * tokens + k * 16, 16), 16), :]
        dx_ref[part, :] = (dh_part.astype(F32) + d_norm).astype(BF16)
        dg_own[0:1, :] += d_gain
        return 0
    lax.fori_loop(0, tokens // 16, input_grad, 0)
    gain_sends = []
    for n, r in enumerate((6, 7, 2, 4, 3, 5, 1)):
        dest = other(r & 1, (r >> 1) & 1, r >> 2)
        gain_sends.append(pltpu.make_async_remote_copy(
            src_ref=dg_own.at[:, rows_of(dest)], dst_ref=dg_all.at[me], send_sem=dg_send.at[n],
            recv_sem=dg_recv.at[n], device_id=(dest,), device_id_type=MESH))
        gain_sends[-1].start()
    dg_all[me] = dg_own[:, rows_of(me)]
    for copy in gain_sends:
        copy.wait_recv()
    dg_ref[...] = jnp.sum(dg_all[...], axis=0)
    for copy in sends + gain_sends:
        copy.wait_send()
    gather.drain()
    for copy in bulk:
        copy.wait()
    for i, dst in enumerate((out1_ref, out3_ref)):
        pltpu.make_async_copy(stage.at[i], dst.at[:, hid_of(me)], loc_sem.at[2 + i]).wait()


def attention_backward_step(heads, dh_all, wo_own, o_t, q_rot, k_rot, v_lin, tables, d_w1, d_w3, w_own, u_t, x_in, gains, d_g2):
    seq_len, model = dh_all.shape
    head_dim = k_rot.shape[1]
    tokens = x_in.shape[0]
    rows_own, hid = model // 8, d_w1.shape[1]
    shape = jax.ShapeDtypeStruct
    vmem, hbm = pl.BlockSpec(memory_space=pltpu.VMEM), pl.BlockSpec(memory_space=pl.ANY)
    dma = pltpu.SemaphoreType.DMA
    return pl.pallas_call(
        functools.partial(attn_bwd_comm_kernel, 'sp', heads), name='attn_bwd_comm',
        in_specs=[vmem] * 8 + [hbm] * 2 + [vmem] * 5,
        out_specs=[vmem] * 4 + [hbm] * 2 + [vmem] * 2,
        out_shape=[shape(wo_own.shape, F32), shape((8 * heads * head_dim, rows_own), F32), shape((8 * head_dim, rows_own), F32),
                   shape((8 * head_dim, rows_own), F32), shape((rows_own, 8 * hid), F32), shape((rows_own, 8 * hid), F32),
                   shape(x_in.shape, BF16), shape((8, rows_own), F32)],
        scratch_shapes=[pltpu.VMEM((8, seq_len, 384), BF16), pltpu.VMEM((heads, seq_len, head_dim), BF16), pltpu.VMEM((heads, seq_len, head_dim), BF16),
                        pltpu.VMEM((8, model), F32), pltpu.VMEM((8, 8, rows_own), F32),
                        pltpu.VMEM((seq_len, head_dim), F32), pltpu.VMEM((seq_len, head_dim), F32),
                        pltpu.VMEM((seq_len, rows_own), F32), pltpu.VMEM((seq_len, rows_own), BF16),
                        pltpu.VMEM((tokens, model), BF16), pltpu.VMEM((2, rows_own, hid), F32),
                        dma((14,)), dma((14,)), dma((7,)), dma((7,)), dma((7,)), dma((7,)), dma((7,)), dma((7,)), dma((4,))],
        compiler_params=pltpu.CompilerParams(collective_id=2, has_side_effects=True, vmem_limit_bytes=63 * 1024 * 1024),
    )(dh_all, wo_own, o_t, q_rot, k_rot, v_lin, *tables, d_w1, d_w3, w_own, u_t, x_in, gains, d_g2)


def mlp_comm_kernel(axis, m_ref, dout_ref, w1_ref, w3_ref, w2_ref, h_ref, g_ref,
                    dw1_ref, dw3_ref, dw2_ref, y_ref, dh_ref, dg2_ref,
                    glu, d_gate, d_up, outbox, chip_sum, inbox, m_blk, do_blk, m_col, do_col, mt_scr, dot_scr, st1, st3, st2, dh_own,
                    part_send, part_recv, mail_send, mail_recv, gat_send, gat_recv, in_sem, col_sem, out_sem, own_sem):
    where = place(axis)
    me, other, first, second = where
    core = lax.rem(me, 2)
    partner = other(1, 0, 0)
    greet(other)
    tokens, model = h_ref.shape
    hid = w1_ref.shape[1]
    tok_of = lambda d: pl.ds(pl.multiple_of(d * tokens, tokens), tokens)
    off_first, off_second = 1 + core, 2 - core

    def block_of(off, flip):
        d_col, d_row = lax.rem(off, 2), lax.div(off, 2)
        col, row = lax.rem(lax.div(me, 2), 2), lax.div(me, 4)
        mix = lambda v, f: v + f - 2 * v * f
        return mix(row, d_row) * 4 + mix(col, d_col) * 2 + mix(core, flip)

    def step_off(step, flip):
        mid_a = off_second * (1 - flip) + off_first * flip
        mid_b = off_first * (1 - flip) + off_second * flip
        return jnp.where(step == 0, 3, jnp.where(step == 1, mid_a, jnp.where(step == 2, mid_b, 0)))

    def fetch(step):
        off = step_off(lax.div(step, 2), 1 - lax.rem(step, 2))
        rows = tok_of(block_of(off, 1 - lax.rem(step, 2)))
        slot = lax.rem(step, 2)
        return (pltpu.make_async_copy(m_ref.at[rows, :], m_blk.at[slot], in_sem.at[0, slot]),
                pltpu.make_async_copy(dout_ref.at[rows, :], do_blk.at[slot], in_sem.at[1, slot]))

    def fetch_cols(j):
        cols = pl.ds(pl.multiple_of(j * 256, 256), 256)
        return (pltpu.make_async_copy(m_ref.at[:, cols], m_col, col_sem.at[0]),
                pltpu.make_async_copy(dout_ref.at[:, cols], do_col, col_sem.at[1]))

    def activations(slot, rows):
        def chunk(j, _):
            cols = pl.ds(pl.multiple_of(j * 256, 256), 256)
            gate = dot(m_blk[slot], w1_ref[:, cols], 1, 0).astype(BF16).astype(F32)
            up = dot(m_blk[slot], w3_ref[:, cols], 1, 0).astype(BF16).astype(F32)
            d_act = dot(do_blk[slot], w2_ref[cols, :], 1, 1).astype(BF16).astype(F32)
            sig = 1.0 / (1.0 + jnp.exp(-gate))
            silu = gate * sig
            glu[rows, cols] = (silu * up).astype(BF16)
            d_up[rows, cols] = (d_act * silu).astype(BF16)
            d_gate[rows, cols] = (d_act * up * (sig + silu * (1.0 - sig))).astype(BF16)
            return 0
        lax.fori_loop(0, hid // 256, chunk, 0)

    def add_mlp_grad(rows, put):
        def chunk(j, _):
            cols = pl.ds(pl.multiple_of(j * 256, 256), 256)
            put(cols, dot(d_gate[rows, :], w1_ref[cols, :], 1, 1) + dot(d_up[rows, :], w3_ref[cols, :], 1, 1))
            return 0
        lax.fori_loop(0, model // 256, chunk, 0)

    def add_mlp_out(rows, put):
        def chunk(j, _):
            cols = pl.ds(pl.multiple_of(j * 256, 256), 256)
            put(cols, dot(glu[rows, :], w2_ref[:, cols], 1, 0))
            return 0
        lax.fori_loop(0, model // 256, chunk, 0)

    def to_partner(step):
        off = step_off(step, 1)
        return pltpu.make_async_remote_copy(
            src_ref=outbox.at[lax.rem(step, 2)], dst_ref=chip_sum.at[off], send_sem=part_send.at[step],
            recv_sem=part_recv.at[off], device_id=(partner,), device_id_type=MESH)

    def from_partner(off):
        return pltpu.make_async_remote_copy(
            src_ref=outbox.at[0], dst_ref=chip_sum.at[off], send_sem=part_send.at[0],
            recv_sem=part_recv.at[off], device_id=(partner,), device_id_type=MESH)

    def mail(kind):
        off = (3, off_first, off_second)[kind]
        dest = (first, first, second)[kind]
        return pltpu.make_async_remote_copy(
            src_ref=chip_sum.at[off], dst_ref=inbox.at[kind], send_sem=mail_send.at[kind],
            recv_sem=mail_recv.at[kind], device_id=(dest,), device_id_type=MESH)

    def scatter_round(prepare, partial):
        def step_body(step, _):
            @pl.when(step >= 2)
            def _():
                to_partner(step - 2).wait_send()

            prepare(2 * step)
            slot = lax.rem(step, 2)

            def put_out(cols, value):
                outbox[slot, :, cols] = value
            partial(tok_of(block_of(step_off(step, 1), 1)), put_out)
            to_partner(step).start()
            prepare(2 * step + 1)
            off = step_off(step, 0)
            from_partner(off).wait_recv()

            def put_sum(cols, value):
                chip_sum[off, :, cols] += value
            partial(tok_of(block_of(off, 0)), put_sum)

            @pl.when(step == 0)
            def _():
                mail(0).start()

            @pl.when(step == 2)
            def _():
                mail(1).start()
                mail(0).wait_recv()

                def add_mail(k, _):
                    part = pl.ds(pl.multiple_of(k * 16, 16), 16)
                    chip_sum[off_second, part, :] += inbox[0, part, :]
                    return 0
                lax.fori_loop(0, tokens // 16, add_mail, 0)
                mail(2).start()
            return 0
        lax.fori_loop(0, 4, step_body, 0)

    def scatter_end():
        mail(1).wait_recv()
        mail(2).wait_recv()

    def scatter_drain():
        to_partner(2).wait_send()
        to_partner(3).wait_send()
        for kind in range(3):
            mail(kind).wait_send()

    for copy in fetch(0):
        copy.start()

    def prepare_grad(half):
        @pl.when(half < 7)
        def _():
            for copy in fetch(half + 1):
                copy.start()
        for copy in fetch(half):
            copy.wait()
        flip = 1 - lax.rem(half, 2)
        activations(lax.rem(half, 2), tok_of(block_of(step_off(lax.div(half, 2), flip), flip)))

    def weight_grads(begin, end):
        for copy in fetch_cols(begin):
            copy.start()

        def body(j, _):
            for copy in fetch_cols(j):
                copy.wait()

            def turn(k, _):
                part = pl.ds(pl.multiple_of(k * 256, 256), 256)
                mt_scr[:, part] = m_col[part, :].T
                dot_scr[:, part] = do_col[part, :].T
                return 0
            lax.fori_loop(0, m_col.shape[0] // 256, turn, 0)

            @pl.when(j + 1 < end)
            def _():
                for copy in fetch_cols(j + 1):
                    copy.start()
            rows = pl.ds(pl.multiple_of(j * 256, 256), 256)
            out = (pltpu.make_async_copy(st1, dw1_ref.at[rows, :], out_sem.at[0]),
                   pltpu.make_async_copy(st3, dw3_ref.at[rows, :], out_sem.at[1]),
                   pltpu.make_async_copy(st2, dw2_ref.at[:, rows], out_sem.at[2]))

            @pl.when(j > begin)
            def _():
                for copy in out:
                    copy.wait()

            def chunk(k, _):
                cols = pl.ds(pl.multiple_of(k * 256, 256), 256)
                st1[:, cols] = dot(mt_scr[...], d_gate[:, cols], 1, 0)
                st3[:, cols] = dot(mt_scr[...], d_up[:, cols], 1, 0)
                st2[cols, :] = dot(dot_scr[...], glu[:, cols], 1, 0).T
                return 0
            lax.fori_loop(0, hid // 256, chunk, 0)
            for copy in out:
                copy.start()
            return 0
        lax.fori_loop(begin, end, body, 0)
        rows = pl.ds((end - 1) * 256, 256)
        for copy in (pltpu.make_async_copy(st1, dw1_ref.at[rows, :], out_sem.at[0]),
                     pltpu.make_async_copy(st3, dw3_ref.at[rows, :], out_sem.at[1]),
                     pltpu.make_async_copy(st2, dw2_ref.at[:, rows], out_sem.at[2])):
            copy.wait()

    scatter_round(prepare_grad, add_mlp_grad)
    own_do = pltpu.make_async_copy(dout_ref.at[tok_of(me), :], dh_own, own_sem.at[0])
    own_do.start()
    weight_grads(0, 4)
    own_do.wait()
    scatter_end()
    dg2_ref[...] = jnp.zeros_like(dg2_ref)

    def hidden_grad(k, _):
        part = pl.ds(pl.multiple_of(k * 16, 16), 16)
        d_mlp = (chip_sum[0, part, :] + inbox[1, part, :] + inbox[2, part, :]).astype(BF16).astype(F32)
        d_norm, d_gain = norm_backward(h_ref[part, :].astype(F32), g_ref[1:2, :], d_mlp)
        dh_own[part, :] = (dh_own[part, :].astype(F32) + d_norm).astype(BF16)
        dg2_ref[...] += d_gain
        return 0
    lax.fori_loop(0, tokens // 16, hidden_grad, 0)
    scatter_drain()
    gather = Gather(lambda d: dh_ref.at[tok_of(d), :], gat_send, gat_recv, where, own=dh_own)
    gather.start()
    own_out = pltpu.make_async_copy(dh_own, dh_ref.at[tok_of(me), :], own_sem.at[1])
    own_out.start()
    weight_grads(4, 8)
    gather.got_first()
    gather.got_second()
    gather.got_partner(0)
    scatter_round(lambda half: None, add_mlp_out)
    gather.got_diag()
    for i in range(1, 4):
        gather.got_partner(i)
    scatter_end()

    def layer_out(k, _):
        part = pl.ds(pl.multiple_of(k * 16, 16), 16)
        y_ref[part, :] = (h_ref[part, :].astype(F32) + (chip_sum[0, part, :] + inbox[1, part, :] + inbox[2, part, :])).astype(BF16)
        return 0
    lax.fori_loop(0, tokens // 16, layer_out, 0)
    scatter_drain()
    gather.drain()
    own_out.wait()


def mlp_step(m_all, dout_all, w1, w3, w2, hidden, gains):
    seq_len, model = m_all.shape
    hid, tokens = w1.shape[1], hidden.shape[0]
    shape = jax.ShapeDtypeStruct
    vmem, hbm = pl.BlockSpec(memory_space=pltpu.VMEM), pl.BlockSpec(memory_space=pl.ANY)
    dma = pltpu.SemaphoreType.DMA
    return pl.pallas_call(
        functools.partial(mlp_comm_kernel, 'sp'), name='mlp_comm',
        in_specs=[hbm] * 2 + [vmem] * 5,
        out_specs=[hbm] * 3 + [vmem, hbm, vmem],
        out_shape=[shape((model, hid), F32), shape((model, hid), F32), shape((hid, model), F32),
                   shape(hidden.shape, BF16), shape((seq_len, model), BF16), shape((1, model), F32)],
        scratch_shapes=[pltpu.VMEM((seq_len, hid), BF16), pltpu.VMEM((seq_len, hid), BF16), pltpu.VMEM((seq_len, hid), BF16),
                        pltpu.VMEM((2, tokens, model), F32), pltpu.VMEM((4, tokens, model), F32), pltpu.VMEM((3, tokens, model), F32),
                        pltpu.VMEM((2, tokens, model), BF16), pltpu.VMEM((2, tokens, model), BF16),
                        pltpu.VMEM((seq_len, 256), BF16), pltpu.VMEM((seq_len, 256), BF16), pltpu.VMEM((256, seq_len), BF16), pltpu.VMEM((256, seq_len), BF16),
                        pltpu.VMEM((256, hid), F32), pltpu.VMEM((256, hid), F32), pltpu.VMEM((hid, 256), F32),
                        pltpu.VMEM((tokens, model), BF16),
                        dma((4,)), dma((4,)), dma((3,)), dma((3,)), dma((7,)), dma((7,)), dma((2, 2)), dma((2,)), dma((3,)), dma((2,))],
        compiler_params=pltpu.CompilerParams(collective_id=1, has_side_effects=True, vmem_limit_bytes=63 * 1024 * 1024),
    )(m_all, dout_all, w1, w3, w2, hidden, gains)


def spread_tables(packed, upper):
    lanes = lax.broadcasted_iota(jnp.int32, packed.shape, 1)
    swapped = pltpu.roll(packed, 64, 1)
    both = jnp.where((lanes < 64) != upper, packed, swapped)
    low = lax.rem(lanes, 64) < 32
    return jnp.where(low, both, pltpu.roll(both, 32, 1)), jnp.where(low, -pltpu.roll(both, 96, 1), both)


def attention_comm_kernel(axis, heads, x_ref, tab_ref, gain_ref, qkvw_ref, wo_ref, wg_ref, wu_ref, dout_ref,
                          q_ref, k_ref, v_ref, ot_ref, ut_ref, cos_ref, sin_ref, gfull_ref, h_ref,
                          m_ref, w1_ref, w3_ref, doutall_ref,
                          x_all, tab_all, gain_all, w_head, wo_all, o_all, u_blk, qkv_blk, o_scr, o_own, h_scr, m_out, stage,
                          g_send, g_recv, w_send, w_recv, x_send, x_recv, t_send, t_recv, wo_send, wo_recv, bulk_send, bulk_recv,
                          o_send, o_recv, do_send, do_recv, m_loc, m_send, m_recv, loc_sem):
    where = place(axis)
    me, other, first, second = where
    core = lax.rem(me, 2)
    partner = other(1, 0, 0)
    greet(other)
    tokens, model = x_ref.shape
    seq_len, head_dim = k_ref.shape
    qw = heads * head_dim
    rows_own, hid = wg_ref.shape[0], w1_ref.shape[1]
    tok_of = lambda d: pl.ds(pl.multiple_of(d * tokens, tokens), tokens)
    cols_of = lambda d: pl.ds(pl.multiple_of(d * rows_own, rows_own), rows_own)
    hid_of = lambda d: pl.ds(pl.multiple_of(d * hid, hid), hid)
    peers = [other(r & 1, (r >> 1) & 1, r >> 2) for r in (6, 2, 4, 7, 3, 5, 1)]

    def to_all(src_of, dst, send_sem, recv_sem):
        return [pltpu.make_async_remote_copy(
            src_ref=src_of(dest), dst_ref=dst, send_sem=send_sem.at[n], recv_sem=recv_sem.at[n],
            device_id=(dest,), device_id_type=MESH) for n, dest in enumerate(peers)]

    small = to_all(lambda dest: gain_ref, gain_all.at[me], g_send, g_recv)
    slices = to_all(lambda dest: qkvw_ref.at[dest], w_head.at[:, cols_of(me)], w_send, w_recv)
    for copy in small + slices:
        copy.start()
    tab_slot = lambda d: tab_all.at[d]
    x_gather = Gather(lambda d: x_all.at[tok_of(d), :], x_send, x_recv, where, own=x_ref)
    t_gather = Gather(tab_slot, t_send, t_recv, where, own=tab_ref)
    t_gather.start()
    x_gather.start()
    wo_gather = Gather(lambda d: wo_all.at[cols_of(d), :], wo_send, wo_recv, where, own=wo_ref)
    do_gather = Gather(lambda d: doutall_ref.at[tok_of(d), :], do_send, do_recv, where, own=dout_ref)
    bulk = []
    for n, dest in enumerate(peers):
        for i, (src, dst) in enumerate(((wg_ref, w1_ref), (wu_ref, w3_ref))):
            bulk.append(pltpu.make_async_remote_copy(
                src_ref=src.at[:, hid_of(dest)], dst_ref=dst.at[cols_of(me), :], send_sem=bulk_send.at[2 * n + i],
                recv_sem=bulk_recv.at[2 * n + i], device_id=(dest,), device_id_type=MESH))

    local = []
    for i, (src, dst) in enumerate(((wg_ref, w1_ref), (wu_ref, w3_ref))):
        local.append((pltpu.make_async_copy(src.at[:, hid_of(me)], stage.at[i], loc_sem.at[i]),
                      pltpu.make_async_copy(stage.at[i], dst.at[cols_of(me), :], loc_sem.at[2 + i])))
        local[-1][0].start()
    own_dout = pltpu.make_async_copy(dout_ref, doutall_ref.at[tok_of(me), :], loc_sem.at[4])
    own_dout.start()
    x_all[tok_of(me), :] = x_ref[...]
    tab_all[me] = tab_ref[...]
    gain_all[me] = gain_ref[...]
    w_head[:, cols_of(me)] = qkvw_ref[me]
    wo_all[cols_of(me), :] = wo_ref[...]
    for load, store in local:
        load.wait()
        store.start()
    for copy in small:
        copy.wait_recv()
    for d in range(8):
        gfull_ref[:, d * rows_own:(d + 1) * rows_own] = gain_all[d]
    for copy in slices:
        copy.wait_recv()

    def use(d):
        base = pl.multiple_of(d * tokens, tokens)

        def norm(k, _):
            part = pl.ds(pl.multiple_of(k * 16, 16), 16)
            x_part = x_all[pl.ds(pl.multiple_of(base + k * 16, 16), 16), :].astype(F32)
            u_blk[part, :] = norm_forward(x_part, gfull_ref[0:1, :]).astype(BF16)
            return 0
        lax.fori_loop(0, tokens // 16, norm, 0)
        ut_ref[:, tok_of(d)] = u_blk[:, cols_of(me)].T
        qkv_blk[...] = dot(u_blk[...], w_head[...], 1, 1).astype(BF16)
        half = tokens // 2
        for part in range(2):
            rows = pl.ds(pl.multiple_of(base + part * half, half), half)
            cos_blk, sin_blk = spread_tables(tab_all[d], part == 1)
            cos_ref[rows, :] = cos_blk
            sin_ref[rows, :] = sin_blk
            source = slice(part * half, (part + 1) * half)
            for pair in range(heads // 2):
                turned = turn_halves(qkv_blk[source, pair * 128:(pair + 1) * 128].astype(F32), cos_blk, sin_blk).astype(BF16)
                q_ref[2 * pair, rows, :] = turned[:, :head_dim]
                q_ref[2 * pair + 1, rows, :] = turned[:, head_dim:]
            turned = turn_halves(qkv_blk[source, qw:].astype(F32), cos_blk, sin_blk).astype(BF16)
            k_ref[rows, :] = turned[:, :head_dim]
            v_ref[rows, :] = qkv_blk[source, qw + head_dim:]

    x_gather.got_first()
    t_gather.got_first()
    x_gather.got_second()
    t_gather.got_second()
    wo_gather.start()
    for copy in bulk:
        copy.start()
    x_gather.got_partner(0)
    t_gather.got_partner(0)

    def use_near(i, _):
        use(jnp.where(i == 0, me, jnp.where(i == 1, first, jnp.where(i == 2, second, partner))))
        return 0
    lax.fori_loop(0, 4, use_near, 0)
    x_gather.got_diag()
    t_gather.got_diag()
    for i in range(1, 4):
        x_gather.got_partner(i)
        t_gather.got_partner(i)

    def use_far(i, _):
        use(jnp.where(i == 0, other(0, 1, 1), jnp.where(i == 1, other(1, 1, 0), jnp.where(i == 2, other(1, 0, 1), other(1, 1, 1)))))
        return 0
    lax.fori_loop(0, 4, use_far, 0)

    def one_head(h, _):
        for start in range(0, seq_len, BLK):
            keys, rows = pl.ds(0, start + BLK), pl.ds(start, BLK)
            probs = probs_transposed(k_ref[keys, :], q_ref[h, rows, :], start)
            o_scr[h, rows, :] = dot(probs.astype(BF16), v_ref[keys, :], 0, 0).astype(BF16)
        return 0
    lax.fori_loop(0, heads, one_head, 0)
    for h in range(heads):
        o_own[:, h * head_dim:(h + 1) * head_dim] = o_scr[h]
    wo_gather.got_first()
    wo_gather.got_second()
    o_gather = Gather(lambda d: o_all.at[:, cols_of(d)], o_send, o_recv, where, own=o_own)
    o_gather.start()
    o_all[:, cols_of(me)] = o_own[...]

    def turn_out(k, _):
        rows = tok_of(k)
        ot_ref[:, rows] = o_own[rows, :].T
        return 0
    lax.fori_loop(0, 8, turn_out, 0)
    wo_gather.got_diag()
    for i in range(4):
        wo_gather.got_partner(i)
    o_gather.got_first()
    o_gather.got_second()
    do_gather.start()
    o_gather.got_partner(0)
    o_gather.got_diag()
    for i in range(1, 4):
        o_gather.got_partner(i)

    def rows_at(i):
        flips = lambda a, b: other(0, a, b)
        return tok_of(jnp.where(i == 0, me, jnp.where(i == 1, flips(1, 0), jnp.where(i == 2, flips(0, 1), flips(1, 1)))))

    def give(i):
        slot = lax.rem(i, 2)
        rows = rows_at(i)
        return (pltpu.make_async_copy(m_out.at[slot], m_ref.at[rows, :], m_loc.at[slot]),
                pltpu.make_async_remote_copy(src_ref=m_out.at[slot], dst_ref=m_ref.at[rows, :], send_sem=m_send.at[i],
                                             recv_sem=m_recv.at[i], device_id=(partner,), device_id_type=MESH))

    def hidden_block(i, _):
        rows = rows_at(i)
        base = rows.start
        slot = lax.rem(i, 2)

        @pl.when(i >= 2)
        def _():
            to_hbm, to_partner = give(i - 2)
            to_hbm.wait()
            to_partner.wait_send()

        def chunk(j, _):
            cols = pl.ds(pl.multiple_of(j * 256, 256), 256)
            h_scr[:, cols] = dot(o_all[rows, :], wo_all[:, cols], 1, 0)
            return 0
        lax.fori_loop(0, model // 256, chunk, 0)

        def norm(k, _):
            part = pl.ds(pl.multiple_of(k * 16, 16), 16)
            x_part = x_all[pl.ds(pl.multiple_of(base + k * 16, 16), 16), :].astype(F32)
            hidden = (x_part + h_scr[part, :]).astype(BF16)

            @pl.when(i == 0)
            def _():
                h_ref[part, :] = hidden
            m_out[slot, part, :] = norm_forward(hidden.astype(F32), gfull_ref[1:2, :]).astype(BF16)
            return 0
        lax.fori_loop(0, tokens // 16, norm, 0)
        for copy in give(i):
            copy.start()

        @pl.when(i == 1)
        def _():
            do_gather.got_first()
            do_gather.got_second()
        return 0
    lax.fori_loop(0, 4, hidden_block, 0)
    do_gather.got_diag()
    for i in range(4):
        do_gather.got_partner(i)
        give(i)[1].wait_recv()
    for i in range(2, 4):
        give(i)[0].wait()
        give(i)[1].wait_send()
    for copy in small + slices:
        copy.wait_send()
    for gather in (x_gather, t_gather, wo_gather, o_gather, do_gather):
        gather.drain()
    for copy in bulk:
        copy.wait()
    for load, store in local:
        store.wait()
    own_dout.wait()


def attention_step(heads, x_in, tab, gains, qkv_rows, wo_own, w_gate, w_up, d_out):
    tokens, model = x_in.shape
    seq_len = 8 * tokens
    head_dim = wo_own.shape[0] // heads
    rows_own, hid = w_gate.shape[0], w_gate.shape[1] // 8
    shape = jax.ShapeDtypeStruct
    vmem, hbm = pl.BlockSpec(memory_space=pltpu.VMEM), pl.BlockSpec(memory_space=pl.ANY)
    dma = pltpu.SemaphoreType.DMA
    return pl.pallas_call(
        functools.partial(attention_comm_kernel, 'sp', heads), name='attention_comm',
        in_specs=[vmem] * 5 + [hbm] * 2 + [vmem],
        out_specs=[vmem] * 9 + [hbm] * 4,
        out_shape=[shape((heads, seq_len, head_dim), BF16), shape((seq_len, head_dim), BF16), shape((seq_len, head_dim), BF16),
                   shape((heads * head_dim, seq_len), BF16), shape((rows_own, seq_len), BF16),
                   shape((seq_len, 128), F32), shape((seq_len, 128), F32), shape((8, model), F32), shape((tokens, model), BF16),
                   shape((seq_len, model), BF16), shape((model, hid), BF16), shape((model, hid), BF16), shape((seq_len, model), BF16)],
        scratch_shapes=[pltpu.VMEM((seq_len, model), BF16), pltpu.VMEM((8, tokens // 2, 128), F32), pltpu.VMEM((8, 8, rows_own), F32),
                        pltpu.VMEM((384, model), BF16), pltpu.VMEM((model, model), BF16), pltpu.VMEM((seq_len, model), BF16),
                        pltpu.VMEM((tokens, model), BF16), pltpu.VMEM((tokens, 384), BF16), pltpu.VMEM((heads, seq_len, head_dim), BF16),
                        pltpu.VMEM((seq_len, heads * head_dim), BF16), pltpu.VMEM((tokens, model), F32), pltpu.VMEM((2, tokens, model), BF16),
                        pltpu.VMEM((2, rows_own, hid), BF16),
                        dma((7,)), dma((7,)), dma((7,)), dma((7,)), dma((7,)), dma((7,)), dma((7,)), dma((7,)), dma((7,)), dma((7,)),
                        dma((14,)), dma((14,)), dma((7,)), dma((7,)), dma((7,)), dma((7,)), dma((2,)), dma((4,)), dma((4,)), dma((5,))],
        compiler_params=pltpu.CompilerParams(collective_id=0, has_side_effects=True, vmem_limit_bytes=63 * 1024 * 1024),
    )(x_in, tab, gains, qkv_rows, wo_own, w_gate, w_up, d_out)


def solution(mesh):
    n_dev = mesh.shape['sp']

    def layer_step(x_in, positions, d_out, norm1_gain, norm2_gain, w_q, w_k, w_v, w_o, w_gate, w_up, w_down):
        tokens, model = x_in.shape
        head_dim = w_q.shape[2]
        heads = w_q.shape[1] // n_dev
        rows_own = w_q.shape[0]
        inv_freq = 1.0 / (ROPE_BASE ** (jnp.arange(head_dim // 2, dtype=F32) * (2.0 / head_dim)))
        angles = positions.astype(F32)[:, None] * inv_freq[None, :]
        table = jnp.concatenate([jnp.cos(angles), jnp.sin(angles)], axis=1)
        table = jnp.concatenate([table[:tokens // 2], table[tokens // 2:]], axis=1)
        gains = jnp.zeros((8, rows_own), F32).at[0].set(norm1_gain.astype(F32)).at[1].set(norm2_gain.astype(F32))
        to_cols = lambda w: w.transpose(1, 2, 0).reshape(n_dev, -1, rows_own)
        qkv_rows = jnp.concatenate([to_cols(w_q), to_cols(w_k), to_cols(w_v)], axis=1)
        wo_own = w_o.reshape(-1, model)
        (q_rot, k_rot, v_lin, o_t, u_t, cos_tab, sin_tab, g_full, hidden,
         mlp_in, w1, w3, dout_all) = attention_step(heads, x_in, table, gains, qkv_rows, wo_own, w_gate, w_up, d_out)
        d_w1s, d_w3s, d_down, y_out, dh_all, d_g2 = mlp_step(mlp_in, dout_all, w1, w3, w_down, hidden, g_full)
        d_wo, d_wq_t, d_wk_t, d_wv_t, d_w1, d_w3, d_x, d_gains = attention_backward_step(
            heads, dh_all, wo_own, o_t, q_rot, k_rot, v_lin, (cos_tab, sin_tab),
            d_w1s, d_w3s, qkv_rows.reshape(-1, rows_own), u_t, x_in, g_full, d_g2)
        from_cols = lambda d, w: d.reshape(w.shape[1], w.shape[2], rows_own).transpose(2, 0, 1)
        return (y_out, d_x, d_gains[0], d_gains[1], from_cols(d_wq_t, w_q), from_cols(d_wk_t, w_k), from_cols(d_wv_t, w_v),
                d_wo.reshape(w_o.shape), d_w1, d_w3, d_down)

    all_rows = P('sp')
    return jax.shard_map(layer_step, mesh=mesh, in_specs=(all_rows,) * 12, out_specs=(all_rows,) * 11, check_vma=False)
```

```python
import functools
import jax
import jax.numpy as jnp
from jax import lax
from jax.experimental import pallas as pl
from jax.experimental.pallas import tpu as pltpu
from jax.sharding import PartitionSpec as P

ROPE_BASE = 10000.0
NORM_EPS = 1e-5
NEG_LARGE = -1e30
F32 = jnp.float32
BF16 = jnp.bfloat16
BLK = 256


def dot(lhs, rhs, lhs_dim, rhs_dim):
    return lax.dot_general(lhs, rhs, (((lhs_dim,), (rhs_dim,)), ((), ())), preferred_element_type=F32)


def norm_forward(hidden, gain_vec):
    inv_rms = lax.rsqrt(jnp.mean(hidden * hidden, axis=-1, keepdims=True) + NORM_EPS)
    return hidden * inv_rms * gain_vec


def probs_transposed(k_rows, q_blk, start):
    scores = dot(k_rows, q_blk, 1, 1)
    rows = lax.broadcasted_iota(jnp.int32, (BLK, BLK), 0)
    cols = lax.broadcasted_iota(jnp.int32, (BLK, BLK), 1)
    tail = jnp.where(rows <= cols, scores[start:], NEG_LARGE)
    scores = jnp.concatenate([scores[:start], tail], axis=0) if start else tail
    top = jnp.max(scores, axis=0, keepdims=True)
    weights = jnp.exp((scores - top) * (q_blk.shape[1] ** -0.5))
    return weights * (1.0 / jnp.sum(weights, axis=0, keepdims=True))


MESH = pl.DeviceIdType.MESH


def place(axis):
    me = lax.axis_index(axis)
    core = lax.rem(me, 2)
    col = lax.rem(lax.div(me, 2), 2)
    row = lax.div(me, 4)

    def other(flip_core, flip_col, flip_row):
        pick = lambda v, f: 1 - v if f else v
        return pick(row, flip_row) * 4 + pick(col, flip_col) * 2 + pick(core, flip_core)

    nbr_x, nbr_y = other(0, 1, 0), other(0, 0, 1)
    first = nbr_x * (1 - core) + nbr_y * core
    second = nbr_y * (1 - core) + nbr_x * core
    return me, other, first, second


def greet(other):
    barrier = pltpu.get_barrier_semaphore()
    for r in range(1, 8):
        pl.semaphore_signal(barrier, inc=1, device_id=(other(r & 1, (r >> 1) & 1, r >> 2),), device_id_type=MESH)
    pl.semaphore_wait(barrier, 7)


class Gather:
    def __init__(self, slot, send_sem, recv_sem, where, own=None):
        me, other, first, second = where
        partner, diag = other(1, 0, 0), other(0, 1, 1)
        own = slot(me) if own is None else own
        self.copies = []
        plan = [(own, me, first), (own, me, second), (own, me, partner), (slot(first), first, second),
                (slot(first), first, partner), (slot(second), second, partner), (slot(diag), diag, partner)]
        for i, (src, what, dest) in enumerate(plan):
            self.copies.append(pltpu.make_async_remote_copy(
                src_ref=src, dst_ref=slot(what), send_sem=send_sem.at[i], recv_sem=recv_sem.at[i],
                device_id=(dest,), device_id_type=MESH))

    def start(self):
        for i in range(3):
            self.copies[i].start()

    def got_first(self):
        self.copies[0].wait_recv()
        self.copies[3].start()
        self.copies[4].start()

    def got_second(self):
        self.copies[1].wait_recv()
        self.copies[5].start()

    def got_diag(self):
        self.copies[3].wait_recv()
        self.copies[6].start()

    def got_partner(self, i):
        self.copies[(2, 4, 5, 6)[i]].wait_recv()

    def drain(self):
        for copy in self.copies:
            copy.wait_send()


def turn_halves(values, cos_blk, sin_blk):
    width = values.shape[1]
    lanes = lax.broadcasted_iota(jnp.int32, values.shape, 1)
    partner = jnp.where(lax.rem(lanes, 64) < 32, pltpu.roll(values, width - 32, 1), pltpu.roll(values, 32, 1))
    return values * cos_blk + partner * sin_blk


def norm_backward(hidden, gain, d_out):
    inv = lax.rsqrt(jnp.mean(hidden * hidden, axis=-1, keepdims=True) + NORM_EPS)
    d_scaled = d_out * gain
    d_hidden = d_scaled * inv - hidden * (inv * inv * inv * jnp.mean(d_scaled * hidden, axis=-1, keepdims=True))
    return d_hidden, jnp.sum(d_out * (hidden * inv), axis=0, keepdims=True)


def attn_bwd_comm_kernel(axis, heads, dh_hbm, wo_hbm, ot_hbm, q_hbm, k_hbm, v_hbm, cos_hbm, sin_hbm,
                         dw1_ref, dw3_ref, wq_hbm, wk_hbm, wv_hbm, ut_hbm, x_hbm, g_hbm, dg2_hbm,
                         dwo_hbm, dwq_hbm, dwk_hbm, dwv_hbm, out1_ref, out3_ref, dx_hbm, dg_hbm,
                         dh_ref, wo_ref, ot_ref, q_ref, k_ref, v_ref, cos_ref, sin_ref, wq_ref, wk_ref, wv_ref, ut_ref, x_ref, g_ref, dg2_ref,
                         dwo_ref, dwq_ref, dwk_ref, dwv_ref, dx_ref, dg_ref,
                         slots, do_scr, dq_scr, dg_own, dg_all, dk_acc, dv_acc, du_acc, du_scr, du_recv, stage,
                         bulk_send, bulk_recv, hg_send, hg_recv, gat_send, gat_recv, du_send, du_rsem, dg_send, dg_recv, loc_sem, ld_sem, st_sem):
    loads = {}
    for i, (name, src, dst) in enumerate((
            ('wo', wo_hbm, wo_ref), ('ot', ot_hbm, ot_ref), ('q', q_hbm, q_ref), ('k', k_hbm, k_ref),
            ('v', v_hbm, v_ref), ('cos', cos_hbm, cos_ref), ('sin', sin_hbm, sin_ref), ('wq', wq_hbm, wq_ref), ('wk', wk_hbm, wk_ref),
            ('wv', wv_hbm, wv_ref), ('ut', ut_hbm, ut_ref), ('x', x_hbm, x_ref), ('g', g_hbm, g_ref), ('dg2', dg2_hbm, dg2_ref),
            ('dh', dh_hbm, dh_ref.at[pl.ds(pl.multiple_of(lax.axis_index(axis) * x_ref.shape[0], x_ref.shape[0]), x_ref.shape[0]), :]))):
        loads[name] = pltpu.make_async_copy(src, dst, ld_sem.at[i])
        loads[name].start()

    def need(*names):
        for name in names:
            loads[name].wait()

    stores = [pltpu.make_async_copy(src, dst, st_sem.at[i]) for i, (src, dst) in enumerate((
        (dwo_ref, dwo_hbm), (dwq_ref, dwq_hbm), (dwk_ref, dwk_hbm), (dwv_ref, dwv_hbm), (dx_ref, dx_hbm), (dg_ref, dg_hbm)))]
    where = place(axis)
    me, other, first, second = where
    greet(other)
    seq_len, head_dim = k_ref.shape
    rows_own, hid = stage.shape[1], stage.shape[2]
    tokens = x_ref.shape[0]
    qw = heads * head_dim
    half_rows = rows_own // 2

    rows_of = lambda d: pl.ds(pl.multiple_of(d * rows_own, rows_own), rows_own)
    hid_of = lambda d: pl.ds(pl.multiple_of(d * hid, hid), hid)
    pairs = ((dw1_ref, out1_ref), (dw3_ref, out3_ref))
    peers = [other(r & 1, (r >> 1) & 1, r >> 2) for r in (2, 4, 6, 3, 5, 7, 1)]
    bulk = []
    for part in range(4):
        src, dst = pairs[part // 2]
        for n, dest in enumerate(peers):
            low = (part % 2) * half_rows
            bulk.append(pltpu.make_async_remote_copy(
                src_ref=src.at[pl.ds(pl.multiple_of(dest * rows_own + low, half_rows), half_rows), :],
                dst_ref=dst.at[pl.ds(low, half_rows), hid_of(me)], send_sem=bulk_send.at[part * 7 + n],
                recv_sem=bulk_recv.at[part * 7 + n], device_id=(dest,), device_id_type=MESH))

    def start_bulk(part):
        for copy in bulk[part * 7:part * 7 + 7]:
            copy.start()
    tok_of = lambda d: pl.ds(pl.multiple_of(d * tokens, tokens), tokens)
    h_gather = Gather(lambda d: dh_ref.at[tok_of(d), :], hg_send, hg_recv, where, own=dh_hbm)
    h_gather.start()
    for i, (src, dst) in enumerate(pairs):
        pltpu.make_async_copy(src.at[rows_of(me), :], stage.at[i], loc_sem.at[i]).start()
    need('dh', 'wo', 'ot')
    h_gather.got_first()
    h_gather.got_second()
    start_bulk(0)
    start_bulk(1)
    h_gather.got_diag()
    for i in range(4):
        h_gather.got_partner(i)

    def split_out_grad(k, _):
        rows = pl.ds(pl.multiple_of(k * BLK, BLK), BLK)
        do_blk = dot(dh_ref[rows, :], wo_ref[...], 1, 1).astype(BF16)
        for h in range(heads):
            do_scr[h, rows, :] = do_blk[:, h * head_dim:(h + 1) * head_dim]
        cols = rows
        dwo_ref[:, cols] = dot(ot_ref[...], dh_ref[:, cols], 1, 0)
        return 0
    lax.fori_loop(0, seq_len // BLK, split_out_grad, 0)
    stores[0].start()

    for i, (src, dst) in enumerate(pairs):
        pltpu.make_async_copy(src.at[rows_of(me), :], stage.at[i], loc_sem.at[i]).wait()
        pltpu.make_async_copy(stage.at[i], dst.at[:, hid_of(me)], loc_sem.at[2 + i]).start()

    need('q', 'k', 'v')
    dk_acc[...] = jnp.zeros_like(dk_acc)
    dv_acc[...] = jnp.zeros_like(dv_acc)
    mine = slots.at[me]

    def one_head(h, _):
        def one_block(start):
            keys = pl.ds(0, start + BLK)
            rows = pl.ds(start, BLK)
            q_blk, do_blk = q_ref[h, rows, :], do_scr[h, rows, :]
            probs = probs_transposed(k_ref[keys, :], q_blk, start)
            d_probs = dot(v_ref[keys, :], do_blk, 1, 1).astype(BF16).astype(F32)
            row_dot = jnp.sum(d_probs * probs, axis=0, keepdims=True)
            d_scores = (probs * (d_probs - row_dot) * (head_dim ** -0.5)).astype(BF16)
            dq_scr[h, rows, :] = dot(d_scores, k_ref[keys, :], 0, 0).astype(BF16)
            dk_acc[keys, :] += dot(d_scores, q_blk, 1, 0)
            dv_acc[keys, :] += dot(probs.astype(BF16), do_blk, 1, 0)
        for start in range(0, seq_len, BLK):
            one_block(start)
        return 0
    lax.fori_loop(0, heads, one_head, 0)
    need('cos', 'sin')
    mine[:, qw:qw + head_dim] = dk_acc[...].astype(BF16)
    mine[:, qw + head_dim:] = dv_acc[...].astype(BF16)
    low = lax.broadcasted_iota(jnp.int32, (BLK, 128), 1) < head_dim

    def turn_back(k, _):
        rows = pl.ds(pl.multiple_of(k * BLK, BLK), BLK)
        cos_blk, sin_blk = cos_ref[rows, :], -sin_ref[rows, :]
        for pair in range(heads // 2):
            both = jnp.concatenate([dq_scr[2 * pair, rows, :], dq_scr[2 * pair + 1, rows, :]], axis=1)
            mine[rows, pair * 128:(pair + 1) * 128] = turn_halves(both.astype(F32), cos_blk, sin_blk).astype(BF16)
        kv = mine[rows, qw:].astype(F32)
        mine[rows, qw:] = jnp.where(low, turn_halves(kv, cos_blk, sin_blk), kv).astype(BF16)
        return 0
    lax.fori_loop(0, seq_len // BLK, turn_back, 0)

    gather = Gather(lambda d: slots.at[d], gat_send, gat_recv, where)
    gather.start()
    du_acc[...] = jnp.zeros_like(du_acc)
    need('wq', 'wk', 'wv', 'ut')

    def use(d):
        q_rows = pl.ds(pl.multiple_of(d * qw, qw), qw)
        kv_rows = pl.ds(pl.multiple_of(d * head_dim, head_dim), head_dim)
        w_all = jnp.concatenate([wq_ref[q_rows, :], wk_ref[kv_rows, :], wv_ref[kv_rows, :]], axis=0)

        def add_rows(k, _):
            rows = pl.ds(pl.multiple_of(k * 512, 512), 512)
            du_acc[rows, :] += dot(slots[d, rows, :], w_all, 1, 0)
            return 0
        lax.fori_loop(0, seq_len // 512, add_rows, 0)
        d_w = dot(ut_ref[...], slots[d], 1, 0).T
        dwq_ref[q_rows, :] = d_w[:qw]
        dwk_ref[kv_rows, :] = d_w[qw:qw + head_dim]
        dwv_ref[kv_rows, :] = d_w[qw + head_dim:]

    def use_many(*devices):
        def body(i, _):
            d = devices[0]
            for n in range(1, len(devices)):
                d = jnp.where(i == n, devices[n], d)
            use(d)
            return 0
        lax.fori_loop(0, len(devices), body, 0)

    use_many(me)
    gather.got_first()
    gather.got_second()
    start_bulk(2)
    gather.got_partner(0)
    use_many(first, second, other(1, 0, 0))
    gather.got_diag()
    for i in range(1, 4):
        gather.got_partner(i)
    use_many(other(0, 1, 1), other(1, 1, 0), other(1, 0, 1), other(1, 1, 1))
    du_scr[...] = du_acc[...].astype(BF16)
    for i in range(1, 4):
        stores[i].start()

    sends = []
    for n, dest in enumerate(peers):
        sends.append(pltpu.make_async_remote_copy(
            src_ref=du_scr.at[tok_of(dest), :], dst_ref=du_recv.at[:, rows_of(me)], send_sem=du_send.at[n],
            recv_sem=du_rsem.at[n], device_id=(dest,), device_id_type=MESH))
        sends[-1].start()
    start_bulk(3)
    du_recv[:, rows_of(me)] = du_scr[tok_of(me), :]
    need('x', 'g', 'dg2')
    for copy in sends:
        copy.wait_recv()
    dg_own[...] = jnp.zeros_like(dg_own)
    dg_own[1:2, :] = dg2_ref[...]

    def input_grad(k, _):
        part = pl.ds(pl.multiple_of(k * 16, 16), 16)
        d_norm, d_gain = norm_backward(x_ref[part, :].astype(F32), g_ref[0:1, :], du_recv[part, :].astype(F32))
        dh_part = dh_ref[pl.ds(pl.multiple_of(me * tokens + k * 16, 16), 16), :]
        dx_ref[part, :] = (dh_part.astype(F32) + d_norm).astype(BF16)
        dg_own[0:1, :] += d_gain
        return 0
    lax.fori_loop(0, tokens // 16, input_grad, 0)
    stores[4].start()
    gain_sends = []
    for n, dest in enumerate(peers):
        gain_sends.append(pltpu.make_async_remote_copy(
            src_ref=dg_own.at[:, rows_of(dest)], dst_ref=dg_all.at[me], send_sem=dg_send.at[n],
            recv_sem=dg_recv.at[n], device_id=(dest,), device_id_type=MESH))
        gain_sends[-1].start()
    dg_all[me] = dg_own[:, rows_of(me)]
    for copy in gain_sends:
        copy.wait_recv()
    dg_ref[...] = jnp.sum(dg_all[...], axis=0)
    stores[5].start()
    for copy in sends + gain_sends:
        copy.wait_send()
    gather.drain()
    h_gather.drain()
    for copy in bulk:
        copy.wait()
    for i, (src, dst) in enumerate(pairs):
        pltpu.make_async_copy(stage.at[i], dst.at[:, hid_of(me)], loc_sem.at[2 + i]).wait()
    for copy in stores:
        copy.wait()


def attention_backward_step(heads, dh_own, wo_own, o_t, q_rot, k_rot, v_lin, tables, d_w1, d_w3, w_q, w_k, w_v, u_t, x_in, gains, d_g2):
    seq_len, model = k_rot.shape[0], x_in.shape[1]
    head_dim = k_rot.shape[1]
    tokens = x_in.shape[0]
    rows_own, hid = model // 8, d_w1.shape[1]
    shape = jax.ShapeDtypeStruct
    hbm = pl.BlockSpec(memory_space=pl.ANY)
    dma = pltpu.SemaphoreType.DMA
    vm = lambda *dims, dtype=BF16: pltpu.VMEM(dims, dtype)
    early = (dh_own, wo_own, o_t, q_rot, k_rot, v_lin, *tables)
    late = (w_q, w_k, w_v, u_t, x_in, gains, d_g2)
    outs = (shape(wo_own.shape, F32), shape(w_q.shape, F32), shape(w_k.shape, F32), shape(w_v.shape, F32))
    ends = (shape(x_in.shape, BF16), shape((8, rows_own), F32))
    return pl.pallas_call(
        functools.partial(attn_bwd_comm_kernel, 'sp', heads), name='attn_bwd_comm',
        in_specs=[hbm] * 17, out_specs=[hbm] * 8,
        out_shape=[*outs, shape((rows_own, 8 * hid), F32), shape((rows_own, 8 * hid), F32), *ends],
        scratch_shapes=[vm(seq_len, model)] + [vm(*t.shape, dtype=t.dtype) for t in early[1:] + late + outs + ends] + [
            vm(8, seq_len, 384), vm(heads, seq_len, head_dim), vm(heads, seq_len, head_dim),
            vm(8, model, dtype=F32), vm(8, 8, rows_own, dtype=F32),
            vm(seq_len, head_dim, dtype=F32), vm(seq_len, head_dim, dtype=F32),
            vm(seq_len, rows_own, dtype=F32), vm(seq_len, rows_own), vm(tokens, model), vm(2, rows_own, hid, dtype=F32),
            dma((28,)), dma((28,)), dma((7,)), dma((7,)), dma((7,)), dma((7,)), dma((7,)), dma((7,)), dma((7,)), dma((7,)), dma((4,)), dma((15,)), dma((6,))],
        compiler_params=pltpu.CompilerParams(collective_id=2, has_side_effects=True, vmem_limit_bytes=63 * 1024 * 1024),
    )(*early, d_w1, d_w3, *late)


def mlp_comm_kernel(axis, m_ref, dout_own, w1_hbm, w3_hbm, w2_hbm, h_hbm, g_hbm,
                    dw1_ref, dw3_ref, dw2_ref, y_hbm, dh_hbm, dg2_hbm, dout_ref,
                    w1_ref, w3_ref, w2_ref, h_ref, g_ref, y_ref, dg2_ref,
                    glu, gate_s, up_s, outbox, chip_sum, inbox, blk, m_col, do_col, mt_scr, dot_scr, st1, st3, st2, dh_own,
                    part_send, part_recv, mail_send, mail_recv, do_send, do_recv,
                    in_sem, col_sem, out_sem, own_sem, ld_sem, credit):
    loads = [pltpu.make_async_copy(src, dst, ld_sem.at[i]) for i, (src, dst) in enumerate((
        (w1_hbm, w1_ref), (w3_hbm, w3_ref), (w2_hbm, w2_ref), (h_hbm, h_ref), (g_hbm, g_ref)))]
    own_in = pltpu.make_async_copy(dout_own, dh_own, own_sem.at[0])
    for copy in loads + [own_in]:
        copy.start()
    where = place(axis)
    me, other, first, second = where
    core = lax.rem(me, 2)
    partner = other(1, 0, 0)
    tokens, model = h_ref.shape
    hid = w1_ref.shape[1]
    tok_of = lambda d: pl.ds(pl.multiple_of(d * tokens, tokens), tokens)
    off_first, off_second = 1 + core, 2 - core

    def block_of(off, flip):
        d_col, d_row = lax.rem(off, 2), lax.div(off, 2)
        col, row = lax.rem(lax.div(me, 2), 2), lax.div(me, 4)
        mix = lambda v, f: v + f - 2 * v * f
        return mix(row, d_row) * 4 + mix(col, d_col) * 2 + mix(core, flip)

    def step_off(step, flip):
        mid_a = off_second * (1 - flip) + off_first * flip
        mid_b = off_first * (1 - flip) + off_second * flip
        return jnp.where(step == 0, 3, jnp.where(step == 1, mid_a, jnp.where(step == 2, mid_b, 0)))

    def half_rows(half):
        flip = 1 - lax.rem(half, 2)
        return tok_of(block_of(step_off(lax.div(half, 2), flip), flip))

    def fetch(half):
        slot = lax.rem(half, 2)
        return pltpu.make_async_copy(m_ref.at[half_rows(half), :], blk.at[slot], in_sem.at[slot])

    def fetch_dout(d):
        slot = lax.rem(d, 2)
        return pltpu.make_async_copy(dout_ref.at[tok_of(d), :], blk.at[slot], in_sem.at[slot])

    def fetch_cols(j):
        cols = pl.ds(pl.multiple_of(j * 256, 256), 256)
        return (pltpu.make_async_copy(m_ref.at[:, cols], m_col, col_sem.at[0]),
                pltpu.make_async_copy(dout_ref.at[:, cols], do_col, col_sem.at[1]))

    def sigmoid(value):
        return 1.0 / (1.0 + jnp.exp(-value))

    def activations(slot, rows):
        def chunk(j, _):
            cols = pl.ds(pl.multiple_of(j * 512, 512), 512)
            gate = dot(blk[slot], w1_ref[:, cols], 1, 0).astype(BF16)
            up = dot(blk[slot], w3_ref[:, cols], 1, 0).astype(BF16)
            gate_s[rows, cols] = gate
            up_s[rows, cols] = up
            gate = gate.astype(F32)
            glu[rows, cols] = (gate * sigmoid(gate) * up.astype(F32)).astype(BF16)
            return 0
        lax.fori_loop(0, hid // 512, chunk, 0)

    def activation_grads(slot, rows):
        def chunk(j, _):
            cols = pl.ds(pl.multiple_of(j * 512, 512), 512)
            d_act = dot(blk[slot], w2_ref[cols, :], 1, 1).astype(BF16).astype(F32)
            gate, up = gate_s[rows, cols].astype(F32), up_s[rows, cols].astype(F32)
            sig = sigmoid(gate)
            silu = gate * sig
            up_s[rows, cols] = (d_act * silu).astype(BF16)
            gate_s[rows, cols] = (d_act * up * (sig + silu * (1.0 - sig))).astype(BF16)
            return 0
        lax.fori_loop(0, hid // 512, chunk, 0)

    def add_mlp_grad(rows, put):
        def chunk(j, _):
            cols = pl.ds(pl.multiple_of(j * 512, 512), 512)
            put(cols, dot(gate_s[rows, :], w1_ref[cols, :], 1, 1) + dot(up_s[rows, :], w3_ref[cols, :], 1, 1))
            return 0
        lax.fori_loop(0, model // 512, chunk, 0)

    def add_mlp_out(rows, put):
        def chunk(j, _):
            cols = pl.ds(pl.multiple_of(j * 512, 512), 512)
            put(cols, dot(glu[rows, :], w2_ref[:, cols], 1, 0))
            return 0
        lax.fori_loop(0, model // 512, chunk, 0)

    def signal(index, device):
        pl.semaphore_signal(credit.at[index], inc=1, device_id=(device,), device_id_type=MESH)

    class Scatter:
        def __init__(self, turn):
            self.turn = turn

        def to_partner(self, step):
            off = step_off(step, 1)
            return pltpu.make_async_remote_copy(
                src_ref=outbox.at[lax.rem(step, 2)], dst_ref=chip_sum.at[off], send_sem=part_send.at[self.turn, step],
                recv_sem=part_recv.at[self.turn, off], device_id=(partner,), device_id_type=MESH)

        def from_partner(self, off):
            return pltpu.make_async_remote_copy(
                src_ref=outbox.at[0], dst_ref=chip_sum.at[off], send_sem=part_send.at[self.turn, 0],
                recv_sem=part_recv.at[self.turn, off], device_id=(partner,), device_id_type=MESH)

        def mail(self, kind):
            off = (3, off_first, off_second)[kind]
            dest = (first, first, second)[kind]
            return pltpu.make_async_remote_copy(
                src_ref=chip_sum.at[off], dst_ref=inbox.at[kind], send_sem=mail_send.at[self.turn, kind],
                recv_sem=mail_recv.at[self.turn, kind], device_id=(dest,), device_id_type=MESH)

        def step(self, step, prepare, partial):
            slot = lax.rem(step, 2)
            prepare(2 * step)

            def put_out(cols, value):
                outbox[slot, :, cols] = value
            partial(half_rows(2 * step), put_out)
            self.to_partner(step).start()
            prepare(2 * step + 1)
            off = step_off(step, 0)
            self.from_partner(off).wait_recv()

            def put_sum(cols, value):
                chip_sum[off, :, cols] += value
            partial(half_rows(2 * step + 1), put_sum)

        def pass_on(self):
            self.mail(0).wait_recv()

            def add_mail(k, _):
                part = pl.ds(pl.multiple_of(k * 16, 16), 16)
                chip_sum[off_second, part, :] += inbox[0, part, :]
                return 0
            lax.fori_loop(0, tokens // 16, add_mail, 0)

    out_round, grad_round = Scatter(0), Scatter(1)

    def prepare_out(half):
        @pl.when(half < 7)
        def _():
            fetch(half + 1).start()
        fetch(half).wait()
        activations(lax.rem(half, 2), half_rows(half))

    def weight_grads(begin, end):
        for copy in fetch_cols(begin):
            copy.start()

        def body(j, _):
            for copy in fetch_cols(j):
                copy.wait()

            def turn(k, _):
                part = pl.ds(pl.multiple_of(k * 256, 256), 256)
                mt_scr[:, part] = m_col[part, :].T
                dot_scr[:, part] = do_col[part, :].T
                return 0
            lax.fori_loop(0, m_col.shape[0] // 256, turn, 0)

            @pl.when(j + 1 < end)
            def _():
                for copy in fetch_cols(j + 1):
                    copy.start()
            rows = pl.ds(pl.multiple_of(j * 256, 256), 256)
            out = (pltpu.make_async_copy(st1, dw1_ref.at[rows, :], out_sem.at[0]),
                   pltpu.make_async_copy(st3, dw3_ref.at[rows, :], out_sem.at[1]),
                   pltpu.make_async_copy(st2, dw2_ref.at[:, rows], out_sem.at[2]))

            @pl.when(j > begin)
            def _():
                for copy in out:
                    copy.wait()

            def chunk(k, _):
                cols = pl.ds(pl.multiple_of(k * 512, 512), 512)
                st1[:, cols] = dot(mt_scr[...], gate_s[:, cols], 1, 0)
                st3[:, cols] = dot(mt_scr[...], up_s[:, cols], 1, 0)
                st2[cols, :] = dot(dot_scr[...], glu[:, cols], 1, 0).T
                return 0
            lax.fori_loop(0, hid // 512, chunk, 0)
            for copy in out:
                copy.start()
            return 0
        lax.fori_loop(begin, end, body, 0)
        rows = pl.ds((end - 1) * 256, 256)
        for copy in (pltpu.make_async_copy(st1, dw1_ref.at[rows, :], out_sem.at[0]),
                     pltpu.make_async_copy(st3, dw3_ref.at[rows, :], out_sem.at[1]),
                     pltpu.make_async_copy(st2, dw2_ref.at[:, rows], out_sem.at[2])):
            copy.wait()

    fetch(0).start()
    greet(other)
    do_gather = Gather(lambda d: dout_ref.at[tok_of(d), :], do_send, do_recv, where, own=dout_own)
    do_gather.start()
    own_in.wait()
    own_out = pltpu.make_async_copy(dh_own, dout_ref.at[tok_of(me), :], own_sem.at[1])
    own_out.start()
    for copy in loads:
        copy.wait()

    def out_step(step, _):
        @pl.when(step >= 2)
        def _():
            out_round.to_partner(step - 2).wait_send()
        out_round.step(step, prepare_out, add_mlp_out)

        @pl.when(step == 0)
        def _():
            out_round.mail(0).start()

        @pl.when(step == 2)
        def _():
            out_round.mail(1).start()
            do_gather.got_first()
            do_gather.got_second()
        return 0
    lax.fori_loop(0, 4, out_step, 0)
    out_round.pass_on()
    out_round.mail(2).start()
    for step in (2, 3):
        out_round.to_partner(step).wait_send()
    out_round.mail(0).wait_send()
    signal(0, partner)
    signal(1, first)
    do_gather.got_diag()
    for i in range(4):
        do_gather.got_partner(i)
    own_out.wait()
    fetch_dout(0).start()

    def grad_block(d, _):
        @pl.when(d < 7)
        def _():
            fetch_dout(d + 1).start()
        fetch_dout(d).wait()
        activation_grads(lax.rem(d, 2), tok_of(d))
        return 0
    lax.fori_loop(0, 8, grad_block, 0)

    pl.semaphore_wait(credit.at[0], 1)
    grad_round.step(0, lambda half: None, add_mlp_grad)
    pl.semaphore_wait(credit.at[1], 1)
    grad_round.mail(0).start()
    weight_grads(0, 2)
    out_round.mail(1).wait_recv()
    out_round.mail(2).wait_recv()

    def layer_out(k, _):
        part = pl.ds(pl.multiple_of(k * 16, 16), 16)
        y_ref[part, :] = (h_ref[part, :].astype(F32) + (chip_sum[0, part, :] + inbox[1, part, :] + inbox[2, part, :])).astype(BF16)
        return 0
    lax.fori_loop(0, tokens // 16, layer_out, 0)
    y_store = pltpu.make_async_copy(y_ref, y_hbm, own_sem.at[2])
    y_store.start()
    out_round.mail(1).wait_send()
    out_round.mail(2).wait_send()
    signal(2, partner)
    signal(3, first)
    signal(4, second)
    pl.semaphore_wait(credit.at[2], 1)

    def grad_step(step, _):
        @pl.when(step >= 2)
        def _():
            grad_round.to_partner(step - 2).wait_send()
        grad_round.step(step, lambda half: None, add_mlp_grad)

        @pl.when(step == 2)
        def _():
            pl.semaphore_wait(credit.at[3], 1)
            grad_round.mail(1).start()
            grad_round.pass_on()
            pl.semaphore_wait(credit.at[4], 1)
            grad_round.mail(2).start()
        return 0
    lax.fori_loop(1, 4, grad_step, 0)
    weight_grads(2, 8)
    grad_round.mail(1).wait_recv()
    grad_round.mail(2).wait_recv()
    dg2_ref[...] = jnp.zeros_like(dg2_ref)

    def hidden_grad(k, _):
        part = pl.ds(pl.multiple_of(k * 16, 16), 16)
        d_mlp = (chip_sum[0, part, :] + inbox[1, part, :] + inbox[2, part, :]).astype(BF16).astype(F32)
        d_norm, d_gain = norm_backward(h_ref[part, :].astype(F32), g_ref[1:2, :], d_mlp)
        dh_own[part, :] = (dh_own[part, :].astype(F32) + d_norm).astype(BF16)
        dg2_ref[...] += d_gain
        return 0
    lax.fori_loop(0, tokens // 16, hidden_grad, 0)
    own_out = pltpu.make_async_copy(dh_own, dh_hbm, own_sem.at[3])
    own_out.start()
    dg2_store = pltpu.make_async_copy(dg2_ref, dg2_hbm, own_sem.at[4])
    dg2_store.start()
    for step in (2, 3):
        grad_round.to_partner(step).wait_send()
    for kind in range(3):
        grad_round.mail(kind).wait_send()
    do_gather.drain()
    own_out.wait()
    y_store.wait()
    dg2_store.wait()


def mlp_step(m_all, d_out, w1, w3, w2, hidden, gains):
    seq_len, model = m_all.shape
    hid, tokens = w1.shape[1], hidden.shape[0]
    shape = jax.ShapeDtypeStruct
    hbm = pl.BlockSpec(memory_space=pl.ANY)
    dma = pltpu.SemaphoreType.DMA
    vm = lambda *dims, dtype=BF16: pltpu.VMEM(dims, dtype)
    return pl.pallas_call(
        functools.partial(mlp_comm_kernel, 'sp'), name='mlp_comm',
        in_specs=[hbm] * 7, out_specs=[hbm] * 7,
        out_shape=[shape((model, hid), F32), shape((model, hid), F32), shape((hid, model), F32),
                   shape(hidden.shape, BF16), shape(hidden.shape, BF16), shape((1, model), F32), shape((seq_len, model), BF16)],
        scratch_shapes=[vm(*t.shape, dtype=t.dtype) for t in (w1, w3, w2, hidden, gains)] + [
            vm(tokens, model), vm(1, model, dtype=F32),
            vm(seq_len, hid), vm(seq_len, hid), vm(seq_len, hid),
            vm(2, tokens, model, dtype=F32), vm(4, tokens, model, dtype=F32), vm(3, tokens, model, dtype=F32),
            vm(2, tokens, model), vm(seq_len, 256), vm(seq_len, 256), vm(256, seq_len), vm(256, seq_len),
            vm(256, hid, dtype=F32), vm(256, hid, dtype=F32), vm(hid, 256, dtype=F32), vm(tokens, model),
            dma((2, 4)), dma((2, 4)), dma((2, 3)), dma((2, 3)), dma((7,)), dma((7,)),
            dma((2,)), dma((2,)), dma((3,)), dma((5,)), dma((5,)), pltpu.SemaphoreType.REGULAR((5,))],
        compiler_params=pltpu.CompilerParams(collective_id=1, has_side_effects=True, vmem_limit_bytes=63 * 1024 * 1024),
    )(m_all, d_out, w1, w3, w2, hidden, gains)[:6]


def spread_tables(packed, upper):
    lanes = lax.broadcasted_iota(jnp.int32, packed.shape, 1)
    swapped = pltpu.roll(packed, 64, 1)
    both = jnp.where((lanes < 64) != upper, packed, swapped)
    low = lax.rem(lanes, 64) < 32
    return jnp.where(low, both, pltpu.roll(both, 32, 1)), jnp.where(low, -pltpu.roll(both, 96, 1), both)


def attention_comm_kernel(axis, heads, x_ref, ang_hbm, gain_ref, wq_ref, wk_ref, wv_ref, wo_ref, wg_ref, wu_ref,
                          q_hbm, k_hbm, v_hbm, ot_hbm, ut_hbm, cos_hbm, sin_hbm, gfull_hbm, h_hbm, m_ref, w1_ref, w3_ref,
                          q_ref, k_ref, v_ref, ot_ref, ut_ref, cos_ref, sin_ref, gfull_ref, h_ref, ang_ref, tab_ref, x_all, tab_all, gain_all, w_head, wo_all, o_all, u_blk, qkv_blk, o_scr, o_own, h_scr, m_out, stage,
                          g_send, g_recv, w_send, w_recv, x_send, x_recv, t_send, t_recv, wo_send, wo_recv, bulk_send, bulk_recv,
                          o_send, o_recv, m_loc, m_send, m_recv, loc_sem, own_sem, st_sem):
    ang_load = pltpu.make_async_copy(ang_hbm, ang_ref, own_sem.at[7])
    ang_load.start()
    where = place(axis)
    me, other, first, second = where
    core = lax.rem(me, 2)
    partner = other(1, 0, 0)
    greet(other)
    tokens, model = x_ref.shape
    seq_len, head_dim = k_ref.shape
    qw = heads * head_dim
    rows_own, hid = wg_ref.shape[0], w1_ref.shape[1]
    tok_of = lambda d: pl.ds(pl.multiple_of(d * tokens, tokens), tokens)
    cols_of = lambda d: pl.ds(pl.multiple_of(d * rows_own, rows_own), rows_own)
    hid_of = lambda d: pl.ds(pl.multiple_of(d * hid, hid), hid)
    peers = [other(r & 1, (r >> 1) & 1, r >> 2) for r in (6, 2, 4, 7, 3, 5, 1)]

    def to_all(src_of, dst, send_sem, recv_sem):
        return [pltpu.make_async_remote_copy(
            src_ref=src_of(dest), dst_ref=dst, send_sem=send_sem.at[n], recv_sem=recv_sem.at[n],
            device_id=(dest,), device_id_type=MESH) for n, dest in enumerate(peers)]

    small = to_all(lambda dest: gain_ref, gain_all.at[me], g_send, g_recv)
    q_of = lambda d: pl.ds(pl.multiple_of(d * qw, qw), qw)
    kv_of = lambda d: pl.ds(pl.multiple_of(d * head_dim, head_dim), head_dim)
    slices = (to_all(lambda dest: wq_ref.at[q_of(dest), :], w_head.at[0:qw, cols_of(me)], w_send.at[0], w_recv.at[0])
              + to_all(lambda dest: wk_ref.at[kv_of(dest), :], w_head.at[qw:qw + head_dim, cols_of(me)], w_send.at[1], w_recv.at[1])
              + to_all(lambda dest: wv_ref.at[kv_of(dest), :], w_head.at[qw + head_dim:, cols_of(me)], w_send.at[2], w_recv.at[2]))
    for copy in small + slices:
        copy.start()
    tab_slot = lambda d: tab_all.at[d]
    x_gather = Gather(lambda d: x_all.at[tok_of(d), :], x_send, x_recv, where, own=x_ref)
    t_gather = Gather(tab_slot, t_send, t_recv, where, own=tab_ref)
    x_gather.start()
    ang_load.wait()
    low = lax.rem(lax.broadcasted_iota(jnp.int32, ang_ref.shape, 1), head_dim) < head_dim // 2
    tab_ref[...] = jnp.where(low, jnp.cos(ang_ref[...]), jnp.sin(ang_ref[...]))
    t_gather.start()
    wo_gather = Gather(lambda d: wo_all.at[cols_of(d), :], wo_send, wo_recv, where, own=wo_ref)
    bulk = []
    part_rows = rows_own // 4
    for part in range(8):
        src, dst = ((wg_ref, w1_ref), (wu_ref, w3_ref))[part // 4]
        low = (part % 4) * part_rows
        for n, dest in enumerate(peers):
            bulk.append(pltpu.make_async_remote_copy(
                src_ref=src.at[pl.ds(low, part_rows), hid_of(dest)],
                dst_ref=dst.at[pl.ds(pl.multiple_of(me * rows_own + low, part_rows), part_rows), :],
                send_sem=bulk_send.at[part * 7 + n], recv_sem=bulk_recv.at[part * 7 + n], device_id=(dest,), device_id_type=MESH))

    def start_bulk(*parts):
        for part in parts:
            for copy in bulk[part * 7:part * 7 + 7]:
                copy.start()

    stores = [pltpu.make_async_copy(src, dst, st_sem.at[i]) for i, (src, dst) in enumerate((
        (q_ref, q_hbm), (k_ref, k_hbm), (v_ref, v_hbm), (ot_ref, ot_hbm), (ut_ref, ut_hbm), (cos_ref, cos_hbm),
        (sin_ref, sin_hbm), (gfull_ref, gfull_hbm), (h_ref, h_hbm)))]
    own = [pltpu.make_async_copy(src, dst, own_sem.at[i]) for i, (src, dst) in enumerate((
        (gain_ref, gain_all.at[me]), (wq_ref.at[q_of(me), :], w_head.at[0:qw, cols_of(me)]),
        (wk_ref.at[kv_of(me), :], w_head.at[qw:qw + head_dim, cols_of(me)]),
        (wv_ref.at[kv_of(me), :], w_head.at[qw + head_dim:, cols_of(me)]),
        (x_ref, x_all.at[tok_of(me), :]), (wo_ref, wo_all.at[cols_of(me), :])))]
    for copy in own:
        copy.start()
    local = []
    for i, (src, dst) in enumerate(((wg_ref, w1_ref), (wu_ref, w3_ref))):
        local.append((pltpu.make_async_copy(src.at[:, hid_of(me)], stage.at[i], loc_sem.at[i]),
                      pltpu.make_async_copy(stage.at[i], dst.at[cols_of(me), :], loc_sem.at[2 + i])))
        local[-1][0].start()
    tab_all[me] = tab_ref[...]
    for load, store in local:
        load.wait()
        store.start()
    for copy in own:
        copy.wait()
    for copy in small:
        copy.wait_recv()
    for d in range(8):
        gfull_ref[:, d * rows_own:(d + 1) * rows_own] = gain_all[d]
    for copy in slices:
        copy.wait_recv()

    def use(d):
        base = pl.multiple_of(d * tokens, tokens)

        def norm(k, _):
            part = pl.ds(pl.multiple_of(k * 16, 16), 16)
            x_part = x_all[pl.ds(pl.multiple_of(base + k * 16, 16), 16), :].astype(F32)
            u_blk[part, :] = norm_forward(x_part, gfull_ref[0:1, :]).astype(BF16)
            return 0
        lax.fori_loop(0, tokens // 16, norm, 0)
        ut_ref[:, tok_of(d)] = u_blk[:, cols_of(me)].T
        qkv_blk[...] = dot(u_blk[...], w_head[...], 1, 1).astype(BF16)
        half = tokens // 2
        for part in range(2):
            rows = pl.ds(pl.multiple_of(base + part * half, half), half)
            cos_blk, sin_blk = spread_tables(tab_all[d], part == 1)
            cos_ref[rows, :] = cos_blk
            sin_ref[rows, :] = sin_blk
            source = slice(part * half, (part + 1) * half)
            for pair in range(heads // 2):
                turned = turn_halves(qkv_blk[source, pair * 128:(pair + 1) * 128].astype(F32), cos_blk, sin_blk).astype(BF16)
                q_ref[2 * pair, rows, :] = turned[:, :head_dim]
                q_ref[2 * pair + 1, rows, :] = turned[:, head_dim:]
            turned = turn_halves(qkv_blk[source, qw:].astype(F32), cos_blk, sin_blk).astype(BF16)
            k_ref[rows, :] = turned[:, :head_dim]
            v_ref[rows, :] = qkv_blk[source, qw + head_dim:]

    x_gather.got_first()
    t_gather.got_first()
    x_gather.got_second()
    t_gather.got_second()
    wo_gather.start()
    start_bulk(0, 1)
    x_gather.got_partner(0)
    t_gather.got_partner(0)

    def use_near(i, _):
        use(jnp.where(i == 0, me, jnp.where(i == 1, first, jnp.where(i == 2, second, partner))))
        return 0
    lax.fori_loop(0, 4, use_near, 0)
    x_gather.got_diag()
    t_gather.got_diag()
    for i in range(1, 4):
        x_gather.got_partner(i)
        t_gather.got_partner(i)

    def use_far(i, _):
        use(jnp.where(i == 0, other(0, 1, 1), jnp.where(i == 1, other(1, 1, 0), jnp.where(i == 2, other(1, 0, 1), other(1, 1, 1)))))
        return 0
    lax.fori_loop(0, 4, use_far, 0)

    def one_head(h, _):
        for start in range(0, seq_len, BLK):
            keys, rows = pl.ds(0, start + BLK), pl.ds(start, BLK)
            probs = probs_transposed(k_ref[keys, :], q_ref[h, rows, :], start)
            o_scr[h, rows, :] = dot(probs.astype(BF16), v_ref[keys, :], 0, 0).astype(BF16)
        return 0
    for i in (0, 1, 2, 4, 5, 6, 7):
        stores[i].start()
    lax.fori_loop(0, heads, one_head, 0)
    for h in range(heads):
        o_own[:, h * head_dim:(h + 1) * head_dim] = o_scr[h]
    o_gather = Gather(lambda d: o_all.at[:, cols_of(d)], o_send, o_recv, where, own=o_own)
    o_gather.start()
    wo_gather.got_first()
    wo_gather.got_second()
    start_bulk(2)
    o_all[:, cols_of(me)] = o_own[...]

    def turn_out(k, _):
        rows = tok_of(k)
        ot_ref[:, rows] = o_own[rows, :].T
        return 0
    lax.fori_loop(0, 8, turn_out, 0)
    stores[3].start()
    wo_gather.got_diag()
    for i in range(4):
        wo_gather.got_partner(i)
    o_gather.got_first()
    o_gather.got_second()
    start_bulk(3)
    o_gather.got_partner(0)
    o_gather.got_diag()
    for i in range(1, 4):
        o_gather.got_partner(i)
    start_bulk(4, 5, 6, 7)

    def rows_at(i):
        flips = lambda a, b: other(0, a, b)
        return tok_of(jnp.where(i == 0, me, jnp.where(i == 1, flips(1, 0), jnp.where(i == 2, flips(0, 1), flips(1, 1)))))

    def give(i):
        slot = lax.rem(i, 2)
        rows = rows_at(i)
        return (pltpu.make_async_copy(m_out.at[slot], m_ref.at[rows, :], m_loc.at[slot]),
                pltpu.make_async_remote_copy(src_ref=m_out.at[slot], dst_ref=m_ref.at[rows, :], send_sem=m_send.at[i],
                                             recv_sem=m_recv.at[i], device_id=(partner,), device_id_type=MESH))

    def hidden_block(i, _):
        rows = rows_at(i)
        base = rows.start
        slot = lax.rem(i, 2)

        @pl.when(i >= 2)
        def _():
            to_hbm, to_partner = give(i - 2)
            to_hbm.wait()
            to_partner.wait_send()

        def chunk(j, _):
            cols = pl.ds(pl.multiple_of(j * 256, 256), 256)
            h_scr[:, cols] = dot(o_all[rows, :], wo_all[:, cols], 1, 0)
            return 0
        lax.fori_loop(0, model // 256, chunk, 0)

        def norm(k, _):
            part = pl.ds(pl.multiple_of(k * 16, 16), 16)
            x_part = x_all[pl.ds(pl.multiple_of(base + k * 16, 16), 16), :].astype(F32)
            hidden = (x_part + h_scr[part, :]).astype(BF16)

            @pl.when(i == 0)
            def _():
                h_ref[part, :] = hidden
            m_out[slot, part, :] = norm_forward(hidden.astype(F32), gfull_ref[1:2, :]).astype(BF16)
            return 0
        lax.fori_loop(0, tokens // 16, norm, 0)
        for copy in give(i):
            copy.start()
        return 0
    lax.fori_loop(0, 4, hidden_block, 0)
    stores[8].start()
    for i in range(4):
        give(i)[1].wait_recv()
    for i in range(2, 4):
        give(i)[0].wait()
        give(i)[1].wait_send()
    for copy in small + slices:
        copy.wait_send()
    for gather in (x_gather, t_gather, wo_gather, o_gather):
        gather.drain()
    for copy in bulk:
        copy.wait()
    for load, store in local:
        store.wait()
    for copy in stores:
        copy.wait()


def attention_step(heads, x_in, angles, gains, w_q, w_k, w_v, wo_own, w_gate, w_up):
    tokens, model = x_in.shape
    seq_len = 8 * tokens
    head_dim = wo_own.shape[0] // heads
    rows_own, hid = w_gate.shape[0], w_gate.shape[1] // 8
    shape = jax.ShapeDtypeStruct
    hbm = pl.BlockSpec(memory_space=pl.ANY)
    dma = pltpu.SemaphoreType.DMA
    vm = lambda *dims, dtype=BF16: pltpu.VMEM(dims, dtype)
    outs = (shape((heads, seq_len, head_dim), BF16), shape((seq_len, head_dim), BF16), shape((seq_len, head_dim), BF16),
            shape((heads * head_dim, seq_len), BF16), shape((rows_own, seq_len), BF16),
            shape((seq_len, 128), F32), shape((seq_len, 128), F32), shape((8, model), F32), shape((tokens, model), BF16))
    pairs = [dma((7,)), dma((7,)), dma((3, 7)), dma((3, 7)), dma((7,)), dma((7,)), dma((7,)), dma((7,)), dma((7,)), dma((7,)),
             dma((56,)), dma((56,)), dma((7,)), dma((7,))]
    return pl.pallas_call(
        functools.partial(attention_comm_kernel, 'sp', heads), name='attention_comm',
        in_specs=[hbm] * 9, out_specs=[hbm] * 12,
        out_shape=[*outs, shape((seq_len, model), BF16), shape((model, hid), BF16), shape((model, hid), BF16)],
        scratch_shapes=[vm(*t.shape, dtype=t.dtype) for t in outs] + [
            vm(tokens // 2, 128, dtype=F32), vm(tokens // 2, 128, dtype=F32), vm(seq_len, model), vm(8, tokens // 2, 128, dtype=F32), vm(8, 8, rows_own, dtype=F32),
            vm(384, model), vm(model, model), vm(seq_len, model), vm(tokens, model), vm(tokens, 384), vm(heads, seq_len, head_dim),
            vm(seq_len, heads * head_dim), vm(tokens, model, dtype=F32), vm(2, tokens, model), vm(2, rows_own, hid)] + pairs + [
            dma((2,)), dma((4,)), dma((4,)), dma((4,)), dma((8,)), dma((9,))],
        compiler_params=pltpu.CompilerParams(collective_id=0, has_side_effects=True, vmem_limit_bytes=63 * 1024 * 1024),
    )(x_in, angles, gains, w_q, w_k, w_v, wo_own, w_gate, w_up)


def hand_over_kernel(plan, *refs):
    n_in = len(plan)
    sources, gains, results = refs[:n_in], refs[n_in], refs[n_in + 1:2 * n_in + 1]
    gain_outs, stages = refs[2 * n_in + 1:2 * n_in + 3], refs[2 * n_in + 3:3 * n_in + 3]
    in_sem, out_sem = refs[3 * n_in + 3:]
    pieces, count = [], 0
    for src, stage, dst, parts in zip(sources, stages, results, plan):
        rows = src.shape[0] // parts
        for p in range(parts):
            part = pl.ds(p * rows, rows)
            pieces.append((pltpu.make_async_copy(src.at[part], stage.at[part], in_sem.at[count]),
                           pltpu.make_async_copy(stage.at[part], dst.at[part], out_sem.at[count])))
            count += 1
    for load, _ in pieces:
        load.start()
    for i in range(2):
        gain_outs[i][...] = gains[i, :]
    for load, store in pieces:
        load.wait()
        store.start()
    for _, store in pieces:
        store.wait()


def hand_over(arrays, gains):
    shape = jax.ShapeDtypeStruct
    plan = tuple(max(1, a.size * a.dtype.itemsize // (1 << 20)) for a in arrays)
    hbm, vmem = pl.BlockSpec(memory_space=pl.ANY), pl.BlockSpec(memory_space=pltpu.VMEM)
    dma = pltpu.SemaphoreType.DMA
    out = pl.pallas_call(
        functools.partial(hand_over_kernel, plan), name='hand_over',
        in_specs=[hbm] * len(arrays) + [vmem], out_specs=[hbm] * len(arrays) + [vmem] * 2,
        out_shape=[shape(a.shape, a.dtype) for a in arrays] + [shape((gains.shape[1],), F32)] * 2,
        scratch_shapes=[pltpu.VMEM(a.shape, a.dtype) for a in arrays] + [dma((sum(plan),)), dma((sum(plan),))],
        compiler_params=pltpu.CompilerParams(vmem_limit_bytes=63 * 1024 * 1024),
    )(*arrays, gains)
    return out


def solution(mesh):
    n_dev = mesh.shape['sp']

    def layer_step(x_in, positions, d_out, norm1_gain, norm2_gain, w_q, w_k, w_v, w_o, w_gate, w_up, w_down):
        tokens, model = x_in.shape
        head_dim = w_q.shape[2]
        heads = w_q.shape[1] // n_dev
        rows_own = w_q.shape[0]
        inv_freq = 1.0 / (ROPE_BASE ** (jnp.arange(head_dim // 2, dtype=F32) * (2.0 / head_dim)))
        half = tokens // 2
        lane = jnp.arange(4 * head_dim // 2)
        turn = jnp.where((lane < head_dim)[None, :], positions[:half, None], positions[half:, None])
        angles = turn.astype(F32) * jnp.tile(inv_freq, 4)[None, :]
        row = jnp.arange(8)[:, None]
        gains = jnp.where(row == 0, norm1_gain[None].astype(F32), jnp.where(row == 1, norm2_gain[None].astype(F32), 0.0))
        flat = lambda w: w.transpose(1, 2, 0).reshape(-1, rows_own)
        wo_own = w_o.reshape(-1, model)
        (q_rot, k_rot, v_lin, o_t, u_t, cos_tab, sin_tab, g_full, hidden,
         mlp_in, w1, w3) = attention_step(heads, x_in, angles, gains, flat(w_q), flat(w_k), flat(w_v), wo_own, w_gate, w_up)
        d_w1s, d_w3s, d_down, y_out, dh_own, d_g2 = mlp_step(mlp_in, d_out, w1, w3, w_down, hidden, g_full)
        d_wo, d_wq_t, d_wk_t, d_wv_t, d_w1, d_w3, d_x, d_gains = attention_backward_step(
            heads, dh_own, wo_own, o_t, q_rot, k_rot, v_lin, (cos_tab, sin_tab),
            d_w1s, d_w3s, flat(w_q), flat(w_k), flat(w_v), u_t, x_in, g_full, d_g2)
        from_cols = lambda d, w: d.reshape(w.shape[1], w.shape[2], rows_own).transpose(2, 0, 1)
        (d_w1, d_w3, d_down, d_wo, d_wq_t, d_wk_t, d_wv_t, y_out, d_x, d_g1, d_g2) = hand_over(
            (d_w1, d_w3, d_down, d_wo, d_wq_t, d_wk_t, d_wv_t, y_out, d_x), d_gains)
        return (y_out, d_x, d_g1, d_g2, from_cols(d_wq_t, w_q), from_cols(d_wk_t, w_k), from_cols(d_wv_t, w_v),
                d_wo.reshape(w_o.shape), d_w1, d_w3, d_down)

    all_rows = P('sp')
    return jax.shard_map(layer_step, mesh=mesh, in_specs=(all_rows,) * 12, out_specs=(all_rows,) * 11, check_vma=False)
```

```python
import functools
import jax
import jax.numpy as jnp
import numpy as np
from jax import lax
from jax.experimental import pallas as pl
from jax.experimental.pallas import tpu as pltpu
from jax.sharding import PartitionSpec as P

ROPE_BASE = 10000.0
NORM_EPS = 1e-5
NEG_LARGE = -1e30
F32 = jnp.float32
BF16 = jnp.bfloat16
BLK = 256


def dot(lhs, rhs, lhs_dim, rhs_dim):
    return lax.dot_general(lhs, rhs, (((lhs_dim,), (rhs_dim,)), ((), ())), preferred_element_type=F32)


def norm_forward(hidden, gain_vec):
    inv_rms = lax.rsqrt(jnp.mean(hidden * hidden, axis=-1, keepdims=True) + NORM_EPS)
    return hidden * inv_rms * gain_vec


def probs_transposed(k_rows, q_blk, start):
    scores = dot(k_rows, q_blk, 1, 1)
    rows = lax.broadcasted_iota(jnp.int32, (BLK, BLK), 0)
    cols = lax.broadcasted_iota(jnp.int32, (BLK, BLK), 1)
    tail = jnp.where(rows <= cols, scores[start:], NEG_LARGE)
    scores = jnp.concatenate([scores[:start], tail], axis=0) if start else tail
    top = jnp.max(scores, axis=0, keepdims=True)
    weights = jnp.exp((scores - top) * (q_blk.shape[1] ** -0.5))
    return weights * (1.0 / jnp.sum(weights, axis=0, keepdims=True))


MESH = pl.DeviceIdType.MESH


def place(axis):
    me = lax.axis_index(axis)
    core = lax.rem(me, 2)
    col = lax.rem(lax.div(me, 2), 2)
    row = lax.div(me, 4)

    def other(flip_core, flip_col, flip_row):
        pick = lambda v, f: 1 - v if f else v
        return pick(row, flip_row) * 4 + pick(col, flip_col) * 2 + pick(core, flip_core)

    nbr_x, nbr_y = other(0, 1, 0), other(0, 0, 1)
    first = nbr_x * (1 - core) + nbr_y * core
    second = nbr_y * (1 - core) + nbr_x * core
    return me, other, first, second


def greet(other):
    barrier = pltpu.get_barrier_semaphore()
    for r in range(1, 8):
        pl.semaphore_signal(barrier, inc=1, device_id=(other(r & 1, (r >> 1) & 1, r >> 2),), device_id_type=MESH)
    pl.semaphore_wait(barrier, 7)


class Gather:
    def __init__(self, slot, send_sem, recv_sem, where, own=None):
        me, other, first, second = where
        partner, diag = other(1, 0, 0), other(0, 1, 1)
        own = slot(me) if own is None else own
        self.copies = []
        plan = [(own, me, first), (own, me, second), (own, me, partner), (slot(first), first, second),
                (slot(first), first, partner), (slot(second), second, partner), (slot(diag), diag, partner)]
        for i, (src, what, dest) in enumerate(plan):
            self.copies.append(pltpu.make_async_remote_copy(
                src_ref=src, dst_ref=slot(what), send_sem=send_sem.at[i], recv_sem=recv_sem.at[i],
                device_id=(dest,), device_id_type=MESH))

    def start(self):
        for i in range(3):
            self.copies[i].start()

    def got_first(self):
        self.copies[0].wait_recv()
        self.copies[3].start()
        self.copies[4].start()

    def got_second(self):
        self.copies[1].wait_recv()
        self.copies[5].start()

    def got_diag(self):
        self.copies[3].wait_recv()
        self.copies[6].start()

    def got_partner(self, i):
        self.copies[(2, 4, 5, 6)[i]].wait_recv()

    def drain(self):
        for copy in self.copies:
            copy.wait_send()


def turn_halves(values, cos_blk, sin_blk):
    width = values.shape[1]
    lanes = lax.broadcasted_iota(jnp.int32, values.shape, 1)
    partner = jnp.where(lax.rem(lanes, 64) < 32, pltpu.roll(values, width - 32, 1), pltpu.roll(values, 32, 1))
    return values * cos_blk + partner * sin_blk


def norm_backward(hidden, gain, d_out):
    inv = lax.rsqrt(jnp.mean(hidden * hidden, axis=-1, keepdims=True) + NORM_EPS)
    d_scaled = d_out * gain
    d_hidden = d_scaled * inv - hidden * (inv * inv * inv * jnp.mean(d_scaled * hidden, axis=-1, keepdims=True))
    return d_hidden, jnp.sum(d_out * (hidden * inv), axis=0, keepdims=True)


def attn_bwd_comm_kernel(axis, heads, dh_hbm, wo_hbm, ot_hbm, q_hbm, k_hbm, v_hbm, cos_hbm, sin_hbm,
                         dw1_ref, dw3_ref, wq_hbm, wk_hbm, wv_hbm, ut_hbm, x_hbm, g_hbm, dg2_hbm,
                         dwo_ref, dwq_ref, dwk_ref, dwv_ref, out1_ref, out3_ref, dx_ref, dg_ref,
                         dh_ref, wo_ref, ot_ref, q_ref, k_ref, v_ref, cos_ref, sin_ref, wq_ref, wk_ref, wv_ref, ut_ref, g_ref, dg2_ref,
                         slots, do_scr, dg_own, dg_all, dk_acc, dv_acc, du_acc, du_scr,
                         bulk_send, bulk_recv, hg_send, hg_recv, gat_send, gat_recv, du_send, du_rsem, dg_send, dg_recv, loc_sem, ld_sem):
    loads = {}
    for i, (name, src, dst) in enumerate((
            ('wo', wo_hbm, wo_ref), ('ot', ot_hbm, ot_ref), ('q', q_hbm, q_ref), ('k', k_hbm, k_ref),
            ('v', v_hbm, v_ref), ('cos', cos_hbm, cos_ref), ('sin', sin_hbm, sin_ref), ('wq', wq_hbm, wq_ref), ('wk', wk_hbm, wk_ref),
            ('wv', wv_hbm, wv_ref), ('ut', ut_hbm, ut_ref), ('g', g_hbm, g_ref), ('dg2', dg2_hbm, dg2_ref),
            ('dh', dh_hbm, dh_ref.at[pl.ds(pl.multiple_of(lax.axis_index(axis) * x_hbm.shape[0], x_hbm.shape[0]), x_hbm.shape[0]), :]))):
        loads[name] = pltpu.make_async_copy(src, dst, ld_sem.at[i])
        loads[name].start()

    def need(*names):
        for name in names:
            loads[name].wait()

    where = place(axis)
    me, other, first, second = where
    greet(other)
    seq_len, head_dim = k_ref.shape
    rows_own, hid = out1_ref.shape[0], dw1_ref.shape[1]
    tokens = x_hbm.shape[0]
    qw = heads * head_dim
    half_rows = rows_own // 2

    rows_of = lambda d: pl.ds(pl.multiple_of(d * rows_own, rows_own), rows_own)
    hid_of = lambda d: pl.ds(pl.multiple_of(d * hid, hid), hid)
    pairs = ((dw1_ref, out1_ref), (dw3_ref, out3_ref))
    peers = [other(r & 1, (r >> 1) & 1, r >> 2) for r in (2, 4, 6, 3, 5, 7, 1)]
    bulk = []
    for part in range(4):
        src, dst = pairs[part // 2]
        for n, dest in enumerate(peers):
            low = (part % 2) * half_rows
            bulk.append(pltpu.make_async_remote_copy(
                src_ref=src.at[pl.ds(pl.multiple_of(dest * rows_own + low, half_rows), half_rows), :],
                dst_ref=dst.at[pl.ds(low, half_rows), hid_of(me)], send_sem=bulk_send.at[part * 7 + n],
                recv_sem=bulk_recv.at[part * 7 + n], device_id=(dest,), device_id_type=MESH))

    def start_bulk(part):
        for copy in bulk[part * 7:part * 7 + 7]:
            copy.start()
    tok_of = lambda d: pl.ds(pl.multiple_of(d * tokens, tokens), tokens)
    h_gather = Gather(lambda d: dh_ref.at[tok_of(d), :], hg_send, hg_recv, where, own=dh_hbm)
    h_gather.start()
    local = [pltpu.make_async_copy(src.at[rows_of(me), :], dst.at[:, hid_of(me)], loc_sem.at[i]) for i, (src, dst) in enumerate(pairs)]
    for copy in local:
        copy.start()
    need('dh', 'wo', 'ot')
    h_gather.got_first()
    h_gather.got_second()
    start_bulk(0)
    start_bulk(1)
    h_gather.got_diag()
    for i in range(4):
        h_gather.got_partner(i)

    def split_out_grad(k, _):
        rows = pl.ds(pl.multiple_of(k * BLK, BLK), BLK)
        do_blk = dot(dh_ref[rows, :], wo_ref[...], 1, 1).astype(BF16)
        for h in range(heads):
            do_scr[h, rows, :] = do_blk[:, h * head_dim:(h + 1) * head_dim]
        cols = rows
        dwo_ref[:, cols] = dot(ot_ref[...], dh_ref[:, cols], 1, 0)
        return 0
    lax.fori_loop(0, seq_len // BLK, split_out_grad, 0)
    x_ref = wo_ref
    x_load = pltpu.make_async_copy(x_hbm, x_ref, ld_sem.at[14])
    x_load.start()


    need('q', 'k', 'v')
    dk_acc[...] = jnp.zeros_like(dk_acc)
    dv_acc[...] = jnp.zeros_like(dv_acc)
    mine = slots.at[me]

    def one_head(h, _):
        def one_block(start):
            keys = pl.ds(0, start + BLK)
            rows = pl.ds(start, BLK)
            q_blk, do_blk = q_ref[h, rows, :], do_scr[h, rows, :]
            probs = probs_transposed(k_ref[keys, :], q_blk, start)
            d_probs = dot(v_ref[keys, :], do_blk, 1, 1).astype(BF16).astype(F32)
            row_dot = jnp.sum(d_probs * probs, axis=0, keepdims=True)
            d_scores = (probs * (d_probs - row_dot) * (head_dim ** -0.5)).astype(BF16)
            do_scr[h, rows, :] = dot(d_scores, k_ref[keys, :], 0, 0).astype(BF16)
            dk_acc[keys, :] += dot(d_scores, q_blk, 1, 0)
            dv_acc[keys, :] += dot(probs.astype(BF16), do_blk, 1, 0)
        for start in range(0, seq_len, BLK):
            one_block(start)
        return 0
    lax.fori_loop(0, heads, one_head, 0)
    need('cos', 'sin')
    mine[:, qw:qw + head_dim] = dk_acc[...].astype(BF16)
    mine[:, qw + head_dim:] = dv_acc[...].astype(BF16)
    low = lax.broadcasted_iota(jnp.int32, (BLK, 128), 1) < head_dim

    def turn_back(k, _):
        rows = pl.ds(pl.multiple_of(k * BLK, BLK), BLK)
        cos_blk, sin_blk = cos_ref[rows, :], -sin_ref[rows, :]
        for pair in range(heads // 2):
            both = jnp.concatenate([do_scr[2 * pair, rows, :], do_scr[2 * pair + 1, rows, :]], axis=1)
            mine[rows, pair * 128:(pair + 1) * 128] = turn_halves(both.astype(F32), cos_blk, sin_blk).astype(BF16)
        kv = mine[rows, qw:].astype(F32)
        mine[rows, qw:] = jnp.where(low, turn_halves(kv, cos_blk, sin_blk), kv).astype(BF16)
        return 0
    lax.fori_loop(0, seq_len // BLK, turn_back, 0)

    gather = Gather(lambda d: slots.at[d], gat_send, gat_recv, where)
    gather.start()
    du_acc[...] = jnp.zeros_like(du_acc)
    need('wq', 'wk', 'wv', 'ut')

    def use(d):
        q_rows = pl.ds(pl.multiple_of(d * qw, qw), qw)
        kv_rows = pl.ds(pl.multiple_of(d * head_dim, head_dim), head_dim)
        w_all = jnp.concatenate([wq_ref[q_rows, :], wk_ref[kv_rows, :], wv_ref[kv_rows, :]], axis=0)

        def add_rows(k, _):
            rows = pl.ds(pl.multiple_of(k * 512, 512), 512)
            du_acc[rows, :] += dot(slots[d, rows, :], w_all, 1, 0)
            return 0
        lax.fori_loop(0, seq_len // 512, add_rows, 0)
        d_w = dot(ut_ref[...], slots[d], 1, 0).T
        dwq_ref[q_rows, :] = d_w[:qw]
        dwk_ref[kv_rows, :] = d_w[qw:qw + head_dim]
        dwv_ref[kv_rows, :] = d_w[qw + head_dim:]

    def use_many(*devices):
        def body(i, _):
            d = devices[0]
            for n in range(1, len(devices)):
                d = jnp.where(i == n, devices[n], d)
            use(d)
            return 0
        lax.fori_loop(0, len(devices), body, 0)

    use_many(me)
    gather.got_first()
    gather.got_second()
    start_bulk(2)
    gather.got_partner(0)
    use_many(first, second, other(1, 0, 0))
    gather.got_diag()
    for i in range(1, 4):
        gather.got_partner(i)
    use_many(other(0, 1, 1), other(1, 1, 0), other(1, 0, 1), other(1, 1, 1))
    du_scr[...] = du_acc[...].astype(BF16)
    sends = []
    for n, dest in enumerate(peers):
        sends.append(pltpu.make_async_remote_copy(
            src_ref=du_scr.at[tok_of(dest), :], dst_ref=ot_ref.at[:, rows_of(me)], send_sem=du_send.at[n],
            recv_sem=du_rsem.at[n], device_id=(dest,), device_id_type=MESH))
        sends[-1].start()
    start_bulk(3)
    ot_ref[:, rows_of(me)] = du_scr[tok_of(me), :]
    need('g', 'dg2')
    x_load.wait()
    for copy in sends:
        copy.wait_recv()
    dg_own[...] = jnp.zeros_like(dg_own)
    dg_own[1:2, :] = dg2_ref[...]

    def input_grad(k, _):
        part = pl.ds(pl.multiple_of(k * 16, 16), 16)
        d_norm, d_gain = norm_backward(x_ref[part, :].astype(F32), g_ref[0:1, :], ot_ref[part, :].astype(F32))
        dh_part = dh_ref[pl.ds(pl.multiple_of(me * tokens + k * 16, 16), 16), :]
        dx_ref[part, :] = (dh_part.astype(F32) + d_norm).astype(BF16)
        dg_own[0:1, :] += d_gain
        return 0
    lax.fori_loop(0, tokens // 16, input_grad, 0)
    gain_sends = []
    for n, dest in enumerate(peers):
        gain_sends.append(pltpu.make_async_remote_copy(
            src_ref=dg_own.at[:, rows_of(dest)], dst_ref=dg_all.at[me], send_sem=dg_send.at[n],
            recv_sem=dg_recv.at[n], device_id=(dest,), device_id_type=MESH))
        gain_sends[-1].start()
    dg_all[me] = dg_own[:, rows_of(me)]
    for copy in gain_sends:
        copy.wait_recv()
    dg_ref[...] = jnp.sum(dg_all[...], axis=0)
    for copy in sends + gain_sends:
        copy.wait_send()
    gather.drain()
    h_gather.drain()
    for copy in bulk:
        copy.wait()
    for copy in local:
        copy.wait()


def attention_backward_step(heads, dh_own, wo_own, o_t, q_rot, k_rot, v_lin, tables, d_w1, d_w3, w_q, w_k, w_v, u_t, x_in, gains, d_g2):
    seq_len, model = k_rot.shape[0], x_in.shape[1]
    head_dim = k_rot.shape[1]
    tokens = x_in.shape[0]
    rows_own, hid = model // 8, d_w1.shape[1]
    shape = jax.ShapeDtypeStruct
    hbm = pl.BlockSpec(memory_space=pl.ANY)
    dma = pltpu.SemaphoreType.DMA
    vm = lambda *dims, dtype=BF16: pltpu.VMEM(dims, dtype)
    early = (dh_own, wo_own, o_t, q_rot, k_rot, v_lin, *tables)
    late = (w_q, w_k, w_v, u_t, x_in, gains, d_g2)
    outs = [(wo_own.shape, F32), (w_q.shape, F32), (w_k.shape, F32), (w_v.shape, F32), ((rows_own, 8 * hid), F32),
            ((rows_own, 8 * hid), F32), (x_in.shape, BF16), ((8, rows_own), F32)]
    vmem = pl.BlockSpec(memory_space=pltpu.VMEM)
    return pl.pallas_call(
        functools.partial(attn_bwd_comm_kernel, 'sp', heads), name='attn_bwd_comm',
        in_specs=[hbm] * 17, out_specs=[vmem] * 8,
        out_shape=[pltpu.VMEM(dims, dtype) for dims, dtype in outs],
        scratch_shapes=[vm(seq_len, model)] + [vm(*t.shape, dtype=t.dtype) for t in early[1:] + late[:4] + late[5:]] + [
            vm(8, seq_len, 384), vm(heads, seq_len, head_dim),
            vm(8, model, dtype=F32), vm(8, 8, rows_own, dtype=F32),
            vm(seq_len, head_dim, dtype=F32), vm(seq_len, head_dim, dtype=F32),
            vm(seq_len, rows_own, dtype=F32), vm(seq_len, rows_own),
            dma((28,)), dma((28,)), dma((7,)), dma((7,)), dma((7,)), dma((7,)), dma((7,)), dma((7,)), dma((7,)), dma((7,)), dma((2,)), dma((15,))],
        compiler_params=pltpu.CompilerParams(collective_id=2, has_side_effects=True, vmem_limit_bytes=43515904),
    )(*early, d_w1, d_w3, *late)


def mlp_comm_kernel(axis, m_ref, dout_own, w1_hbm, w3_hbm, w2_hbm, h_hbm, g_hbm,
                    dw1_ref, dw3_ref, dw2_ref, y_hbm, dh_hbm, dg2_hbm, dout_ref,
                    w1_ref, w3_ref, w2_ref, h_ref, g_ref, y_ref, dg2_ref,
                    glu, gate_s, up_s, outbox, chip_sum, inbox, blk, m_col, do_col, mt_scr, dot_scr, st1, st3, st2, dh_own,
                    part_send, part_recv, mail_send, mail_recv, do_send, do_recv,
                    in_sem, col_sem, out_sem, own_sem, ld_sem, credit):
    loads = [pltpu.make_async_copy(src, dst, ld_sem.at[i]) for i, (src, dst) in enumerate((
        (w1_hbm, w1_ref), (w3_hbm, w3_ref), (w2_hbm, w2_ref), (h_hbm, h_ref), (g_hbm, g_ref)))]
    own_in = pltpu.make_async_copy(dout_own, dh_own, own_sem.at[0])
    for copy in loads + [own_in]:
        copy.start()
    where = place(axis)
    me, other, first, second = where
    core = lax.rem(me, 2)
    partner = other(1, 0, 0)
    tokens, model = h_ref.shape
    hid = w1_ref.shape[1]
    tok_of = lambda d: pl.ds(pl.multiple_of(d * tokens, tokens), tokens)
    off_first, off_second = 1 + core, 2 - core

    def block_of(off, flip):
        d_col, d_row = lax.rem(off, 2), lax.div(off, 2)
        col, row = lax.rem(lax.div(me, 2), 2), lax.div(me, 4)
        mix = lambda v, f: v + f - 2 * v * f
        return mix(row, d_row) * 4 + mix(col, d_col) * 2 + mix(core, flip)

    def step_off(step, flip):
        mid_a = off_second * (1 - flip) + off_first * flip
        mid_b = off_first * (1 - flip) + off_second * flip
        return jnp.where(step == 0, 3, jnp.where(step == 1, mid_a, jnp.where(step == 2, mid_b, 0)))

    def half_rows(half):
        flip = 1 - lax.rem(half, 2)
        return tok_of(block_of(step_off(lax.div(half, 2), flip), flip))

    def fetch(half):
        slot = lax.rem(half, 2)
        return pltpu.make_async_copy(m_ref.at[half_rows(half), :], blk.at[slot], in_sem.at[slot])

    def fetch_dout(d):
        slot = lax.rem(d, 2)
        return pltpu.make_async_copy(dout_ref.at[tok_of(d), :], blk.at[slot], in_sem.at[slot])

    def fetch_cols(j):
        cols = pl.ds(pl.multiple_of(j * 256, 256), 256)
        return (pltpu.make_async_copy(m_ref.at[:, cols], m_col, col_sem.at[0]),
                pltpu.make_async_copy(dout_ref.at[:, cols], do_col, col_sem.at[1]))

    def sigmoid(value):
        return 1.0 / (1.0 + jnp.exp(-value))

    def activations(slot, rows):
        def chunk(j, _):
            cols = pl.ds(pl.multiple_of(j * 512, 512), 512)
            gate = dot(blk[slot], w1_ref[:, cols], 1, 0).astype(BF16)
            up = dot(blk[slot], w3_ref[:, cols], 1, 0).astype(BF16)
            gate_s[rows, cols] = gate
            up_s[rows, cols] = up
            gate = gate.astype(F32)
            glu[rows, cols] = (gate * sigmoid(gate) * up.astype(F32)).astype(BF16)
            return 0
        lax.fori_loop(0, hid // 512, chunk, 0)

    def activation_grads(slot, rows):
        def chunk(j, _):
            cols = pl.ds(pl.multiple_of(j * 512, 512), 512)
            d_act = dot(blk[slot], w2_ref[cols, :], 1, 1).astype(BF16).astype(F32)
            gate, up = gate_s[rows, cols].astype(F32), up_s[rows, cols].astype(F32)
            sig = sigmoid(gate)
            silu = gate * sig
            up_s[rows, cols] = (d_act * silu).astype(BF16)
            gate_s[rows, cols] = (d_act * up * (sig + silu * (1.0 - sig))).astype(BF16)
            return 0
        lax.fori_loop(0, hid // 512, chunk, 0)

    def add_mlp_grad(rows, put):
        def chunk(j, _):
            cols = pl.ds(pl.multiple_of(j * 512, 512), 512)
            put(cols, dot(gate_s[rows, :], w1_ref[cols, :], 1, 1) + dot(up_s[rows, :], w3_ref[cols, :], 1, 1))
            return 0
        lax.fori_loop(0, model // 512, chunk, 0)

    def add_mlp_out(rows, put):
        def chunk(j, _):
            cols = pl.ds(pl.multiple_of(j * 512, 512), 512)
            put(cols, dot(glu[rows, :], w2_ref[:, cols], 1, 0))
            return 0
        lax.fori_loop(0, model // 512, chunk, 0)

    def signal(index, device):
        pl.semaphore_signal(credit.at[index], inc=1, device_id=(device,), device_id_type=MESH)

    class Scatter:
        def __init__(self, turn):
            self.turn = turn

        def to_partner(self, step):
            off = step_off(step, 1)
            return pltpu.make_async_remote_copy(
                src_ref=outbox.at[lax.rem(step, 2)], dst_ref=chip_sum.at[off], send_sem=part_send.at[self.turn, step],
                recv_sem=part_recv.at[self.turn, off], device_id=(partner,), device_id_type=MESH)

        def from_partner(self, off):
            return pltpu.make_async_remote_copy(
                src_ref=outbox.at[0], dst_ref=chip_sum.at[off], send_sem=part_send.at[self.turn, 0],
                recv_sem=part_recv.at[self.turn, off], device_id=(partner,), device_id_type=MESH)

        def mail(self, kind):
            off = (3, off_first, off_second)[kind]
            dest = (first, first, second)[kind]
            return pltpu.make_async_remote_copy(
                src_ref=chip_sum.at[off], dst_ref=inbox.at[kind], send_sem=mail_send.at[self.turn, kind],
                recv_sem=mail_recv.at[self.turn, kind], device_id=(dest,), device_id_type=MESH)

        def step(self, step, prepare, partial):
            slot = lax.rem(step, 2)
            prepare(2 * step)

            def put_out(cols, value):
                outbox[slot, :, cols] = value
            partial(half_rows(2 * step), put_out)
            self.to_partner(step).start()
            prepare(2 * step + 1)
            off = step_off(step, 0)
            self.from_partner(off).wait_recv()

            def put_sum(cols, value):
                chip_sum[off, :, cols] += value
            partial(half_rows(2 * step + 1), put_sum)

        def pass_on(self):
            self.mail(0).wait_recv()

            def add_mail(k, _):
                part = pl.ds(pl.multiple_of(k * 16, 16), 16)
                chip_sum[off_second, part, :] += inbox[0, part, :]
                return 0
            lax.fori_loop(0, tokens // 16, add_mail, 0)

    out_round, grad_round = Scatter(0), Scatter(1)

    def prepare_out(half):
        @pl.when(half < 7)
        def _():
            fetch(half + 1).start()
        fetch(half).wait()
        activations(lax.rem(half, 2), half_rows(half))

    def weight_grads(begin, end):
        for copy in fetch_cols(begin):
            copy.start()

        def body(j, _):
            for copy in fetch_cols(j):
                copy.wait()

            def turn(k, _):
                part = pl.ds(pl.multiple_of(k * 256, 256), 256)
                mt_scr[:, part] = m_col[part, :].T
                dot_scr[:, part] = do_col[part, :].T
                return 0
            lax.fori_loop(0, m_col.shape[0] // 256, turn, 0)

            @pl.when(j + 1 < end)
            def _():
                for copy in fetch_cols(j + 1):
                    copy.start()
            rows = pl.ds(pl.multiple_of(j * 256, 256), 256)
            out = (pltpu.make_async_copy(st1, dw1_ref.at[rows, :], out_sem.at[0]),
                   pltpu.make_async_copy(st3, dw3_ref.at[rows, :], out_sem.at[1]),
                   pltpu.make_async_copy(st2, dw2_ref.at[:, rows], out_sem.at[2]))

            @pl.when(j > begin)
            def _():
                for copy in out:
                    copy.wait()

            def chunk(k, _):
                cols = pl.ds(pl.multiple_of(k * 512, 512), 512)
                st1[:, cols] = dot(mt_scr[...], gate_s[:, cols], 1, 0)
                st3[:, cols] = dot(mt_scr[...], up_s[:, cols], 1, 0)
                st2[cols, :] = dot(dot_scr[...], glu[:, cols], 1, 0).T
                return 0
            lax.fori_loop(0, hid // 512, chunk, 0)
            for copy in out:
                copy.start()
            return 0
        lax.fori_loop(begin, end, body, 0)
        rows = pl.ds((end - 1) * 256, 256)
        for copy in (pltpu.make_async_copy(st1, dw1_ref.at[rows, :], out_sem.at[0]),
                     pltpu.make_async_copy(st3, dw3_ref.at[rows, :], out_sem.at[1]),
                     pltpu.make_async_copy(st2, dw2_ref.at[:, rows], out_sem.at[2])):
            copy.wait()

    fetch(0).start()
    greet(other)
    do_gather = Gather(lambda d: dout_ref.at[tok_of(d), :], do_send, do_recv, where, own=dout_own)
    do_gather.start()
    own_in.wait()
    own_out = pltpu.make_async_copy(dh_own, dout_ref.at[tok_of(me), :], own_sem.at[1])
    own_out.start()
    for copy in loads:
        copy.wait()

    def out_step(step, _):
        @pl.when(step >= 2)
        def _():
            out_round.to_partner(step - 2).wait_send()
        out_round.step(step, prepare_out, add_mlp_out)

        @pl.when(step == 0)
        def _():
            out_round.mail(0).start()

        @pl.when(step == 2)
        def _():
            out_round.mail(1).start()
            do_gather.got_first()
            do_gather.got_second()
        return 0
    lax.fori_loop(0, 4, out_step, 0)
    out_round.pass_on()
    out_round.mail(2).start()
    for step in (2, 3):
        out_round.to_partner(step).wait_send()
    out_round.mail(0).wait_send()
    signal(0, partner)
    signal(1, first)
    do_gather.got_diag()
    for i in range(4):
        do_gather.got_partner(i)
    own_out.wait()
    fetch_dout(0).start()

    def grad_block(d, _):
        @pl.when(d < 7)
        def _():
            fetch_dout(d + 1).start()
        fetch_dout(d).wait()
        activation_grads(lax.rem(d, 2), tok_of(d))
        return 0
    lax.fori_loop(0, 8, grad_block, 0)

    pl.semaphore_wait(credit.at[0], 1)
    grad_round.step(0, lambda half: None, add_mlp_grad)
    pl.semaphore_wait(credit.at[1], 1)
    grad_round.mail(0).start()
    weight_grads(0, 2)
    out_round.mail(1).wait_recv()
    out_round.mail(2).wait_recv()

    def layer_out(k, _):
        part = pl.ds(pl.multiple_of(k * 16, 16), 16)
        y_ref[part, :] = (h_ref[part, :].astype(F32) + (chip_sum[0, part, :] + inbox[1, part, :] + inbox[2, part, :])).astype(BF16)
        return 0
    lax.fori_loop(0, tokens // 16, layer_out, 0)
    y_store = pltpu.make_async_copy(y_ref, y_hbm, own_sem.at[2])
    y_store.start()
    out_round.mail(1).wait_send()
    out_round.mail(2).wait_send()
    signal(2, partner)
    signal(3, first)
    signal(4, second)
    pl.semaphore_wait(credit.at[2], 1)

    def grad_step(step, _):
        @pl.when(step >= 2)
        def _():
            grad_round.to_partner(step - 2).wait_send()
        grad_round.step(step, lambda half: None, add_mlp_grad)

        @pl.when(step == 2)
        def _():
            pl.semaphore_wait(credit.at[3], 1)
            grad_round.mail(1).start()
            grad_round.pass_on()
            pl.semaphore_wait(credit.at[4], 1)
            grad_round.mail(2).start()
        return 0
    lax.fori_loop(1, 4, grad_step, 0)
    weight_grads(2, 8)
    grad_round.mail(1).wait_recv()
    grad_round.mail(2).wait_recv()
    dg2_ref[...] = jnp.zeros_like(dg2_ref)

    def hidden_grad(k, _):
        part = pl.ds(pl.multiple_of(k * 16, 16), 16)
        d_mlp = (chip_sum[0, part, :] + inbox[1, part, :] + inbox[2, part, :]).astype(BF16).astype(F32)
        d_norm, d_gain = norm_backward(h_ref[part, :].astype(F32), g_ref[1:2, :], d_mlp)
        dh_own[part, :] = (dh_own[part, :].astype(F32) + d_norm).astype(BF16)
        dg2_ref[...] += d_gain
        return 0
    lax.fori_loop(0, tokens // 16, hidden_grad, 0)
    own_out = pltpu.make_async_copy(dh_own, dh_hbm, own_sem.at[3])
    own_out.start()
    dg2_store = pltpu.make_async_copy(dg2_ref, dg2_hbm, own_sem.at[4])
    dg2_store.start()
    for step in (2, 3):
        grad_round.to_partner(step).wait_send()
    for kind in range(3):
        grad_round.mail(kind).wait_send()
    do_gather.drain()
    own_out.wait()
    y_store.wait()
    dg2_store.wait()


def mlp_step(m_all, d_out, w1, w3, w2, hidden, gains):
    seq_len, model = m_all.shape
    hid, tokens = w1.shape[1], hidden.shape[0]
    shape = jax.ShapeDtypeStruct
    hbm = pl.BlockSpec(memory_space=pl.ANY)
    dma = pltpu.SemaphoreType.DMA
    vm = lambda *dims, dtype=BF16: pltpu.VMEM(dims, dtype)
    return pl.pallas_call(
        functools.partial(mlp_comm_kernel, 'sp'), name='mlp_comm',
        in_specs=[hbm] * 7, out_specs=[hbm] * 7,
        out_shape=[shape((model, hid), F32), shape((model, hid), F32), shape((hid, model), F32),
                   shape(hidden.shape, BF16), shape(hidden.shape, BF16), shape((1, model), F32), shape((seq_len, model), BF16)],
        scratch_shapes=[vm(*t.shape, dtype=t.dtype) for t in (w1, w3, w2, hidden, gains)] + [
            vm(tokens, model), vm(1, model, dtype=F32),
            vm(seq_len, hid), vm(seq_len, hid), vm(seq_len, hid),
            vm(2, tokens, model, dtype=F32), vm(4, tokens, model, dtype=F32), vm(3, tokens, model, dtype=F32),
            vm(2, tokens, model), vm(seq_len, 256), vm(seq_len, 256), vm(256, seq_len), vm(256, seq_len),
            vm(256, hid, dtype=F32), vm(256, hid, dtype=F32), vm(hid, 256, dtype=F32), vm(tokens, model),
            dma((2, 4)), dma((2, 4)), dma((2, 3)), dma((2, 3)), dma((7,)), dma((7,)),
            dma((2,)), dma((2,)), dma((3,)), dma((5,)), dma((5,)), pltpu.SemaphoreType.REGULAR((5,))],
        compiler_params=pltpu.CompilerParams(collective_id=1, has_side_effects=True, vmem_limit_bytes=63 * 1024 * 1024),
    )(m_all, d_out, w1, w3, w2, hidden, gains)[:6]


def spread_tables(packed, upper):
    lanes = lax.broadcasted_iota(jnp.int32, packed.shape, 1)
    swapped = pltpu.roll(packed, 64, 1)
    both = jnp.where((lanes < 64) != upper, packed, swapped)
    low = lax.rem(lanes, 64) < 32
    return jnp.where(low, both, pltpu.roll(both, 32, 1)), jnp.where(low, -pltpu.roll(both, 96, 1), both)


def attention_comm_kernel(axis, heads, x_ref, pos_ref, gain1_ref, gain2_ref, freq_ref, wq_ref, wk_ref, wv_ref, wo_ref, wg_ref, wu_ref,
                          q_hbm, k_hbm, v_hbm, ot_hbm, ut_hbm, cos_hbm, sin_hbm, gfull_hbm, h_hbm, m_ref, w1_ref, w3_ref,
                          q_ref, k_ref, v_ref, ot_ref, ut_ref, cos_ref, sin_ref, gfull_ref, h_ref, gain_ref, x_all, gain_all, w_head, wo_all, o_all, u_blk, qkv_blk, o_scr, o_own, h_scr, m_out, stage,
                          g_send, g_recv, w_send, w_recv, x_send, x_recv, wo_send, wo_recv, bulk_send, bulk_recv,
                          o_send, o_recv, m_loc, m_send, m_recv, loc_sem, own_sem, st_sem):
    gain_ref[...] = jnp.zeros_like(gain_ref)
    gain_ref[0:1, :] = gain1_ref[...].astype(F32).reshape(1, -1)
    gain_ref[1:2, :] = gain2_ref[...].astype(F32).reshape(1, -1)
    gain_ref[2:3, :] = pos_ref[...].astype(F32).reshape(1, -1)
    where = place(axis)
    me, other, first, second = where
    core = lax.rem(me, 2)
    partner = other(1, 0, 0)
    greet(other)
    tokens, model = x_ref.shape
    seq_len, head_dim = k_ref.shape
    qw = heads * head_dim
    rows_own, hid = wg_ref.shape[0], w1_ref.shape[1]
    tok_of = lambda d: pl.ds(pl.multiple_of(d * tokens, tokens), tokens)
    cols_of = lambda d: pl.ds(pl.multiple_of(d * rows_own, rows_own), rows_own)
    hid_of = lambda d: pl.ds(pl.multiple_of(d * hid, hid), hid)
    peers = [other(r & 1, (r >> 1) & 1, r >> 2) for r in (6, 2, 4, 7, 3, 5, 1)]

    def to_all(src_of, dst, send_sem, recv_sem):
        return [pltpu.make_async_remote_copy(
            src_ref=src_of(dest), dst_ref=dst, send_sem=send_sem.at[n], recv_sem=recv_sem.at[n],
            device_id=(dest,), device_id_type=MESH) for n, dest in enumerate(peers)]

    small = to_all(lambda dest: gain_ref, gain_all.at[me], g_send, g_recv)
    q_of = lambda d: pl.ds(pl.multiple_of(d * qw, qw), qw)
    kv_of = lambda d: pl.ds(pl.multiple_of(d * head_dim, head_dim), head_dim)
    slices = (to_all(lambda dest: wq_ref.at[q_of(dest), :], w_head.at[0:qw, cols_of(me)], w_send.at[0], w_recv.at[0])
              + to_all(lambda dest: wk_ref.at[kv_of(dest), :], w_head.at[qw:qw + head_dim, cols_of(me)], w_send.at[1], w_recv.at[1])
              + to_all(lambda dest: wv_ref.at[kv_of(dest), :], w_head.at[qw + head_dim:, cols_of(me)], w_send.at[2], w_recv.at[2]))
    for copy in small + slices:
        copy.start()
    x_gather = Gather(lambda d: x_all.at[tok_of(d), :], x_send, x_recv, where, own=x_ref)
    x_gather.start()
    wo_gather = Gather(lambda d: wo_all.at[cols_of(d), :], wo_send, wo_recv, where, own=wo_ref)
    bulk = []
    part_rows = rows_own // 4
    for part in range(8):
        src, dst = ((wg_ref, w1_ref), (wu_ref, w3_ref))[part // 4]
        low = (part % 4) * part_rows
        for n, dest in enumerate(peers):
            bulk.append(pltpu.make_async_remote_copy(
                src_ref=src.at[pl.ds(low, part_rows), hid_of(dest)],
                dst_ref=dst.at[pl.ds(pl.multiple_of(me * rows_own + low, part_rows), part_rows), :],
                send_sem=bulk_send.at[part * 7 + n], recv_sem=bulk_recv.at[part * 7 + n], device_id=(dest,), device_id_type=MESH))

    def start_bulk(*parts):
        for part in parts:
            for copy in bulk[part * 7:part * 7 + 7]:
                copy.start()

    stores = [pltpu.make_async_copy(src, dst, st_sem.at[i]) for i, (src, dst) in enumerate((
        (q_ref, q_hbm), (k_ref, k_hbm), (v_ref, v_hbm), (ot_ref, ot_hbm), (ut_ref, ut_hbm), (cos_ref, cos_hbm),
        (sin_ref, sin_hbm), (gfull_ref, gfull_hbm), (h_ref, h_hbm)))]
    own = [pltpu.make_async_copy(src, dst, own_sem.at[i]) for i, (src, dst) in enumerate((
        (gain_ref, gain_all.at[me]), (wq_ref.at[q_of(me), :], w_head.at[0:qw, cols_of(me)]),
        (wk_ref.at[kv_of(me), :], w_head.at[qw:qw + head_dim, cols_of(me)]),
        (wv_ref.at[kv_of(me), :], w_head.at[qw + head_dim:, cols_of(me)]),
        (x_ref, x_all.at[tok_of(me), :]), (wo_ref, wo_all.at[cols_of(me), :])))]
    for copy in own:
        copy.start()
    local = []
    for i, (src, dst) in enumerate(((wg_ref, w1_ref), (wu_ref, w3_ref))):
        local.append((pltpu.make_async_copy(src.at[:, hid_of(me)], stage.at[i], loc_sem.at[i]),
                      pltpu.make_async_copy(stage.at[i], dst.at[cols_of(me), :], loc_sem.at[2 + i])))
        local[-1][0].start()
    for load, store in local:
        load.wait()
        store.start()
    for copy in own:
        copy.wait()
    for copy in small:
        copy.wait_recv()
    for d in range(8):
        gfull_ref[:, d * rows_own:(d + 1) * rows_own] = gain_all[d]
    for copy in slices:
        copy.wait_recv()

    def use(d):
        base = pl.multiple_of(d * tokens, tokens)

        def norm(k, _):
            part = pl.ds(pl.multiple_of(k * 16, 16), 16)
            x_part = x_all[pl.ds(pl.multiple_of(base + k * 16, 16), 16), :].astype(F32)
            u_blk[part, :] = norm_forward(x_part, gfull_ref[0:1, :]).astype(BF16)
            return 0
        lax.fori_loop(0, tokens // 16, norm, 0)
        ut_ref[:, tok_of(d)] = u_blk[:, cols_of(me)].T
        qkv_blk[...] = dot(u_blk[...], w_head[...], 1, 1).astype(BF16)
        half = tokens // 2
        where_to = gain_all[d, 2:3, :]
        lanes = lax.broadcasted_iota(jnp.int32, (half, 2 * head_dim), 1)
        by_row = lambda lo: jnp.broadcast_to(where_to[:, lo:lo + half], (2 * head_dim, half)).T
        angles = jnp.where(lanes < head_dim, by_row(0), by_row(half)) * freq_ref[...]
        packed = jnp.where(lax.rem(lanes, head_dim) < head_dim // 2, jnp.cos(angles), jnp.sin(angles))
        for part in range(2):
            rows = pl.ds(pl.multiple_of(base + part * half, half), half)
            cos_blk, sin_blk = spread_tables(packed, part == 1)
            cos_ref[rows, :] = cos_blk
            sin_ref[rows, :] = sin_blk
            source = slice(part * half, (part + 1) * half)
            for pair in range(heads // 2):
                turned = turn_halves(qkv_blk[source, pair * 128:(pair + 1) * 128].astype(F32), cos_blk, sin_blk).astype(BF16)
                q_ref[2 * pair, rows, :] = turned[:, :head_dim]
                q_ref[2 * pair + 1, rows, :] = turned[:, head_dim:]
            turned = turn_halves(qkv_blk[source, qw:].astype(F32), cos_blk, sin_blk).astype(BF16)
            k_ref[rows, :] = turned[:, :head_dim]
            v_ref[rows, :] = qkv_blk[source, qw + head_dim:]

    x_gather.got_first()
    x_gather.got_second()
    wo_gather.start()
    start_bulk(0, 1)
    x_gather.got_partner(0)

    def use_near(i, _):
        use(jnp.where(i == 0, me, jnp.where(i == 1, first, jnp.where(i == 2, second, partner))))
        return 0
    lax.fori_loop(0, 4, use_near, 0)
    x_gather.got_diag()
    for i in range(1, 4):
        x_gather.got_partner(i)

    def use_far(i, _):
        use(jnp.where(i == 0, other(0, 1, 1), jnp.where(i == 1, other(1, 1, 0), jnp.where(i == 2, other(1, 0, 1), other(1, 1, 1)))))
        return 0
    lax.fori_loop(0, 4, use_far, 0)

    def one_head(h, _):
        for start in range(0, seq_len, BLK):
            keys, rows = pl.ds(0, start + BLK), pl.ds(start, BLK)
            probs = probs_transposed(k_ref[keys, :], q_ref[h, rows, :], start)
            o_scr[h, rows, :] = dot(probs.astype(BF16), v_ref[keys, :], 0, 0).astype(BF16)
        return 0
    for i in (0, 1, 2, 4, 5, 6, 7):
        stores[i].start()
    lax.fori_loop(0, heads, one_head, 0)
    for h in range(heads):
        o_own[:, h * head_dim:(h + 1) * head_dim] = o_scr[h]
    o_gather = Gather(lambda d: o_all.at[:, cols_of(d)], o_send, o_recv, where, own=o_own)
    o_gather.start()
    wo_gather.got_first()
    wo_gather.got_second()
    start_bulk(2)
    o_all[:, cols_of(me)] = o_own[...]

    def turn_out(k, _):
        rows = tok_of(k)
        ot_ref[:, rows] = o_own[rows, :].T
        return 0
    lax.fori_loop(0, 8, turn_out, 0)
    stores[3].start()
    wo_gather.got_diag()
    for i in range(4):
        wo_gather.got_partner(i)
    o_gather.got_first()
    o_gather.got_second()
    start_bulk(3)
    o_gather.got_partner(0)
    o_gather.got_diag()
    for i in range(1, 4):
        o_gather.got_partner(i)
    start_bulk(4, 5, 6, 7)

    def rows_at(i):
        flips = lambda a, b: other(0, a, b)
        return tok_of(jnp.where(i == 0, me, jnp.where(i == 1, flips(1, 0), jnp.where(i == 2, flips(0, 1), flips(1, 1)))))

    def give(i):
        slot = lax.rem(i, 2)
        rows = rows_at(i)
        return (pltpu.make_async_copy(m_out.at[slot], m_ref.at[rows, :], m_loc.at[slot]),
                pltpu.make_async_remote_copy(src_ref=m_out.at[slot], dst_ref=m_ref.at[rows, :], send_sem=m_send.at[i],
                                             recv_sem=m_recv.at[i], device_id=(partner,), device_id_type=MESH))

    def hidden_block(i, _):
        rows = rows_at(i)
        base = rows.start
        slot = lax.rem(i, 2)

        @pl.when(i >= 2)
        def _():
            to_hbm, to_partner = give(i - 2)
            to_hbm.wait()
            to_partner.wait_send()

        def chunk(j, _):
            cols = pl.ds(pl.multiple_of(j * 256, 256), 256)
            h_scr[:, cols] = dot(o_all[rows, :], wo_all[:, cols], 1, 0)
            return 0
        lax.fori_loop(0, model // 256, chunk, 0)

        def norm(k, _):
            part = pl.ds(pl.multiple_of(k * 16, 16), 16)
            x_part = x_all[pl.ds(pl.multiple_of(base + k * 16, 16), 16), :].astype(F32)
            hidden = (x_part + h_scr[part, :]).astype(BF16)

            @pl.when(i == 0)
            def _():
                h_ref[part, :] = hidden
            m_out[slot, part, :] = norm_forward(hidden.astype(F32), gfull_ref[1:2, :]).astype(BF16)
            return 0
        lax.fori_loop(0, tokens // 16, norm, 0)
        for copy in give(i):
            copy.start()
        return 0
    lax.fori_loop(0, 4, hidden_block, 0)
    stores[8].start()
    for i in range(4):
        give(i)[1].wait_recv()
    for i in range(2, 4):
        give(i)[0].wait()
        give(i)[1].wait_send()
    for copy in small + slices:
        copy.wait_send()
    for gather in (x_gather, wo_gather, o_gather):
        gather.drain()
    for copy in bulk:
        copy.wait()
    for load, store in local:
        store.wait()
    for copy in stores:
        copy.wait()


def attention_step(heads, x_in, positions, gain1, gain2, w_q, w_k, w_v, wo_own, w_gate, w_up):
    tokens, model = x_in.shape
    seq_len = 8 * tokens
    head_dim = wo_own.shape[0] // heads
    rows_own, hid = w_gate.shape[0], w_gate.shape[1] // 8
    shape = jax.ShapeDtypeStruct
    hbm, vmem = pl.BlockSpec(memory_space=pl.ANY), pl.BlockSpec(memory_space=pltpu.VMEM)
    dma = pltpu.SemaphoreType.DMA
    vm = lambda *dims, dtype=BF16: pltpu.VMEM(dims, dtype)
    steps = np.arange(head_dim // 2, dtype=np.float32) * np.float32(2.0 / head_dim)
    freq = np.tile(np.float32(1.0) / (np.float32(ROPE_BASE) ** steps), 4)[None]
    outs = (shape((heads, seq_len, head_dim), BF16), shape((seq_len, head_dim), BF16), shape((seq_len, head_dim), BF16),
            shape((heads * head_dim, seq_len), BF16), shape((rows_own, seq_len), BF16),
            shape((seq_len, 128), F32), shape((seq_len, 128), F32), shape((8, model), F32), shape((tokens, model), BF16))
    pairs = [dma((7,)), dma((7,)), dma((3, 7)), dma((3, 7)), dma((7,)), dma((7,)), dma((7,)), dma((7,)),
             dma((56,)), dma((56,)), dma((7,)), dma((7,))]
    return pl.pallas_call(
        functools.partial(attention_comm_kernel, 'sp', heads), name='attention_comm',
        in_specs=[hbm] + [vmem] * 4 + [hbm] * 6, out_specs=[hbm] * 12,
        out_shape=[*outs, shape((seq_len, model), BF16), shape((model, hid), BF16), shape((model, hid), BF16)],
        scratch_shapes=[vm(*t.shape, dtype=t.dtype) for t in outs] + [
            vm(8, rows_own, dtype=F32), vm(seq_len, model), vm(8, 8, rows_own, dtype=F32),
            vm(384, model), vm(model, model), vm(seq_len, model), vm(tokens, model), vm(tokens, 384), vm(heads, seq_len, head_dim),
            vm(seq_len, heads * head_dim), vm(tokens, model, dtype=F32), vm(2, tokens, model), vm(2, rows_own, hid)] + pairs + [
            dma((2,)), dma((4,)), dma((4,)), dma((4,)), dma((8,)), dma((9,))],
        compiler_params=pltpu.CompilerParams(collective_id=0, has_side_effects=True, vmem_limit_bytes=63 * 1024 * 1024),
    )(x_in, positions, gain1, gain2, jnp.asarray(freq), w_q, w_k, w_v, wo_own, w_gate, w_up)


def hand_over_kernel(n_far, n_near, *refs):
    n_in = n_far + n_near
    sources, gains, results = refs[:n_in], refs[n_in], refs[n_in + 1:2 * n_in + 1]
    gain_outs, stages = refs[2 * n_in + 1:2 * n_in + 3], refs[2 * n_in + 3:2 * n_in + 3 + n_far]
    in_sem, out_sem = refs[2 * n_in + 3 + n_far:]
    loads = [pltpu.make_async_copy(sources[i], stages[i], in_sem.at[i]) for i in range(n_far)]
    stores = [pltpu.make_async_copy(stages[i] if i < n_far else sources[i], results[i], out_sem.at[i]) for i in range(n_in)]
    for load in loads:
        load.start()
    for store in stores[n_far:]:
        store.start()
    for i in range(2):
        gain_outs[i][...] = gains[i, :]
    for load, store in zip(loads, stores):
        load.wait()
        store.start()
    for store in stores:
        store.wait()


def hand_over(far, near, gains):
    shape = jax.ShapeDtypeStruct
    arrays = far + near
    hbm, vmem = pl.BlockSpec(memory_space=pltpu.HBM), pl.BlockSpec(memory_space=pltpu.VMEM)
    dma = pltpu.SemaphoreType.DMA
    return pl.pallas_call(
        functools.partial(hand_over_kernel, len(far), len(near)), name='hand_over',
        in_specs=[hbm] * len(far) + [vmem] * (len(near) + 1), out_specs=[hbm] * len(arrays) + [vmem] * 2,
        out_shape=[shape(a.shape, a.dtype) for a in arrays] + [shape((gains.shape[1],), F32)] * 2,
        scratch_shapes=[pltpu.VMEM(a.shape, a.dtype) for a in far] + [dma((len(far),)), dma((len(arrays),))],
        compiler_params=pltpu.CompilerParams(vmem_limit_bytes=12 * 1024 * 1024),
    )(*[pltpu.with_memory_space_constraint(a, pltpu.HBM) for a in far],
      *[pltpu.with_memory_space_constraint(a, pltpu.VMEM) for a in near + (gains,)])


def solution(mesh):
    n_dev = mesh.shape['sp']

    def layer_step(x_in, positions, d_out, norm1_gain, norm2_gain, w_q, w_k, w_v, w_o, w_gate, w_up, w_down):
        tokens, model = x_in.shape
        head_dim = w_q.shape[2]
        heads = w_q.shape[1] // n_dev
        rows_own = w_q.shape[0]
        flat = lambda w: w.transpose(1, 2, 0).reshape(-1, rows_own)
        wo_own = w_o.reshape(-1, model)
        (q_rot, k_rot, v_lin, o_t, u_t, cos_tab, sin_tab, g_full, hidden,
         mlp_in, w1, w3) = attention_step(heads, x_in, positions, norm1_gain, norm2_gain, flat(w_q), flat(w_k), flat(w_v), wo_own, w_gate, w_up)
        d_w1s, d_w3s, d_down, y_out, dh_own, d_g2 = mlp_step(mlp_in, d_out, w1, w3, w_down, hidden, g_full)
        d_wo, d_wq_t, d_wk_t, d_wv_t, d_w1, d_w3, d_x, d_gains = attention_backward_step(
            heads, dh_own, wo_own, o_t, q_rot, k_rot, v_lin, (cos_tab, sin_tab),
            d_w1s, d_w3s, flat(w_q), flat(w_k), flat(w_v), u_t, x_in, g_full, d_g2)
        from_cols = lambda d, w: d.reshape(w.shape[1], w.shape[2], rows_own).transpose(2, 0, 1)
        (d_down, y_out, d_w1, d_w3, d_wo, d_wq_t, d_wk_t, d_wv_t, d_x, d_g1, d_g2) = hand_over(
            (d_down, y_out), (d_w1, d_w3, d_wo, d_wq_t, d_wk_t, d_wv_t, d_x), d_gains)
        return (y_out, d_x, d_g1, d_g2, from_cols(d_wq_t, w_q), from_cols(d_wk_t, w_k), from_cols(d_wv_t, w_v),
                d_wo.reshape(w_o.shape), d_w1, d_w3, d_down)

    all_rows = P('sp')
    return jax.shard_map(layer_step, mesh=mesh, in_specs=(all_rows,) * 12, out_specs=(all_rows,) * 11, check_vma=False)
```

```python
import functools
import jax
import jax.numpy as jnp
import numpy as np
from jax import lax
from jax.experimental import pallas as pl
from jax.experimental.pallas import tpu as pltpu
from jax.sharding import PartitionSpec as P

ROPE_BASE = 10000.0
NORM_EPS = 1e-5
NEG_LARGE = -1e30
F32 = jnp.float32
BF16 = jnp.bfloat16
BLK = 256


def dot(lhs, rhs, lhs_dim, rhs_dim):
    return lax.dot_general(lhs, rhs, (((lhs_dim,), (rhs_dim,)), ((), ())), preferred_element_type=F32)


def norm_forward(hidden, gain_vec):
    inv_rms = lax.rsqrt(jnp.mean(hidden * hidden, axis=-1, keepdims=True) + NORM_EPS)
    return hidden * inv_rms * gain_vec


def probs_transposed(k_rows, q_blk, start):
    scores = dot(k_rows, q_blk, 1, 1)
    rows = lax.broadcasted_iota(jnp.int32, (BLK, BLK), 0)
    cols = lax.broadcasted_iota(jnp.int32, (BLK, BLK), 1)
    tail = jnp.where(rows <= cols, scores[start:], NEG_LARGE)
    scores = jnp.concatenate([scores[:start], tail], axis=0) if start else tail
    top = jnp.max(scores, axis=0, keepdims=True)
    weights = jnp.exp((scores - top) * (q_blk.shape[1] ** -0.5))
    return weights * (1.0 / jnp.sum(weights, axis=0, keepdims=True))


MESH = pl.DeviceIdType.MESH


def place(axis):
    me = lax.axis_index(axis)
    core = lax.rem(me, 2)
    col = lax.rem(lax.div(me, 2), 2)
    row = lax.div(me, 4)

    def other(flip_core, flip_col, flip_row):
        pick = lambda v, f: 1 - v if f else v
        return pick(row, flip_row) * 4 + pick(col, flip_col) * 2 + pick(core, flip_core)

    nbr_x, nbr_y = other(0, 1, 0), other(0, 0, 1)
    first = nbr_x * (1 - core) + nbr_y * core
    second = nbr_y * (1 - core) + nbr_x * core
    return me, other, first, second


def greet(other):
    barrier = pltpu.get_barrier_semaphore()
    for r in range(1, 8):
        pl.semaphore_signal(barrier, inc=1, device_id=(other(r & 1, (r >> 1) & 1, r >> 2),), device_id_type=MESH)
    pl.semaphore_wait(barrier, 7)


class Gather:
    def __init__(self, slot, send_sem, recv_sem, where, own=None):
        me, other, first, second = where
        partner, diag = other(1, 0, 0), other(0, 1, 1)
        own = slot(me) if own is None else own
        self.copies = []
        plan = [(own, me, first), (own, me, second), (own, me, partner), (slot(first), first, second),
                (slot(first), first, partner), (slot(second), second, partner), (slot(diag), diag, partner)]
        for i, (src, what, dest) in enumerate(plan):
            self.copies.append(pltpu.make_async_remote_copy(
                src_ref=src, dst_ref=slot(what), send_sem=send_sem.at[i], recv_sem=recv_sem.at[i],
                device_id=(dest,), device_id_type=MESH))

    def start(self):
        for i in range(3):
            self.copies[i].start()

    def got_first(self):
        self.copies[0].wait_recv()
        self.copies[3].start()
        self.copies[4].start()

    def got_second(self):
        self.copies[1].wait_recv()
        self.copies[5].start()

    def got_diag(self):
        self.copies[3].wait_recv()
        self.copies[6].start()

    def got_partner(self, i):
        self.copies[(2, 4, 5, 6)[i]].wait_recv()

    def drain(self):
        for copy in self.copies:
            copy.wait_send()


def turn_halves(values, cos_blk, sin_blk):
    width = values.shape[1]
    lanes = lax.broadcasted_iota(jnp.int32, values.shape, 1)
    partner = jnp.where(lax.rem(lanes, 64) < 32, pltpu.roll(values, width - 32, 1), pltpu.roll(values, 32, 1))
    return values * cos_blk + partner * sin_blk


def norm_backward(hidden, gain, d_out):
    inv = lax.rsqrt(jnp.mean(hidden * hidden, axis=-1, keepdims=True) + NORM_EPS)
    d_scaled = d_out * gain
    d_hidden = d_scaled * inv - hidden * (inv * inv * inv * jnp.mean(d_scaled * hidden, axis=-1, keepdims=True))
    return d_hidden, jnp.sum(d_out * (hidden * inv), axis=0, keepdims=True)


def attn_bwd_comm_kernel(axis, heads, dh_hbm, wo_hbm, ot_hbm, q_hbm, k_hbm, v_hbm, cos_hbm, sin_hbm,
                         dw1_ref, dw3_ref, wq_hbm, wk_hbm, wv_hbm, ut_hbm, x_hbm, g_hbm, dg2_hbm,
                         dwo_ref, dwq_ref, dwk_ref, dwv_ref, out1_ref, out3_ref, dx_ref, dg_ref,
                         dh_ref, wo_ref, ot_ref, q_ref, k_ref, v_ref, cos_ref, sin_ref, wq_ref, wk_ref, wv_ref, ut_ref, g_ref, dg2_ref,
                         slots, do_scr, dg_own, dg_all, dk_acc, dv_acc, du_acc, du_scr,
                         bulk_send, bulk_recv, hg_send, hg_recv, gat_send, gat_recv, du_send, du_rsem, dg_send, dg_recv, loc_sem, ld_sem):
    loads = {}
    for i, (name, src, dst) in enumerate((
            ('wo', wo_hbm, wo_ref), ('ot', ot_hbm, ot_ref), ('q', q_hbm, q_ref), ('k', k_hbm, k_ref),
            ('v', v_hbm, v_ref), ('cos', cos_hbm, cos_ref), ('sin', sin_hbm, sin_ref), ('wq', wq_hbm, wq_ref), ('wk', wk_hbm, wk_ref),
            ('wv', wv_hbm, wv_ref), ('ut', ut_hbm, ut_ref), ('g', g_hbm, g_ref), ('dg2', dg2_hbm, dg2_ref),
            ('dh', dh_hbm, dh_ref.at[pl.ds(pl.multiple_of(lax.axis_index(axis) * x_hbm.shape[0], x_hbm.shape[0]), x_hbm.shape[0]), :]))):
        loads[name] = pltpu.make_async_copy(src, dst, ld_sem.at[i])
        loads[name].start()

    def need(*names):
        for name in names:
            loads[name].wait()

    where = place(axis)
    me, other, first, second = where
    greet(other)
    seq_len, head_dim = k_ref.shape
    rows_own, hid = out1_ref.shape[0], dw1_ref.shape[1]
    tokens = x_hbm.shape[0]
    qw = heads * head_dim

    rows_of = lambda d: pl.ds(pl.multiple_of(d * rows_own, rows_own), rows_own)
    hid_of = lambda d: pl.ds(pl.multiple_of(d * hid, hid), hid)
    pairs = ((dw1_ref, out1_ref), (dw3_ref, out3_ref))
    peers = [other(r & 1, (r >> 1) & 1, r >> 2) for r in (2, 4, 6, 3, 5, 7, 1)]
    bulk, parts = [], []
    for src, dst in pairs:
        for low, high in ((0, 8), (8, rows_own // 2), (rows_own // 2, rows_own)):
            parts.append(range(len(bulk), len(bulk) + len(peers)))
            for dest in peers:
                bulk.append(pltpu.make_async_remote_copy(
                    src_ref=src.at[pl.ds(pl.multiple_of(dest * rows_own + low, 8), high - low), :],
                    dst_ref=dst.at[pl.ds(low, high - low), hid_of(me)], send_sem=bulk_send.at[len(bulk)],
                    recv_sem=bulk_recv.at[len(bulk)], device_id=(dest,), device_id_type=MESH))

    def start_bulk(*which):
        for part in which:
            for i in parts[part]:
                bulk[i].start()
    tok_of = lambda d: pl.ds(pl.multiple_of(d * tokens, tokens), tokens)
    h_gather = Gather(lambda d: dh_ref.at[tok_of(d), :], hg_send, hg_recv, where, own=dh_hbm)
    h_gather.start()
    start_bulk(0)
    local = [pltpu.make_async_copy(src.at[rows_of(me), :], dst.at[:, hid_of(me)], loc_sem.at[i]) for i, (src, dst) in enumerate(pairs)]
    for copy in local:
        copy.start()
    need('dh', 'wo', 'ot')
    h_gather.got_first()
    h_gather.got_second()
    start_bulk(1, 2)
    h_gather.got_diag()
    for i in range(4):
        h_gather.got_partner(i)

    def split_out_grad(k, _):
        rows = pl.ds(pl.multiple_of(k * BLK, BLK), BLK)
        do_blk = dot(dh_ref[rows, :], wo_ref[...], 1, 1).astype(BF16)
        for h in range(heads):
            do_scr[h, rows, :] = do_blk[:, h * head_dim:(h + 1) * head_dim]
        cols = rows
        dwo_ref[:, cols] = dot(ot_ref[...], dh_ref[:, cols], 1, 0)
        return 0
    lax.fori_loop(0, seq_len // BLK, split_out_grad, 0)
    x_ref = wo_ref
    x_load = pltpu.make_async_copy(x_hbm, x_ref, ld_sem.at[14])
    x_load.start()


    need('q', 'k', 'v')
    dk_acc[...] = jnp.zeros_like(dk_acc)
    dv_acc[...] = jnp.zeros_like(dv_acc)
    mine = slots.at[me]

    def one_head(h, _):
        def one_block(start):
            keys = pl.ds(0, start + BLK)
            rows = pl.ds(start, BLK)
            q_blk, do_blk = q_ref[h, rows, :], do_scr[h, rows, :]
            probs = probs_transposed(k_ref[keys, :], q_blk, start)
            d_probs = dot(v_ref[keys, :], do_blk, 1, 1).astype(BF16).astype(F32)
            row_dot = jnp.sum(d_probs * probs, axis=0, keepdims=True)
            d_scores = (probs * (d_probs - row_dot) * (head_dim ** -0.5)).astype(BF16)
            do_scr[h, rows, :] = dot(d_scores, k_ref[keys, :], 0, 0).astype(BF16)
            dk_acc[keys, :] += dot(d_scores, q_blk, 1, 0)
            dv_acc[keys, :] += dot(probs.astype(BF16), do_blk, 1, 0)
        for start in range(0, seq_len, BLK):
            one_block(start)
        return 0
    lax.fori_loop(0, heads, one_head, 0)
    need('cos', 'sin')
    mine[:, qw:qw + head_dim] = dk_acc[...].astype(BF16)
    mine[:, qw + head_dim:] = dv_acc[...].astype(BF16)
    low = lax.broadcasted_iota(jnp.int32, (BLK, 128), 1) < head_dim

    def turn_back(k, _):
        rows = pl.ds(pl.multiple_of(k * BLK, BLK), BLK)
        cos_blk, sin_blk = cos_ref[rows, :], -sin_ref[rows, :]
        for pair in range(heads // 2):
            both = jnp.concatenate([do_scr[2 * pair, rows, :], do_scr[2 * pair + 1, rows, :]], axis=1)
            mine[rows, pair * 128:(pair + 1) * 128] = turn_halves(both.astype(F32), cos_blk, sin_blk).astype(BF16)
        kv = mine[rows, qw:].astype(F32)
        mine[rows, qw:] = jnp.where(low, turn_halves(kv, cos_blk, sin_blk), kv).astype(BF16)
        return 0
    lax.fori_loop(0, seq_len // BLK, turn_back, 0)

    gather = Gather(lambda d: slots.at[d], gat_send, gat_recv, where)
    gather.start()
    start_bulk(3)
    du_acc[...] = jnp.zeros_like(du_acc)
    need('wq', 'wk', 'wv', 'ut')

    def use(d):
        q_rows = pl.ds(pl.multiple_of(d * qw, qw), qw)
        kv_rows = pl.ds(pl.multiple_of(d * head_dim, head_dim), head_dim)
        w_all = jnp.concatenate([wq_ref[q_rows, :], wk_ref[kv_rows, :], wv_ref[kv_rows, :]], axis=0)

        def add_rows(k, _):
            rows = pl.ds(pl.multiple_of(k * 512, 512), 512)
            du_acc[rows, :] += dot(slots[d, rows, :], w_all, 1, 0)
            return 0
        lax.fori_loop(0, seq_len // 512, add_rows, 0)
        d_w = dot(ut_ref[...], slots[d], 1, 0).T
        dwq_ref[q_rows, :] = d_w[:qw]
        dwk_ref[kv_rows, :] = d_w[qw:qw + head_dim]
        dwv_ref[kv_rows, :] = d_w[qw + head_dim:]

    def use_many(*devices):
        def body(i, _):
            d = devices[0]
            for n in range(1, len(devices)):
                d = jnp.where(i == n, devices[n], d)
            use(d)
            return 0
        lax.fori_loop(0, len(devices), body, 0)

    use_many(me)
    gather.got_first()
    gather.got_second()
    start_bulk(4)
    gather.got_partner(0)
    use_many(first, second, other(1, 0, 0))
    gather.got_diag()
    for i in range(1, 4):
        gather.got_partner(i)
    use_many(other(0, 1, 1), other(1, 1, 0), other(1, 0, 1), other(1, 1, 1))
    du_scr[...] = du_acc[...].astype(BF16)
    sends = []
    for n, dest in enumerate(peers):
        sends.append(pltpu.make_async_remote_copy(
            src_ref=du_scr.at[tok_of(dest), :], dst_ref=ot_ref.at[:, rows_of(me)], send_sem=du_send.at[n],
            recv_sem=du_rsem.at[n], device_id=(dest,), device_id_type=MESH))
        sends[-1].start()
    start_bulk(5)
    ot_ref[:, rows_of(me)] = du_scr[tok_of(me), :]
    need('g', 'dg2')
    x_load.wait()
    for copy in sends:
        copy.wait_recv()
    dg_own[...] = jnp.zeros_like(dg_own)
    dg_own[1:2, :] = dg2_ref[...]

    def input_grad(k, _):
        part = pl.ds(pl.multiple_of(k * 16, 16), 16)
        d_norm, d_gain = norm_backward(x_ref[part, :].astype(F32), g_ref[0:1, :], ot_ref[part, :].astype(F32))
        dh_part = dh_ref[pl.ds(pl.multiple_of(me * tokens + k * 16, 16), 16), :]
        dx_ref[part, :] = (dh_part.astype(F32) + d_norm).astype(BF16)
        dg_own[0:1, :] += d_gain
        return 0
    lax.fori_loop(0, tokens // 16, input_grad, 0)
    gain_sends = []
    for n, dest in enumerate(peers):
        gain_sends.append(pltpu.make_async_remote_copy(
            src_ref=dg_own.at[:, rows_of(dest)], dst_ref=dg_all.at[me], send_sem=dg_send.at[n],
            recv_sem=dg_recv.at[n], device_id=(dest,), device_id_type=MESH))
        gain_sends[-1].start()
    dg_all[me] = dg_own[:, rows_of(me)]
    for copy in gain_sends:
        copy.wait_recv()
    dg_ref[...] = jnp.sum(dg_all[...], axis=0)
    for copy in sends + gain_sends:
        copy.wait_send()
    gather.drain()
    h_gather.drain()
    for copy in bulk:
        copy.wait()
    for copy in local:
        copy.wait()


def attention_backward_step(heads, dh_own, wo_own, o_t, q_rot, k_rot, v_lin, tables, d_w1, d_w3, w_q, w_k, w_v, u_t, x_in, gains, d_g2):
    seq_len, model = k_rot.shape[0], x_in.shape[1]
    head_dim = k_rot.shape[1]
    tokens = x_in.shape[0]
    rows_own, hid = model // 8, d_w1.shape[1]
    shape = jax.ShapeDtypeStruct
    hbm = pl.BlockSpec(memory_space=pl.ANY)
    dma = pltpu.SemaphoreType.DMA
    vm = lambda *dims, dtype=BF16: pltpu.VMEM(dims, dtype)
    early = (dh_own, wo_own, o_t, q_rot, k_rot, v_lin, *tables)
    late = (w_q, w_k, w_v, u_t, x_in, gains, d_g2)
    outs = [(wo_own.shape, F32), (w_q.shape, F32), (w_k.shape, F32), (w_v.shape, F32), ((rows_own, 8 * hid), F32),
            ((rows_own, 8 * hid), F32), (x_in.shape, BF16), ((8, rows_own), F32)]
    vmem = pl.BlockSpec(memory_space=pltpu.VMEM)
    return pl.pallas_call(
        functools.partial(attn_bwd_comm_kernel, 'sp', heads), name='attn_bwd_comm',
        in_specs=[hbm] * 17, out_specs=[vmem] * 8,
        out_shape=[pltpu.VMEM(dims, dtype) for dims, dtype in outs],
        scratch_shapes=[vm(seq_len, model)] + [vm(*t.shape, dtype=t.dtype) for t in early[1:] + late[:4] + late[5:]] + [
            vm(8, seq_len, 384), vm(heads, seq_len, head_dim),
            vm(8, model, dtype=F32), vm(8, 8, rows_own, dtype=F32),
            vm(seq_len, head_dim, dtype=F32), vm(seq_len, head_dim, dtype=F32),
            vm(seq_len, rows_own, dtype=F32), vm(seq_len, rows_own),
            dma((42,)), dma((42,)), dma((7,)), dma((7,)), dma((7,)), dma((7,)), dma((7,)), dma((7,)), dma((7,)), dma((7,)), dma((2,)), dma((15,))],
        compiler_params=pltpu.CompilerParams(collective_id=2, has_side_effects=True, vmem_limit_bytes=43515904),
    )(*early, d_w1, d_w3, *late)


def mlp_comm_kernel(axis, m_ref, dout_own, w1_hbm, w3_hbm, w2_hbm, h_hbm, g_hbm,
                    dw1_ref, dw3_ref, dw2_ref, y_hbm, dh_hbm, dg2_hbm, dout_ref,
                    w1_ref, w3_ref, w2_ref, h_ref, g_ref, y_ref, dg2_ref,
                    glu, gate_s, up_s, outbox, chip_sum, inbox, blk, m_col, do_col, mt_scr, dot_scr, st1, st3, st2, dh_own,
                    part_send, part_recv, mail_send, mail_recv, do_send, do_recv,
                    in_sem, col_sem, out_sem, own_sem, ld_sem, credit):
    loads = [pltpu.make_async_copy(src, dst, ld_sem.at[i]) for i, (src, dst) in enumerate((
        (w1_hbm, w1_ref), (w3_hbm, w3_ref), (w2_hbm, w2_ref), (h_hbm, h_ref), (g_hbm, g_ref)))]
    own_in = pltpu.make_async_copy(dout_own, dh_own, own_sem.at[0])
    for copy in loads + [own_in]:
        copy.start()
    where = place(axis)
    me, other, first, second = where
    core = lax.rem(me, 2)
    partner = other(1, 0, 0)
    tokens, model = h_ref.shape
    hid = w1_ref.shape[1]
    tok_of = lambda d: pl.ds(pl.multiple_of(d * tokens, tokens), tokens)
    off_first, off_second = 1 + core, 2 - core

    def block_of(off, flip):
        d_col, d_row = lax.rem(off, 2), lax.div(off, 2)
        col, row = lax.rem(lax.div(me, 2), 2), lax.div(me, 4)
        mix = lambda v, f: v + f - 2 * v * f
        return mix(row, d_row) * 4 + mix(col, d_col) * 2 + mix(core, flip)

    def step_off(step, flip):
        mid_a = off_second * (1 - flip) + off_first * flip
        mid_b = off_first * (1 - flip) + off_second * flip
        return jnp.where(step == 0, 3, jnp.where(step == 1, mid_a, jnp.where(step == 2, mid_b, 0)))

    def half_rows(half):
        flip = 1 - lax.rem(half, 2)
        return tok_of(block_of(step_off(lax.div(half, 2), flip), flip))

    def fetch(half):
        slot = lax.rem(half, 2)
        return pltpu.make_async_copy(m_ref.at[half_rows(half), :], blk.at[slot], in_sem.at[slot])

    def fetch_dout(d):
        slot = lax.rem(d, 2)
        return pltpu.make_async_copy(dout_ref.at[tok_of(d), :], blk.at[slot], in_sem.at[slot])

    def fetch_cols(j):
        cols = pl.ds(pl.multiple_of(j * 256, 256), 256)
        return (pltpu.make_async_copy(m_ref.at[:, cols], m_col, col_sem.at[0]),
                pltpu.make_async_copy(dout_ref.at[:, cols], do_col, col_sem.at[1]))

    def sigmoid(value):
        return 1.0 / (1.0 + jnp.exp(-value))

    def activations(slot, rows):
        def chunk(j, _):
            cols = pl.ds(pl.multiple_of(j * 512, 512), 512)
            gate = dot(blk[slot], w1_ref[:, cols], 1, 0).astype(BF16)
            up = dot(blk[slot], w3_ref[:, cols], 1, 0).astype(BF16)
            gate_s[rows, cols] = gate
            up_s[rows, cols] = up
            gate = gate.astype(F32)
            glu[rows, cols] = (gate * sigmoid(gate) * up.astype(F32)).astype(BF16)
            return 0
        lax.fori_loop(0, hid // 512, chunk, 0)

    def activation_grads(slot, rows):
        def chunk(j, _):
            cols = pl.ds(pl.multiple_of(j * 512, 512), 512)
            d_act = dot(blk[slot], w2_ref[cols, :], 1, 1).astype(BF16).astype(F32)
            gate, up = gate_s[rows, cols].astype(F32), up_s[rows, cols].astype(F32)
            sig = sigmoid(gate)
            silu = gate * sig
            up_s[rows, cols] = (d_act * silu).astype(BF16)
            gate_s[rows, cols] = (d_act * up * (sig + silu * (1.0 - sig))).astype(BF16)
            return 0
        lax.fori_loop(0, hid // 512, chunk, 0)

    def add_mlp_grad(rows, put):
        def chunk(j, _):
            cols = pl.ds(pl.multiple_of(j * 512, 512), 512)
            put(cols, dot(gate_s[rows, :], w1_ref[cols, :], 1, 1) + dot(up_s[rows, :], w3_ref[cols, :], 1, 1))
            return 0
        lax.fori_loop(0, model // 512, chunk, 0)

    def add_mlp_out(rows, put):
        def chunk(j, _):
            cols = pl.ds(pl.multiple_of(j * 512, 512), 512)
            put(cols, dot(glu[rows, :], w2_ref[:, cols], 1, 0))
            return 0
        lax.fori_loop(0, model // 512, chunk, 0)

    def signal(index, device):
        pl.semaphore_signal(credit.at[index], inc=1, device_id=(device,), device_id_type=MESH)

    class Scatter:
        def __init__(self, turn):
            self.turn = turn

        def to_partner(self, step):
            off = step_off(step, 1)
            return pltpu.make_async_remote_copy(
                src_ref=outbox.at[lax.rem(step, 2)], dst_ref=chip_sum.at[off], send_sem=part_send.at[self.turn, step],
                recv_sem=part_recv.at[self.turn, off], device_id=(partner,), device_id_type=MESH)

        def from_partner(self, off):
            return pltpu.make_async_remote_copy(
                src_ref=outbox.at[0], dst_ref=chip_sum.at[off], send_sem=part_send.at[self.turn, 0],
                recv_sem=part_recv.at[self.turn, off], device_id=(partner,), device_id_type=MESH)

        def mail(self, kind):
            off = (3, off_first, off_second)[kind]
            dest = (first, first, second)[kind]
            return pltpu.make_async_remote_copy(
                src_ref=chip_sum.at[off], dst_ref=inbox.at[kind], send_sem=mail_send.at[self.turn, kind],
                recv_sem=mail_recv.at[self.turn, kind], device_id=(dest,), device_id_type=MESH)

        def step(self, step, prepare, partial):
            self.first_half(step, prepare, partial)
            self.second_half(step, prepare, partial)

        def first_half(self, step, prepare, partial):
            slot = lax.rem(step, 2)
            prepare(2 * step)

            def put_out(cols, value):
                outbox[slot, :, cols] = value
            partial(half_rows(2 * step), put_out)

        def second_half(self, step, prepare, partial):
            self.to_partner(step).start()
            prepare(2 * step + 1)
            off = step_off(step, 0)
            self.from_partner(off).wait_recv()

            def put_sum(cols, value):
                chip_sum[off, :, cols] += value
            partial(half_rows(2 * step + 1), put_sum)

        def pass_on(self):
            self.mail(0).wait_recv()

            def add_mail(k, _):
                part = pl.ds(pl.multiple_of(k * 16, 16), 16)
                chip_sum[off_second, part, :] += inbox[0, part, :]
                return 0
            lax.fori_loop(0, tokens // 16, add_mail, 0)

    out_round, grad_round = Scatter(0), Scatter(1)

    def prepare_out(half):
        @pl.when(half < 7)
        def _():
            fetch(half + 1).start()
        fetch(half).wait()
        activations(lax.rem(half, 2), half_rows(half))

    def weight_grads(begin, end):
        for copy in fetch_cols(begin):
            copy.start()

        def body(j, _):
            for copy in fetch_cols(j):
                copy.wait()

            def turn(k, _):
                part = pl.ds(pl.multiple_of(k * 256, 256), 256)
                mt_scr[:, part] = m_col[part, :].T
                dot_scr[:, part] = do_col[part, :].T
                return 0
            lax.fori_loop(0, m_col.shape[0] // 256, turn, 0)

            @pl.when(j + 1 < end)
            def _():
                for copy in fetch_cols(j + 1):
                    copy.start()
            rows = pl.ds(pl.multiple_of(j * 256, 256), 256)
            out = (pltpu.make_async_copy(st1, dw1_ref.at[rows, :], out_sem.at[0]),
                   pltpu.make_async_copy(st3, dw3_ref.at[rows, :], out_sem.at[1]),
                   pltpu.make_async_copy(st2, dw2_ref.at[:, rows], out_sem.at[2]))

            @pl.when(j > begin)
            def _():
                for copy in out:
                    copy.wait()

            def chunk(k, _):
                cols = pl.ds(pl.multiple_of(k * 512, 512), 512)
                st1[:, cols] = dot(mt_scr[...], gate_s[:, cols], 1, 0)
                st3[:, cols] = dot(mt_scr[...], up_s[:, cols], 1, 0)
                st2[cols, :] = dot(dot_scr[...], glu[:, cols], 1, 0).T
                return 0
            lax.fori_loop(0, hid // 512, chunk, 0)
            for copy in out:
                copy.start()
            return 0
        lax.fori_loop(begin, end, body, 0)
        rows = pl.ds((end - 1) * 256, 256)
        for copy in (pltpu.make_async_copy(st1, dw1_ref.at[rows, :], out_sem.at[0]),
                     pltpu.make_async_copy(st3, dw3_ref.at[rows, :], out_sem.at[1]),
                     pltpu.make_async_copy(st2, dw2_ref.at[:, rows], out_sem.at[2])):
            copy.wait()

    fetch(0).start()
    greet(other)
    do_gather = Gather(lambda d: dout_ref.at[tok_of(d), :], do_send, do_recv, where, own=dout_own)
    do_gather.start()
    own_in.wait()
    own_out = pltpu.make_async_copy(dh_own, dout_ref.at[tok_of(me), :], own_sem.at[1])
    own_out.start()
    for copy in loads:
        copy.wait()

    def out_step(step, _):
        @pl.when(step >= 2)
        def _():
            out_round.to_partner(step - 2).wait_send()
        out_round.step(step, prepare_out, add_mlp_out)

        @pl.when(step == 0)
        def _():
            out_round.mail(0).start()

        @pl.when(step == 2)
        def _():
            out_round.mail(1).start()
            do_gather.got_first()
            do_gather.got_second()
        return 0
    lax.fori_loop(0, 4, out_step, 0)
    out_round.pass_on()
    out_round.mail(2).start()
    for step in (2, 3):
        out_round.to_partner(step).wait_send()
    out_round.mail(0).wait_send()
    signal(0, partner)
    signal(1, first)
    do_gather.got_diag()
    for i in range(4):
        do_gather.got_partner(i)
    own_out.wait()
    fetch_dout(0).start()

    def grad_block(d, _):
        @pl.when(d < 7)
        def _():
            fetch_dout(d + 1).start()
        fetch_dout(d).wait()
        activation_grads(lax.rem(d, 2), tok_of(d))
        return 0
    lax.fori_loop(0, 8, grad_block, 0)

    as_is = lambda half: None
    grad_round.first_half(0, as_is, add_mlp_grad)
    pl.semaphore_wait(credit.at[0], 1)
    grad_round.second_half(0, as_is, add_mlp_grad)
    pl.semaphore_wait(credit.at[1], 1)
    grad_round.mail(0).start()
    weight_grads(0, 2)
    grad_round.first_half(1, as_is, add_mlp_grad)
    out_round.mail(1).wait_recv()
    out_round.mail(2).wait_recv()

    def layer_out(k, _):
        part = pl.ds(pl.multiple_of(k * 16, 16), 16)
        y_ref[part, :] = (h_ref[part, :].astype(F32) + (chip_sum[0, part, :] + inbox[1, part, :] + inbox[2, part, :])).astype(BF16)
        return 0
    lax.fori_loop(0, tokens // 16, layer_out, 0)
    y_store = pltpu.make_async_copy(y_ref, y_hbm, own_sem.at[2])
    y_store.start()
    out_round.mail(1).wait_send()
    out_round.mail(2).wait_send()
    signal(2, partner)
    signal(3, first)
    signal(4, second)
    pl.semaphore_wait(credit.at[2], 1)

    grad_round.second_half(1, as_is, add_mlp_grad)

    def grad_step(step, _):
        grad_round.to_partner(step - 2).wait_send()
        grad_round.step(step, as_is, add_mlp_grad)

        @pl.when(step == 2)
        def _():
            pl.semaphore_wait(credit.at[3], 1)
            grad_round.mail(1).start()
            grad_round.pass_on()
            pl.semaphore_wait(credit.at[4], 1)
            grad_round.mail(2).start()
        return 0
    lax.fori_loop(2, 4, grad_step, 0)
    weight_grads(2, 8)
    grad_round.mail(1).wait_recv()
    grad_round.mail(2).wait_recv()
    dg2_ref[...] = jnp.zeros_like(dg2_ref)

    def hidden_grad(k, _):
        part = pl.ds(pl.multiple_of(k * 16, 16), 16)
        d_mlp = (chip_sum[0, part, :] + inbox[1, part, :] + inbox[2, part, :]).astype(BF16).astype(F32)
        d_norm, d_gain = norm_backward(h_ref[part, :].astype(F32), g_ref[1:2, :], d_mlp)
        dh_own[part, :] = (dh_own[part, :].astype(F32) + d_norm).astype(BF16)
        dg2_ref[...] += d_gain
        return 0
    lax.fori_loop(0, tokens // 16, hidden_grad, 0)
    own_out = pltpu.make_async_copy(dh_own, dh_hbm, own_sem.at[3])
    own_out.start()
    dg2_store = pltpu.make_async_copy(dg2_ref, dg2_hbm, own_sem.at[4])
    dg2_store.start()
    for step in (2, 3):
        grad_round.to_partner(step).wait_send()
    for kind in range(3):
        grad_round.mail(kind).wait_send()
    do_gather.drain()
    own_out.wait()
    y_store.wait()
    dg2_store.wait()


def mlp_step(m_all, d_out, w1, w3, w2, hidden, gains):
    seq_len, model = m_all.shape
    hid, tokens = w1.shape[1], hidden.shape[0]
    shape = jax.ShapeDtypeStruct
    hbm = pl.BlockSpec(memory_space=pl.ANY)
    dma = pltpu.SemaphoreType.DMA
    vm = lambda *dims, dtype=BF16: pltpu.VMEM(dims, dtype)
    return pl.pallas_call(
        functools.partial(mlp_comm_kernel, 'sp'), name='mlp_comm',
        in_specs=[hbm] * 7, out_specs=[hbm] * 7,
        out_shape=[shape((model, hid), F32), shape((model, hid), F32), shape((hid, model), F32),
                   shape(hidden.shape, BF16), shape(hidden.shape, BF16), shape((1, model), F32), shape((seq_len, model), BF16)],
        scratch_shapes=[vm(*t.shape, dtype=t.dtype) for t in (w1, w3, w2, hidden, gains)] + [
            vm(tokens, model), vm(1, model, dtype=F32),
            vm(seq_len, hid), vm(seq_len, hid), vm(seq_len, hid),
            vm(2, tokens, model, dtype=F32), vm(4, tokens, model, dtype=F32), vm(3, tokens, model, dtype=F32),
            vm(2, tokens, model), vm(seq_len, 256), vm(seq_len, 256), vm(256, seq_len), vm(256, seq_len),
            vm(256, hid, dtype=F32), vm(256, hid, dtype=F32), vm(hid, 256, dtype=F32), vm(tokens, model),
            dma((2, 4)), dma((2, 4)), dma((2, 3)), dma((2, 3)), dma((7,)), dma((7,)),
            dma((2,)), dma((2,)), dma((3,)), dma((5,)), dma((5,)), pltpu.SemaphoreType.REGULAR((5,))],
        compiler_params=pltpu.CompilerParams(collective_id=1, has_side_effects=True, vmem_limit_bytes=63 * 1024 * 1024),
    )(m_all, d_out, w1, w3, w2, hidden, gains)[:6]


def spread_tables(packed, upper):
    lanes = lax.broadcasted_iota(jnp.int32, packed.shape, 1)
    swapped = pltpu.roll(packed, 64, 1)
    both = jnp.where((lanes < 64) != upper, packed, swapped)
    low = lax.rem(lanes, 64) < 32
    return jnp.where(low, both, pltpu.roll(both, 32, 1)), jnp.where(low, -pltpu.roll(both, 96, 1), both)


def attention_comm_kernel(axis, heads, x_ref, pos_ref, gain1_ref, gain2_ref, freq_ref, wq_ref, wk_ref, wv_ref, wo_ref, wg_ref, wu_ref,
                          q_hbm, k_hbm, v_hbm, ot_hbm, ut_hbm, cos_hbm, sin_hbm, gfull_hbm, h_hbm, m_ref, w1_ref, w3_ref,
                          q_ref, k_ref, v_ref, ot_ref, ut_ref, cos_ref, sin_ref, gfull_ref, h_ref, gain_ref, x_all, gain_all, w_head, wo_all, o_all, u_blk, qkv_blk, o_scr, o_own, h_scr, m_out, stage,
                          g_send, g_recv, w_send, w_recv, x_send, x_recv, wo_send, wo_recv, bulk_send, bulk_recv,
                          o_send, o_recv, m_loc, m_send, m_recv, loc_sem, own_sem, st_sem):
    gain_ref[...] = jnp.zeros_like(gain_ref)
    gain_ref[0:1, :] = gain1_ref[...].astype(F32).reshape(1, -1)
    gain_ref[1:2, :] = gain2_ref[...].astype(F32).reshape(1, -1)
    gain_ref[2:3, :] = pos_ref[...].astype(F32).reshape(1, -1)
    where = place(axis)
    me, other, first, second = where
    core = lax.rem(me, 2)
    partner = other(1, 0, 0)
    greet(other)
    tokens, model = x_ref.shape
    seq_len, head_dim = k_ref.shape
    qw = heads * head_dim
    rows_own, hid = wg_ref.shape[0], w1_ref.shape[1]
    tok_of = lambda d: pl.ds(pl.multiple_of(d * tokens, tokens), tokens)
    cols_of = lambda d: pl.ds(pl.multiple_of(d * rows_own, rows_own), rows_own)
    hid_of = lambda d: pl.ds(pl.multiple_of(d * hid, hid), hid)
    peers = [other(r & 1, (r >> 1) & 1, r >> 2) for r in (6, 2, 4, 7, 3, 5, 1)]

    def to_all(src_of, dst, send_sem, recv_sem):
        return [pltpu.make_async_remote_copy(
            src_ref=src_of(dest), dst_ref=dst, send_sem=send_sem.at[n], recv_sem=recv_sem.at[n],
            device_id=(dest,), device_id_type=MESH) for n, dest in enumerate(peers)]

    small = to_all(lambda dest: gain_ref, gain_all.at[me], g_send, g_recv)
    q_of = lambda d: pl.ds(pl.multiple_of(d * qw, qw), qw)
    kv_of = lambda d: pl.ds(pl.multiple_of(d * head_dim, head_dim), head_dim)
    slices = (to_all(lambda dest: wq_ref.at[q_of(dest), :], w_head.at[0:qw, cols_of(me)], w_send.at[0], w_recv.at[0])
              + to_all(lambda dest: wk_ref.at[kv_of(dest), :], w_head.at[qw:qw + head_dim, cols_of(me)], w_send.at[1], w_recv.at[1])
              + to_all(lambda dest: wv_ref.at[kv_of(dest), :], w_head.at[qw + head_dim:, cols_of(me)], w_send.at[2], w_recv.at[2]))
    for copy in small + slices:
        copy.start()
    x_gather = Gather(lambda d: x_all.at[tok_of(d), :], x_send, x_recv, where, own=x_ref)
    x_gather.start()
    wo_gather = Gather(lambda d: wo_all.at[cols_of(d), :], wo_send, wo_recv, where, own=wo_ref)
    bulk, parts = [], []
    quarter = rows_own // 4
    for src, dst in ((wg_ref, w1_ref), (wu_ref, w3_ref)):
        for low, high in ((0, 16), (16, quarter), (quarter, 2 * quarter), (2 * quarter, 3 * quarter), (3 * quarter, rows_own)):
            parts.append(range(len(bulk), len(bulk) + len(peers)))
            for dest in peers:
                bulk.append(pltpu.make_async_remote_copy(
                    src_ref=src.at[pl.ds(low, high - low), hid_of(dest)],
                    dst_ref=dst.at[pl.ds(pl.multiple_of(me * rows_own + low, 16), high - low), :],
                    send_sem=bulk_send.at[len(bulk)], recv_sem=bulk_recv.at[len(bulk)], device_id=(dest,), device_id_type=MESH))

    def start_bulk(*which):
        for part in which:
            for i in parts[part]:
                bulk[i].start()
    start_bulk(0)

    stores = [pltpu.make_async_copy(src, dst, st_sem.at[i]) for i, (src, dst) in enumerate((
        (q_ref, q_hbm), (k_ref, k_hbm), (v_ref, v_hbm), (ot_ref, ot_hbm), (ut_ref, ut_hbm), (cos_ref, cos_hbm),
        (sin_ref, sin_hbm), (gfull_ref, gfull_hbm), (h_ref, h_hbm)))]
    own = [pltpu.make_async_copy(src, dst, own_sem.at[i]) for i, (src, dst) in enumerate((
        (gain_ref, gain_all.at[me]), (wq_ref.at[q_of(me), :], w_head.at[0:qw, cols_of(me)]),
        (wk_ref.at[kv_of(me), :], w_head.at[qw:qw + head_dim, cols_of(me)]),
        (wv_ref.at[kv_of(me), :], w_head.at[qw + head_dim:, cols_of(me)]),
        (x_ref, x_all.at[tok_of(me), :]), (wo_ref, wo_all.at[cols_of(me), :])))]
    for copy in own:
        copy.start()
    local = []
    for i, (src, dst) in enumerate(((wg_ref, w1_ref), (wu_ref, w3_ref))):
        local.append((pltpu.make_async_copy(src.at[:, hid_of(me)], stage.at[i], loc_sem.at[i]),
                      pltpu.make_async_copy(stage.at[i], dst.at[cols_of(me), :], loc_sem.at[2 + i])))
        local[-1][0].start()
    for load, store in local:
        load.wait()
        store.start()
    for copy in own:
        copy.wait()
    for copy in small:
        copy.wait_recv()
    for d in range(8):
        gfull_ref[:, d * rows_own:(d + 1) * rows_own] = gain_all[d]
    for copy in slices:
        copy.wait_recv()

    def use(d):
        base = pl.multiple_of(d * tokens, tokens)

        def norm(k, _):
            part = pl.ds(pl.multiple_of(k * 16, 16), 16)
            x_part = x_all[pl.ds(pl.multiple_of(base + k * 16, 16), 16), :].astype(F32)
            u_blk[part, :] = norm_forward(x_part, gfull_ref[0:1, :]).astype(BF16)
            return 0
        lax.fori_loop(0, tokens // 16, norm, 0)
        ut_ref[:, tok_of(d)] = u_blk[:, cols_of(me)].T
        qkv_blk[...] = dot(u_blk[...], w_head[...], 1, 1).astype(BF16)
        half = tokens // 2
        where_to = gain_all[d, 2:3, :]
        lanes = lax.broadcasted_iota(jnp.int32, (half, 2 * head_dim), 1)
        by_row = lambda lo: jnp.broadcast_to(where_to[:, lo:lo + half], (2 * head_dim, half)).T
        angles = jnp.where(lanes < head_dim, by_row(0), by_row(half)) * freq_ref[...]
        packed = jnp.where(lax.rem(lanes, head_dim) < head_dim // 2, jnp.cos(angles), jnp.sin(angles))
        for part in range(2):
            rows = pl.ds(pl.multiple_of(base + part * half, half), half)
            cos_blk, sin_blk = spread_tables(packed, part == 1)
            cos_ref[rows, :] = cos_blk
            sin_ref[rows, :] = sin_blk
            source = slice(part * half, (part + 1) * half)
            for pair in range(heads // 2):
                turned = turn_halves(qkv_blk[source, pair * 128:(pair + 1) * 128].astype(F32), cos_blk, sin_blk).astype(BF16)
                q_ref[2 * pair, rows, :] = turned[:, :head_dim]
                q_ref[2 * pair + 1, rows, :] = turned[:, head_dim:]
            turned = turn_halves(qkv_blk[source, qw:].astype(F32), cos_blk, sin_blk).astype(BF16)
            k_ref[rows, :] = turned[:, :head_dim]
            v_ref[rows, :] = qkv_blk[source, qw + head_dim:]

    x_gather.got_first()
    x_gather.got_second()
    wo_gather.start()
    start_bulk(1, 2, 3)
    x_gather.got_partner(0)

    def use_near(i, _):
        use(jnp.where(i == 0, me, jnp.where(i == 1, first, jnp.where(i == 2, second, partner))))
        return 0
    lax.fori_loop(0, 4, use_near, 0)
    x_gather.got_diag()
    for i in range(1, 4):
        x_gather.got_partner(i)

    def use_far(i, _):
        use(jnp.where(i == 0, other(0, 1, 1), jnp.where(i == 1, other(1, 1, 0), jnp.where(i == 2, other(1, 0, 1), other(1, 1, 1)))))
        return 0
    lax.fori_loop(0, 4, use_far, 0)

    def one_head(h, _):
        for start in range(0, seq_len, BLK):
            keys, rows = pl.ds(0, start + BLK), pl.ds(start, BLK)
            probs = probs_transposed(k_ref[keys, :], q_ref[h, rows, :], start)
            o_scr[h, rows, :] = dot(probs.astype(BF16), v_ref[keys, :], 0, 0).astype(BF16)
        return 0
    for i in (0, 1, 2, 4, 5, 6, 7):
        stores[i].start()
    lax.fori_loop(0, heads, one_head, 0)
    for h in range(heads):
        o_own[:, h * head_dim:(h + 1) * head_dim] = o_scr[h]
    o_gather = Gather(lambda d: o_all.at[:, cols_of(d)], o_send, o_recv, where, own=o_own)
    o_gather.start()
    wo_gather.got_first()
    wo_gather.got_second()
    start_bulk(4)
    o_all[:, cols_of(me)] = o_own[...]

    def turn_out(k, _):
        rows = tok_of(k)
        ot_ref[:, rows] = o_own[rows, :].T
        return 0
    lax.fori_loop(0, 8, turn_out, 0)
    stores[3].start()
    wo_gather.got_diag()
    for i in range(4):
        wo_gather.got_partner(i)
    o_gather.got_first()
    o_gather.got_second()
    start_bulk(5, 6)
    o_gather.got_partner(0)
    o_gather.got_diag()
    for i in range(1, 4):
        o_gather.got_partner(i)
    start_bulk(7, 8, 9)

    def rows_at(i):
        flips = lambda a, b: other(0, a, b)
        return tok_of(jnp.where(i == 0, me, jnp.where(i == 1, flips(1, 0), jnp.where(i == 2, flips(0, 1), flips(1, 1)))))

    def give(i):
        slot = lax.rem(i, 2)
        rows = rows_at(i)
        return (pltpu.make_async_copy(m_out.at[slot], m_ref.at[rows, :], m_loc.at[slot]),
                pltpu.make_async_remote_copy(src_ref=m_out.at[slot], dst_ref=m_ref.at[rows, :], send_sem=m_send.at[i],
                                             recv_sem=m_recv.at[i], device_id=(partner,), device_id_type=MESH))

    def hidden_block(i, _):
        rows = rows_at(i)
        base = rows.start
        slot = lax.rem(i, 2)

        @pl.when(i >= 2)
        def _():
            to_hbm, to_partner = give(i - 2)
            to_hbm.wait()
            to_partner.wait_send()

        def chunk(j, _):
            cols = pl.ds(pl.multiple_of(j * 256, 256), 256)
            h_scr[:, cols] = dot(o_all[rows, :], wo_all[:, cols], 1, 0)
            return 0
        lax.fori_loop(0, model // 256, chunk, 0)

        def norm(k, _):
            part = pl.ds(pl.multiple_of(k * 16, 16), 16)
            x_part = x_all[pl.ds(pl.multiple_of(base + k * 16, 16), 16), :].astype(F32)
            hidden = (x_part + h_scr[part, :]).astype(BF16)

            @pl.when(i == 0)
            def _():
                h_ref[part, :] = hidden
            m_out[slot, part, :] = norm_forward(hidden.astype(F32), gfull_ref[1:2, :]).astype(BF16)
            return 0
        lax.fori_loop(0, tokens // 16, norm, 0)
        for copy in give(i):
            copy.start()
        return 0
    lax.fori_loop(0, 4, hidden_block, 0)
    stores[8].start()
    for i in range(4):
        give(i)[1].wait_recv()
    for i in range(2, 4):
        give(i)[0].wait()
        give(i)[1].wait_send()
    for copy in small + slices:
        copy.wait_send()
    for gather in (x_gather, wo_gather, o_gather):
        gather.drain()
    for copy in bulk:
        copy.wait()
    for load, store in local:
        store.wait()
    for copy in stores:
        copy.wait()


def attention_step(heads, x_in, positions, gain1, gain2, w_q, w_k, w_v, wo_own, w_gate, w_up):
    tokens, model = x_in.shape
    seq_len = 8 * tokens
    head_dim = wo_own.shape[0] // heads
    rows_own, hid = w_gate.shape[0], w_gate.shape[1] // 8
    shape = jax.ShapeDtypeStruct
    hbm, vmem = pl.BlockSpec(memory_space=pl.ANY), pl.BlockSpec(memory_space=pltpu.VMEM)
    dma = pltpu.SemaphoreType.DMA
    vm = lambda *dims, dtype=BF16: pltpu.VMEM(dims, dtype)
    steps = np.arange(head_dim // 2, dtype=np.float32) * np.float32(2.0 / head_dim)
    freq = np.tile(np.float32(1.0) / (np.float32(ROPE_BASE) ** steps), 4)[None]
    outs = (shape((heads, seq_len, head_dim), BF16), shape((seq_len, head_dim), BF16), shape((seq_len, head_dim), BF16),
            shape((heads * head_dim, seq_len), BF16), shape((rows_own, seq_len), BF16),
            shape((seq_len, 128), F32), shape((seq_len, 128), F32), shape((8, model), F32), shape((tokens, model), BF16))
    pairs = [dma((7,)), dma((7,)), dma((3, 7)), dma((3, 7)), dma((7,)), dma((7,)), dma((7,)), dma((7,)),
             dma((70,)), dma((70,)), dma((7,)), dma((7,))]
    return pl.pallas_call(
        functools.partial(attention_comm_kernel, 'sp', heads), name='attention_comm',
        in_specs=[hbm] + [vmem] * 4 + [hbm] * 6, out_specs=[hbm] * 12,
        out_shape=[*outs, shape((seq_len, model), BF16), shape((model, hid), BF16), shape((model, hid), BF16)],
        scratch_shapes=[vm(*t.shape, dtype=t.dtype) for t in outs] + [
            vm(8, rows_own, dtype=F32), vm(seq_len, model), vm(8, 8, rows_own, dtype=F32),
            vm(384, model), vm(model, model), vm(seq_len, model), vm(tokens, model), vm(tokens, 384), vm(heads, seq_len, head_dim),
            vm(seq_len, heads * head_dim), vm(tokens, model, dtype=F32), vm(2, tokens, model), vm(2, rows_own, hid)] + pairs + [
            dma((2,)), dma((4,)), dma((4,)), dma((4,)), dma((8,)), dma((9,))],
        compiler_params=pltpu.CompilerParams(collective_id=0, has_side_effects=True, vmem_limit_bytes=63 * 1024 * 1024),
    )(x_in, positions, gain1, gain2, jnp.asarray(freq), w_q, w_k, w_v, wo_own, w_gate, w_up)


def hand_over_kernel(n_far, n_near, *refs):
    n_in = n_far + n_near
    sources, gains, results = refs[:n_in], refs[n_in], refs[n_in + 1:2 * n_in + 1]
    gain_outs, stages = refs[2 * n_in + 1:2 * n_in + 3], refs[2 * n_in + 3:2 * n_in + 3 + n_far]
    in_sem, out_sem = refs[2 * n_in + 3 + n_far:]
    loads = [pltpu.make_async_copy(sources[i], stages[i], in_sem.at[i]) for i in range(n_far)]
    stores = [pltpu.make_async_copy(stages[i] if i < n_far else sources[i], results[i], out_sem.at[i]) for i in range(n_in)]
    for load in loads:
        load.start()
    for store in stores[n_far:]:
        store.start()
    for i in range(2):
        gain_outs[i][...] = gains[i, :]
    for load, store in zip(loads, stores):
        load.wait()
        store.start()
    for store in stores:
        store.wait()


def hand_over(far, near, gains):
    shape = jax.ShapeDtypeStruct
    arrays = far + near
    hbm, vmem = pl.BlockSpec(memory_space=pltpu.HBM), pl.BlockSpec(memory_space=pltpu.VMEM)
    dma = pltpu.SemaphoreType.DMA
    return pl.pallas_call(
        functools.partial(hand_over_kernel, len(far), len(near)), name='hand_over',
        in_specs=[hbm] * len(far) + [vmem] * (len(near) + 1), out_specs=[hbm] * len(arrays) + [vmem] * 2,
        out_shape=[shape(a.shape, a.dtype) for a in arrays] + [shape((gains.shape[1],), F32)] * 2,
        scratch_shapes=[pltpu.VMEM(a.shape, a.dtype) for a in far] + [dma((len(far),)), dma((len(arrays),))],
        compiler_params=pltpu.CompilerParams(vmem_limit_bytes=12 * 1024 * 1024),
    )(*[pltpu.with_memory_space_constraint(a, pltpu.HBM) for a in far],
      *[pltpu.with_memory_space_constraint(a, pltpu.VMEM) for a in near + (gains,)])


def solution(mesh):
    n_dev = mesh.shape['sp']

    def layer_step(x_in, positions, d_out, norm1_gain, norm2_gain, w_q, w_k, w_v, w_o, w_gate, w_up, w_down):
        tokens, model = x_in.shape
        head_dim = w_q.shape[2]
        heads = w_q.shape[1] // n_dev
        rows_own = w_q.shape[0]
        flat = lambda w: w.transpose(1, 2, 0).reshape(-1, rows_own)
        wo_own = w_o.reshape(-1, model)
        (q_rot, k_rot, v_lin, o_t, u_t, cos_tab, sin_tab, g_full, hidden,
         mlp_in, w1, w3) = attention_step(heads, x_in, positions, norm1_gain, norm2_gain, flat(w_q), flat(w_k), flat(w_v), wo_own, w_gate, w_up)
        d_w1s, d_w3s, d_down, y_out, dh_own, d_g2 = mlp_step(mlp_in, d_out, w1, w3, w_down, hidden, g_full)
        d_wo, d_wq_t, d_wk_t, d_wv_t, d_w1, d_w3, d_x, d_gains = attention_backward_step(
            heads, dh_own, wo_own, o_t, q_rot, k_rot, v_lin, (cos_tab, sin_tab),
            d_w1s, d_w3s, flat(w_q), flat(w_k), flat(w_v), u_t, x_in, g_full, d_g2)
        from_cols = lambda d, w: d.reshape(w.shape[1], w.shape[2], rows_own).transpose(2, 0, 1)
        (d_down, y_out, d_w1, d_w3, d_wo, d_wq_t, d_wk_t, d_wv_t, d_x, d_g1, d_g2) = hand_over(
            (d_down, y_out), (d_w1, d_w3, d_wo, d_wq_t, d_wk_t, d_wv_t, d_x), d_gains)
        return (y_out, d_x, d_g1, d_g2, from_cols(d_wq_t, w_q), from_cols(d_wk_t, w_k), from_cols(d_wv_t, w_v),
                d_wo.reshape(w_o.shape), d_w1, d_w3, d_down)

    all_rows = P('sp')
    return jax.shard_map(layer_step, mesh=mesh, in_specs=(all_rows,) * 12, out_specs=(all_rows,) * 11, check_vma=False)
```

```python
import functools
import jax
import jax.numpy as jnp
import numpy as np
from jax import lax
from jax.experimental import pallas as pl
from jax.experimental.pallas import tpu as pltpu
from jax.sharding import PartitionSpec as P

ROPE_BASE = 10000.0
NORM_EPS = 1e-5
NEG_LARGE = -1e30
F32 = jnp.float32
BF16 = jnp.bfloat16
BLK = 256


def dot(lhs, rhs, lhs_dim, rhs_dim):
    return lax.dot_general(lhs, rhs, (((lhs_dim,), (rhs_dim,)), ((), ())), preferred_element_type=F32)


def norm_forward(hidden, gain_vec):
    inv_rms = lax.rsqrt(jnp.mean(hidden * hidden, axis=-1, keepdims=True) + NORM_EPS)
    return hidden * inv_rms * gain_vec


def probs_transposed(k_rows, q_blk, start):
    scores = dot(k_rows, q_blk, 1, 1)
    rows = lax.broadcasted_iota(jnp.int32, (BLK, BLK), 0)
    cols = lax.broadcasted_iota(jnp.int32, (BLK, BLK), 1)
    tail = jnp.where(rows <= cols, scores[start:], NEG_LARGE)
    scores = jnp.concatenate([scores[:start], tail], axis=0) if start else tail
    top = jnp.max(scores, axis=0, keepdims=True)
    weights = jnp.exp((scores - top) * (q_blk.shape[1] ** -0.5))
    return weights * (1.0 / jnp.sum(weights, axis=0, keepdims=True))


MESH = pl.DeviceIdType.MESH


def place(axis):
    me = lax.axis_index(axis)
    core = lax.rem(me, 2)
    col = lax.rem(lax.div(me, 2), 2)
    row = lax.div(me, 4)

    def other(flip_core, flip_col, flip_row):
        pick = lambda v, f: 1 - v if f else v
        return pick(row, flip_row) * 4 + pick(col, flip_col) * 2 + pick(core, flip_core)

    nbr_x, nbr_y = other(0, 1, 0), other(0, 0, 1)
    first = nbr_x * (1 - core) + nbr_y * core
    second = nbr_y * (1 - core) + nbr_x * core
    return me, other, first, second


def greet(other):
    barrier = pltpu.get_barrier_semaphore()
    for r in range(1, 8):
        pl.semaphore_signal(barrier, inc=1, device_id=(other(r & 1, (r >> 1) & 1, r >> 2),), device_id_type=MESH)
    pl.semaphore_wait(barrier, 7)


class Gather:
    def __init__(self, slot, send_sem, recv_sem, where, seven, own=None):
        me, other, first, second = where
        partner, diag = other(1, 0, 0), other(0, 1, 1)
        own = slot(me) if own is None else own
        self.copies = []
        plan = [(own, me, first), (own, me, second), (own, me, partner), (slot(first), first, second),
                (slot(first), first, partner), (slot(second), second, partner), (slot(diag), diag, partner)]
        for i, (src, what, dest) in enumerate(plan):
            self.copies.append(pltpu.make_async_remote_copy(
                src_ref=src, dst_ref=slot(what), send_sem=send_sem.at[0], recv_sem=recv_sem.at[i],
                device_id=(dest,), device_id_type=MESH))
        self.sent = pltpu.make_async_remote_copy(
            src_ref=seven, dst_ref=seven, send_sem=send_sem.at[0], recv_sem=recv_sem.at[0],
            device_id=(partner,), device_id_type=MESH)

    def start(self):
        for i in range(3):
            self.copies[i].start()

    def got_first(self):
        self.copies[0].wait_recv()
        self.copies[3].start()
        self.copies[4].start()

    def got_second(self):
        self.copies[1].wait_recv()
        self.copies[5].start()

    def got_diag(self):
        self.copies[3].wait_recv()
        self.copies[6].start()

    def got_partner(self, i):
        self.copies[(2, 4, 5, 6)[i]].wait_recv()

    def drain(self):
        self.sent.wait_send()


def turn_halves(values, cos_blk, sin_blk):
    width = values.shape[1]
    lanes = lax.broadcasted_iota(jnp.int32, values.shape, 1)
    partner = jnp.where(lax.rem(lanes, 64) < 32, pltpu.roll(values, width - 32, 1), pltpu.roll(values, 32, 1))
    return values * cos_blk + partner * sin_blk


def norm_backward(hidden, gain, d_out):
    inv = lax.rsqrt(jnp.mean(hidden * hidden, axis=-1, keepdims=True) + NORM_EPS)
    d_scaled = d_out * gain
    d_hidden = d_scaled * inv - hidden * (inv * inv * inv * jnp.mean(d_scaled * hidden, axis=-1, keepdims=True))
    return d_hidden, jnp.sum(d_out * (hidden * inv), axis=0, keepdims=True)


def attn_bwd_comm_kernel(axis, heads, dh_hbm, wo_hbm, ot_hbm, q_hbm, k_hbm, v_hbm, cos_hbm, sin_hbm,
                         dw1_ref, dw3_ref, wq_hbm, wk_hbm, wv_hbm, ut_hbm, x_hbm, g_hbm, dg2_hbm, ddown_hbm, y_hbm,
                         dwo_ref, dwq_ref, dwk_ref, dwv_ref, out1_ref, out3_ref, dx_ref, dg_ref, ddown_ref, y_ref,
                         dh_own, wo_ref, ot_ref, q_ref, k_ref, v_ref, cos_ref, sin_ref, wq_ref, wk_ref, wv_ref, ut_ref, g_ref, dg2_ref,
                         pool, do_scr, dg_own, dg_all, dk_acc, dv_acc, du_acc,
                         bulk_send, bulk_recv, hg_send, hg_recv, gat_send, gat_recv, du_send, du_rsem, dg_send, dg_recv, loc_sem, ld_sem, credit):
    loads = {}
    for i, (name, src, dst) in enumerate((
            ('wo', wo_hbm, wo_ref), ('ot', ot_hbm, ot_ref), ('q', q_hbm, q_ref), ('k', k_hbm, k_ref),
            ('v', v_hbm, v_ref), ('cos', cos_hbm, cos_ref), ('sin', sin_hbm, sin_ref), ('wq', wq_hbm, wq_ref), ('wk', wk_hbm, wk_ref),
            ('wv', wv_hbm, wv_ref), ('ut', ut_hbm, ut_ref), ('g', g_hbm, g_ref), ('dg2', dg2_hbm, dg2_ref),
            ('dh', dh_hbm, dh_own), ('ddown', ddown_hbm, ddown_ref), ('y', y_hbm, y_ref))):
        loads[name] = pltpu.make_async_copy(src, dst, ld_sem.at[i])
        loads[name].start()

    def need(*names):
        for name in names:
            loads[name].wait()

    where = place(axis)
    me, other, first, second = where
    greet(other)
    seq_len, head_dim = k_ref.shape
    rows_own, hid = out1_ref.shape[0], dw1_ref.shape[1]
    tokens, model = x_hbm.shape
    qw = heads * head_dim

    rows_of = lambda d: pl.ds(pl.multiple_of(d * rows_own, rows_own), rows_own)
    hid_of = lambda d: pl.ds(pl.multiple_of(d * hid, hid), hid)
    pairs = ((dw1_ref, out1_ref), (dw3_ref, out3_ref))
    peers = [other(r & 1, (r >> 1) & 1, r >> 2) for r in (2, 4, 6, 3, 5, 7, 1)]
    bulk, parts = [], []
    for mat, (src, dst) in enumerate(pairs):
        for low, high in ((0, 8), (8, rows_own // 2), (rows_own // 2, rows_own)):
            parts.append(range(len(bulk), len(bulk) + len(peers)))
            for dest in peers:
                bulk.append(pltpu.make_async_remote_copy(
                    src_ref=src.at[pl.ds(pl.multiple_of(dest * rows_own + low, 8), high - low), :],
                    dst_ref=dst.at[pl.ds(low, high - low), hid_of(me)], send_sem=bulk_send.at[mat],
                    recv_sem=bulk_recv.at[mat], device_id=(dest,), device_id_type=MESH))

    def start_bulk(*which):
        for part in which:
            for i in parts[part]:
                bulk[i].start()
    tok_of = lambda d: pl.ds(pl.multiple_of(d * tokens, tokens), tokens)
    dh_ref = pool.at[:, 0:model]
    h_gather = Gather(lambda d: dh_ref.at[tok_of(d), :], hg_send, hg_recv, where, dh_ref.at[pl.ds(0, 7 * tokens), :], own=dh_hbm)
    h_gather.start()
    start_bulk(0)
    local = [pltpu.make_async_copy(src.at[rows_of(me), :], dst.at[:, hid_of(me)], loc_sem.at[i]) for i, (src, dst) in enumerate(pairs)]
    for copy in local:
        copy.start()
    need('dh', 'wo', 'ot')
    pool[tok_of(me), 0:model] = dh_own[...]
    h_gather.got_first()
    h_gather.got_second()
    start_bulk(1, 2)
    h_gather.got_diag()
    for i in range(4):
        h_gather.got_partner(i)

    def split_out_grad(k, _):
        rows = pl.ds(pl.multiple_of(k * BLK, BLK), BLK)
        do_blk = dot(pool[rows, 0:model], wo_ref[...], 1, 1).astype(BF16)
        for h in range(heads):
            do_scr[h, rows, :] = do_blk[:, h * head_dim:(h + 1) * head_dim]
        cols = rows
        dwo_ref[:, cols] = dot(ot_ref[...], pool[:, cols], 1, 0)
        return 0
    lax.fori_loop(0, seq_len // BLK, split_out_grad, 0)
    h_gather.drain()
    for i, device in enumerate((first, second, other(1, 0, 0))):
        pl.semaphore_signal(credit.at[i], inc=1, device_id=(device,), device_id_type=MESH)
    x_ref = wo_ref
    x_load = pltpu.make_async_copy(x_hbm, x_ref, ld_sem.at[16])
    x_load.start()


    need('q', 'k', 'v')
    dk_acc[...] = jnp.zeros_like(dk_acc)
    dv_acc[...] = jnp.zeros_like(dv_acc)
    slot_cols = lambda d, off, width: pl.ds(pl.multiple_of(d * 384 + off, 128), width)

    def one_head(h, _):
        def one_block(start):
            keys = pl.ds(0, start + BLK)
            rows = pl.ds(start, BLK)
            q_blk, do_blk = q_ref[h, rows, :], do_scr[h, rows, :]
            probs = probs_transposed(k_ref[keys, :], q_blk, start)
            d_probs = dot(v_ref[keys, :], do_blk, 1, 1).astype(BF16).astype(F32)
            row_dot = jnp.sum(d_probs * probs, axis=0, keepdims=True)
            d_scores = (probs * (d_probs - row_dot) * (head_dim ** -0.5)).astype(BF16)
            do_scr[h, rows, :] = dot(d_scores, k_ref[keys, :], 0, 0).astype(BF16)
            dk_acc[keys, :] += dot(d_scores, q_blk, 1, 0)
            dv_acc[keys, :] += dot(probs.astype(BF16), do_blk, 1, 0)
        for start in range(0, seq_len, BLK):
            one_block(start)
        return 0
    lax.fori_loop(0, heads, one_head, 0)
    need('cos', 'sin')
    low = lax.broadcasted_iota(jnp.int32, (BLK, 128), 1) < head_dim

    def turn_back(k, _):
        rows = pl.ds(pl.multiple_of(k * BLK, BLK), BLK)
        cos_blk, sin_blk = cos_ref[rows, :], -sin_ref[rows, :]
        for pair in range(heads // 2):
            both = jnp.concatenate([do_scr[2 * pair, rows, :], do_scr[2 * pair + 1, rows, :]], axis=1)
            pool[rows, slot_cols(me, pair * 128, 128)] = turn_halves(both.astype(F32), cos_blk, sin_blk).astype(BF16)
        kv = jnp.concatenate([dk_acc[rows, :], dv_acc[rows, :]], axis=1).astype(BF16).astype(F32)
        pool[rows, slot_cols(me, qw, 128)] = jnp.where(low, turn_halves(kv, cos_blk, sin_blk), kv).astype(BF16)
        return 0
    lax.fori_loop(0, seq_len // BLK, turn_back, 0)

    gather = Gather(lambda d: pool.at[:, slot_cols(d, 0, 384)], gat_send, gat_recv, where, pool.at[:, pl.ds(0, 7 * 384)])
    for i in range(3):
        pl.semaphore_wait(credit.at[i], 1)
    gather.start()
    start_bulk(3)
    du_acc[...] = jnp.zeros_like(du_acc)
    need('wq', 'wk', 'wv', 'ut')

    def use(d):
        q_rows = pl.ds(pl.multiple_of(d * qw, qw), qw)
        kv_rows = pl.ds(pl.multiple_of(d * head_dim, head_dim), head_dim)
        w_all = jnp.concatenate([wq_ref[q_rows, :], wk_ref[kv_rows, :], wv_ref[kv_rows, :]], axis=0)

        def add_rows(k, _):
            rows = pl.ds(pl.multiple_of(k * 512, 512), 512)
            du_acc[rows, :] += dot(pool[rows, slot_cols(d, 0, 384)], w_all, 1, 0)
            return 0
        lax.fori_loop(0, seq_len // 512, add_rows, 0)
        d_w = dot(ut_ref[...], pool[:, slot_cols(d, 0, 384)], 1, 0).T
        dwq_ref[q_rows, :] = d_w[:qw]
        dwk_ref[kv_rows, :] = d_w[qw:qw + head_dim]
        dwv_ref[kv_rows, :] = d_w[qw + head_dim:]

    def use_many(*devices):
        def body(i, _):
            d = devices[0]
            for n in range(1, len(devices)):
                d = jnp.where(i == n, devices[n], d)
            use(d)
            return 0
        lax.fori_loop(0, len(devices), body, 0)

    use_many(me)
    gather.got_first()
    gather.got_second()
    start_bulk(4)
    gather.got_partner(0)
    use_many(first, second, other(1, 0, 0))
    gather.got_diag()
    for i in range(1, 4):
        gather.got_partner(i)
    use_many(other(0, 1, 1), other(1, 1, 0), other(1, 0, 1), other(1, 1, 1))
    gather.drain()
    du_scr = pool.at[:, 0:rows_own]

    def round_du(k, _):
        rows = pl.ds(pl.multiple_of(k * BLK, BLK), BLK)
        pool[rows, 0:rows_own] = du_acc[rows, :].astype(BF16)
        return 0
    lax.fori_loop(0, seq_len // BLK, round_du, 0)
    for dest in peers:
        pltpu.make_async_remote_copy(
            src_ref=du_scr.at[tok_of(dest), :], dst_ref=ot_ref.at[:, rows_of(me)], send_sem=du_send.at[0],
            recv_sem=du_rsem.at[0], device_id=(dest,), device_id_type=MESH).start()
    start_bulk(5)
    ot_ref[:, rows_of(me)] = pool[tok_of(me), 0:rows_own]
    need('g', 'dg2')
    x_load.wait()
    got = ot_ref.at[:, pl.ds(0, 7 * rows_own)]
    pltpu.make_async_copy(got, got, du_rsem.at[0]).wait()
    dg_own[...] = jnp.zeros_like(dg_own)
    dg_own[1:2, :] = dg2_ref[...]

    def input_grad(k, _):
        part = pl.ds(pl.multiple_of(k * 16, 16), 16)
        d_norm, d_gain = norm_backward(x_ref[part, :].astype(F32), g_ref[0:1, :], ot_ref[part, :].astype(F32))
        dh_part = dh_own[part, :]
        dx_ref[part, :] = (dh_part.astype(F32) + d_norm).astype(BF16)
        dg_own[0:1, :] += d_gain
        return 0
    lax.fori_loop(0, tokens // 16, input_grad, 0)
    for dest in peers:
        pltpu.make_async_remote_copy(
            src_ref=dg_own.at[:, rows_of(dest)], dst_ref=dg_all.at[me], send_sem=dg_send.at[0],
            recv_sem=dg_recv.at[0], device_id=(dest,), device_id_type=MESH).start()
    dg_all[me] = dg_own[:, rows_of(me)]
    got = dg_all.at[pl.ds(0, 7)]
    pltpu.make_async_copy(got, got, dg_recv.at[0]).wait()
    dg_ref[...] = jnp.sum(dg_all[...], axis=0)
    for sent, sem in ((du_scr.at[pl.ds(0, 7 * tokens), :], du_send), (dg_own.at[:, pl.ds(0, 7 * rows_own)], dg_send)):
        pltpu.make_async_copy(sent, sent, sem.at[0]).wait()
    need('ddown', 'y')
    for mat, (src, dst) in enumerate(pairs):
        sent, got = src.at[pl.ds(0, 7 * rows_own), :], dst.at[:, pl.ds(0, 7 * hid)]
        pltpu.make_async_copy(sent, sent, bulk_send.at[mat]).wait()
        pltpu.make_async_copy(got, got, bulk_recv.at[mat]).wait()
    for copy in local:
        copy.wait()


def attention_backward_step(heads, dh_own, wo_own, o_t, q_rot, k_rot, v_lin, tables, d_w1, d_w3, w_q, w_k, w_v, u_t, x_in, gains, d_g2, d_down, y_out):
    seq_len, model = k_rot.shape[0], x_in.shape[1]
    head_dim = k_rot.shape[1]
    tokens = x_in.shape[0]
    rows_own, hid = model // 8, d_w1.shape[1]
    shape = jax.ShapeDtypeStruct
    hbm = pl.BlockSpec(memory_space=pl.ANY)
    dma = pltpu.SemaphoreType.DMA
    vm = lambda *dims, dtype=BF16: pltpu.VMEM(dims, dtype)
    early = (dh_own, wo_own, o_t, q_rot, k_rot, v_lin, *tables)
    late = (w_q, w_k, w_v, u_t, x_in, gains, d_g2)
    outs = [(wo_own.shape, F32), (w_q.shape, F32), (w_k.shape, F32), (w_v.shape, F32), ((rows_own, 8 * hid), F32),
            ((rows_own, 8 * hid), F32), (x_in.shape, BF16), ((8, rows_own), F32), (d_down.shape, F32), (y_out.shape, BF16)]
    vmem, far = pl.BlockSpec(memory_space=pltpu.VMEM), pl.BlockSpec(memory_space=pltpu.HBM)
    return pl.pallas_call(
        functools.partial(attn_bwd_comm_kernel, 'sp', heads), name='attn_bwd_comm',
        in_specs=[hbm] * 17 + [far] * 2, out_specs=[vmem] * 10,
        out_shape=[pltpu.VMEM(dims, dtype) for dims, dtype in outs],
        scratch_shapes=[vm(*t.shape, dtype=t.dtype) for t in early + late[:4] + late[5:]] + [
            vm(seq_len, 8 * 384), vm(heads, seq_len, head_dim),
            vm(8, model, dtype=F32), vm(8, 8, rows_own, dtype=F32),
            vm(seq_len, head_dim, dtype=F32), vm(seq_len, head_dim, dtype=F32),
            vm(seq_len, rows_own, dtype=F32),
            dma((2,)), dma((2,)), dma((1,)), dma((7,)), dma((1,)), dma((7,)), dma((1,)), dma((1,)), dma((1,)), dma((1,)), dma((2,)), dma((17,)), pltpu.SemaphoreType.REGULAR((3,))],
        compiler_params=pltpu.CompilerParams(collective_id=2, has_side_effects=True, vmem_limit_bytes=34340864),
    )(*early, d_w1, d_w3, *late, *[pltpu.with_memory_space_constraint(a, pltpu.HBM) for a in (d_down, y_out)])


def mlp_comm_kernel(axis, m_ref, dout_own, w1_hbm, w3_hbm, w2_hbm, h_hbm, g_hbm,
                    dw1_ref, dw3_ref, dw2_ref, y_hbm, dh_hbm, dg2_hbm, dout_ref,
                    w1_ref, w3_ref, w2_ref, h_ref, g_ref, y_ref, dg2_ref,
                    glu, gate_s, up_s, outbox, chip_sum, inbox, blk, m_col, do_col, mt_scr, dot_scr, st1, st3, st2, dh_own,
                    part_send, part_recv, mail_send, mail_recv, do_send, do_recv,
                    in_sem, col_sem, out_sem, own_sem, ld_sem, credit):
    loads = [pltpu.make_async_copy(src, dst, ld_sem.at[i]) for i, (src, dst) in enumerate((
        (w1_hbm, w1_ref), (w3_hbm, w3_ref), (w2_hbm, w2_ref), (h_hbm, h_ref), (g_hbm, g_ref)))]
    own_in = pltpu.make_async_copy(dout_own, dh_own, own_sem.at[0])
    for copy in loads + [own_in]:
        copy.start()
    where = place(axis)
    me, other, first, second = where
    core = lax.rem(me, 2)
    partner = other(1, 0, 0)
    tokens, model = h_ref.shape
    hid = w1_ref.shape[1]
    tok_of = lambda d: pl.ds(pl.multiple_of(d * tokens, tokens), tokens)
    off_first, off_second = 1 + core, 2 - core

    def block_of(off, flip):
        d_col, d_row = lax.rem(off, 2), lax.div(off, 2)
        col, row = lax.rem(lax.div(me, 2), 2), lax.div(me, 4)
        mix = lambda v, f: v + f - 2 * v * f
        return mix(row, d_row) * 4 + mix(col, d_col) * 2 + mix(core, flip)

    def step_off(step, flip):
        mid_a = off_second * (1 - flip) + off_first * flip
        mid_b = off_first * (1 - flip) + off_second * flip
        return jnp.where(step == 0, 3, jnp.where(step == 1, mid_a, jnp.where(step == 2, mid_b, 0)))

    def half_rows(half):
        flip = 1 - lax.rem(half, 2)
        return tok_of(block_of(step_off(lax.div(half, 2), flip), flip))

    def fetch(half):
        slot = lax.rem(half, 2)
        return pltpu.make_async_copy(m_ref.at[half_rows(half), :], blk.at[slot], in_sem.at[slot])

    def fetch_dout(d):
        slot = lax.rem(d, 2)
        return pltpu.make_async_copy(dout_ref.at[tok_of(d), :], blk.at[slot], in_sem.at[slot])

    def fetch_cols(j):
        cols = pl.ds(pl.multiple_of(j * 256, 256), 256)
        return (pltpu.make_async_copy(m_ref.at[:, cols], m_col, col_sem.at[0]),
                pltpu.make_async_copy(dout_ref.at[:, cols], do_col, col_sem.at[1]))

    def sigmoid(value):
        return 1.0 / (1.0 + jnp.exp(-value))

    def activations(slot, rows):
        def chunk(j, _):
            cols = pl.ds(pl.multiple_of(j * 512, 512), 512)
            gate = dot(blk[slot], w1_ref[:, cols], 1, 0).astype(BF16)
            up = dot(blk[slot], w3_ref[:, cols], 1, 0).astype(BF16)
            gate_s[rows, cols] = gate
            up_s[rows, cols] = up
            gate = gate.astype(F32)
            glu[rows, cols] = (gate * sigmoid(gate) * up.astype(F32)).astype(BF16)
            return 0
        lax.fori_loop(0, hid // 512, chunk, 0)

    def activation_grads(slot, rows):
        def chunk(j, _):
            cols = pl.ds(pl.multiple_of(j * 512, 512), 512)
            d_act = dot(blk[slot], w2_ref[cols, :], 1, 1).astype(BF16).astype(F32)
            gate, up = gate_s[rows, cols].astype(F32), up_s[rows, cols].astype(F32)
            sig = sigmoid(gate)
            silu = gate * sig
            up_s[rows, cols] = (d_act * silu).astype(BF16)
            gate_s[rows, cols] = (d_act * up * (sig + silu * (1.0 - sig))).astype(BF16)
            return 0
        lax.fori_loop(0, hid // 512, chunk, 0)

    def add_mlp_grad(rows, put):
        def chunk(j, _):
            cols = pl.ds(pl.multiple_of(j * 512, 512), 512)
            put(cols, dot(gate_s[rows, :], w1_ref[cols, :], 1, 1) + dot(up_s[rows, :], w3_ref[cols, :], 1, 1))
            return 0
        lax.fori_loop(0, model // 512, chunk, 0)

    def add_mlp_out(rows, put):
        def chunk(j, _):
            cols = pl.ds(pl.multiple_of(j * 512, 512), 512)
            put(cols, dot(glu[rows, :], w2_ref[:, cols], 1, 0))
            return 0
        lax.fori_loop(0, model // 512, chunk, 0)

    def signal(index, device):
        pl.semaphore_signal(credit.at[index], inc=1, device_id=(device,), device_id_type=MESH)

    class Scatter:
        def __init__(self, turn):
            self.turn = turn

        def to_partner(self, step):
            off = step_off(step, 1)
            return pltpu.make_async_remote_copy(
                src_ref=outbox.at[lax.rem(step, 2)], dst_ref=chip_sum.at[off], send_sem=part_send.at[self.turn, step],
                recv_sem=part_recv.at[self.turn, off], device_id=(partner,), device_id_type=MESH)

        def from_partner(self, off):
            return pltpu.make_async_remote_copy(
                src_ref=outbox.at[0], dst_ref=chip_sum.at[off], send_sem=part_send.at[self.turn, 0],
                recv_sem=part_recv.at[self.turn, off], device_id=(partner,), device_id_type=MESH)

        def mail(self, kind):
            off = (3, off_first, off_second)[kind]
            dest = (first, first, second)[kind]
            return pltpu.make_async_remote_copy(
                src_ref=chip_sum.at[off], dst_ref=inbox.at[kind], send_sem=mail_send.at[self.turn, kind],
                recv_sem=mail_recv.at[self.turn, kind], device_id=(dest,), device_id_type=MESH)

        def step(self, step, prepare, partial):
            self.first_half(step, prepare, partial)
            self.second_half(step, prepare, partial)

        def first_half(self, step, prepare, partial):
            slot = lax.rem(step, 2)
            prepare(2 * step)

            def put_out(cols, value):
                outbox[slot, :, cols] = value
            partial(half_rows(2 * step), put_out)

        def second_half(self, step, prepare, partial):
            self.to_partner(step).start()
            prepare(2 * step + 1)
            off = step_off(step, 0)
            self.from_partner(off).wait_recv()

            def put_sum(cols, value):
                chip_sum[off, :, cols] += value
            partial(half_rows(2 * step + 1), put_sum)

        def pass_on(self):
            self.mail(0).wait_recv()

            def add_mail(k, _):
                part = pl.ds(pl.multiple_of(k * 16, 16), 16)
                chip_sum[off_second, part, :] += inbox[0, part, :]
                return 0
            lax.fori_loop(0, tokens // 16, add_mail, 0)

    out_round, grad_round = Scatter(0), Scatter(1)

    def prepare_out(half):
        @pl.when(half < 7)
        def _():
            fetch(half + 1).start()
        fetch(half).wait()
        activations(lax.rem(half, 2), half_rows(half))

    def weight_grads(begin, end):
        for copy in fetch_cols(begin):
            copy.start()

        def body(j, _):
            for copy in fetch_cols(j):
                copy.wait()

            def turn(k, _):
                part = pl.ds(pl.multiple_of(k * 256, 256), 256)
                mt_scr[:, part] = m_col[part, :].T
                dot_scr[:, part] = do_col[part, :].T
                return 0
            lax.fori_loop(0, m_col.shape[0] // 256, turn, 0)

            @pl.when(j + 1 < end)
            def _():
                for copy in fetch_cols(j + 1):
                    copy.start()
            rows = pl.ds(pl.multiple_of(j * 256, 256), 256)
            out = (pltpu.make_async_copy(st1, dw1_ref.at[rows, :], out_sem.at[0]),
                   pltpu.make_async_copy(st3, dw3_ref.at[rows, :], out_sem.at[1]),
                   pltpu.make_async_copy(st2, dw2_ref.at[:, rows], out_sem.at[2]))

            @pl.when(j > begin)
            def _():
                for copy in out:
                    copy.wait()

            def chunk(k, _):
                cols = pl.ds(pl.multiple_of(k * 512, 512), 512)
                st1[:, cols] = dot(mt_scr[...], gate_s[:, cols], 1, 0)
                st3[:, cols] = dot(mt_scr[...], up_s[:, cols], 1, 0)
                st2[cols, :] = dot(dot_scr[...], glu[:, cols], 1, 0).T
                return 0
            lax.fori_loop(0, hid // 512, chunk, 0)
            for copy in out:
                copy.start()
            return 0
        lax.fori_loop(begin, end, body, 0)
        rows = pl.ds((end - 1) * 256, 256)
        for copy in (pltpu.make_async_copy(st1, dw1_ref.at[rows, :], out_sem.at[0]),
                     pltpu.make_async_copy(st3, dw3_ref.at[rows, :], out_sem.at[1]),
                     pltpu.make_async_copy(st2, dw2_ref.at[:, rows], out_sem.at[2])):
            copy.wait()

    fetch(0).start()
    greet(other)
    do_gather = Gather(lambda d: dout_ref.at[tok_of(d), :], do_send, do_recv, where, dout_ref.at[pl.ds(0, 7 * tokens), :], own=dout_own)
    do_gather.start()
    own_in.wait()
    own_out = pltpu.make_async_copy(dh_own, dout_ref.at[tok_of(me), :], own_sem.at[1])
    own_out.start()
    for copy in loads:
        copy.wait()

    def out_step(step, _):
        @pl.when(step >= 2)
        def _():
            out_round.to_partner(step - 2).wait_send()
        out_round.step(step, prepare_out, add_mlp_out)

        @pl.when(step == 0)
        def _():
            out_round.mail(0).start()

        @pl.when(step == 2)
        def _():
            out_round.mail(1).start()
            do_gather.got_first()
            do_gather.got_second()
        return 0
    lax.fori_loop(0, 4, out_step, 0)
    out_round.pass_on()
    out_round.mail(2).start()
    for step in (2, 3):
        out_round.to_partner(step).wait_send()
    out_round.mail(0).wait_send()
    signal(0, partner)
    signal(1, first)
    do_gather.got_diag()
    for i in range(4):
        do_gather.got_partner(i)
    own_out.wait()
    fetch_dout(0).start()

    def grad_block(d, _):
        @pl.when(d < 7)
        def _():
            fetch_dout(d + 1).start()
        fetch_dout(d).wait()
        activation_grads(lax.rem(d, 2), tok_of(d))
        return 0
    lax.fori_loop(0, 8, grad_block, 0)

    as_is = lambda half: None
    grad_round.first_half(0, as_is, add_mlp_grad)
    pl.semaphore_wait(credit.at[0], 1)
    grad_round.second_half(0, as_is, add_mlp_grad)
    pl.semaphore_wait(credit.at[1], 1)
    grad_round.mail(0).start()
    weight_grads(0, 2)
    grad_round.first_half(1, as_is, add_mlp_grad)
    out_round.mail(1).wait_recv()
    out_round.mail(2).wait_recv()

    def layer_out(k, _):
        part = pl.ds(pl.multiple_of(k * 16, 16), 16)
        y_ref[part, :] = (h_ref[part, :].astype(F32) + (chip_sum[0, part, :] + inbox[1, part, :] + inbox[2, part, :])).astype(BF16)
        return 0
    lax.fori_loop(0, tokens // 16, layer_out, 0)
    y_store = pltpu.make_async_copy(y_ref, y_hbm, own_sem.at[2])
    y_store.start()
    out_round.mail(1).wait_send()
    out_round.mail(2).wait_send()
    signal(2, partner)
    signal(3, first)
    signal(4, second)
    pl.semaphore_wait(credit.at[2], 1)

    grad_round.second_half(1, as_is, add_mlp_grad)

    def grad_step(step, _):
        grad_round.to_partner(step - 2).wait_send()
        grad_round.step(step, as_is, add_mlp_grad)

        @pl.when(step == 2)
        def _():
            pl.semaphore_wait(credit.at[3], 1)
            grad_round.mail(1).start()
            grad_round.pass_on()
            pl.semaphore_wait(credit.at[4], 1)
            grad_round.mail(2).start()
        return 0
    lax.fori_loop(2, 4, grad_step, 0)
    weight_grads(2, 8)
    grad_round.mail(1).wait_recv()
    grad_round.mail(2).wait_recv()
    dg2_ref[...] = jnp.zeros_like(dg2_ref)

    def hidden_grad(k, _):
        part = pl.ds(pl.multiple_of(k * 16, 16), 16)
        d_mlp = (chip_sum[0, part, :] + inbox[1, part, :] + inbox[2, part, :]).astype(BF16).astype(F32)
        d_norm, d_gain = norm_backward(h_ref[part, :].astype(F32), g_ref[1:2, :], d_mlp)
        dh_own[part, :] = (dh_own[part, :].astype(F32) + d_norm).astype(BF16)
        dg2_ref[...] += d_gain
        return 0
    lax.fori_loop(0, tokens // 16, hidden_grad, 0)
    own_out = pltpu.make_async_copy(dh_own, dh_hbm, own_sem.at[3])
    own_out.start()
    dg2_store = pltpu.make_async_copy(dg2_ref, dg2_hbm, own_sem.at[4])
    dg2_store.start()
    for step in (2, 3):
        grad_round.to_partner(step).wait_send()
    for kind in range(3):
        grad_round.mail(kind).wait_send()
    do_gather.drain()
    own_out.wait()
    y_store.wait()
    dg2_store.wait()


def mlp_step(m_all, d_out, w1, w3, w2, hidden, gains):
    seq_len, model = m_all.shape
    hid, tokens = w1.shape[1], hidden.shape[0]
    shape = jax.ShapeDtypeStruct
    hbm = pl.BlockSpec(memory_space=pl.ANY)
    dma = pltpu.SemaphoreType.DMA
    vm = lambda *dims, dtype=BF16: pltpu.VMEM(dims, dtype)
    return pl.pallas_call(
        functools.partial(mlp_comm_kernel, 'sp'), name='mlp_comm',
        in_specs=[hbm] * 7, out_specs=[hbm] * 7,
        out_shape=[shape((model, hid), F32), shape((model, hid), F32), shape((hid, model), F32),
                   shape(hidden.shape, BF16), shape(hidden.shape, BF16), shape((1, model), F32), shape((seq_len, model), BF16)],
        scratch_shapes=[vm(*t.shape, dtype=t.dtype) for t in (w1, w3, w2, hidden, gains)] + [
            vm(tokens, model), vm(1, model, dtype=F32),
            vm(seq_len, hid), vm(seq_len, hid), vm(seq_len, hid),
            vm(2, tokens, model, dtype=F32), vm(4, tokens, model, dtype=F32), vm(3, tokens, model, dtype=F32),
            vm(2, tokens, model), vm(seq_len, 256), vm(seq_len, 256), vm(256, seq_len), vm(256, seq_len),
            vm(256, hid, dtype=F32), vm(256, hid, dtype=F32), vm(hid, 256, dtype=F32), vm(tokens, model),
            dma((2, 4)), dma((2, 4)), dma((2, 3)), dma((2, 3)), dma((1,)), dma((7,)),
            dma((2,)), dma((2,)), dma((3,)), dma((5,)), dma((5,)), pltpu.SemaphoreType.REGULAR((5,))],
        compiler_params=pltpu.CompilerParams(collective_id=1, has_side_effects=True, vmem_limit_bytes=63 * 1024 * 1024),
    )(m_all, d_out, w1, w3, w2, hidden, gains)[:6]


def spread_tables(packed, upper):
    lanes = lax.broadcasted_iota(jnp.int32, packed.shape, 1)
    swapped = pltpu.roll(packed, 64, 1)
    both = jnp.where((lanes < 64) != upper, packed, swapped)
    low = lax.rem(lanes, 64) < 32
    return jnp.where(low, both, pltpu.roll(both, 32, 1)), jnp.where(low, -pltpu.roll(both, 96, 1), both)


def attention_comm_kernel(axis, heads, x_ref, pos_ref, gain1_ref, gain2_ref, freq_ref, wq_ref, wk_ref, wv_ref, wo_ref, wg_ref, wu_ref,
                          q_hbm, k_hbm, v_hbm, ot_hbm, ut_hbm, cos_hbm, sin_hbm, gfull_hbm, h_hbm, m_ref, w1_ref, w3_ref,
                          q_ref, k_ref, v_ref, ot_ref, ut_ref, cos_ref, sin_ref, gfull_ref, h_ref, gain_ref, x_all, gain_all, w_head, wo_all, o_all, u_blk, qkv_blk, o_scr, o_own, h_scr, m_out, stage,
                          g_send, g_recv, w_send, w_recv, x_send, x_recv, wo_send, wo_recv, bulk_send, bulk_recv,
                          o_send, o_recv, m_loc, m_send, m_recv, loc_sem, own_sem, st_sem):
    gain_ref[...] = jnp.zeros_like(gain_ref)
    gain_ref[0:1, :] = gain1_ref[...].astype(F32).reshape(1, -1)
    gain_ref[1:2, :] = gain2_ref[...].astype(F32).reshape(1, -1)
    gain_ref[2:3, :] = pos_ref[...].astype(F32).reshape(1, -1)
    where = place(axis)
    me, other, first, second = where
    core = lax.rem(me, 2)
    partner = other(1, 0, 0)
    greet(other)
    tokens, model = x_ref.shape
    seq_len, head_dim = k_ref.shape
    qw = heads * head_dim
    rows_own, hid = wg_ref.shape[0], w1_ref.shape[1]
    tok_of = lambda d: pl.ds(pl.multiple_of(d * tokens, tokens), tokens)
    cols_of = lambda d: pl.ds(pl.multiple_of(d * rows_own, rows_own), rows_own)
    hid_of = lambda d: pl.ds(pl.multiple_of(d * hid, hid), hid)
    peers = [other(r & 1, (r >> 1) & 1, r >> 2) for r in (6, 2, 4, 7, 3, 5, 1)]

    def to_all(src_of, dst, seven, sems):
        copies = [pltpu.make_async_remote_copy(
            src_ref=src_of(dest), dst_ref=dst, send_sem=sems[0], recv_sem=sems[1],
            device_id=(dest,), device_id_type=MESH) for dest in peers]
        for copy in copies:
            copy.start()
        return pltpu.make_async_remote_copy(src_ref=seven, dst_ref=seven, send_sem=sems[0], recv_sem=sems[1],
                                            device_id=(partner,), device_id_type=MESH)

    q_of = lambda d: pl.ds(pl.multiple_of(d * qw, qw), qw)
    kv_of = lambda d: pl.ds(pl.multiple_of(d * head_dim, head_dim), head_dim)
    seven_rows = pl.ds(0, 7 * rows_own)
    small = [to_all(lambda dest: gain_ref, gain_all.at[me], gain_all.at[pl.ds(0, 7)], (g_send.at[0], g_recv.at[0]))]
    slices = []
    for i, (src, rows, low, high) in enumerate(((wq_ref, q_of, 0, qw), (wk_ref, kv_of, qw, qw + head_dim),
                                                (wv_ref, kv_of, qw + head_dim, qw + 2 * head_dim))):
        slices.append(to_all(lambda dest: src.at[rows(dest), :], w_head.at[low:high, cols_of(me)],
                             w_head.at[low:high, seven_rows], (w_send.at[i], w_recv.at[i])))
    x_gather = Gather(lambda d: x_all.at[tok_of(d), :], x_send, x_recv, where, x_all.at[pl.ds(0, 7 * tokens), :], own=x_ref)
    x_gather.start()
    wo_gather = Gather(lambda d: wo_all.at[cols_of(d), :], wo_send, wo_recv, where, wo_all.at[pl.ds(0, 7 * rows_own), :], own=wo_ref)
    bulk, parts = [], []
    quarter = rows_own // 4
    for mat, (src, dst) in enumerate(((wg_ref, w1_ref), (wu_ref, w3_ref))):
        for low, high in ((0, 16), (16, quarter), (quarter, 2 * quarter), (2 * quarter, 3 * quarter), (3 * quarter, rows_own)):
            parts.append(range(len(bulk), len(bulk) + len(peers)))
            for dest in peers:
                bulk.append(pltpu.make_async_remote_copy(
                    src_ref=src.at[pl.ds(low, high - low), hid_of(dest)],
                    dst_ref=dst.at[pl.ds(pl.multiple_of(me * rows_own + low, 16), high - low), :],
                    send_sem=bulk_send.at[mat], recv_sem=bulk_recv.at[mat], device_id=(dest,), device_id_type=MESH))

    def start_bulk(*which):
        for part in which:
            for i in parts[part]:
                bulk[i].start()
    start_bulk(0)

    stores = [pltpu.make_async_copy(src, dst, st_sem.at[i]) for i, (src, dst) in enumerate((
        (q_ref, q_hbm), (k_ref, k_hbm), (v_ref, v_hbm), (ot_ref, ot_hbm), (ut_ref, ut_hbm), (cos_ref, cos_hbm),
        (sin_ref, sin_hbm), (gfull_ref, gfull_hbm), (h_ref, h_hbm)))]
    own = [pltpu.make_async_copy(src, dst, own_sem.at[i]) for i, (src, dst) in enumerate((
        (gain_ref, gain_all.at[me]), (wq_ref.at[q_of(me), :], w_head.at[0:qw, cols_of(me)]),
        (wk_ref.at[kv_of(me), :], w_head.at[qw:qw + head_dim, cols_of(me)]),
        (wv_ref.at[kv_of(me), :], w_head.at[qw + head_dim:, cols_of(me)]),
        (x_ref, x_all.at[tok_of(me), :]), (wo_ref, wo_all.at[cols_of(me), :])))]
    for copy in own:
        copy.start()
    local = []
    for i, (src, dst) in enumerate(((wg_ref, w1_ref), (wu_ref, w3_ref))):
        local.append((pltpu.make_async_copy(src.at[:, hid_of(me)], stage.at[i], loc_sem.at[i]),
                      pltpu.make_async_copy(stage.at[i], dst.at[cols_of(me), :], loc_sem.at[2 + i])))
        local[-1][0].start()
    for load, store in local:
        load.wait()
        store.start()
    for copy in own:
        copy.wait()
    for copy in small:
        copy.wait_recv()
    for d in range(8):
        gfull_ref[:, d * rows_own:(d + 1) * rows_own] = gain_all[d]
    for copy in slices:
        copy.wait_recv()

    def use(d):
        base = pl.multiple_of(d * tokens, tokens)

        def norm(k, _):
            part = pl.ds(pl.multiple_of(k * 16, 16), 16)
            x_part = x_all[pl.ds(pl.multiple_of(base + k * 16, 16), 16), :].astype(F32)
            u_blk[part, :] = norm_forward(x_part, gfull_ref[0:1, :]).astype(BF16)
            return 0
        lax.fori_loop(0, tokens // 16, norm, 0)
        ut_ref[:, tok_of(d)] = u_blk[:, cols_of(me)].T
        qkv_blk[...] = dot(u_blk[...], w_head[...], 1, 1).astype(BF16)
        half = tokens // 2
        where_to = gain_all[d, 2:3, :]
        lanes = lax.broadcasted_iota(jnp.int32, (half, 2 * head_dim), 1)
        by_row = lambda lo: jnp.broadcast_to(where_to[:, lo:lo + half], (2 * head_dim, half)).T
        angles = jnp.where(lanes < head_dim, by_row(0), by_row(half)) * freq_ref[...]
        packed = jnp.where(lax.rem(lanes, head_dim) < head_dim // 2, jnp.cos(angles), jnp.sin(angles))
        for part in range(2):
            rows = pl.ds(pl.multiple_of(base + part * half, half), half)
            cos_blk, sin_blk = spread_tables(packed, part == 1)
            cos_ref[rows, :] = cos_blk
            sin_ref[rows, :] = sin_blk
            source = slice(part * half, (part + 1) * half)
            for pair in range(heads // 2):
                turned = turn_halves(qkv_blk[source, pair * 128:(pair + 1) * 128].astype(F32), cos_blk, sin_blk).astype(BF16)
                q_ref[2 * pair, rows, :] = turned[:, :head_dim]
                q_ref[2 * pair + 1, rows, :] = turned[:, head_dim:]
            turned = turn_halves(qkv_blk[source, qw:].astype(F32), cos_blk, sin_blk).astype(BF16)
            k_ref[rows, :] = turned[:, :head_dim]
            v_ref[rows, :] = qkv_blk[source, qw + head_dim:]

    x_gather.got_first()
    x_gather.got_second()
    wo_gather.start()
    start_bulk(1, 2, 3)
    x_gather.got_partner(0)

    def use_near(i, _):
        use(jnp.where(i == 0, me, jnp.where(i == 1, first, jnp.where(i == 2, second, partner))))
        return 0
    lax.fori_loop(0, 4, use_near, 0)
    x_gather.got_diag()
    for i in range(1, 4):
        x_gather.got_partner(i)

    def use_far(i, _):
        use(jnp.where(i == 0, other(0, 1, 1), jnp.where(i == 1, other(1, 1, 0), jnp.where(i == 2, other(1, 0, 1), other(1, 1, 1)))))
        return 0
    lax.fori_loop(0, 4, use_far, 0)

    def one_head(h, _):
        for start in range(0, seq_len, BLK):
            keys, rows = pl.ds(0, start + BLK), pl.ds(start, BLK)
            probs = probs_transposed(k_ref[keys, :], q_ref[h, rows, :], start)
            o_scr[h, rows, :] = dot(probs.astype(BF16), v_ref[keys, :], 0, 0).astype(BF16)
        return 0
    for i in (0, 1, 2, 4, 5, 6, 7):
        stores[i].start()
    lax.fori_loop(0, heads, one_head, 0)
    for h in range(heads):
        o_own[:, h * head_dim:(h + 1) * head_dim] = o_scr[h]
    o_gather = Gather(lambda d: o_all.at[:, cols_of(d)], o_send, o_recv, where, o_all.at[:, pl.ds(0, 7 * rows_own)], own=o_own)
    o_gather.start()
    wo_gather.got_first()
    wo_gather.got_second()
    start_bulk(4)
    o_all[:, cols_of(me)] = o_own[...]

    def turn_out(k, _):
        rows = tok_of(k)
        ot_ref[:, rows] = o_own[rows, :].T
        return 0
    lax.fori_loop(0, 8, turn_out, 0)
    stores[3].start()
    wo_gather.got_diag()
    for i in range(4):
        wo_gather.got_partner(i)
    o_gather.got_first()
    o_gather.got_second()
    start_bulk(5, 6)
    o_gather.got_partner(0)
    o_gather.got_diag()
    for i in range(1, 4):
        o_gather.got_partner(i)
    start_bulk(7, 8, 9)

    def rows_at(i):
        flips = lambda a, b: other(0, a, b)
        return tok_of(jnp.where(i == 0, me, jnp.where(i == 1, flips(1, 0), jnp.where(i == 2, flips(0, 1), flips(1, 1)))))

    def give(i):
        slot = lax.rem(i, 2)
        rows = rows_at(i)
        return (pltpu.make_async_copy(m_out.at[slot], m_ref.at[rows, :], m_loc.at[slot]),
                pltpu.make_async_remote_copy(src_ref=m_out.at[slot], dst_ref=m_ref.at[rows, :], send_sem=m_send.at[i],
                                             recv_sem=m_recv.at[i], device_id=(partner,), device_id_type=MESH))

    def hidden_block(i, _):
        rows = rows_at(i)
        base = rows.start
        slot = lax.rem(i, 2)

        @pl.when(i >= 2)
        def _():
            to_hbm, to_partner = give(i - 2)
            to_hbm.wait()
            to_partner.wait_send()

        def chunk(j, _):
            cols = pl.ds(pl.multiple_of(j * 256, 256), 256)
            h_scr[:, cols] = dot(o_all[rows, :], wo_all[:, cols], 1, 0)
            return 0
        lax.fori_loop(0, model // 256, chunk, 0)

        def norm(k, _):
            part = pl.ds(pl.multiple_of(k * 16, 16), 16)
            x_part = x_all[pl.ds(pl.multiple_of(base + k * 16, 16), 16), :].astype(F32)
            hidden = (x_part + h_scr[part, :]).astype(BF16)

            @pl.when(i == 0)
            def _():
                h_ref[part, :] = hidden
            m_out[slot, part, :] = norm_forward(hidden.astype(F32), gfull_ref[1:2, :]).astype(BF16)
            return 0
        lax.fori_loop(0, tokens // 16, norm, 0)
        for copy in give(i):
            copy.start()
        return 0
    lax.fori_loop(0, 4, hidden_block, 0)
    stores[8].start()
    for i in range(4):
        give(i)[1].wait_recv()
    for i in range(2, 4):
        give(i)[0].wait()
        give(i)[1].wait_send()
    for copy in small + slices:
        copy.wait_send()
    for gather in (x_gather, wo_gather, o_gather):
        gather.drain()
    for mat, dst in enumerate((w1_ref, w3_ref)):
        seven = dst.at[pl.ds(0, 7 * rows_own), :]
        pltpu.make_async_remote_copy(src_ref=seven, dst_ref=seven, send_sem=bulk_send.at[mat], recv_sem=bulk_recv.at[mat],
                                     device_id=(partner,), device_id_type=MESH).wait()
    for load, store in local:
        store.wait()
    for copy in stores:
        copy.wait()


def attention_step(heads, x_in, positions, gain1, gain2, w_q, w_k, w_v, wo_own, w_gate, w_up):
    tokens, model = x_in.shape
    seq_len = 8 * tokens
    head_dim = wo_own.shape[0] // heads
    rows_own, hid = w_gate.shape[0], w_gate.shape[1] // 8
    shape = jax.ShapeDtypeStruct
    hbm, vmem = pl.BlockSpec(memory_space=pl.ANY), pl.BlockSpec(memory_space=pltpu.VMEM)
    dma = pltpu.SemaphoreType.DMA
    vm = lambda *dims, dtype=BF16: pltpu.VMEM(dims, dtype)
    steps = np.arange(head_dim // 2, dtype=np.float32) * np.float32(2.0 / head_dim)
    freq = np.tile(np.float32(1.0) / (np.float32(ROPE_BASE) ** steps), 4)[None]
    outs = (shape((heads, seq_len, head_dim), BF16), shape((seq_len, head_dim), BF16), shape((seq_len, head_dim), BF16),
            shape((heads * head_dim, seq_len), BF16), shape((rows_own, seq_len), BF16),
            shape((seq_len, 128), F32), shape((seq_len, 128), F32), shape((8, model), F32), shape((tokens, model), BF16))
    pairs = [dma((1,)), dma((1,)), dma((3,)), dma((3,)), dma((1,)), dma((7,)), dma((1,)), dma((7,)),
             dma((2,)), dma((2,)), dma((1,)), dma((7,))]
    return pl.pallas_call(
        functools.partial(attention_comm_kernel, 'sp', heads), name='attention_comm',
        in_specs=[hbm] + [vmem] * 4 + [hbm] * 6, out_specs=[hbm] * 12,
        out_shape=[*outs, shape((seq_len, model), BF16), shape((model, hid), BF16), shape((model, hid), BF16)],
        scratch_shapes=[vm(*t.shape, dtype=t.dtype) for t in outs] + [
            vm(8, rows_own, dtype=F32), vm(seq_len, model), vm(8, 8, rows_own, dtype=F32),
            vm(384, model), vm(model, model), vm(seq_len, model), vm(tokens, model), vm(tokens, 384), vm(heads, seq_len, head_dim),
            vm(seq_len, heads * head_dim), vm(tokens, model, dtype=F32), vm(2, tokens, model), vm(2, rows_own, hid)] + pairs + [
            dma((2,)), dma((4,)), dma((4,)), dma((4,)), dma((8,)), dma((9,))],
        compiler_params=pltpu.CompilerParams(collective_id=0, has_side_effects=True, vmem_limit_bytes=63 * 1024 * 1024),
    )(x_in, positions, gain1, gain2, jnp.asarray(freq), w_q, w_k, w_v, wo_own, w_gate, w_up)


def hand_over_kernel(n_in, *refs):
    sources, gains, results = refs[:n_in], refs[n_in], refs[n_in + 1:2 * n_in + 1]
    gain_outs, sem = refs[2 * n_in + 1:2 * n_in + 3], refs[2 * n_in + 3]
    stores = [pltpu.make_async_copy(sources[i], results[i], sem.at[i]) for i in range(n_in)]
    for store in stores:
        store.start()
    for i in range(2):
        gain_outs[i][...] = gains[i, :]
    for store in stores:
        store.wait()


def hand_over(arrays, gains):
    shape = jax.ShapeDtypeStruct
    hbm, vmem = pl.BlockSpec(memory_space=pltpu.HBM), pl.BlockSpec(memory_space=pltpu.VMEM)
    return pl.pallas_call(
        functools.partial(hand_over_kernel, len(arrays)), name='hand_over',
        in_specs=[vmem] * (len(arrays) + 1), out_specs=[hbm] * len(arrays) + [vmem] * 2,
        out_shape=[shape(a.shape, a.dtype) for a in arrays] + [shape((gains.shape[1],), F32)] * 2,
        scratch_shapes=[pltpu.SemaphoreType.DMA((len(arrays),))],
        compiler_params=pltpu.CompilerParams(vmem_limit_bytes=1024 * 1024),
    )(*[pltpu.with_memory_space_constraint(a, pltpu.VMEM) for a in arrays + (gains,)])


def solution(mesh):
    n_dev = mesh.shape['sp']

    def layer_step(x_in, positions, d_out, norm1_gain, norm2_gain, w_q, w_k, w_v, w_o, w_gate, w_up, w_down):
        tokens, model = x_in.shape
        head_dim = w_q.shape[2]
        heads = w_q.shape[1] // n_dev
        rows_own = w_q.shape[0]
        flat = lambda w: w.transpose(1, 2, 0).reshape(-1, rows_own)
        wo_own = w_o.reshape(-1, model)
        (q_rot, k_rot, v_lin, o_t, u_t, cos_tab, sin_tab, g_full, hidden,
         mlp_in, w1, w3) = attention_step(heads, x_in, positions, norm1_gain, norm2_gain, flat(w_q), flat(w_k), flat(w_v), wo_own, w_gate, w_up)
        d_w1s, d_w3s, d_down, y_out, dh_own, d_g2 = mlp_step(mlp_in, d_out, w1, w3, w_down, hidden, g_full)
        d_wo, d_wq_t, d_wk_t, d_wv_t, d_w1, d_w3, d_x, d_gains, d_down, y_out = attention_backward_step(
            heads, dh_own, wo_own, o_t, q_rot, k_rot, v_lin, (cos_tab, sin_tab),
            d_w1s, d_w3s, flat(w_q), flat(w_k), flat(w_v), u_t, x_in, g_full, d_g2, d_down, y_out)
        from_cols = lambda d, w: d.reshape(w.shape[1], w.shape[2], rows_own).transpose(2, 0, 1)
        (d_down, y_out, d_w1, d_w3, d_wo, d_wq_t, d_wk_t, d_wv_t, d_x, d_g1, d_g2) = hand_over(
            (d_down, y_out, d_w1, d_w3, d_wo, d_wq_t, d_wk_t, d_wv_t, d_x), d_gains)
        return (y_out, d_x, d_g1, d_g2, from_cols(d_wq_t, w_q), from_cols(d_wk_t, w_k), from_cols(d_wv_t, w_v),
                d_wo.reshape(w_o.shape), d_w1, d_w3, d_down)

    all_rows = P('sp')
    return jax.shard_map(layer_step, mesh=mesh, in_specs=(all_rows,) * 12, out_specs=(all_rows,) * 11, check_vma=False)
```

```python
import functools
import jax
import jax.numpy as jnp
import numpy as np
from jax import lax
from jax.experimental import pallas as pl
from jax.experimental.pallas import tpu as pltpu
from jax.sharding import PartitionSpec as P

ROPE_BASE = 10000.0
NORM_EPS = 1e-5
NEG_LARGE = -1e30
F32 = jnp.float32
BF16 = jnp.bfloat16
BLK = 256


def dot(lhs, rhs, lhs_dim, rhs_dim):
    return lax.dot_general(lhs, rhs, (((lhs_dim,), (rhs_dim,)), ((), ())), preferred_element_type=F32)


def norm_forward(hidden, gain_vec):
    inv_rms = lax.rsqrt(jnp.mean(hidden * hidden, axis=-1, keepdims=True) + NORM_EPS)
    return hidden * inv_rms * gain_vec


def probs_transposed(k_rows, q_blk, start):
    scores = dot(k_rows, q_blk, 1, 1)
    rows = lax.broadcasted_iota(jnp.int32, (BLK, BLK), 0)
    cols = lax.broadcasted_iota(jnp.int32, (BLK, BLK), 1)
    tail = jnp.where(rows <= cols, scores[start:], NEG_LARGE)
    scores = jnp.concatenate([scores[:start], tail], axis=0) if start else tail
    top = jnp.max(scores, axis=0, keepdims=True)
    weights = jnp.exp((scores - top) * (q_blk.shape[1] ** -0.5))
    return weights * (1.0 / jnp.sum(weights, axis=0, keepdims=True))


MESH = pl.DeviceIdType.MESH


def place(axis):
    me = lax.axis_index(axis)
    core = lax.rem(me, 2)
    col = lax.rem(lax.div(me, 2), 2)
    row = lax.div(me, 4)

    def other(flip_core, flip_col, flip_row):
        pick = lambda v, f: 1 - v if f else v
        return pick(row, flip_row) * 4 + pick(col, flip_col) * 2 + pick(core, flip_core)

    nbr_x, nbr_y = other(0, 1, 0), other(0, 0, 1)
    first = nbr_x * (1 - core) + nbr_y * core
    second = nbr_y * (1 - core) + nbr_x * core
    return me, other, first, second


def greet(other):
    barrier = pltpu.get_barrier_semaphore()
    for r in range(1, 8):
        pl.semaphore_signal(barrier, inc=1, device_id=(other(r & 1, (r >> 1) & 1, r >> 2),), device_id_type=MESH)
    pl.semaphore_wait(barrier, 7)


class Gather:
    def __init__(self, slot, send_sem, recv_sem, where, seven, own=None):
        me, other, first, second = where
        partner, diag = other(1, 0, 0), other(0, 1, 1)
        own = slot(me) if own is None else own
        self.copies = []
        plan = [(own, me, first), (own, me, second), (own, me, partner), (slot(first), first, second),
                (slot(first), first, partner), (slot(second), second, partner), (slot(diag), diag, partner)]
        for i, (src, what, dest) in enumerate(plan):
            self.copies.append(pltpu.make_async_remote_copy(
                src_ref=src, dst_ref=slot(what), send_sem=send_sem.at[0], recv_sem=recv_sem.at[i],
                device_id=(dest,), device_id_type=MESH))
        self.sent = pltpu.make_async_remote_copy(
            src_ref=seven, dst_ref=seven, send_sem=send_sem.at[0], recv_sem=recv_sem.at[0],
            device_id=(partner,), device_id_type=MESH)

    def start(self):
        for i in range(3):
            self.copies[i].start()

    def got_first(self):
        self.copies[0].wait_recv()
        self.copies[3].start()
        self.copies[4].start()

    def got_second(self):
        self.copies[1].wait_recv()
        self.copies[5].start()

    def got_diag(self):
        self.copies[3].wait_recv()
        self.copies[6].start()

    def got_partner(self, i):
        self.copies[(2, 4, 5, 6)[i]].wait_recv()

    def drain(self):
        self.sent.wait_send()


def turn_halves(values, cos_blk, sin_blk):
    width = values.shape[1]
    lanes = lax.broadcasted_iota(jnp.int32, values.shape, 1)
    partner = jnp.where(lax.rem(lanes, 64) < 32, pltpu.roll(values, width - 32, 1), pltpu.roll(values, 32, 1))
    return values * cos_blk + partner * sin_blk


def norm_backward(hidden, gain, d_out):
    inv = lax.rsqrt(jnp.mean(hidden * hidden, axis=-1, keepdims=True) + NORM_EPS)
    d_scaled = d_out * gain
    d_hidden = d_scaled * inv - hidden * (inv * inv * inv * jnp.mean(d_scaled * hidden, axis=-1, keepdims=True))
    return d_hidden, jnp.sum(d_out * (hidden * inv), axis=0, keepdims=True)


def attn_bwd_comm_kernel(axis, heads, dh_hbm, wo_hbm, ot_hbm, q_hbm, k_hbm, v_hbm, cos_hbm, sin_hbm,
                         dw1_ref, dw3_ref, wq_hbm, wk_hbm, wv_hbm, ut_hbm, x_hbm, g_hbm, dg2_hbm, ddown_hbm, y_hbm,
                         dwo_ref, dwq_ref, dwk_ref, dwv_ref, out1_ref, out3_ref, dx_ref, dg_ref, ddown_ref, y_ref,
                         dh_own, wo_ref, ot_ref, q_ref, k_ref, v_ref, cos_ref, sin_ref, wq_ref, wk_ref, wv_ref, ut_ref, g_ref, dg2_ref,
                         pool, do_scr, dg_own, dg_all, dk_acc, dv_acc, du_acc,
                         bulk_send, bulk_recv, hg_send, hg_recv, gat_send, gat_recv, du_send, du_rsem, dg_send, dg_recv, loc_sem, ld_sem, credit):
    loads = {}
    for i, (name, src, dst) in enumerate((
            ('wo', wo_hbm, wo_ref), ('ot', ot_hbm, ot_ref), ('q', q_hbm, q_ref), ('k', k_hbm, k_ref),
            ('v', v_hbm, v_ref), ('cos', cos_hbm, cos_ref), ('sin', sin_hbm, sin_ref), ('wq', wq_hbm, wq_ref), ('wk', wk_hbm, wk_ref),
            ('wv', wv_hbm, wv_ref), ('ut', ut_hbm, ut_ref), ('g', g_hbm, g_ref), ('dg2', dg2_hbm, dg2_ref),
            ('dh', dh_hbm, dh_own), ('ddown', ddown_hbm, ddown_ref), ('y', y_hbm, y_ref))):
        loads[name] = pltpu.make_async_copy(src, dst, ld_sem.at[i])
        loads[name].start()

    def need(*names):
        for name in names:
            loads[name].wait()

    where = place(axis)
    me, other, first, second = where
    greet(other)
    seq_len, head_dim = k_ref.shape
    rows_own, hid = out1_ref.shape[0], dw1_ref.shape[1]
    tokens, model = x_hbm.shape
    qw = heads * head_dim

    rows_of = lambda d: pl.ds(pl.multiple_of(d * rows_own, rows_own), rows_own)
    hid_of = lambda d: pl.ds(pl.multiple_of(d * hid, hid), hid)
    pairs = ((dw1_ref, out1_ref), (dw3_ref, out3_ref))
    peers = [other(r & 1, (r >> 1) & 1, r >> 2) for r in (2, 4, 6, 3, 5, 7, 1)]
    bulk, parts = [], []
    for mat, (src, dst) in enumerate(pairs):
        for low, high in ((0, 8), (8, rows_own // 2), (rows_own // 2, rows_own)):
            parts.append(range(len(bulk), len(bulk) + len(peers)))
            for dest in peers:
                bulk.append(pltpu.make_async_remote_copy(
                    src_ref=src.at[pl.ds(pl.multiple_of(dest * rows_own + low, 8), high - low), :],
                    dst_ref=dst.at[pl.ds(low, high - low), hid_of(me)], send_sem=bulk_send.at[mat],
                    recv_sem=bulk_recv.at[mat], device_id=(dest,), device_id_type=MESH))

    def start_bulk(*which):
        for part in which:
            for i in parts[part]:
                bulk[i].start()
    tok_of = lambda d: pl.ds(pl.multiple_of(d * tokens, tokens), tokens)
    dh_ref = pool.at[:, 0:model]
    h_gather = Gather(lambda d: dh_ref.at[tok_of(d), :], hg_send, hg_recv, where, dh_ref.at[pl.ds(0, 7 * tokens), :], own=dh_hbm)
    h_gather.start()
    start_bulk(0)
    local = [pltpu.make_async_copy(src.at[rows_of(me), :], dst.at[:, hid_of(me)], loc_sem.at[i]) for i, (src, dst) in enumerate(pairs)]
    for copy in local:
        copy.start()
    need('dh', 'wo', 'ot')
    pool[tok_of(me), 0:model] = dh_own[...]
    h_gather.got_first()
    h_gather.got_second()
    start_bulk(1, 2)
    h_gather.got_diag()
    for i in range(4):
        h_gather.got_partner(i)

    def split_out_grad(k, _):
        rows = pl.ds(pl.multiple_of(k * BLK, BLK), BLK)
        do_blk = dot(pool[rows, 0:model], wo_ref[...], 1, 1).astype(BF16)
        for h in range(heads):
            do_scr[h, rows, :] = do_blk[:, h * head_dim:(h + 1) * head_dim]
        cols = rows
        dwo_ref[:, cols] = dot(ot_ref[...], pool[:, cols], 1, 0)
        return 0
    lax.fori_loop(0, seq_len // BLK, split_out_grad, 0)
    h_gather.drain()
    for i, device in enumerate((first, second, other(1, 0, 0))):
        pl.semaphore_signal(credit.at[i], inc=1, device_id=(device,), device_id_type=MESH)
    x_ref = wo_ref
    x_load = pltpu.make_async_copy(x_hbm, x_ref, ld_sem.at[16])
    x_load.start()


    need('q', 'k', 'v')
    dk_acc[...] = jnp.zeros_like(dk_acc)
    dv_acc[...] = jnp.zeros_like(dv_acc)
    slot_cols = lambda d, off, width: pl.ds(pl.multiple_of(d * 384 + off, 128), width)

    def one_head(h, _):
        def one_block(start):
            keys = pl.ds(0, start + BLK)
            rows = pl.ds(start, BLK)
            q_blk, do_blk = q_ref[h, rows, :], do_scr[h, rows, :]
            probs = probs_transposed(k_ref[keys, :], q_blk, start)
            d_probs = dot(v_ref[keys, :], do_blk, 1, 1).astype(BF16).astype(F32)
            row_dot = jnp.sum(d_probs * probs, axis=0, keepdims=True)
            d_scores = (probs * (d_probs - row_dot) * (head_dim ** -0.5)).astype(BF16)
            do_scr[h, rows, :] = dot(d_scores, k_ref[keys, :], 0, 0).astype(BF16)
            dk_acc[keys, :] += dot(d_scores, q_blk, 1, 0)
            dv_acc[keys, :] += dot(probs.astype(BF16), do_blk, 1, 0)
        for start in range(0, seq_len, BLK):
            one_block(start)
        return 0
    lax.fori_loop(0, heads, one_head, 0)
    need('cos', 'sin')
    low = lax.broadcasted_iota(jnp.int32, (BLK, 128), 1) < head_dim

    def turn_back(k, _):
        rows = pl.ds(pl.multiple_of(k * BLK, BLK), BLK)
        cos_blk, sin_blk = cos_ref[rows, :], -sin_ref[rows, :]
        for pair in range(heads // 2):
            both = jnp.concatenate([do_scr[2 * pair, rows, :], do_scr[2 * pair + 1, rows, :]], axis=1)
            pool[rows, slot_cols(me, pair * 128, 128)] = turn_halves(both.astype(F32), cos_blk, sin_blk).astype(BF16)
        kv = jnp.concatenate([dk_acc[rows, :], dv_acc[rows, :]], axis=1).astype(BF16).astype(F32)
        pool[rows, slot_cols(me, qw, 128)] = jnp.where(low, turn_halves(kv, cos_blk, sin_blk), kv).astype(BF16)
        return 0
    lax.fori_loop(0, seq_len // BLK, turn_back, 0)

    gather = Gather(lambda d: pool.at[:, slot_cols(d, 0, 384)], gat_send, gat_recv, where, pool.at[:, pl.ds(0, 7 * 384)])
    for i in range(3):
        pl.semaphore_wait(credit.at[i], 1)
    gather.start()
    start_bulk(3)
    du_acc[...] = jnp.zeros_like(du_acc)
    need('wq', 'wk', 'wv', 'ut')

    def use(d):
        q_rows = pl.ds(pl.multiple_of(d * qw, qw), qw)
        kv_rows = pl.ds(pl.multiple_of(d * head_dim, head_dim), head_dim)
        w_all = jnp.concatenate([wq_ref[q_rows, :], wk_ref[kv_rows, :], wv_ref[kv_rows, :]], axis=0)

        def add_rows(k, _):
            rows = pl.ds(pl.multiple_of(k * 512, 512), 512)
            du_acc[rows, :] += dot(pool[rows, slot_cols(d, 0, 384)], w_all, 1, 0)
            return 0
        lax.fori_loop(0, seq_len // 512, add_rows, 0)
        d_w = dot(ut_ref[...], pool[:, slot_cols(d, 0, 384)], 1, 0).T
        dwq_ref[q_rows, :] = d_w[:qw]
        dwk_ref[kv_rows, :] = d_w[qw:qw + head_dim]
        dwv_ref[kv_rows, :] = d_w[qw + head_dim:]

    def use_many(*devices):
        def body(i, _):
            d = devices[0]
            for n in range(1, len(devices)):
                d = jnp.where(i == n, devices[n], d)
            use(d)
            return 0
        lax.fori_loop(0, len(devices), body, 0)

    use_many(me)
    gather.got_first()
    gather.got_second()
    start_bulk(4)
    gather.got_partner(0)
    use_many(first, second, other(1, 0, 0))
    gather.got_diag()
    for i in range(1, 4):
        gather.got_partner(i)
    use_many(other(0, 1, 1), other(1, 1, 0), other(1, 0, 1), other(1, 1, 1))
    gather.drain()
    du_scr = pool.at[:, 0:rows_own]

    def round_du(k, _):
        rows = pl.ds(pl.multiple_of(k * BLK, BLK), BLK)
        pool[rows, 0:rows_own] = du_acc[rows, :].astype(BF16)
        return 0
    lax.fori_loop(0, seq_len // BLK, round_du, 0)
    for dest in peers:
        pltpu.make_async_remote_copy(
            src_ref=du_scr.at[tok_of(dest), :], dst_ref=ot_ref.at[:, rows_of(me)], send_sem=du_send.at[0],
            recv_sem=du_rsem.at[0], device_id=(dest,), device_id_type=MESH).start()
    start_bulk(5)
    ot_ref[:, rows_of(me)] = pool[tok_of(me), 0:rows_own]
    need('g', 'dg2')
    x_load.wait()
    got = ot_ref.at[:, pl.ds(0, 7 * rows_own)]
    pltpu.make_async_copy(got, got, du_rsem.at[0]).wait()
    dg_own[...] = jnp.zeros_like(dg_own)
    dg_own[1:2, :] = dg2_ref[...]

    def input_grad(k, _):
        part = pl.ds(pl.multiple_of(k * 16, 16), 16)
        d_norm, d_gain = norm_backward(x_ref[part, :].astype(F32), g_ref[0:1, :], ot_ref[part, :].astype(F32))
        dh_part = dh_own[part, :]
        dx_ref[part, :] = (dh_part.astype(F32) + d_norm).astype(BF16)
        dg_own[0:1, :] += d_gain
        return 0
    lax.fori_loop(0, tokens // 16, input_grad, 0)
    for dest in peers:
        pltpu.make_async_remote_copy(
            src_ref=dg_own.at[:, rows_of(dest)], dst_ref=dg_all.at[me], send_sem=dg_send.at[0],
            recv_sem=dg_recv.at[0], device_id=(dest,), device_id_type=MESH).start()
    dg_all[me] = dg_own[:, rows_of(me)]
    got = dg_all.at[pl.ds(0, 7)]
    pltpu.make_async_copy(got, got, dg_recv.at[0]).wait()
    dg_ref[...] = jnp.sum(dg_all[...], axis=0)
    for sent, sem in ((du_scr.at[pl.ds(0, 7 * tokens), :], du_send), (dg_own.at[:, pl.ds(0, 7 * rows_own)], dg_send)):
        pltpu.make_async_copy(sent, sent, sem.at[0]).wait()
    need('ddown', 'y')
    for mat, (src, dst) in enumerate(pairs):
        sent, got = src.at[pl.ds(0, 7 * rows_own), :], dst.at[:, pl.ds(0, 7 * hid)]
        pltpu.make_async_copy(sent, sent, bulk_send.at[mat]).wait()
        pltpu.make_async_copy(got, got, bulk_recv.at[mat]).wait()
    for copy in local:
        copy.wait()


def attention_backward_step(heads, dh_own, wo_own, o_t, q_rot, k_rot, v_lin, tables, d_w1, d_w3, w_q, w_k, w_v, u_t, x_in, gains, d_g2, d_down, y_out):
    seq_len, model = k_rot.shape[0], x_in.shape[1]
    head_dim = k_rot.shape[1]
    tokens = x_in.shape[0]
    rows_own, hid = model // 8, d_w1.shape[1]
    shape = jax.ShapeDtypeStruct
    hbm = pl.BlockSpec(memory_space=pl.ANY)
    dma = pltpu.SemaphoreType.DMA
    vm = lambda *dims, dtype=BF16: pltpu.VMEM(dims, dtype)
    early = (dh_own, wo_own, o_t, q_rot, k_rot, v_lin, *tables)
    late = (w_q, w_k, w_v, u_t, x_in, gains, d_g2)
    outs = [(wo_own.shape, F32), (w_q.shape, F32), (w_k.shape, F32), (w_v.shape, F32), ((rows_own, 8 * hid), F32),
            ((rows_own, 8 * hid), F32), (x_in.shape, BF16), ((8, rows_own), F32), (d_down.shape, F32), (y_out.shape, BF16)]
    vmem, far = pl.BlockSpec(memory_space=pltpu.VMEM), pl.BlockSpec(memory_space=pltpu.HBM)
    return pl.pallas_call(
        functools.partial(attn_bwd_comm_kernel, 'sp', heads), name='attn_bwd_comm',
        in_specs=[hbm] * 17 + [far] * 2, out_specs=[vmem] * 10,
        out_shape=[pltpu.VMEM(dims, dtype) for dims, dtype in outs],
        scratch_shapes=[vm(*t.shape, dtype=t.dtype) for t in early + late[:4] + late[5:]] + [
            vm(seq_len, 8 * 384), vm(heads, seq_len, head_dim),
            vm(8, model, dtype=F32), vm(8, 8, rows_own, dtype=F32),
            vm(seq_len, head_dim, dtype=F32), vm(seq_len, head_dim, dtype=F32),
            vm(seq_len, rows_own, dtype=F32),
            dma((2,)), dma((2,)), dma((1,)), dma((7,)), dma((1,)), dma((7,)), dma((1,)), dma((1,)), dma((1,)), dma((1,)), dma((2,)), dma((17,)), pltpu.SemaphoreType.REGULAR((3,))],
        compiler_params=pltpu.CompilerParams(collective_id=2, has_side_effects=True, vmem_limit_bytes=34340864),
    )(*early, d_w1, d_w3, *late, *[pltpu.with_memory_space_constraint(a, pltpu.HBM) for a in (d_down, y_out)])


def mlp_comm_kernel(axis, m_ref, dout_own, w1_hbm, w3_hbm, w2_hbm, h_hbm, g_hbm,
                    dw1_ref, dw3_ref, dw2_ref, y_hbm, dh_hbm, dg2_hbm, dout_ref,
                    w1_ref, w3_ref, w2_ref, h_ref, g_ref, y_ref, dg2_ref,
                    glu, gate_s, up_s, outbox, chip_sum, inbox, blk, m_col, do_col, mt_scr, dot_scr, st1, st3, st2, dh_own,
                    part_send, part_recv, mail_send, mail_recv, do_send, do_recv,
                    in_sem, col_sem, out_sem, own_sem, ld_sem, credit):
    loads = [pltpu.make_async_copy(src, dst, ld_sem.at[i]) for i, (src, dst) in enumerate((
        (w1_hbm, w1_ref), (w3_hbm, w3_ref), (w2_hbm, w2_ref), (h_hbm, h_ref), (g_hbm, g_ref)))]
    own_in = pltpu.make_async_copy(dout_own, dh_own, own_sem.at[0])
    for copy in loads + [own_in]:
        copy.start()
    where = place(axis)
    me, other, first, second = where
    core = lax.rem(me, 2)
    partner = other(1, 0, 0)
    tokens, model = h_ref.shape
    hid = w1_ref.shape[1]
    tok_of = lambda d: pl.ds(pl.multiple_of(d * tokens, tokens), tokens)
    off_first, off_second = 1 + core, 2 - core

    def block_of(off, flip):
        d_col, d_row = lax.rem(off, 2), lax.div(off, 2)
        col, row = lax.rem(lax.div(me, 2), 2), lax.div(me, 4)
        mix = lambda v, f: v + f - 2 * v * f
        return mix(row, d_row) * 4 + mix(col, d_col) * 2 + mix(core, flip)

    def step_off(step, flip):
        mid_a = off_second * (1 - flip) + off_first * flip
        mid_b = off_first * (1 - flip) + off_second * flip
        return jnp.where(step == 0, 3, jnp.where(step == 1, mid_a, jnp.where(step == 2, mid_b, 0)))

    def half_rows(half):
        flip = 1 - lax.rem(half, 2)
        return tok_of(block_of(step_off(lax.div(half, 2), flip), flip))

    def fetch(half):
        slot = lax.rem(half, 2)
        return pltpu.make_async_copy(m_ref.at[half_rows(half), :], blk.at[slot], in_sem.at[slot])

    def fetch_dout(d):
        slot = lax.rem(d, 2)
        return pltpu.make_async_copy(dout_ref.at[tok_of(d), :], blk.at[slot], in_sem.at[slot])

    def fetch_cols(j):
        cols = pl.ds(pl.multiple_of(j * 256, 256), 256)
        return (pltpu.make_async_copy(m_ref.at[:, cols], m_col, col_sem.at[0]),
                pltpu.make_async_copy(dout_ref.at[:, cols], do_col, col_sem.at[1]))

    def sigmoid(value):
        return 1.0 / (1.0 + jnp.exp(-value))

    def activations(slot, rows):
        def chunk(j, _):
            cols = pl.ds(pl.multiple_of(j * 512, 512), 512)
            gate = dot(blk[slot], w1_ref[:, cols], 1, 0).astype(BF16)
            up = dot(blk[slot], w3_ref[:, cols], 1, 0).astype(BF16)
            gate_s[rows, cols] = gate
            up_s[rows, cols] = up
            gate = gate.astype(F32)
            glu[rows, cols] = (gate * sigmoid(gate) * up.astype(F32)).astype(BF16)
            return 0
        lax.fori_loop(0, hid // 512, chunk, 0)

    def activation_grads(slot, rows):
        def chunk(j, _):
            cols = pl.ds(pl.multiple_of(j * 512, 512), 512)
            d_act = dot(blk[slot], w2_ref[cols, :], 1, 1).astype(BF16).astype(F32)
            gate, up = gate_s[rows, cols].astype(F32), up_s[rows, cols].astype(F32)
            sig = sigmoid(gate)
            silu = gate * sig
            up_s[rows, cols] = (d_act * silu).astype(BF16)
            gate_s[rows, cols] = (d_act * up * (sig + silu * (1.0 - sig))).astype(BF16)
            return 0
        lax.fori_loop(0, hid // 512, chunk, 0)

    def add_mlp_grad(rows, put):
        def chunk(j, _):
            cols = pl.ds(pl.multiple_of(j * 512, 512), 512)
            put(cols, dot(gate_s[rows, :], w1_ref[cols, :], 1, 1) + dot(up_s[rows, :], w3_ref[cols, :], 1, 1))
            return 0
        lax.fori_loop(0, model // 512, chunk, 0)

    def add_mlp_out(rows, put):
        def chunk(j, _):
            cols = pl.ds(pl.multiple_of(j * 512, 512), 512)
            put(cols, dot(glu[rows, :], w2_ref[:, cols], 1, 0))
            return 0
        lax.fori_loop(0, model // 512, chunk, 0)

    def signal(index, device):
        pl.semaphore_signal(credit.at[index], inc=1, device_id=(device,), device_id_type=MESH)

    class Scatter:
        def __init__(self, turn):
            self.turn = turn

        def to_partner(self, step):
            off = step_off(step, 1)
            return pltpu.make_async_remote_copy(
                src_ref=outbox.at[lax.rem(step, 2)], dst_ref=chip_sum.at[off], send_sem=part_send.at[self.turn, step],
                recv_sem=part_recv.at[self.turn, off], device_id=(partner,), device_id_type=MESH)

        def from_partner(self, off):
            return pltpu.make_async_remote_copy(
                src_ref=outbox.at[0], dst_ref=chip_sum.at[off], send_sem=part_send.at[self.turn, 0],
                recv_sem=part_recv.at[self.turn, off], device_id=(partner,), device_id_type=MESH)

        def mail(self, kind):
            off = (3, off_first, off_second)[kind]
            dest = (first, first, second)[kind]
            return pltpu.make_async_remote_copy(
                src_ref=chip_sum.at[off], dst_ref=inbox.at[kind], send_sem=mail_send.at[self.turn, kind],
                recv_sem=mail_recv.at[self.turn, kind], device_id=(dest,), device_id_type=MESH)

        def step(self, step, prepare, partial):
            self.first_half(step, prepare, partial)
            self.second_half(step, prepare, partial)

        def first_half(self, step, prepare, partial):
            slot = lax.rem(step, 2)
            prepare(2 * step)

            def put_out(cols, value):
                outbox[slot, :, cols] = value
            partial(half_rows(2 * step), put_out)

        def second_half(self, step, prepare, partial):
            self.to_partner(step).start()
            prepare(2 * step + 1)
            off = step_off(step, 0)
            self.from_partner(off).wait_recv()

            def put_sum(cols, value):
                chip_sum[off, :, cols] += value
            partial(half_rows(2 * step + 1), put_sum)

        def pass_on(self):
            self.mail(0).wait_recv()

            def add_mail(k, _):
                part = pl.ds(pl.multiple_of(k * 16, 16), 16)
                chip_sum[off_second, part, :] += inbox[0, part, :]
                return 0
            lax.fori_loop(0, tokens // 16, add_mail, 0)

    out_round, grad_round = Scatter(0), Scatter(1)

    def prepare_out(half):
        @pl.when(half < 7)
        def _():
            fetch(half + 1).start()
        fetch(half).wait()
        activations(lax.rem(half, 2), half_rows(half))

    def weight_grads(begin, end):
        for copy in fetch_cols(begin):
            copy.start()

        def body(j, _):
            for copy in fetch_cols(j):
                copy.wait()

            def turn(k, _):
                part = pl.ds(pl.multiple_of(k * 256, 256), 256)
                mt_scr[:, part] = m_col[part, :].T
                dot_scr[:, part] = do_col[part, :].T
                return 0
            lax.fori_loop(0, m_col.shape[0] // 256, turn, 0)

            @pl.when(j + 1 < end)
            def _():
                for copy in fetch_cols(j + 1):
                    copy.start()
            rows = pl.ds(pl.multiple_of(j * 256, 256), 256)
            out = (pltpu.make_async_copy(st1, dw1_ref.at[rows, :], out_sem.at[0]),
                   pltpu.make_async_copy(st3, dw3_ref.at[rows, :], out_sem.at[1]),
                   pltpu.make_async_copy(st2, dw2_ref.at[:, rows], out_sem.at[2]))

            @pl.when(j > begin)
            def _():
                for copy in out:
                    copy.wait()

            def chunk(k, _):
                cols = pl.ds(pl.multiple_of(k * 512, 512), 512)
                st1[:, cols] = dot(mt_scr[...], gate_s[:, cols], 1, 0)
                st3[:, cols] = dot(mt_scr[...], up_s[:, cols], 1, 0)
                st2[cols, :] = dot(dot_scr[...], glu[:, cols], 1, 0).T
                return 0
            lax.fori_loop(0, hid // 512, chunk, 0)
            for copy in out:
                copy.start()
            return 0
        lax.fori_loop(begin, end, body, 0)
        rows = pl.ds((end - 1) * 256, 256)
        for copy in (pltpu.make_async_copy(st1, dw1_ref.at[rows, :], out_sem.at[0]),
                     pltpu.make_async_copy(st3, dw3_ref.at[rows, :], out_sem.at[1]),
                     pltpu.make_async_copy(st2, dw2_ref.at[:, rows], out_sem.at[2])):
            copy.wait()

    fetch(0).start()
    greet(other)
    do_gather = Gather(lambda d: dout_ref.at[tok_of(d), :], do_send, do_recv, where, dout_ref.at[pl.ds(0, 7 * tokens), :], own=dout_own)
    do_gather.start()
    own_in.wait()
    own_out = pltpu.make_async_copy(dh_own, dout_ref.at[tok_of(me), :], own_sem.at[1])
    own_out.start()
    for copy in loads:
        copy.wait()

    def out_step(step, _):
        @pl.when(step >= 2)
        def _():
            out_round.to_partner(step - 2).wait_send()
        out_round.step(step, prepare_out, add_mlp_out)

        @pl.when(step == 0)
        def _():
            out_round.mail(0).start()

        @pl.when(step == 2)
        def _():
            out_round.mail(1).start()
            do_gather.got_first()
            do_gather.got_second()
        return 0
    lax.fori_loop(0, 4, out_step, 0)
    out_round.pass_on()
    out_round.mail(2).start()
    for step in (2, 3):
        out_round.to_partner(step).wait_send()
    out_round.mail(0).wait_send()
    signal(0, partner)
    signal(1, first)
    do_gather.got_diag()
    for i in range(4):
        do_gather.got_partner(i)
    own_out.wait()
    fetch_dout(0).start()

    def grad_block(d, _):
        @pl.when(d < 7)
        def _():
            fetch_dout(d + 1).start()
        fetch_dout(d).wait()
        activation_grads(lax.rem(d, 2), tok_of(d))
        return 0
    lax.fori_loop(0, 8, grad_block, 0)

    as_is = lambda half: None
    grad_round.first_half(0, as_is, add_mlp_grad)
    pl.semaphore_wait(credit.at[0], 1)
    grad_round.second_half(0, as_is, add_mlp_grad)
    pl.semaphore_wait(credit.at[1], 1)
    grad_round.mail(0).start()
    weight_grads(0, 2)
    grad_round.first_half(1, as_is, add_mlp_grad)
    out_round.mail(1).wait_recv()
    out_round.mail(2).wait_recv()

    def layer_out(k, _):
        part = pl.ds(pl.multiple_of(k * 16, 16), 16)
        y_ref[part, :] = (h_ref[part, :].astype(F32) + (chip_sum[0, part, :] + inbox[1, part, :] + inbox[2, part, :])).astype(BF16)
        return 0
    lax.fori_loop(0, tokens // 16, layer_out, 0)
    y_store = pltpu.make_async_copy(y_ref, y_hbm, own_sem.at[2])
    y_store.start()
    out_round.mail(1).wait_send()
    out_round.mail(2).wait_send()
    signal(2, partner)
    signal(3, first)
    signal(4, second)
    pl.semaphore_wait(credit.at[2], 1)

    grad_round.second_half(1, as_is, add_mlp_grad)

    def grad_step(step, _):
        grad_round.to_partner(step - 2).wait_send()
        grad_round.step(step, as_is, add_mlp_grad)

        @pl.when(step == 2)
        def _():
            pl.semaphore_wait(credit.at[3], 1)
            grad_round.mail(1).start()
            grad_round.pass_on()
            pl.semaphore_wait(credit.at[4], 1)
            grad_round.mail(2).start()
        return 0
    lax.fori_loop(2, 4, grad_step, 0)
    weight_grads(2, 8)
    grad_round.mail(1).wait_recv()
    grad_round.mail(2).wait_recv()
    dg2_ref[...] = jnp.zeros_like(dg2_ref)

    def hidden_grad(k, _):
        part = pl.ds(pl.multiple_of(k * 16, 16), 16)
        d_mlp = (chip_sum[0, part, :] + inbox[1, part, :] + inbox[2, part, :]).astype(BF16).astype(F32)
        d_norm, d_gain = norm_backward(h_ref[part, :].astype(F32), g_ref[1:2, :], d_mlp)
        dh_own[part, :] = (dh_own[part, :].astype(F32) + d_norm).astype(BF16)
        dg2_ref[...] += d_gain
        return 0
    lax.fori_loop(0, tokens // 16, hidden_grad, 0, unroll=4)
    own_out = pltpu.make_async_copy(dh_own, dh_hbm, own_sem.at[3])
    own_out.start()
    dg2_store = pltpu.make_async_copy(dg2_ref, dg2_hbm, own_sem.at[4])
    dg2_store.start()
    for step in (2, 3):
        grad_round.to_partner(step).wait_send()
    for kind in range(3):
        grad_round.mail(kind).wait_send()
    do_gather.drain()
    own_out.wait()
    y_store.wait()
    dg2_store.wait()


def mlp_step(m_all, d_out, w1, w3, w2, hidden, gains):
    seq_len, model = m_all.shape
    hid, tokens = w1.shape[1], hidden.shape[0]
    shape = jax.ShapeDtypeStruct
    hbm = pl.BlockSpec(memory_space=pl.ANY)
    dma = pltpu.SemaphoreType.DMA
    vm = lambda *dims, dtype=BF16: pltpu.VMEM(dims, dtype)
    return pl.pallas_call(
        functools.partial(mlp_comm_kernel, 'sp'), name='mlp_comm',
        in_specs=[hbm] * 7, out_specs=[hbm] * 7,
        out_shape=[shape((model, hid), F32), shape((model, hid), F32), shape((hid, model), F32),
                   shape(hidden.shape, BF16), shape(hidden.shape, BF16), shape((1, model), F32), shape((seq_len, model), BF16)],
        scratch_shapes=[vm(*t.shape, dtype=t.dtype) for t in (w1, w3, w2, hidden, gains)] + [
            vm(tokens, model), vm(1, model, dtype=F32),
            vm(seq_len, hid), vm(seq_len, hid), vm(seq_len, hid),
            vm(2, tokens, model, dtype=F32), vm(4, tokens, model, dtype=F32), vm(3, tokens, model, dtype=F32),
            vm(2, tokens, model), vm(seq_len, 256), vm(seq_len, 256), vm(256, seq_len), vm(256, seq_len),
            vm(256, hid, dtype=F32), vm(256, hid, dtype=F32), vm(hid, 256, dtype=F32), vm(tokens, model),
            dma((2, 4)), dma((2, 4)), dma((2, 3)), dma((2, 3)), dma((1,)), dma((7,)),
            dma((2,)), dma((2,)), dma((3,)), dma((5,)), dma((5,)), pltpu.SemaphoreType.REGULAR((5,))],
        compiler_params=pltpu.CompilerParams(collective_id=1, has_side_effects=True, vmem_limit_bytes=63 * 1024 * 1024),
    )(m_all, d_out, w1, w3, w2, hidden, gains)[:6]


def spread_tables(packed, upper):
    lanes = lax.broadcasted_iota(jnp.int32, packed.shape, 1)
    swapped = pltpu.roll(packed, 64, 1)
    both = jnp.where((lanes < 64) != upper, packed, swapped)
    low = lax.rem(lanes, 64) < 32
    return jnp.where(low, both, pltpu.roll(both, 32, 1)), jnp.where(low, -pltpu.roll(both, 96, 1), both)


def attention_comm_kernel(axis, heads, x_ref, pos_hbm, gain1_hbm, gain2_hbm, freq_hbm, wq_ref, wk_ref, wv_ref, wo_ref, wg_ref, wu_ref,
                          q_hbm, k_hbm, v_hbm, ot_hbm, ut_hbm, cos_hbm, sin_hbm, gfull_hbm, h_hbm, m_ref, w1_ref, w3_ref,
                          q_ref, k_ref, v_ref, ot_ref, ut_ref, cos_ref, sin_ref, gfull_ref, h_ref, pos_ref, gain1_ref, gain2_ref, freq_ref, gain_ref, x_all, gain_all, w_head, wo_all, o_all, u_blk, qkv_blk, o_scr, o_own, h_scr, m_out, stage,
                          g_send, g_recv, w_send, w_recv, x_send, x_recv, wo_send, wo_recv, bulk_send, bulk_recv,
                          o_send, o_recv, m_loc, m_send, m_recv, loc_sem, own_sem, st_sem):
    tiny = [pltpu.make_async_copy(src, dst, own_sem.at[8 + i]) for i, (src, dst) in enumerate((
        (gain1_hbm, gain1_ref), (gain2_hbm, gain2_ref), (pos_hbm, pos_ref), (freq_hbm, freq_ref)))]
    for copy in tiny:
        copy.start()
    where = place(axis)
    me, other, first, second = where
    core = lax.rem(me, 2)
    partner = other(1, 0, 0)
    greet(other)
    tokens, model = x_ref.shape
    seq_len, head_dim = k_ref.shape
    qw = heads * head_dim
    rows_own, hid = wg_ref.shape[0], w1_ref.shape[1]
    tok_of = lambda d: pl.ds(pl.multiple_of(d * tokens, tokens), tokens)
    cols_of = lambda d: pl.ds(pl.multiple_of(d * rows_own, rows_own), rows_own)
    hid_of = lambda d: pl.ds(pl.multiple_of(d * hid, hid), hid)
    peers = [other(r & 1, (r >> 1) & 1, r >> 2) for r in (6, 2, 4, 7, 3, 5, 1)]

    def to_all(src_of, dst, seven, sems):
        copies = [pltpu.make_async_remote_copy(
            src_ref=src_of(dest), dst_ref=dst, send_sem=sems[0], recv_sem=sems[1],
            device_id=(dest,), device_id_type=MESH) for dest in peers]
        for copy in copies:
            copy.start()
        return pltpu.make_async_remote_copy(src_ref=seven, dst_ref=seven, send_sem=sems[0], recv_sem=sems[1],
                                            device_id=(partner,), device_id_type=MESH)

    q_of = lambda d: pl.ds(pl.multiple_of(d * qw, qw), qw)
    kv_of = lambda d: pl.ds(pl.multiple_of(d * head_dim, head_dim), head_dim)
    seven_rows = pl.ds(0, 7 * rows_own)
    slices = []
    for i, (src, rows, low, high) in enumerate(((wq_ref, q_of, 0, qw), (wk_ref, kv_of, qw, qw + head_dim),
                                                (wv_ref, kv_of, qw + head_dim, qw + 2 * head_dim))):
        slices.append(to_all(lambda dest: src.at[rows(dest), :], w_head.at[low:high, cols_of(me)],
                             w_head.at[low:high, seven_rows], (w_send.at[i], w_recv.at[i])))
    x_gather = Gather(lambda d: x_all.at[tok_of(d), :], x_send, x_recv, where, x_all.at[pl.ds(0, 7 * tokens), :], own=x_ref)
    x_gather.start()
    for copy in tiny:
        copy.wait()
    gain_ref[...] = jnp.zeros_like(gain_ref)
    gain_ref[0:1, :] = gain1_ref[...].astype(F32).reshape(1, -1)
    gain_ref[1:2, :] = gain2_ref[...].astype(F32).reshape(1, -1)
    gain_ref[2:3, :] = pos_ref[...].astype(F32).reshape(1, -1)
    small = [to_all(lambda dest: gain_ref, gain_all.at[me], gain_all.at[pl.ds(0, 7)], (g_send.at[0], g_recv.at[0]))]
    wo_gather = Gather(lambda d: wo_all.at[cols_of(d), :], wo_send, wo_recv, where, wo_all.at[pl.ds(0, 7 * rows_own), :], own=wo_ref)
    bulk, parts = [], []
    quarter = rows_own // 4
    for mat, (src, dst) in enumerate(((wg_ref, w1_ref), (wu_ref, w3_ref))):
        for low, high in ((0, 16), (16, quarter), (quarter, 2 * quarter), (2 * quarter, 3 * quarter), (3 * quarter, rows_own)):
            parts.append(range(len(bulk), len(bulk) + len(peers)))
            for dest in peers:
                bulk.append(pltpu.make_async_remote_copy(
                    src_ref=src.at[pl.ds(low, high - low), hid_of(dest)],
                    dst_ref=dst.at[pl.ds(pl.multiple_of(me * rows_own + low, 16), high - low), :],
                    send_sem=bulk_send.at[mat], recv_sem=bulk_recv.at[mat], device_id=(dest,), device_id_type=MESH))

    def start_bulk(*which):
        for part in which:
            for i in parts[part]:
                bulk[i].start()
    start_bulk(0)

    stores = [pltpu.make_async_copy(src, dst, st_sem.at[i]) for i, (src, dst) in enumerate((
        (q_ref, q_hbm), (k_ref, k_hbm), (v_ref, v_hbm), (ot_ref, ot_hbm), (ut_ref, ut_hbm), (cos_ref, cos_hbm),
        (sin_ref, sin_hbm), (gfull_ref, gfull_hbm), (h_ref, h_hbm)))]
    own = [pltpu.make_async_copy(src, dst, own_sem.at[i]) for i, (src, dst) in enumerate((
        (gain_ref, gain_all.at[me]), (wq_ref.at[q_of(me), :], w_head.at[0:qw, cols_of(me)]),
        (wk_ref.at[kv_of(me), :], w_head.at[qw:qw + head_dim, cols_of(me)]),
        (wv_ref.at[kv_of(me), :], w_head.at[qw + head_dim:, cols_of(me)]),
        (x_ref, x_all.at[tok_of(me), :]), (wo_ref, wo_all.at[cols_of(me), :])))]
    for copy in own:
        copy.start()
    local = []
    for i, (src, dst) in enumerate(((wg_ref, w1_ref), (wu_ref, w3_ref))):
        local.append((pltpu.make_async_copy(src.at[:, hid_of(me)], stage.at[i], loc_sem.at[i]),
                      pltpu.make_async_copy(stage.at[i], dst.at[cols_of(me), :], loc_sem.at[2 + i])))
        local[-1][0].start()
    for load, store in local:
        load.wait()
        store.start()
    for copy in own:
        copy.wait()
    for copy in small:
        copy.wait_recv()
    for d in range(8):
        gfull_ref[:, d * rows_own:(d + 1) * rows_own] = gain_all[d]
    for copy in slices:
        copy.wait_recv()

    def use(d):
        base = pl.multiple_of(d * tokens, tokens)

        def norm(k, _):
            part = pl.ds(pl.multiple_of(k * 16, 16), 16)
            x_part = x_all[pl.ds(pl.multiple_of(base + k * 16, 16), 16), :].astype(F32)
            u_blk[part, :] = norm_forward(x_part, gfull_ref[0:1, :]).astype(BF16)
            return 0
        lax.fori_loop(0, tokens // 16, norm, 0)
        ut_ref[:, tok_of(d)] = u_blk[:, cols_of(me)].T
        qkv_blk[...] = dot(u_blk[...], w_head[...], 1, 1).astype(BF16)
        half = tokens // 2
        where_to = gain_all[d, 2:3, :]
        lanes = lax.broadcasted_iota(jnp.int32, (half, 2 * head_dim), 1)
        by_row = lambda lo: jnp.broadcast_to(where_to[:, lo:lo + half], (2 * head_dim, half)).T
        angles = jnp.where(lanes < head_dim, by_row(0), by_row(half)) * freq_ref[...]
        packed = jnp.where(lax.rem(lanes, head_dim) < head_dim // 2, jnp.cos(angles), jnp.sin(angles))
        for part in range(2):
            rows = pl.ds(pl.multiple_of(base + part * half, half), half)
            cos_blk, sin_blk = spread_tables(packed, part == 1)
            cos_ref[rows, :] = cos_blk
            sin_ref[rows, :] = sin_blk
            source = slice(part * half, (part + 1) * half)
            for pair in range(heads // 2):
                turned = turn_halves(qkv_blk[source, pair * 128:(pair + 1) * 128].astype(F32), cos_blk, sin_blk).astype(BF16)
                q_ref[2 * pair, rows, :] = turned[:, :head_dim]
                q_ref[2 * pair + 1, rows, :] = turned[:, head_dim:]
            turned = turn_halves(qkv_blk[source, qw:].astype(F32), cos_blk, sin_blk).astype(BF16)
            k_ref[rows, :] = turned[:, :head_dim]
            v_ref[rows, :] = qkv_blk[source, qw + head_dim:]

    x_gather.got_first()
    x_gather.got_second()
    wo_gather.start()
    start_bulk(1, 2, 3)
    x_gather.got_partner(0)

    def use_near(i, _):
        use(jnp.where(i == 0, me, jnp.where(i == 1, first, jnp.where(i == 2, second, partner))))
        return 0
    lax.fori_loop(0, 4, use_near, 0)
    x_gather.got_diag()
    for i in range(1, 4):
        x_gather.got_partner(i)

    def use_far(i, _):
        use(jnp.where(i == 0, other(0, 1, 1), jnp.where(i == 1, other(1, 1, 0), jnp.where(i == 2, other(1, 0, 1), other(1, 1, 1)))))
        return 0
    lax.fori_loop(0, 4, use_far, 0)

    def one_head(h, _):
        for start in range(0, seq_len, BLK):
            keys, rows = pl.ds(0, start + BLK), pl.ds(start, BLK)
            probs = probs_transposed(k_ref[keys, :], q_ref[h, rows, :], start)
            o_scr[h, rows, :] = dot(probs.astype(BF16), v_ref[keys, :], 0, 0).astype(BF16)
        return 0
    for i in (0, 1, 2, 4, 5, 6, 7):
        stores[i].start()
    lax.fori_loop(0, heads, one_head, 0)
    for h in range(heads):
        o_own[:, h * head_dim:(h + 1) * head_dim] = o_scr[h]
    o_gather = Gather(lambda d: o_all.at[:, cols_of(d)], o_send, o_recv, where, o_all.at[:, pl.ds(0, 7 * rows_own)], own=o_own)
    o_gather.start()
    wo_gather.got_first()
    wo_gather.got_second()
    start_bulk(4)
    o_all[:, cols_of(me)] = o_own[...]

    def turn_out(k, _):
        rows = tok_of(k)
        ot_ref[:, rows] = o_own[rows, :].T
        return 0
    lax.fori_loop(0, 8, turn_out, 0)
    stores[3].start()
    wo_gather.got_diag()
    for i in range(4):
        wo_gather.got_partner(i)
    o_gather.got_first()
    o_gather.got_second()
    start_bulk(5, 6)
    o_gather.got_partner(0)
    o_gather.got_diag()
    for i in range(1, 4):
        o_gather.got_partner(i)
    start_bulk(7, 8, 9)

    def rows_at(i):
        flips = lambda a, b: other(0, a, b)
        return tok_of(jnp.where(i == 0, me, jnp.where(i == 1, flips(1, 0), jnp.where(i == 2, flips(0, 1), flips(1, 1)))))

    def give(i):
        slot = lax.rem(i, 2)
        rows = rows_at(i)
        return (pltpu.make_async_copy(m_out.at[slot], m_ref.at[rows, :], m_loc.at[slot]),
                pltpu.make_async_remote_copy(src_ref=m_out.at[slot], dst_ref=m_ref.at[rows, :], send_sem=m_send.at[i],
                                             recv_sem=m_recv.at[i], device_id=(partner,), device_id_type=MESH))

    def hidden_block(i, _):
        rows = rows_at(i)
        base = rows.start
        slot = lax.rem(i, 2)

        @pl.when(i >= 2)
        def _():
            to_hbm, to_partner = give(i - 2)
            to_hbm.wait()
            to_partner.wait_send()

        def chunk(j, _):
            cols = pl.ds(pl.multiple_of(j * 256, 256), 256)
            h_scr[:, cols] = dot(o_all[rows, :], wo_all[:, cols], 1, 0)
            return 0
        lax.fori_loop(0, model // 256, chunk, 0)

        def norm(k, _):
            part = pl.ds(pl.multiple_of(k * 16, 16), 16)
            x_part = x_all[pl.ds(pl.multiple_of(base + k * 16, 16), 16), :].astype(F32)
            hidden = (x_part + h_scr[part, :]).astype(BF16)

            @pl.when(i == 0)
            def _():
                h_ref[part, :] = hidden
            m_out[slot, part, :] = norm_forward(hidden.astype(F32), gfull_ref[1:2, :]).astype(BF16)
            return 0
        lax.fori_loop(0, tokens // 16, norm, 0)
        for copy in give(i):
            copy.start()
        return 0
    lax.fori_loop(0, 4, hidden_block, 0)
    stores[8].start()
    for i in range(4):
        give(i)[1].wait_recv()
    for i in range(2, 4):
        give(i)[0].wait()
        give(i)[1].wait_send()
    for copy in small + slices:
        copy.wait_send()
    for gather in (x_gather, wo_gather, o_gather):
        gather.drain()
    for mat, dst in enumerate((w1_ref, w3_ref)):
        seven = dst.at[pl.ds(0, 7 * rows_own), :]
        pltpu.make_async_remote_copy(src_ref=seven, dst_ref=seven, send_sem=bulk_send.at[mat], recv_sem=bulk_recv.at[mat],
                                     device_id=(partner,), device_id_type=MESH).wait()
    for load, store in local:
        store.wait()
    for copy in stores:
        copy.wait()


def attention_step(heads, x_in, positions, gain1, gain2, w_q, w_k, w_v, wo_own, w_gate, w_up):
    tokens, model = x_in.shape
    seq_len = 8 * tokens
    head_dim = wo_own.shape[0] // heads
    rows_own, hid = w_gate.shape[0], w_gate.shape[1] // 8
    shape = jax.ShapeDtypeStruct
    hbm = pl.BlockSpec(memory_space=pl.ANY)
    dma = pltpu.SemaphoreType.DMA
    vm = lambda *dims, dtype=BF16: pltpu.VMEM(dims, dtype)
    steps = np.arange(head_dim // 2, dtype=np.float32) * np.float32(2.0 / head_dim)
    freq = np.tile(np.float32(1.0) / (np.float32(ROPE_BASE) ** steps), 4)[None]
    outs = (shape((heads, seq_len, head_dim), BF16), shape((seq_len, head_dim), BF16), shape((seq_len, head_dim), BF16),
            shape((heads * head_dim, seq_len), BF16), shape((rows_own, seq_len), BF16),
            shape((seq_len, 128), F32), shape((seq_len, 128), F32), shape((8, model), F32), shape((tokens, model), BF16))
    pairs = [dma((1,)), dma((1,)), dma((3,)), dma((3,)), dma((1,)), dma((7,)), dma((1,)), dma((7,)),
             dma((2,)), dma((2,)), dma((1,)), dma((7,))]
    return pl.pallas_call(
        functools.partial(attention_comm_kernel, 'sp', heads), name='attention_comm',
        in_specs=[hbm] * 11, out_specs=[hbm] * 12,
        out_shape=[*outs, shape((seq_len, model), BF16), shape((model, hid), BF16), shape((model, hid), BF16)],
        scratch_shapes=[vm(*t.shape, dtype=t.dtype) for t in outs] + [
            vm(tokens, dtype=jnp.int32), vm(rows_own), vm(rows_own), vm(1, 2 * head_dim, dtype=F32),
            vm(8, rows_own, dtype=F32), vm(seq_len, model), vm(8, 8, rows_own, dtype=F32),
            vm(384, model), vm(model, model), vm(seq_len, model), vm(tokens, model), vm(tokens, 384), vm(heads, seq_len, head_dim),
            vm(seq_len, heads * head_dim), vm(tokens, model, dtype=F32), vm(2, tokens, model), vm(2, rows_own, hid)] + pairs + [
            dma((2,)), dma((4,)), dma((4,)), dma((4,)), dma((12,)), dma((9,))],
        compiler_params=pltpu.CompilerParams(collective_id=0, has_side_effects=True, vmem_limit_bytes=63 * 1024 * 1024),
    )(x_in, positions, gain1, gain2, jnp.asarray(freq), w_q, w_k, w_v, wo_own, w_gate, w_up)


def hand_over_kernel(n_in, *refs):
    sources, gains, results = refs[:n_in], refs[n_in], refs[n_in + 1:2 * n_in + 1]
    gain_outs, sem = refs[2 * n_in + 1:2 * n_in + 3], refs[2 * n_in + 3]
    stores = [pltpu.make_async_copy(sources[i], results[i], sem.at[i]) for i in range(n_in)]
    for store in stores:
        store.start()
    for i in range(2):
        gain_outs[i][...] = gains[i, :]
    for store in stores:
        store.wait()


def hand_over(arrays, gains):
    shape = jax.ShapeDtypeStruct
    hbm, vmem = pl.BlockSpec(memory_space=pltpu.HBM), pl.BlockSpec(memory_space=pltpu.VMEM)
    return pl.pallas_call(
        functools.partial(hand_over_kernel, len(arrays)), name='hand_over',
        in_specs=[vmem] * (len(arrays) + 1), out_specs=[hbm] * len(arrays) + [vmem] * 2,
        out_shape=[shape(a.shape, a.dtype) for a in arrays] + [shape((gains.shape[1],), F32)] * 2,
        scratch_shapes=[pltpu.SemaphoreType.DMA((len(arrays),))],
        compiler_params=pltpu.CompilerParams(vmem_limit_bytes=1024 * 1024),
    )(*[pltpu.with_memory_space_constraint(a, pltpu.VMEM) for a in arrays + (gains,)])


def solution(mesh):
    n_dev = mesh.shape['sp']

    def layer_step(x_in, positions, d_out, norm1_gain, norm2_gain, w_q, w_k, w_v, w_o, w_gate, w_up, w_down):
        tokens, model = x_in.shape
        head_dim = w_q.shape[2]
        heads = w_q.shape[1] // n_dev
        rows_own = w_q.shape[0]
        flat = lambda w: w.transpose(1, 2, 0).reshape(-1, rows_own)
        wo_own = w_o.reshape(-1, model)
        (q_rot, k_rot, v_lin, o_t, u_t, cos_tab, sin_tab, g_full, hidden,
         mlp_in, w1, w3) = attention_step(heads, x_in, positions, norm1_gain, norm2_gain, flat(w_q), flat(w_k), flat(w_v), wo_own, w_gate, w_up)
        d_w1s, d_w3s, d_down, y_out, dh_own, d_g2 = mlp_step(mlp_in, d_out, w1, w3, w_down, hidden, g_full)
        d_wo, d_wq_t, d_wk_t, d_wv_t, d_w1, d_w3, d_x, d_gains, d_down, y_out = attention_backward_step(
            heads, dh_own, wo_own, o_t, q_rot, k_rot, v_lin, (cos_tab, sin_tab),
            d_w1s, d_w3s, flat(w_q), flat(w_k), flat(w_v), u_t, x_in, g_full, d_g2, d_down, y_out)
        from_cols = lambda d, w: d.reshape(w.shape[1], w.shape[2], rows_own).transpose(2, 0, 1)
        (d_down, y_out, d_w1, d_w3, d_wo, d_wq_t, d_wk_t, d_wv_t, d_x, d_g1, d_g2) = hand_over(
            (d_down, y_out, d_w1, d_w3, d_wo, d_wq_t, d_wk_t, d_wv_t, d_x), d_gains)
        return (y_out, d_x, d_g1, d_g2, from_cols(d_wq_t, w_q), from_cols(d_wk_t, w_k), from_cols(d_wv_t, w_v),
                d_wo.reshape(w_o.shape), d_w1, d_w3, d_down)

    all_rows = P('sp')
    return jax.shard_map(layer_step, mesh=mesh, in_specs=(all_rows,) * 12, out_specs=(all_rows,) * 11, check_vma=False)
```

```python
import functools
import jax
import jax.numpy as jnp
import numpy as np
from jax import lax
from jax.experimental import pallas as pl
from jax.experimental.pallas import tpu as pltpu
from jax.sharding import PartitionSpec as P

ROPE_BASE = 10000.0
NORM_EPS = 1e-5
NEG_LARGE = -1e30
F32 = jnp.float32
BF16 = jnp.bfloat16
BLK = 256
EARLY_ROWS = 8


def dot(lhs, rhs, lhs_dim, rhs_dim):
    return lax.dot_general(lhs, rhs, (((lhs_dim,), (rhs_dim,)), ((), ())), preferred_element_type=F32)


def norm_forward(hidden, gain_vec):
    inv_rms = lax.rsqrt(jnp.mean(hidden * hidden, axis=-1, keepdims=True) + NORM_EPS)
    return hidden * inv_rms * gain_vec


def probs_transposed(k_rows, q_blk, start):
    scores = dot(k_rows, q_blk, 1, 1)
    rows = lax.broadcasted_iota(jnp.int32, (BLK, BLK), 0)
    cols = lax.broadcasted_iota(jnp.int32, (BLK, BLK), 1)
    tail = jnp.where(rows <= cols, scores[start:], NEG_LARGE)
    scores = jnp.concatenate([scores[:start], tail], axis=0) if start else tail
    top = jnp.max(scores, axis=0, keepdims=True)
    weights = jnp.exp((scores - top) * (q_blk.shape[1] ** -0.5))
    return weights * (1.0 / jnp.sum(weights, axis=0, keepdims=True))


MESH = pl.DeviceIdType.MESH


def place(axis):
    me = lax.axis_index(axis)
    core = lax.rem(me, 2)
    col = lax.rem(lax.div(me, 2), 2)
    row = lax.div(me, 4)

    def other(flip_core, flip_col, flip_row):
        pick = lambda v, f: 1 - v if f else v
        return pick(row, flip_row) * 4 + pick(col, flip_col) * 2 + pick(core, flip_core)

    nbr_x, nbr_y = other(0, 1, 0), other(0, 0, 1)
    first = nbr_x * (1 - core) + nbr_y * core
    second = nbr_y * (1 - core) + nbr_x * core
    return me, other, first, second


def greet(other):
    barrier = pltpu.get_barrier_semaphore()
    for r in range(1, 8):
        pl.semaphore_signal(barrier, inc=1, device_id=(other(r & 1, (r >> 1) & 1, r >> 2),), device_id_type=MESH)
    pl.semaphore_wait(barrier, 7)


class Gather:
    def __init__(self, slot, send_sem, recv_sem, where, seven, own=None):
        me, other, first, second = where
        partner, diag = other(1, 0, 0), other(0, 1, 1)
        own = slot(me) if own is None else own
        self.copies = []
        plan = [(own, me, first), (own, me, second), (own, me, partner), (slot(first), first, second),
                (slot(first), first, partner), (slot(second), second, partner), (slot(diag), diag, partner)]
        for i, (src, what, dest) in enumerate(plan):
            self.copies.append(pltpu.make_async_remote_copy(
                src_ref=src, dst_ref=slot(what), send_sem=send_sem.at[0], recv_sem=recv_sem.at[i],
                device_id=(dest,), device_id_type=MESH))
        self.sent = pltpu.make_async_remote_copy(
            src_ref=seven, dst_ref=seven, send_sem=send_sem.at[0], recv_sem=recv_sem.at[0],
            device_id=(partner,), device_id_type=MESH)

    def start(self):
        for i in range(3):
            self.copies[i].start()

    def got_first(self):
        self.copies[0].wait_recv()
        self.copies[3].start()
        self.copies[4].start()

    def got_second(self):
        self.copies[1].wait_recv()
        self.copies[5].start()

    def got_diag(self):
        self.copies[3].wait_recv()
        self.copies[6].start()

    def got_partner(self, i):
        self.copies[(2, 4, 5, 6)[i]].wait_recv()

    def drain(self):
        self.sent.wait_send()


def turn_halves(values, cos_blk, sin_blk):
    width = values.shape[1]
    lanes = lax.broadcasted_iota(jnp.int32, values.shape, 1)
    partner = jnp.where(lax.rem(lanes, 64) < 32, pltpu.roll(values, width - 32, 1), pltpu.roll(values, 32, 1))
    return values * cos_blk + partner * sin_blk


def norm_backward(hidden, gain, d_out):
    inv = lax.rsqrt(jnp.mean(hidden * hidden, axis=-1, keepdims=True) + NORM_EPS)
    d_scaled = d_out * gain
    d_hidden = d_scaled * inv - hidden * (inv * inv * inv * jnp.mean(d_scaled * hidden, axis=-1, keepdims=True))
    return d_hidden, jnp.sum(d_out * (hidden * inv), axis=0, keepdims=True)


def attn_bwd_comm_kernel(axis, heads, dh_hbm, wo_hbm, ot_hbm, q_hbm, k_hbm, v_hbm, cos_hbm, sin_hbm,
                         dw1_ref, dw3_ref, wq_hbm, wk_hbm, wv_hbm, ut_hbm, x_hbm, g_hbm, dg2_hbm, ddown_hbm, y_hbm, early_hbm,
                         dwo_ref, dwq_ref, dwk_ref, dwv_ref, out1_ref, out3_ref, dx_ref, dg_ref, ddown_ref, y_ref,
                         dh_own, wo_ref, ot_ref, q_ref, k_ref, v_ref, cos_ref, sin_ref, wq_ref, wk_ref, wv_ref, ut_ref, g_ref, dg2_ref,
                         pool, do_scr, dg_own, dg_all, dk_acc, dv_acc, du_acc,
                         bulk_send, bulk_recv, hg_send, hg_recv, gat_send, gat_recv, du_send, du_rsem, dg_send, dg_recv, loc_sem, ld_sem, credit):
    loads = {}
    for i, (name, src, dst) in enumerate((
            ('wo', wo_hbm, wo_ref), ('ot', ot_hbm, ot_ref), ('q', q_hbm, q_ref), ('k', k_hbm, k_ref),
            ('v', v_hbm, v_ref), ('cos', cos_hbm, cos_ref), ('sin', sin_hbm, sin_ref), ('wq', wq_hbm, wq_ref), ('wk', wk_hbm, wk_ref),
            ('wv', wv_hbm, wv_ref), ('ut', ut_hbm, ut_ref), ('g', g_hbm, g_ref), ('dg2', dg2_hbm, dg2_ref),
            ('dh', dh_hbm, dh_own), ('ddown', ddown_hbm, ddown_ref), ('y', y_hbm, y_ref))):
        loads[name] = pltpu.make_async_copy(src, dst, ld_sem.at[i])
        loads[name].start()

    def need(*names):
        for name in names:
            loads[name].wait()

    where = place(axis)
    me, other, first, second = where
    greet(other)
    seq_len, head_dim = k_ref.shape
    rows_own, hid = out1_ref.shape[0], dw1_ref.shape[1]
    tokens, model = x_hbm.shape
    qw = heads * head_dim

    rows_of = lambda d: pl.ds(pl.multiple_of(d * rows_own, rows_own), rows_own)
    hid_of = lambda d: pl.ds(pl.multiple_of(d * hid, hid), hid)
    pairs = ((dw1_ref, out1_ref), (dw3_ref, out3_ref))
    peers = [other(r & 1, (r >> 1) & 1, r >> 2) for r in (2, 4, 6, 3, 5, 7, 1)]
    bulk, parts = [], []
    for mat, (src, dst) in enumerate(pairs):
        skip = (EARLY_ROWS, 0)[mat]
        for low, high in ((skip, skip + 8), (skip + 8, rows_own // 2), (rows_own // 2, rows_own)):
            parts.append(range(len(bulk), len(bulk) + len(peers)))
            for dest in peers:
                bulk.append(pltpu.make_async_remote_copy(
                    src_ref=src.at[pl.ds(pl.multiple_of(dest * rows_own + low, 8), high - low), :],
                    dst_ref=dst.at[pl.ds(low, high - low), hid_of(me)], send_sem=bulk_send.at[mat],
                    recv_sem=bulk_recv.at[mat], device_id=(dest,), device_id_type=MESH))

    def start_bulk(*which):
        for part in which:
            for i in parts[part]:
                bulk[i].start()
    tok_of = lambda d: pl.ds(pl.multiple_of(d * tokens, tokens), tokens)
    dh_ref = pool.at[:, 0:model]
    h_gather = Gather(lambda d: dh_ref.at[tok_of(d), :], hg_send, hg_recv, where, dh_ref.at[pl.ds(0, 7 * tokens), :], own=dh_hbm)
    h_gather.start()
    start_bulk(0)
    local = [pltpu.make_async_copy(src.at[rows_of(me), :], dst.at[:, hid_of(me)], loc_sem.at[i]) for i, (src, dst) in enumerate(pairs)]
    for copy in local:
        copy.start()
    for dest in peers:
        pltpu.make_async_copy(early_hbm.at[:, hid_of(dest)], out1_ref.at[0:EARLY_ROWS, hid_of(dest)], loc_sem.at[2]).start()
    need('dh', 'wo', 'ot')
    pool[tok_of(me), 0:model] = dh_own[...]
    h_gather.got_first()
    h_gather.got_second()
    start_bulk(1, 2)
    h_gather.got_diag()
    for i in range(4):
        h_gather.got_partner(i)

    def split_out_grad(k, _):
        rows = pl.ds(pl.multiple_of(k * BLK, BLK), BLK)
        do_blk = dot(pool[rows, 0:model], wo_ref[...], 1, 1).astype(BF16)
        for h in range(heads):
            do_scr[h, rows, :] = do_blk[:, h * head_dim:(h + 1) * head_dim]
        cols = rows
        dwo_ref[:, cols] = dot(ot_ref[...], pool[:, cols], 1, 0)
        return 0
    lax.fori_loop(0, seq_len // BLK, split_out_grad, 0)
    h_gather.drain()
    for i, device in enumerate((first, second, other(1, 0, 0))):
        pl.semaphore_signal(credit.at[i], inc=1, device_id=(device,), device_id_type=MESH)
    x_ref = wo_ref
    x_load = pltpu.make_async_copy(x_hbm, x_ref, ld_sem.at[16])
    x_load.start()


    need('q', 'k', 'v')
    dk_acc[...] = jnp.zeros_like(dk_acc)
    dv_acc[...] = jnp.zeros_like(dv_acc)
    slot_cols = lambda d, off, width: pl.ds(pl.multiple_of(d * 384 + off, 128), width)

    def one_head(h, _):
        def one_block(start):
            keys = pl.ds(0, start + BLK)
            rows = pl.ds(start, BLK)
            q_blk, do_blk = q_ref[h, rows, :], do_scr[h, rows, :]
            probs = probs_transposed(k_ref[keys, :], q_blk, start)
            d_probs = dot(v_ref[keys, :], do_blk, 1, 1).astype(BF16).astype(F32)
            row_dot = jnp.sum(d_probs * probs, axis=0, keepdims=True)
            d_scores = (probs * (d_probs - row_dot) * (head_dim ** -0.5)).astype(BF16)
            do_scr[h, rows, :] = dot(d_scores, k_ref[keys, :], 0, 0).astype(BF16)
            dk_acc[keys, :] += dot(d_scores, q_blk, 1, 0)
            dv_acc[keys, :] += dot(probs.astype(BF16), do_blk, 1, 0)
        for start in range(0, seq_len, BLK):
            one_block(start)
        return 0
    lax.fori_loop(0, heads, one_head, 0)
    need('cos', 'sin')
    low = lax.broadcasted_iota(jnp.int32, (BLK, 128), 1) < head_dim

    def turn_back(k, _):
        rows = pl.ds(pl.multiple_of(k * BLK, BLK), BLK)
        cos_blk, sin_blk = cos_ref[rows, :], -sin_ref[rows, :]
        for pair in range(heads // 2):
            both = jnp.concatenate([do_scr[2 * pair, rows, :], do_scr[2 * pair + 1, rows, :]], axis=1)
            pool[rows, slot_cols(me, pair * 128, 128)] = turn_halves(both.astype(F32), cos_blk, sin_blk).astype(BF16)
        kv = jnp.concatenate([dk_acc[rows, :], dv_acc[rows, :]], axis=1).astype(BF16).astype(F32)
        pool[rows, slot_cols(me, qw, 128)] = jnp.where(low, turn_halves(kv, cos_blk, sin_blk), kv).astype(BF16)
        return 0
    lax.fori_loop(0, seq_len // BLK, turn_back, 0)

    gather = Gather(lambda d: pool.at[:, slot_cols(d, 0, 384)], gat_send, gat_recv, where, pool.at[:, pl.ds(0, 7 * 384)])
    for i in range(3):
        pl.semaphore_wait(credit.at[i], 1)
    gather.start()
    start_bulk(3)
    du_acc[...] = jnp.zeros_like(du_acc)
    need('wq', 'wk', 'wv', 'ut')

    def use(d):
        q_rows = pl.ds(pl.multiple_of(d * qw, qw), qw)
        kv_rows = pl.ds(pl.multiple_of(d * head_dim, head_dim), head_dim)
        w_all = jnp.concatenate([wq_ref[q_rows, :], wk_ref[kv_rows, :], wv_ref[kv_rows, :]], axis=0)

        def add_rows(k, _):
            rows = pl.ds(pl.multiple_of(k * 512, 512), 512)
            du_acc[rows, :] += dot(pool[rows, slot_cols(d, 0, 384)], w_all, 1, 0)
            return 0
        lax.fori_loop(0, seq_len // 512, add_rows, 0)
        d_w = dot(ut_ref[...], pool[:, slot_cols(d, 0, 384)], 1, 0).T
        dwq_ref[q_rows, :] = d_w[:qw]
        dwk_ref[kv_rows, :] = d_w[qw:qw + head_dim]
        dwv_ref[kv_rows, :] = d_w[qw + head_dim:]

    def use_many(*devices):
        def body(i, _):
            d = devices[0]
            for n in range(1, len(devices)):
                d = jnp.where(i == n, devices[n], d)
            use(d)
            return 0
        lax.fori_loop(0, len(devices), body, 0)

    use_many(me)
    gather.got_first()
    gather.got_second()
    start_bulk(4)
    gather.got_partner(0)
    use_many(first, second, other(1, 0, 0))
    gather.got_diag()
    for i in range(1, 4):
        gather.got_partner(i)
    use_many(other(0, 1, 1), other(1, 1, 0), other(1, 0, 1), other(1, 1, 1))
    gather.drain()
    du_scr = pool.at[:, 0:rows_own]

    def round_du(k, _):
        rows = pl.ds(pl.multiple_of(k * BLK, BLK), BLK)
        pool[rows, 0:rows_own] = du_acc[rows, :].astype(BF16)
        return 0
    lax.fori_loop(0, seq_len // BLK, round_du, 0)
    for dest in peers:
        pltpu.make_async_remote_copy(
            src_ref=du_scr.at[tok_of(dest), :], dst_ref=ot_ref.at[:, rows_of(me)], send_sem=du_send.at[0],
            recv_sem=du_rsem.at[0], device_id=(dest,), device_id_type=MESH).start()
    start_bulk(5)
    ot_ref[:, rows_of(me)] = pool[tok_of(me), 0:rows_own]
    need('g', 'dg2')
    x_load.wait()
    got = ot_ref.at[:, pl.ds(0, 7 * rows_own)]
    pltpu.make_async_copy(got, got, du_rsem.at[0]).wait()
    dg_own[...] = jnp.zeros_like(dg_own)
    dg_own[1:2, :] = dg2_ref[...]

    def input_grad(k, _):
        part = pl.ds(pl.multiple_of(k * 16, 16), 16)
        d_norm, d_gain = norm_backward(x_ref[part, :].astype(F32), g_ref[0:1, :], ot_ref[part, :].astype(F32))
        dh_part = dh_own[part, :]
        dx_ref[part, :] = (dh_part.astype(F32) + d_norm).astype(BF16)
        dg_own[0:1, :] += d_gain
        return 0
    lax.fori_loop(0, tokens // 16, input_grad, 0)
    for dest in peers:
        pltpu.make_async_remote_copy(
            src_ref=dg_own.at[:, rows_of(dest)], dst_ref=dg_all.at[me], send_sem=dg_send.at[0],
            recv_sem=dg_recv.at[0], device_id=(dest,), device_id_type=MESH).start()
    dg_all[me] = dg_own[:, rows_of(me)]
    got = dg_all.at[pl.ds(0, 7)]
    pltpu.make_async_copy(got, got, dg_recv.at[0]).wait()
    dg_ref[...] = jnp.sum(dg_all[...], axis=0)
    for sent, sem in ((du_scr.at[pl.ds(0, 7 * tokens), :], du_send), (dg_own.at[:, pl.ds(0, 7 * rows_own)], dg_send)):
        pltpu.make_async_copy(sent, sent, sem.at[0]).wait()
    need('ddown', 'y')
    for mat, (src, dst) in enumerate(pairs):
        rows = rows_own - (EARLY_ROWS, 0)[mat]
        sent, got = src.at[pl.ds(0, 7 * rows), :], dst.at[0:rows, pl.ds(0, 7 * hid)]
        pltpu.make_async_copy(sent, sent, bulk_send.at[mat]).wait()
        pltpu.make_async_copy(got, got, bulk_recv.at[mat]).wait()
    for copy in local:
        copy.wait()
    seven = out1_ref.at[0:EARLY_ROWS, pl.ds(0, 7 * hid)]
    pltpu.make_async_copy(seven, seven, loc_sem.at[2]).wait()


def attention_backward_step(heads, dh_own, wo_own, o_t, q_rot, k_rot, v_lin, tables, d_w1, d_w3, w_q, w_k, w_v, u_t, x_in, gains, d_g2, d_down, y_out, early_rows):
    seq_len, model = k_rot.shape[0], x_in.shape[1]
    head_dim = k_rot.shape[1]
    tokens = x_in.shape[0]
    rows_own, hid = model // 8, d_w1.shape[1]
    shape = jax.ShapeDtypeStruct
    hbm = pl.BlockSpec(memory_space=pl.ANY)
    dma = pltpu.SemaphoreType.DMA
    vm = lambda *dims, dtype=BF16: pltpu.VMEM(dims, dtype)
    early = (dh_own, wo_own, o_t, q_rot, k_rot, v_lin, *tables)
    late = (w_q, w_k, w_v, u_t, x_in, gains, d_g2)
    outs = [(wo_own.shape, F32), (w_q.shape, F32), (w_k.shape, F32), (w_v.shape, F32), ((rows_own, 8 * hid), F32),
            ((rows_own, 8 * hid), F32), (x_in.shape, BF16), ((8, rows_own), F32), (d_down.shape, F32), (y_out.shape, BF16)]
    vmem, far = pl.BlockSpec(memory_space=pltpu.VMEM), pl.BlockSpec(memory_space=pltpu.HBM)
    return pl.pallas_call(
        functools.partial(attn_bwd_comm_kernel, 'sp', heads), name='attn_bwd_comm',
        in_specs=[hbm] * 17 + [far] * 3, out_specs=[vmem] * 10,
        out_shape=[pltpu.VMEM(dims, dtype) for dims, dtype in outs],
        scratch_shapes=[vm(*t.shape, dtype=t.dtype) for t in early + late[:4] + late[5:]] + [
            vm(seq_len, 8 * 384), vm(heads, seq_len, head_dim),
            vm(8, model, dtype=F32), vm(8, 8, rows_own, dtype=F32),
            vm(seq_len, head_dim, dtype=F32), vm(seq_len, head_dim, dtype=F32),
            vm(seq_len, rows_own, dtype=F32),
            dma((2,)), dma((2,)), dma((1,)), dma((7,)), dma((1,)), dma((7,)), dma((1,)), dma((1,)), dma((1,)), dma((1,)), dma((3,)), dma((17,)), pltpu.SemaphoreType.REGULAR((3,))],
        compiler_params=pltpu.CompilerParams(collective_id=2, has_side_effects=True, vmem_limit_bytes=34340864),
    )(*early, d_w1, d_w3, *late, *[pltpu.with_memory_space_constraint(a, pltpu.HBM) for a in (d_down, y_out, early_rows)])


def mlp_comm_kernel(axis, m_ref, dout_own, w1_hbm, w3_hbm, w2_hbm, h_hbm, g_hbm,
                    dw1_ref, dw3_ref, dw2_ref, y_hbm, dh_hbm, dg2_hbm, early_ref, dout_ref,
                    w1_ref, w3_ref, w2_ref, h_ref, g_ref, y_ref, dg2_ref,
                    glu, gate_s, up_s, outbox, chip_sum, inbox, blk, m_col, do_col, mt_scr, dot_scr, st1, st3, st2, dh_own,
                    part_send, part_recv, mail_send, mail_recv, do_send, do_recv,
                    in_sem, col_sem, out_sem, own_sem, ld_sem, early_sem, credit):
    loads = [pltpu.make_async_copy(src, dst, ld_sem.at[i]) for i, (src, dst) in enumerate((
        (w1_hbm, w1_ref), (w3_hbm, w3_ref), (w2_hbm, w2_ref), (h_hbm, h_ref), (g_hbm, g_ref)))]
    own_in = pltpu.make_async_copy(dout_own, dh_own, own_sem.at[0])
    for copy in loads + [own_in]:
        copy.start()
    where = place(axis)
    me, other, first, second = where
    core = lax.rem(me, 2)
    partner = other(1, 0, 0)
    tokens, model = h_ref.shape
    hid = w1_ref.shape[1]
    tok_of = lambda d: pl.ds(pl.multiple_of(d * tokens, tokens), tokens)
    off_first, off_second = 1 + core, 2 - core

    def block_of(off, flip):
        d_col, d_row = lax.rem(off, 2), lax.div(off, 2)
        col, row = lax.rem(lax.div(me, 2), 2), lax.div(me, 4)
        mix = lambda v, f: v + f - 2 * v * f
        return mix(row, d_row) * 4 + mix(col, d_col) * 2 + mix(core, flip)

    def step_off(step, flip):
        mid_a = off_second * (1 - flip) + off_first * flip
        mid_b = off_first * (1 - flip) + off_second * flip
        return jnp.where(step == 0, 3, jnp.where(step == 1, mid_a, jnp.where(step == 2, mid_b, 0)))

    def half_rows(half):
        flip = 1 - lax.rem(half, 2)
        return tok_of(block_of(step_off(lax.div(half, 2), flip), flip))

    def fetch(half):
        slot = lax.rem(half, 2)
        return pltpu.make_async_copy(m_ref.at[half_rows(half), :], blk.at[slot], in_sem.at[slot])

    def fetch_dout(d):
        slot = lax.rem(d, 2)
        return pltpu.make_async_copy(dout_ref.at[tok_of(d), :], blk.at[slot], in_sem.at[slot])

    def fetch_cols(j):
        cols = pl.ds(pl.multiple_of(j * 256, 256), 256)
        return (pltpu.make_async_copy(m_ref.at[:, cols], m_col, col_sem.at[0]),
                pltpu.make_async_copy(dout_ref.at[:, cols], do_col, col_sem.at[1]))

    def sigmoid(value):
        return 1.0 / (1.0 + jnp.exp(-value))

    def activations(slot, rows):
        def chunk(j, _):
            cols = pl.ds(pl.multiple_of(j * 512, 512), 512)
            gate = dot(blk[slot], w1_ref[:, cols], 1, 0).astype(BF16)
            up = dot(blk[slot], w3_ref[:, cols], 1, 0).astype(BF16)
            gate_s[rows, cols] = gate
            up_s[rows, cols] = up
            gate = gate.astype(F32)
            glu[rows, cols] = (gate * sigmoid(gate) * up.astype(F32)).astype(BF16)
            return 0
        lax.fori_loop(0, hid // 512, chunk, 0)

    def activation_grads(slot, rows):
        def chunk(j, _):
            cols = pl.ds(pl.multiple_of(j * 512, 512), 512)
            d_act = dot(blk[slot], w2_ref[cols, :], 1, 1).astype(BF16).astype(F32)
            gate, up = gate_s[rows, cols].astype(F32), up_s[rows, cols].astype(F32)
            sig = sigmoid(gate)
            silu = gate * sig
            up_s[rows, cols] = (d_act * silu).astype(BF16)
            gate_s[rows, cols] = (d_act * up * (sig + silu * (1.0 - sig))).astype(BF16)
            return 0
        lax.fori_loop(0, hid // 512, chunk, 0)

    def add_mlp_grad(rows, put):
        def chunk(j, _):
            cols = pl.ds(pl.multiple_of(j * 512, 512), 512)
            put(cols, dot(gate_s[rows, :], w1_ref[cols, :], 1, 1) + dot(up_s[rows, :], w3_ref[cols, :], 1, 1))
            return 0
        lax.fori_loop(0, model // 512, chunk, 0)

    def add_mlp_out(rows, put):
        def chunk(j, _):
            cols = pl.ds(pl.multiple_of(j * 512, 512), 512)
            put(cols, dot(glu[rows, :], w2_ref[:, cols], 1, 0))
            return 0
        lax.fori_loop(0, model // 512, chunk, 0)

    def signal(index, device):
        pl.semaphore_signal(credit.at[index], inc=1, device_id=(device,), device_id_type=MESH)

    class Scatter:
        def __init__(self, turn):
            self.turn = turn

        def to_partner(self, step):
            off = step_off(step, 1)
            return pltpu.make_async_remote_copy(
                src_ref=outbox.at[lax.rem(step, 2)], dst_ref=chip_sum.at[off], send_sem=part_send.at[self.turn, step],
                recv_sem=part_recv.at[self.turn, off], device_id=(partner,), device_id_type=MESH)

        def from_partner(self, off):
            return pltpu.make_async_remote_copy(
                src_ref=outbox.at[0], dst_ref=chip_sum.at[off], send_sem=part_send.at[self.turn, 0],
                recv_sem=part_recv.at[self.turn, off], device_id=(partner,), device_id_type=MESH)

        def mail(self, kind):
            off = (3, off_first, off_second)[kind]
            dest = (first, first, second)[kind]
            return pltpu.make_async_remote_copy(
                src_ref=chip_sum.at[off], dst_ref=inbox.at[kind], send_sem=mail_send.at[self.turn, kind],
                recv_sem=mail_recv.at[self.turn, kind], device_id=(dest,), device_id_type=MESH)

        def step(self, step, prepare, partial):
            self.first_half(step, prepare, partial)
            self.second_half(step, prepare, partial)

        def first_half(self, step, prepare, partial):
            slot = lax.rem(step, 2)
            prepare(2 * step)

            def put_out(cols, value):
                outbox[slot, :, cols] = value
            partial(half_rows(2 * step), put_out)

        def second_half(self, step, prepare, partial):
            self.to_partner(step).start()
            prepare(2 * step + 1)
            off = step_off(step, 0)
            self.from_partner(off).wait_recv()

            def put_sum(cols, value):
                chip_sum[off, :, cols] += value
            partial(half_rows(2 * step + 1), put_sum)

        def pass_on(self):
            self.mail(0).wait_recv()

            def add_mail(k, _):
                part = pl.ds(pl.multiple_of(k * 16, 16), 16)
                chip_sum[off_second, part, :] += inbox[0, part, :]
                return 0
            lax.fori_loop(0, tokens // 16, add_mail, 0)

    out_round, grad_round = Scatter(0), Scatter(1)

    def prepare_out(half):
        @pl.when(half < 7)
        def _():
            fetch(half + 1).start()
        fetch(half).wait()
        activations(lax.rem(half, 2), half_rows(half))

    def weight_grads(begin, end):
        for copy in fetch_cols(begin):
            copy.start()

        def body(j, _):
            for copy in fetch_cols(j):
                copy.wait()

            def turn(k, _):
                part = pl.ds(pl.multiple_of(k * 256, 256), 256)
                mt_scr[:, part] = m_col[part, :].T
                dot_scr[:, part] = do_col[part, :].T
                return 0
            lax.fori_loop(0, m_col.shape[0] // 256, turn, 0)

            @pl.when(j + 1 < end)
            def _():
                for copy in fetch_cols(j + 1):
                    copy.start()
            rows = pl.ds(pl.multiple_of(j * 256, 256), 256)
            out = (pltpu.make_async_copy(st1, dw1_ref.at[rows, :], out_sem.at[0]),
                   pltpu.make_async_copy(st3, dw3_ref.at[rows, :], out_sem.at[1]),
                   pltpu.make_async_copy(st2, dw2_ref.at[:, rows], out_sem.at[2]))

            @pl.when(j > begin)
            def _():
                for copy in out:
                    copy.wait()

            def chunk(k, _):
                cols = pl.ds(pl.multiple_of(k * 512, 512), 512)
                st1[:, cols] = dot(mt_scr[...], gate_s[:, cols], 1, 0)
                st3[:, cols] = dot(mt_scr[...], up_s[:, cols], 1, 0)
                st2[cols, :] = dot(dot_scr[...], glu[:, cols], 1, 0).T
                return 0
            lax.fori_loop(0, hid // 512, chunk, 0)
            for copy in out:
                copy.start()
            return 0
        lax.fori_loop(begin, end, body, 0)
        rows = pl.ds((end - 1) * 256, 256)
        for copy in (pltpu.make_async_copy(st1, dw1_ref.at[rows, :], out_sem.at[0]),
                     pltpu.make_async_copy(st3, dw3_ref.at[rows, :], out_sem.at[1]),
                     pltpu.make_async_copy(st2, dw2_ref.at[:, rows], out_sem.at[2])):
            copy.wait()

    fetch(0).start()
    greet(other)
    do_gather = Gather(lambda d: dout_ref.at[tok_of(d), :], do_send, do_recv, where, dout_ref.at[pl.ds(0, 7 * tokens), :], own=dout_own)
    do_gather.start()
    own_in.wait()
    own_out = pltpu.make_async_copy(dh_own, dout_ref.at[tok_of(me), :], own_sem.at[1])
    own_out.start()
    for copy in loads:
        copy.wait()

    def out_step(step, _):
        @pl.when(step >= 2)
        def _():
            out_round.to_partner(step - 2).wait_send()
        out_round.step(step, prepare_out, add_mlp_out)

        @pl.when(step == 0)
        def _():
            out_round.mail(0).start()

        @pl.when(step == 2)
        def _():
            out_round.mail(1).start()
            do_gather.got_first()
            do_gather.got_second()
        return 0
    lax.fori_loop(0, 4, out_step, 0)
    out_round.pass_on()
    out_round.mail(2).start()
    for step in (2, 3):
        out_round.to_partner(step).wait_send()
    out_round.mail(0).wait_send()
    signal(0, partner)
    signal(1, first)
    do_gather.got_diag()
    for i in range(4):
        do_gather.got_partner(i)
    own_out.wait()
    fetch_dout(0).start()

    def grad_block(d, _):
        @pl.when(d < 7)
        def _():
            fetch_dout(d + 1).start()
        fetch_dout(d).wait()
        activation_grads(lax.rem(d, 2), tok_of(d))
        return 0
    lax.fori_loop(0, 8, grad_block, 0)

    as_is = lambda half: None
    grad_round.first_half(0, as_is, add_mlp_grad)
    pl.semaphore_wait(credit.at[0], 1)
    grad_round.second_half(0, as_is, add_mlp_grad)
    pl.semaphore_wait(credit.at[1], 1)
    grad_round.mail(0).start()
    weight_grads(0, 2)
    grad_round.first_half(1, as_is, add_mlp_grad)
    out_round.mail(1).wait_recv()
    out_round.mail(2).wait_recv()

    def layer_out(k, _):
        part = pl.ds(pl.multiple_of(k * 16, 16), 16)
        y_ref[part, :] = (h_ref[part, :].astype(F32) + (chip_sum[0, part, :] + inbox[1, part, :] + inbox[2, part, :])).astype(BF16)
        return 0
    lax.fori_loop(0, tokens // 16, layer_out, 0)
    y_store = pltpu.make_async_copy(y_ref, y_hbm, own_sem.at[2])
    y_store.start()
    out_round.mail(1).wait_send()
    out_round.mail(2).wait_send()
    signal(2, partner)
    signal(3, first)
    signal(4, second)
    pl.semaphore_wait(credit.at[2], 1)

    grad_round.second_half(1, as_is, add_mlp_grad)

    def grad_step(step, _):
        grad_round.to_partner(step - 2).wait_send()
        grad_round.step(step, as_is, add_mlp_grad)

        @pl.when(step == 2)
        def _():
            pl.semaphore_wait(credit.at[3], 1)
            grad_round.mail(1).start()
            grad_round.pass_on()
            pl.semaphore_wait(credit.at[4], 1)
            grad_round.mail(2).start()
        return 0
    lax.fori_loop(2, 4, grad_step, 0)
    weight_grads(2, 8)
    rows = early_ref.shape[0]
    for r in (2, 4, 6, 3, 5, 7, 1):
        dest = other(r & 1, (r >> 1) & 1, r >> 2)
        pltpu.make_async_remote_copy(
            src_ref=dw1_ref.at[pl.ds(pl.multiple_of(dest * 256, 256), rows), :],
            dst_ref=early_ref.at[:, pl.ds(pl.multiple_of(me * hid, hid), hid)], send_sem=early_sem.at[0],
            recv_sem=early_sem.at[1], device_id=(dest,), device_id_type=MESH).start()
    grad_round.mail(1).wait_recv()
    grad_round.mail(2).wait_recv()
    dg2_ref[...] = jnp.zeros_like(dg2_ref)

    def hidden_grad(k, _):
        part = pl.ds(pl.multiple_of(k * 16, 16), 16)
        d_mlp = (chip_sum[0, part, :] + inbox[1, part, :] + inbox[2, part, :]).astype(BF16).astype(F32)
        d_norm, d_gain = norm_backward(h_ref[part, :].astype(F32), g_ref[1:2, :], d_mlp)
        dh_own[part, :] = (dh_own[part, :].astype(F32) + d_norm).astype(BF16)
        dg2_ref[...] += d_gain
        return 0
    lax.fori_loop(0, tokens // 16, hidden_grad, 0, unroll=4)
    own_out = pltpu.make_async_copy(dh_own, dh_hbm, own_sem.at[3])
    own_out.start()
    dg2_store = pltpu.make_async_copy(dg2_ref, dg2_hbm, own_sem.at[4])
    dg2_store.start()
    for step in (2, 3):
        grad_round.to_partner(step).wait_send()
    for kind in range(3):
        grad_round.mail(kind).wait_send()
    seven = early_ref.at[:, pl.ds(0, 7 * hid)]
    for i in range(2):
        pltpu.make_async_copy(seven, seven, early_sem.at[i]).wait()
    do_gather.drain()
    own_out.wait()
    y_store.wait()
    dg2_store.wait()


def mlp_step(m_all, d_out, w1, w3, w2, hidden, gains):
    seq_len, model = m_all.shape
    hid, tokens = w1.shape[1], hidden.shape[0]
    shape = jax.ShapeDtypeStruct
    hbm = pl.BlockSpec(memory_space=pl.ANY)
    dma = pltpu.SemaphoreType.DMA
    vm = lambda *dims, dtype=BF16: pltpu.VMEM(dims, dtype)
    return pl.pallas_call(
        functools.partial(mlp_comm_kernel, 'sp'), name='mlp_comm',
        in_specs=[hbm] * 7, out_specs=[hbm] * 8,
        out_shape=[shape((model, hid), F32), shape((model, hid), F32), shape((hid, model), F32),
                   shape(hidden.shape, BF16), shape(hidden.shape, BF16), shape((1, model), F32), shape((EARLY_ROWS, 8 * hid), F32),
                   shape((seq_len, model), BF16)],
        scratch_shapes=[vm(*t.shape, dtype=t.dtype) for t in (w1, w3, w2, hidden, gains)] + [
            vm(tokens, model), vm(1, model, dtype=F32),
            vm(seq_len, hid), vm(seq_len, hid), vm(seq_len, hid),
            vm(2, tokens, model, dtype=F32), vm(4, tokens, model, dtype=F32), vm(3, tokens, model, dtype=F32),
            vm(2, tokens, model), vm(seq_len, 256), vm(seq_len, 256), vm(256, seq_len), vm(256, seq_len),
            vm(256, hid, dtype=F32), vm(256, hid, dtype=F32), vm(hid, 256, dtype=F32), vm(tokens, model),
            dma((2, 4)), dma((2, 4)), dma((2, 3)), dma((2, 3)), dma((1,)), dma((7,)),
            dma((2,)), dma((2,)), dma((3,)), dma((5,)), dma((5,)), dma((2,)), pltpu.SemaphoreType.REGULAR((5,))],
        compiler_params=pltpu.CompilerParams(collective_id=1, has_side_effects=True, vmem_limit_bytes=63 * 1024 * 1024),
    )(m_all, d_out, w1, w3, w2, hidden, gains)[:7]


def spread_tables(packed, upper):
    lanes = lax.broadcasted_iota(jnp.int32, packed.shape, 1)
    swapped = pltpu.roll(packed, 64, 1)
    both = jnp.where((lanes < 64) != upper, packed, swapped)
    low = lax.rem(lanes, 64) < 32
    return jnp.where(low, both, pltpu.roll(both, 32, 1)), jnp.where(low, -pltpu.roll(both, 96, 1), both)


def attention_comm_kernel(axis, heads, x_ref, pos_hbm, gain1_hbm, gain2_hbm, freq_hbm, wq_ref, wk_ref, wv_ref, wo_ref, wg_ref, wu_ref,
                          q_hbm, k_hbm, v_hbm, ot_hbm, ut_hbm, cos_hbm, sin_hbm, gfull_hbm, h_hbm, m_ref, w1_ref, w3_ref,
                          q_ref, k_ref, v_ref, ot_ref, ut_ref, cos_ref, sin_ref, gfull_ref, h_ref, pos_ref, gain1_ref, gain2_ref, freq_ref, gain_ref, x_all, gain_all, w_head, wo_all, o_all, u_blk, qkv_blk, o_scr, o_own, h_scr, m_out, stage,
                          g_send, g_recv, w_send, w_recv, x_send, x_recv, wo_send, wo_recv, bulk_send, bulk_recv,
                          o_send, o_recv, m_loc, m_send, m_recv, loc_sem, own_sem, st_sem):
    tiny = [pltpu.make_async_copy(src, dst, own_sem.at[8 + i]) for i, (src, dst) in enumerate((
        (gain1_hbm, gain1_ref), (gain2_hbm, gain2_ref), (pos_hbm, pos_ref), (freq_hbm, freq_ref)))]
    for copy in tiny:
        copy.start()
    where = place(axis)
    me, other, first, second = where
    core = lax.rem(me, 2)
    partner = other(1, 0, 0)
    greet(other)
    tokens, model = x_ref.shape
    seq_len, head_dim = k_ref.shape
    qw = heads * head_dim
    rows_own, hid = wg_ref.shape[0], w1_ref.shape[1]
    tok_of = lambda d: pl.ds(pl.multiple_of(d * tokens, tokens), tokens)
    cols_of = lambda d: pl.ds(pl.multiple_of(d * rows_own, rows_own), rows_own)
    hid_of = lambda d: pl.ds(pl.multiple_of(d * hid, hid), hid)
    peers = [other(r & 1, (r >> 1) & 1, r >> 2) for r in (6, 2, 4, 7, 3, 5, 1)]

    def to_all(src_of, dst, seven, sems):
        copies = [pltpu.make_async_remote_copy(
            src_ref=src_of(dest), dst_ref=dst, send_sem=sems[0], recv_sem=sems[1],
            device_id=(dest,), device_id_type=MESH) for dest in peers]
        for copy in copies:
            copy.start()
        return pltpu.make_async_remote_copy(src_ref=seven, dst_ref=seven, send_sem=sems[0], recv_sem=sems[1],
                                            device_id=(partner,), device_id_type=MESH)

    q_of = lambda d: pl.ds(pl.multiple_of(d * qw, qw), qw)
    kv_of = lambda d: pl.ds(pl.multiple_of(d * head_dim, head_dim), head_dim)
    seven_rows = pl.ds(0, 7 * rows_own)
    slices = []
    for i, (src, rows, low, high) in enumerate(((wq_ref, q_of, 0, qw), (wk_ref, kv_of, qw, qw + head_dim),
                                                (wv_ref, kv_of, qw + head_dim, qw + 2 * head_dim))):
        slices.append(to_all(lambda dest: src.at[rows(dest), :], w_head.at[low:high, cols_of(me)],
                             w_head.at[low:high, seven_rows], (w_send.at[i], w_recv.at[i])))
    x_gather = Gather(lambda d: x_all.at[tok_of(d), :], x_send, x_recv, where, x_all.at[pl.ds(0, 7 * tokens), :], own=x_ref)
    x_gather.start()
    for copy in tiny:
        copy.wait()
    gain_ref[...] = jnp.zeros_like(gain_ref)
    gain_ref[0:1, :] = gain1_ref[...].astype(F32).reshape(1, -1)
    gain_ref[1:2, :] = gain2_ref[...].astype(F32).reshape(1, -1)
    gain_ref[2:3, :] = pos_ref[...].astype(F32).reshape(1, -1)
    small = [to_all(lambda dest: gain_ref, gain_all.at[me], gain_all.at[pl.ds(0, 7)], (g_send.at[0], g_recv.at[0]))]
    wo_gather = Gather(lambda d: wo_all.at[cols_of(d), :], wo_send, wo_recv, where, wo_all.at[pl.ds(0, 7 * rows_own), :], own=wo_ref)
    bulk, parts = [], []
    quarter = rows_own // 4
    for mat, (src, dst) in enumerate(((wg_ref, w1_ref), (wu_ref, w3_ref))):
        for low, high in ((0, 16), (16, quarter), (quarter, 2 * quarter), (2 * quarter, 3 * quarter), (3 * quarter, rows_own)):
            parts.append(range(len(bulk), len(bulk) + len(peers)))
            for dest in peers:
                bulk.append(pltpu.make_async_remote_copy(
                    src_ref=src.at[pl.ds(low, high - low), hid_of(dest)],
                    dst_ref=dst.at[pl.ds(pl.multiple_of(me * rows_own + low, 16), high - low), :],
                    send_sem=bulk_send.at[mat], recv_sem=bulk_recv.at[mat], device_id=(dest,), device_id_type=MESH))

    def start_bulk(*which):
        for part in which:
            for i in parts[part]:
                bulk[i].start()
    start_bulk(0)

    stores = [pltpu.make_async_copy(src, dst, st_sem.at[i]) for i, (src, dst) in enumerate((
        (q_ref, q_hbm), (k_ref, k_hbm), (v_ref, v_hbm), (ot_ref, ot_hbm), (ut_ref, ut_hbm), (cos_ref, cos_hbm),
        (sin_ref, sin_hbm), (gfull_ref, gfull_hbm), (h_ref, h_hbm)))]
    own = [pltpu.make_async_copy(src, dst, own_sem.at[i]) for i, (src, dst) in enumerate((
        (gain_ref, gain_all.at[me]), (wq_ref.at[q_of(me), :], w_head.at[0:qw, cols_of(me)]),
        (wk_ref.at[kv_of(me), :], w_head.at[qw:qw + head_dim, cols_of(me)]),
        (wv_ref.at[kv_of(me), :], w_head.at[qw + head_dim:, cols_of(me)]),
        (x_ref, x_all.at[tok_of(me), :]), (wo_ref, wo_all.at[cols_of(me), :])))]
    for copy in own:
        copy.start()
    local = []
    for i, (src, dst) in enumerate(((wg_ref, w1_ref), (wu_ref, w3_ref))):
        local.append((pltpu.make_async_copy(src.at[:, hid_of(me)], stage.at[i], loc_sem.at[i]),
                      pltpu.make_async_copy(stage.at[i], dst.at[cols_of(me), :], loc_sem.at[2 + i])))
        local[-1][0].start()
    for load, store in local:
        load.wait()
        store.start()
    for copy in own:
        copy.wait()
    for copy in small:
        copy.wait_recv()
    for d in range(8):
        gfull_ref[:, d * rows_own:(d + 1) * rows_own] = gain_all[d]
    for copy in slices:
        copy.wait_recv()

    def use(d):
        base = pl.multiple_of(d * tokens, tokens)

        def norm(k, _):
            part = pl.ds(pl.multiple_of(k * 16, 16), 16)
            x_part = x_all[pl.ds(pl.multiple_of(base + k * 16, 16), 16), :].astype(F32)
            u_blk[part, :] = norm_forward(x_part, gfull_ref[0:1, :]).astype(BF16)
            return 0
        lax.fori_loop(0, tokens // 16, norm, 0)
        ut_ref[:, tok_of(d)] = u_blk[:, cols_of(me)].T
        qkv_blk[...] = dot(u_blk[...], w_head[...], 1, 1).astype(BF16)
        half = tokens // 2
        where_to = gain_all[d, 2:3, :]
        lanes = lax.broadcasted_iota(jnp.int32, (half, 2 * head_dim), 1)
        by_row = lambda lo: jnp.broadcast_to(where_to[:, lo:lo + half], (2 * head_dim, half)).T
        angles = jnp.where(lanes < head_dim, by_row(0), by_row(half)) * freq_ref[...]
        packed = jnp.where(lax.rem(lanes, head_dim) < head_dim // 2, jnp.cos(angles), jnp.sin(angles))
        for part in range(2):
            rows = pl.ds(pl.multiple_of(base + part * half, half), half)
            cos_blk, sin_blk = spread_tables(packed, part == 1)
            cos_ref[rows, :] = cos_blk
            sin_ref[rows, :] = sin_blk
            source = slice(part * half, (part + 1) * half)
            for pair in range(heads // 2):
                turned = turn_halves(qkv_blk[source, pair * 128:(pair + 1) * 128].astype(F32), cos_blk, sin_blk).astype(BF16)
                q_ref[2 * pair, rows, :] = turned[:, :head_dim]
                q_ref[2 * pair + 1, rows, :] = turned[:, head_dim:]
            turned = turn_halves(qkv_blk[source, qw:].astype(F32), cos_blk, sin_blk).astype(BF16)
            k_ref[rows, :] = turned[:, :head_dim]
            v_ref[rows, :] = qkv_blk[source, qw + head_dim:]

    x_gather.got_first()
    x_gather.got_second()
    wo_gather.start()
    start_bulk(1, 2, 3)
    x_gather.got_partner(0)

    def use_near(i, _):
        use(jnp.where(i == 0, me, jnp.where(i == 1, first, jnp.where(i == 2, second, partner))))
        return 0
    lax.fori_loop(0, 4, use_near, 0)
    x_gather.got_diag()
    for i in range(1, 4):
        x_gather.got_partner(i)

    def use_far(i, _):
        use(jnp.where(i == 0, other(0, 1, 1), jnp.where(i == 1, other(1, 1, 0), jnp.where(i == 2, other(1, 0, 1), other(1, 1, 1)))))
        return 0
    lax.fori_loop(0, 4, use_far, 0)

    def one_head(h, _):
        for start in range(0, seq_len, BLK):
            keys, rows = pl.ds(0, start + BLK), pl.ds(start, BLK)
            probs = probs_transposed(k_ref[keys, :], q_ref[h, rows, :], start)
            o_scr[h, rows, :] = dot(probs.astype(BF16), v_ref[keys, :], 0, 0).astype(BF16)
        return 0
    for i in (0, 1, 2, 4, 5, 6, 7):
        stores[i].start()
    lax.fori_loop(0, heads, one_head, 0)
    for h in range(heads):
        o_own[:, h * head_dim:(h + 1) * head_dim] = o_scr[h]
    o_gather = Gather(lambda d: o_all.at[:, cols_of(d)], o_send, o_recv, where, o_all.at[:, pl.ds(0, 7 * rows_own)], own=o_own)
    o_gather.start()
    wo_gather.got_first()
    wo_gather.got_second()
    start_bulk(4)
    o_all[:, cols_of(me)] = o_own[...]

    def turn_out(k, _):
        rows = tok_of(k)
        ot_ref[:, rows] = o_own[rows, :].T
        return 0
    lax.fori_loop(0, 8, turn_out, 0)
    stores[3].start()
    wo_gather.got_diag()
    for i in range(4):
        wo_gather.got_partner(i)
    o_gather.got_first()
    o_gather.got_second()
    start_bulk(5, 6)
    o_gather.got_partner(0)
    o_gather.got_diag()
    for i in range(1, 4):
        o_gather.got_partner(i)
    start_bulk(7, 8, 9)

    def rows_at(i):
        flips = lambda a, b: other(0, a, b)
        return tok_of(jnp.where(i == 0, me, jnp.where(i == 1, flips(1, 0), jnp.where(i == 2, flips(0, 1), flips(1, 1)))))

    def give(i):
        slot = lax.rem(i, 2)
        rows = rows_at(i)
        return (pltpu.make_async_copy(m_out.at[slot], m_ref.at[rows, :], m_loc.at[slot]),
                pltpu.make_async_remote_copy(src_ref=m_out.at[slot], dst_ref=m_ref.at[rows, :], send_sem=m_send.at[i],
                                             recv_sem=m_recv.at[i], device_id=(partner,), device_id_type=MESH))

    def hidden_block(i, _):
        rows = rows_at(i)
        base = rows.start
        slot = lax.rem(i, 2)

        @pl.when(i >= 2)
        def _():
            to_hbm, to_partner = give(i - 2)
            to_hbm.wait()
            to_partner.wait_send()

        def chunk(j, _):
            cols = pl.ds(pl.multiple_of(j * 256, 256), 256)
            h_scr[:, cols] = dot(o_all[rows, :], wo_all[:, cols], 1, 0)
            return 0
        lax.fori_loop(0, model // 256, chunk, 0)

        def norm(k, _):
            part = pl.ds(pl.multiple_of(k * 16, 16), 16)
            x_part = x_all[pl.ds(pl.multiple_of(base + k * 16, 16), 16), :].astype(F32)
            hidden = (x_part + h_scr[part, :]).astype(BF16)

            @pl.when(i == 0)
            def _():
                h_ref[part, :] = hidden
            m_out[slot, part, :] = norm_forward(hidden.astype(F32), gfull_ref[1:2, :]).astype(BF16)
            return 0
        lax.fori_loop(0, tokens // 16, norm, 0)
        for copy in give(i):
            copy.start()
        return 0
    lax.fori_loop(0, 4, hidden_block, 0)
    stores[8].start()
    for i in range(4):
        give(i)[1].wait_recv()
    for i in range(2, 4):
        give(i)[0].wait()
        give(i)[1].wait_send()
    for copy in small + slices:
        copy.wait_send()
    for gather in (x_gather, wo_gather, o_gather):
        gather.drain()
    for mat, dst in enumerate((w1_ref, w3_ref)):
        seven = dst.at[pl.ds(0, 7 * rows_own), :]
        pltpu.make_async_remote_copy(src_ref=seven, dst_ref=seven, send_sem=bulk_send.at[mat], recv_sem=bulk_recv.at[mat],
                                     device_id=(partner,), device_id_type=MESH).wait()
    for load, store in local:
        store.wait()
    for copy in stores:
        copy.wait()


def attention_step(heads, x_in, positions, gain1, gain2, w_q, w_k, w_v, wo_own, w_gate, w_up):
    tokens, model = x_in.shape
    seq_len = 8 * tokens
    head_dim = wo_own.shape[0] // heads
    rows_own, hid = w_gate.shape[0], w_gate.shape[1] // 8
    shape = jax.ShapeDtypeStruct
    hbm = pl.BlockSpec(memory_space=pl.ANY)
    dma = pltpu.SemaphoreType.DMA
    vm = lambda *dims, dtype=BF16: pltpu.VMEM(dims, dtype)
    steps = np.arange(head_dim // 2, dtype=np.float32) * np.float32(2.0 / head_dim)
    freq = np.tile(np.float32(1.0) / (np.float32(ROPE_BASE) ** steps), 4)[None]
    outs = (shape((heads, seq_len, head_dim), BF16), shape((seq_len, head_dim), BF16), shape((seq_len, head_dim), BF16),
            shape((heads * head_dim, seq_len), BF16), shape((rows_own, seq_len), BF16),
            shape((seq_len, 128), F32), shape((seq_len, 128), F32), shape((8, model), F32), shape((tokens, model), BF16))
    pairs = [dma((1,)), dma((1,)), dma((3,)), dma((3,)), dma((1,)), dma((7,)), dma((1,)), dma((7,)),
             dma((2,)), dma((2,)), dma((1,)), dma((7,))]
    return pl.pallas_call(
        functools.partial(attention_comm_kernel, 'sp', heads), name='attention_comm',
        in_specs=[hbm] * 11, out_specs=[hbm] * 12,
        out_shape=[*outs, shape((seq_len, model), BF16), shape((model, hid), BF16), shape((model, hid), BF16)],
        scratch_shapes=[vm(*t.shape, dtype=t.dtype) for t in outs] + [
            vm(tokens, dtype=jnp.int32), vm(rows_own), vm(rows_own), vm(1, 2 * head_dim, dtype=F32),
            vm(8, rows_own, dtype=F32), vm(seq_len, model), vm(8, 8, rows_own, dtype=F32),
            vm(384, model), vm(model, model), vm(seq_len, model), vm(tokens, model), vm(tokens, 384), vm(heads, seq_len, head_dim),
            vm(seq_len, heads * head_dim), vm(tokens, model, dtype=F32), vm(2, tokens, model), vm(2, rows_own, hid)] + pairs + [
            dma((2,)), dma((4,)), dma((4,)), dma((4,)), dma((12,)), dma((9,))],
        compiler_params=pltpu.CompilerParams(collective_id=0, has_side_effects=True, vmem_limit_bytes=63 * 1024 * 1024),
    )(x_in, positions, gain1, gain2, jnp.asarray(freq), w_q, w_k, w_v, wo_own, w_gate, w_up)


def hand_over_kernel(n_in, *refs):
    sources, gains, results = refs[:n_in], refs[n_in], refs[n_in + 1:2 * n_in + 1]
    gain_outs, sem = refs[2 * n_in + 1:2 * n_in + 3], refs[2 * n_in + 3]
    stores = [pltpu.make_async_copy(sources[i], results[i], sem.at[i]) for i in range(n_in)]
    for store in stores:
        store.start()
    for i in range(2):
        gain_outs[i][...] = gains[i, :]
    for store in stores:
        store.wait()


def hand_over(arrays, gains):
    shape = jax.ShapeDtypeStruct
    hbm, vmem = pl.BlockSpec(memory_space=pltpu.HBM), pl.BlockSpec(memory_space=pltpu.VMEM)
    return pl.pallas_call(
        functools.partial(hand_over_kernel, len(arrays)), name='hand_over',
        in_specs=[vmem] * (len(arrays) + 1), out_specs=[hbm] * len(arrays) + [vmem] * 2,
        out_shape=[shape(a.shape, a.dtype) for a in arrays] + [shape((gains.shape[1],), F32)] * 2,
        scratch_shapes=[pltpu.SemaphoreType.DMA((len(arrays),))],
        compiler_params=pltpu.CompilerParams(vmem_limit_bytes=1024 * 1024),
    )(*[pltpu.with_memory_space_constraint(a, pltpu.VMEM) for a in arrays + (gains,)])


def solution(mesh):
    n_dev = mesh.shape['sp']

    def layer_step(x_in, positions, d_out, norm1_gain, norm2_gain, w_q, w_k, w_v, w_o, w_gate, w_up, w_down):
        tokens, model = x_in.shape
        head_dim = w_q.shape[2]
        heads = w_q.shape[1] // n_dev
        rows_own = w_q.shape[0]
        flat = lambda w: w.transpose(1, 2, 0).reshape(-1, rows_own)
        wo_own = w_o.reshape(-1, model)
        (q_rot, k_rot, v_lin, o_t, u_t, cos_tab, sin_tab, g_full, hidden,
         mlp_in, w1, w3) = attention_step(heads, x_in, positions, norm1_gain, norm2_gain, flat(w_q), flat(w_k), flat(w_v), wo_own, w_gate, w_up)
        d_w1s, d_w3s, d_down, y_out, dh_own, d_g2, early = mlp_step(mlp_in, d_out, w1, w3, w_down, hidden, g_full)
        d_wo, d_wq_t, d_wk_t, d_wv_t, d_w1, d_w3, d_x, d_gains, d_down, y_out = attention_backward_step(
            heads, dh_own, wo_own, o_t, q_rot, k_rot, v_lin, (cos_tab, sin_tab),
            d_w1s, d_w3s, flat(w_q), flat(w_k), flat(w_v), u_t, x_in, g_full, d_g2, d_down, y_out, early)
        from_cols = lambda d, w: d.reshape(w.shape[1], w.shape[2], rows_own).transpose(2, 0, 1)
        (d_down, y_out, d_w1, d_w3, d_wo, d_wq_t, d_wk_t, d_wv_t, d_x, d_g1, d_g2) = hand_over(
            (d_down, y_out, d_w1, d_w3, d_wo, d_wq_t, d_wk_t, d_wv_t, d_x), d_gains)
        return (y_out, d_x, d_g1, d_g2, from_cols(d_wq_t, w_q), from_cols(d_wk_t, w_k), from_cols(d_wv_t, w_v),
                d_wo.reshape(w_o.shape), d_w1, d_w3, d_down)

    all_rows = P('sp')
    return jax.shard_map(layer_step, mesh=mesh, in_specs=(all_rows,) * 12, out_specs=(all_rows,) * 11, check_vma=False)
```

```python
import functools
import jax
import jax.numpy as jnp
import numpy as np
from jax import lax
from jax.experimental import pallas as pl
from jax.experimental.pallas import tpu as pltpu
from jax.sharding import PartitionSpec as P

ROPE_BASE = 10000.0
NORM_EPS = 1e-5
NEG_LARGE = -1e30
F32 = jnp.float32
BF16 = jnp.bfloat16
BLK = 256
EARLY_ROWS = 8


def dot(lhs, rhs, lhs_dim, rhs_dim):
    return lax.dot_general(lhs, rhs, (((lhs_dim,), (rhs_dim,)), ((), ())), preferred_element_type=F32)


def norm_forward(hidden, gain_vec):
    inv_rms = lax.rsqrt(jnp.mean(hidden * hidden, axis=-1, keepdims=True) + NORM_EPS)
    return hidden * inv_rms * gain_vec


def probs_transposed(k_rows, q_blk, start):
    scores = dot(k_rows, q_blk, 1, 1)
    rows = lax.broadcasted_iota(jnp.int32, (BLK, BLK), 0)
    cols = lax.broadcasted_iota(jnp.int32, (BLK, BLK), 1)
    tail = jnp.where(rows <= cols, scores[start:], NEG_LARGE)
    scores = jnp.concatenate([scores[:start], tail], axis=0) if start else tail
    top = jnp.max(scores, axis=0, keepdims=True)
    weights = jnp.exp((scores - top) * (q_blk.shape[1] ** -0.5))
    return weights * (1.0 / jnp.sum(weights, axis=0, keepdims=True))


MESH = pl.DeviceIdType.MESH


def place(axis):
    me = lax.axis_index(axis)
    core = lax.rem(me, 2)
    col = lax.rem(lax.div(me, 2), 2)
    row = lax.div(me, 4)

    def other(flip_core, flip_col, flip_row):
        pick = lambda v, f: 1 - v if f else v
        return pick(row, flip_row) * 4 + pick(col, flip_col) * 2 + pick(core, flip_core)

    nbr_x, nbr_y = other(0, 1, 0), other(0, 0, 1)
    first = nbr_x * (1 - core) + nbr_y * core
    second = nbr_y * (1 - core) + nbr_x * core
    return me, other, first, second


def greet(other):
    barrier = pltpu.get_barrier_semaphore()
    for r in range(1, 8):
        pl.semaphore_signal(barrier, inc=1, device_id=(other(r & 1, (r >> 1) & 1, r >> 2),), device_id_type=MESH)
    pl.semaphore_wait(barrier, 7)


class Gather:
    def __init__(self, slot, send_sem, recv_sem, where, seven, own=None):
        me, other, first, second = where
        partner, diag = other(1, 0, 0), other(0, 1, 1)
        own = slot(me) if own is None else own
        self.copies = []
        plan = [(own, me, first), (own, me, second), (own, me, partner), (slot(first), first, second),
                (slot(first), first, partner), (slot(second), second, partner), (slot(diag), diag, partner)]
        for i, (src, what, dest) in enumerate(plan):
            self.copies.append(pltpu.make_async_remote_copy(
                src_ref=src, dst_ref=slot(what), send_sem=send_sem.at[0], recv_sem=recv_sem.at[i],
                device_id=(dest,), device_id_type=MESH))
        self.sent = pltpu.make_async_remote_copy(
            src_ref=seven, dst_ref=seven, send_sem=send_sem.at[0], recv_sem=recv_sem.at[0],
            device_id=(partner,), device_id_type=MESH)

    def start(self):
        for i in range(3):
            self.copies[i].start()

    def got_first(self):
        self.copies[0].wait_recv()
        self.copies[3].start()
        self.copies[4].start()

    def got_second(self):
        self.copies[1].wait_recv()
        self.copies[5].start()

    def got_diag(self):
        self.copies[3].wait_recv()
        self.copies[6].start()

    def got_partner(self, i):
        self.copies[(2, 4, 5, 6)[i]].wait_recv()

    def drain(self):
        self.sent.wait_send()


def turn_halves(values, cos_blk, sin_blk):
    width = values.shape[1]
    lanes = lax.broadcasted_iota(jnp.int32, values.shape, 1)
    partner = jnp.where(lax.rem(lanes, 64) < 32, pltpu.roll(values, width - 32, 1), pltpu.roll(values, 32, 1))
    return values * cos_blk + partner * sin_blk


def norm_backward(hidden, gain, d_out):
    inv = lax.rsqrt(jnp.mean(hidden * hidden, axis=-1, keepdims=True) + NORM_EPS)
    d_scaled = d_out * gain
    d_hidden = d_scaled * inv - hidden * (inv * inv * inv * jnp.mean(d_scaled * hidden, axis=-1, keepdims=True))
    return d_hidden, jnp.sum(d_out * (hidden * inv), axis=0, keepdims=True)


def attn_bwd_comm_kernel(axis, heads, dh_hbm, wo_hbm, ot_hbm, q_hbm, k_hbm, v_hbm, cos_hbm, sin_hbm,
                         dw1_ref, dw3_ref, wq_hbm, wk_hbm, wv_hbm, ut_hbm, x_hbm, g_hbm, dg2_hbm, ddown_hbm, y_hbm, early_hbm,
                         dwo_ref, dwq_ref, dwk_ref, dwv_ref, out1_ref, out3_ref, dx_ref, dg_ref, ddown_ref, y_ref,
                         dh_own, wo_ref, ot_ref, q_ref, k_ref, v_ref, cos_ref, sin_ref, wq_ref, wk_ref, wv_ref, ut_ref, g_ref, dg2_ref,
                         pool, do_scr, dg_own, dg_all, dk_acc, dv_acc, du_acc,
                         bulk_send, bulk_recv, hg_send, hg_recv, gat_send, gat_recv, du_send, du_rsem, dg_send, dg_recv, loc_sem, ld_sem, credit):
    loads = {}
    for i, (name, src, dst) in enumerate((
            ('wo', wo_hbm, wo_ref), ('ot', ot_hbm, ot_ref), ('q', q_hbm, q_ref), ('k', k_hbm, k_ref),
            ('v', v_hbm, v_ref), ('cos', cos_hbm, cos_ref), ('sin', sin_hbm, sin_ref), ('wq', wq_hbm, wq_ref), ('wk', wk_hbm, wk_ref),
            ('wv', wv_hbm, wv_ref), ('ut', ut_hbm, ut_ref), ('g', g_hbm, g_ref), ('dg2', dg2_hbm, dg2_ref),
            ('dh', dh_hbm, dh_own), ('ddown', ddown_hbm, ddown_ref), ('y', y_hbm, y_ref))):
        loads[name] = pltpu.make_async_copy(src, dst, ld_sem.at[i])
        loads[name].start()

    def need(*names):
        for name in names:
            loads[name].wait()

    where = place(axis)
    me, other, first, second = where
    greet(other)
    seq_len, head_dim = k_ref.shape
    rows_own, hid = out1_ref.shape[0], dw1_ref.shape[1]
    tokens, model = x_hbm.shape
    qw = heads * head_dim

    rows_of = lambda d: pl.ds(pl.multiple_of(d * rows_own, rows_own), rows_own)
    hid_of = lambda d: pl.ds(pl.multiple_of(d * hid, hid), hid)
    pairs = ((dw1_ref, out1_ref), (dw3_ref, out3_ref))
    peers = [other(r & 1, (r >> 1) & 1, r >> 2) for r in (2, 4, 6, 3, 5, 7, 1)]
    bulk, parts = [], []
    for mat, (src, dst) in enumerate(pairs):
        skip = (EARLY_ROWS, 0)[mat]
        for low, high in ((skip, skip + 16), (skip + 16, rows_own // 2), (rows_own // 2, rows_own)):
            parts.append(range(len(bulk), len(bulk) + len(peers)))
            for dest in peers:
                bulk.append(pltpu.make_async_remote_copy(
                    src_ref=src.at[pl.ds(pl.multiple_of(dest * rows_own + low, 8), high - low), :],
                    dst_ref=dst.at[pl.ds(low, high - low), hid_of(me)], send_sem=bulk_send.at[mat],
                    recv_sem=bulk_recv.at[mat], device_id=(dest,), device_id_type=MESH))

    def start_bulk(*which):
        for part in which:
            for i in parts[part]:
                bulk[i].start()
    tok_of = lambda d: pl.ds(pl.multiple_of(d * tokens, tokens), tokens)
    dh_ref = pool.at[:, 0:model]
    h_gather = Gather(lambda d: dh_ref.at[tok_of(d), :], hg_send, hg_recv, where, dh_ref.at[pl.ds(0, 7 * tokens), :], own=dh_hbm)
    h_gather.start()
    start_bulk(0)
    local = [pltpu.make_async_copy(src.at[rows_of(me), :], dst.at[:, hid_of(me)], loc_sem.at[i]) for i, (src, dst) in enumerate(pairs)]
    for copy in local:
        copy.start()
    for dest in peers:
        pltpu.make_async_copy(early_hbm.at[:, hid_of(dest)], out1_ref.at[0:EARLY_ROWS, hid_of(dest)], loc_sem.at[2]).start()
    need('dh', 'wo', 'ot')
    pool[tok_of(me), 0:model] = dh_own[...]
    h_gather.got_first()
    h_gather.got_second()
    start_bulk(1, 2)
    h_gather.got_diag()
    for i in range(4):
        h_gather.got_partner(i)

    def split_out_grad(k, _):
        rows = pl.ds(pl.multiple_of(k * BLK, BLK), BLK)
        do_blk = dot(pool[rows, 0:model], wo_ref[...], 1, 1).astype(BF16)
        for h in range(heads):
            do_scr[h, rows, :] = do_blk[:, h * head_dim:(h + 1) * head_dim]
        cols = rows
        dwo_ref[:, cols] = dot(ot_ref[...], pool[:, cols], 1, 0)
        return 0
    lax.fori_loop(0, seq_len // BLK, split_out_grad, 0)
    h_gather.drain()
    for i, device in enumerate((first, second, other(1, 0, 0))):
        pl.semaphore_signal(credit.at[i], inc=1, device_id=(device,), device_id_type=MESH)
    x_ref = wo_ref
    x_load = pltpu.make_async_copy(x_hbm, x_ref, ld_sem.at[16])
    x_load.start()


    need('q', 'k', 'v')
    dk_acc[...] = jnp.zeros_like(dk_acc)
    dv_acc[...] = jnp.zeros_like(dv_acc)
    slot_cols = lambda d, off, width: pl.ds(pl.multiple_of(d * 384 + off, 128), width)

    def one_head(h, _):
        def one_block(start):
            keys = pl.ds(0, start + BLK)
            rows = pl.ds(start, BLK)
            q_blk, do_blk = q_ref[h, rows, :], do_scr[h, rows, :]
            probs = probs_transposed(k_ref[keys, :], q_blk, start)
            d_probs = dot(v_ref[keys, :], do_blk, 1, 1).astype(BF16).astype(F32)
            row_dot = jnp.sum(d_probs * probs, axis=0, keepdims=True)
            d_scores = (probs * (d_probs - row_dot) * (head_dim ** -0.5)).astype(BF16)
            do_scr[h, rows, :] = dot(d_scores, k_ref[keys, :], 0, 0).astype(BF16)
            dk_acc[keys, :] += dot(d_scores, q_blk, 1, 0)
            dv_acc[keys, :] += dot(probs.astype(BF16), do_blk, 1, 0)
        for start in range(0, seq_len, BLK):
            one_block(start)
        return 0
    lax.fori_loop(0, heads, one_head, 0)
    need('cos', 'sin')
    low = lax.broadcasted_iota(jnp.int32, (BLK, 128), 1) < head_dim

    def turn_back(k, _):
        rows = pl.ds(pl.multiple_of(k * BLK, BLK), BLK)
        cos_blk, sin_blk = cos_ref[rows, :], -sin_ref[rows, :]
        for pair in range(heads // 2):
            both = jnp.concatenate([do_scr[2 * pair, rows, :], do_scr[2 * pair + 1, rows, :]], axis=1)
            pool[rows, slot_cols(me, pair * 128, 128)] = turn_halves(both.astype(F32), cos_blk, sin_blk).astype(BF16)
        kv = jnp.concatenate([dk_acc[rows, :], dv_acc[rows, :]], axis=1).astype(BF16).astype(F32)
        pool[rows, slot_cols(me, qw, 128)] = jnp.where(low, turn_halves(kv, cos_blk, sin_blk), kv).astype(BF16)
        return 0
    lax.fori_loop(0, seq_len // BLK, turn_back, 0)

    gather = Gather(lambda d: pool.at[:, slot_cols(d, 0, 384)], gat_send, gat_recv, where, pool.at[:, pl.ds(0, 7 * 384)])
    for i in range(3):
        pl.semaphore_wait(credit.at[i], 1)
    gather.start()
    start_bulk(3)
    du_acc[...] = jnp.zeros_like(du_acc)
    need('wq', 'wk', 'wv', 'ut')

    def use(d):
        q_rows = pl.ds(pl.multiple_of(d * qw, qw), qw)
        kv_rows = pl.ds(pl.multiple_of(d * head_dim, head_dim), head_dim)
        w_all = jnp.concatenate([wq_ref[q_rows, :], wk_ref[kv_rows, :], wv_ref[kv_rows, :]], axis=0)

        def add_rows(k, _):
            rows = pl.ds(pl.multiple_of(k * 512, 512), 512)
            du_acc[rows, :] += dot(pool[rows, slot_cols(d, 0, 384)], w_all, 1, 0)
            return 0
        lax.fori_loop(0, seq_len // 512, add_rows, 0)
        d_w = dot(ut_ref[...], pool[:, slot_cols(d, 0, 384)], 1, 0).T
        dwq_ref[q_rows, :] = d_w[:qw]
        dwk_ref[kv_rows, :] = d_w[qw:qw + head_dim]
        dwv_ref[kv_rows, :] = d_w[qw + head_dim:]

    def use_many(*devices):
        def body(i, _):
            d = devices[0]
            for n in range(1, len(devices)):
                d = jnp.where(i == n, devices[n], d)
            use(d)
            return 0
        lax.fori_loop(0, len(devices), body, 0)

    use_many(me)
    gather.got_first()
    gather.got_second()
    start_bulk(4)
    gather.got_partner(0)
    use_many(first, second, other(1, 0, 0))
    gather.got_diag()
    for i in range(1, 4):
        gather.got_partner(i)
    use_many(other(0, 1, 1), other(1, 1, 0), other(1, 0, 1), other(1, 1, 1))
    gather.drain()
    du_scr = pool.at[:, 0:rows_own]

    def round_du(k, _):
        rows = pl.ds(pl.multiple_of(k * BLK, BLK), BLK)
        pool[rows, 0:rows_own] = du_acc[rows, :].astype(BF16)
        return 0
    lax.fori_loop(0, seq_len // BLK, round_du, 0)
    for dest in peers:
        pltpu.make_async_remote_copy(
            src_ref=du_scr.at[tok_of(dest), :], dst_ref=ot_ref.at[:, rows_of(me)], send_sem=du_send.at[0],
            recv_sem=du_rsem.at[0], device_id=(dest,), device_id_type=MESH).start()
    start_bulk(5)
    ot_ref[:, rows_of(me)] = pool[tok_of(me), 0:rows_own]
    need('g', 'dg2')
    x_load.wait()
    got = ot_ref.at[:, pl.ds(0, 7 * rows_own)]
    pltpu.make_async_copy(got, got, du_rsem.at[0]).wait()
    dg_own[...] = jnp.zeros_like(dg_own)
    dg_own[1:2, :] = dg2_ref[...]

    def input_grad(k, _):
        part = pl.ds(pl.multiple_of(k * 16, 16), 16)
        d_norm, d_gain = norm_backward(x_ref[part, :].astype(F32), g_ref[0:1, :], ot_ref[part, :].astype(F32))
        dh_part = dh_own[part, :]
        dx_ref[part, :] = (dh_part.astype(F32) + d_norm).astype(BF16)
        dg_own[0:1, :] += d_gain
        return 0
    lax.fori_loop(0, tokens // 16, input_grad, 0)
    for dest in peers:
        pltpu.make_async_remote_copy(
            src_ref=dg_own.at[:, rows_of(dest)], dst_ref=dg_all.at[me], send_sem=dg_send.at[0],
            recv_sem=dg_recv.at[0], device_id=(dest,), device_id_type=MESH).start()
    dg_all[me] = dg_own[:, rows_of(me)]
    got = dg_all.at[pl.ds(0, 7)]
    pltpu.make_async_copy(got, got, dg_recv.at[0]).wait()
    dg_ref[...] = jnp.sum(dg_all[...], axis=0)
    for sent, sem in ((du_scr.at[pl.ds(0, 7 * tokens), :], du_send), (dg_own.at[:, pl.ds(0, 7 * rows_own)], dg_send)):
        pltpu.make_async_copy(sent, sent, sem.at[0]).wait()
    need('ddown', 'y')
    for copy in local:
        copy.wait()
    seven = out1_ref.at[0:EARLY_ROWS, pl.ds(0, 7 * hid)]
    pltpu.make_async_copy(seven, seven, loc_sem.at[2]).wait()
    for mat, (src, dst) in enumerate(pairs):
        rows = rows_own - (EARLY_ROWS, 0)[mat]
        sent, got = src.at[pl.ds(0, 7 * rows), :], dst.at[0:rows, pl.ds(0, 7 * hid)]
        pltpu.make_async_copy(sent, sent, bulk_send.at[mat]).wait()
        pltpu.make_async_copy(got, got, bulk_recv.at[mat]).wait()


def attention_backward_step(heads, dh_own, wo_own, o_t, q_rot, k_rot, v_lin, tables, d_w1, d_w3, w_q, w_k, w_v, u_t, x_in, gains, d_g2, d_down, y_out, early_rows):
    seq_len, model = k_rot.shape[0], x_in.shape[1]
    head_dim = k_rot.shape[1]
    tokens = x_in.shape[0]
    rows_own, hid = model // 8, d_w1.shape[1]
    shape = jax.ShapeDtypeStruct
    hbm = pl.BlockSpec(memory_space=pl.ANY)
    dma = pltpu.SemaphoreType.DMA
    vm = lambda *dims, dtype=BF16: pltpu.VMEM(dims, dtype)
    early = (dh_own, wo_own, o_t, q_rot, k_rot, v_lin, *tables)
    late = (w_q, w_k, w_v, u_t, x_in, gains, d_g2)
    outs = [(wo_own.shape, F32), (w_q.shape, F32), (w_k.shape, F32), (w_v.shape, F32), ((rows_own, 8 * hid), F32),
            ((rows_own, 8 * hid), F32), (x_in.shape, BF16), ((8, rows_own), F32), (d_down.shape, F32), (y_out.shape, BF16)]
    vmem, far = pl.BlockSpec(memory_space=pltpu.VMEM), pl.BlockSpec(memory_space=pltpu.HBM)
    return pl.pallas_call(
        functools.partial(attn_bwd_comm_kernel, 'sp', heads), name='attn_bwd_comm',
        in_specs=[hbm] * 17 + [far] * 3, out_specs=[vmem] * 10,
        out_shape=[pltpu.VMEM(dims, dtype) for dims, dtype in outs],
        scratch_shapes=[vm(*t.shape, dtype=t.dtype) for t in early + late[:4] + late[5:]] + [
            vm(seq_len, 8 * 384), vm(heads, seq_len, head_dim),
            vm(8, model, dtype=F32), vm(8, 8, rows_own, dtype=F32),
            vm(seq_len, head_dim, dtype=F32), vm(seq_len, head_dim, dtype=F32),
            vm(seq_len, rows_own, dtype=F32),
            dma((2,)), dma((2,)), dma((1,)), dma((7,)), dma((1,)), dma((7,)), dma((1,)), dma((1,)), dma((1,)), dma((1,)), dma((3,)), dma((17,)), pltpu.SemaphoreType.REGULAR((3,))],
        compiler_params=pltpu.CompilerParams(collective_id=2, has_side_effects=True, vmem_limit_bytes=34340864),
    )(*early, d_w1, d_w3, *late, *[pltpu.with_memory_space_constraint(a, pltpu.HBM) for a in (d_down, y_out, early_rows)])


def mlp_comm_kernel(axis, m_ref, dout_own, w1_hbm, w3_hbm, w2_hbm, h_hbm, g_hbm,
                    dw1_ref, dw3_ref, dw2_ref, y_hbm, dh_hbm, dg2_hbm, early_ref, dout_ref,
                    w1_ref, w3_ref, w2_ref, h_ref, g_ref, y_ref, dg2_ref,
                    glu, gate_s, up_s, outbox, chip_sum, inbox, blk, m_col, do_col, mt_scr, dot_scr, st1, st3, st2, dh_own,
                    part_send, part_recv, mail_send, mail_recv, do_send, do_recv,
                    in_sem, col_sem, out_sem, own_sem, ld_sem, early_sem, credit):
    loads = [pltpu.make_async_copy(src, dst, ld_sem.at[i]) for i, (src, dst) in enumerate((
        (w1_hbm, w1_ref), (w3_hbm, w3_ref), (w2_hbm, w2_ref), (h_hbm, h_ref), (g_hbm, g_ref)))]
    own_in = pltpu.make_async_copy(dout_own, dh_own, own_sem.at[0])
    for copy in loads + [own_in]:
        copy.start()
    where = place(axis)
    me, other, first, second = where
    core = lax.rem(me, 2)
    partner = other(1, 0, 0)
    tokens, model = h_ref.shape
    hid = w1_ref.shape[1]
    tok_of = lambda d: pl.ds(pl.multiple_of(d * tokens, tokens), tokens)
    off_first, off_second = 1 + core, 2 - core

    def block_of(off, flip):
        d_col, d_row = lax.rem(off, 2), lax.div(off, 2)
        col, row = lax.rem(lax.div(me, 2), 2), lax.div(me, 4)
        mix = lambda v, f: v + f - 2 * v * f
        return mix(row, d_row) * 4 + mix(col, d_col) * 2 + mix(core, flip)

    def step_off(step, flip):
        mid_a = off_second * (1 - flip) + off_first * flip
        mid_b = off_first * (1 - flip) + off_second * flip
        return jnp.where(step == 0, 3, jnp.where(step == 1, mid_a, jnp.where(step == 2, mid_b, 0)))

    def half_rows(half):
        flip = 1 - lax.rem(half, 2)
        return tok_of(block_of(step_off(lax.div(half, 2), flip), flip))

    def fetch(half):
        slot = lax.rem(half, 2)
        return pltpu.make_async_copy(m_ref.at[half_rows(half), :], blk.at[slot], in_sem.at[slot])

    def fetch_dout(d):
        slot = lax.rem(d, 2)
        return pltpu.make_async_copy(dout_ref.at[tok_of(d), :], blk.at[slot], in_sem.at[slot])

    def fetch_cols(j):
        cols = pl.ds(pl.multiple_of(j * 256, 256), 256)
        return (pltpu.make_async_copy(m_ref.at[:, cols], m_col, col_sem.at[0]),
                pltpu.make_async_copy(dout_ref.at[:, cols], do_col, col_sem.at[1]))

    def sigmoid(value):
        return 1.0 / (1.0 + jnp.exp(-value))

    def activations(slot, rows):
        def chunk(j, _):
            cols = pl.ds(pl.multiple_of(j * 512, 512), 512)
            gate = dot(blk[slot], w1_ref[:, cols], 1, 0).astype(BF16)
            up = dot(blk[slot], w3_ref[:, cols], 1, 0).astype(BF16)
            gate_s[rows, cols] = gate
            up_s[rows, cols] = up
            gate = gate.astype(F32)
            glu[rows, cols] = (gate * sigmoid(gate) * up.astype(F32)).astype(BF16)
            return 0
        lax.fori_loop(0, hid // 512, chunk, 0)

    def activation_grads(slot, rows):
        def chunk(j, _):
            cols = pl.ds(pl.multiple_of(j * 512, 512), 512)
            d_act = dot(blk[slot], w2_ref[cols, :], 1, 1).astype(BF16).astype(F32)
            gate, up = gate_s[rows, cols].astype(F32), up_s[rows, cols].astype(F32)
            sig = sigmoid(gate)
            silu = gate * sig
            up_s[rows, cols] = (d_act * silu).astype(BF16)
            gate_s[rows, cols] = (d_act * up * (sig + silu * (1.0 - sig))).astype(BF16)
            return 0
        lax.fori_loop(0, hid // 512, chunk, 0)

    def add_mlp_grad(rows, put):
        def chunk(j, _):
            cols = pl.ds(pl.multiple_of(j * 512, 512), 512)
            put(cols, dot(gate_s[rows, :], w1_ref[cols, :], 1, 1) + dot(up_s[rows, :], w3_ref[cols, :], 1, 1))
            return 0
        lax.fori_loop(0, model // 512, chunk, 0)

    def add_mlp_out(rows, put):
        def chunk(j, _):
            cols = pl.ds(pl.multiple_of(j * 512, 512), 512)
            put(cols, dot(glu[rows, :], w2_ref[:, cols], 1, 0))
            return 0
        lax.fori_loop(0, model // 512, chunk, 0)

    def signal(index, device):
        pl.semaphore_signal(credit.at[index], inc=1, device_id=(device,), device_id_type=MESH)

    class Scatter:
        def __init__(self, turn):
            self.turn = turn

        def to_partner(self, step):
            off = step_off(step, 1)
            return pltpu.make_async_remote_copy(
                src_ref=outbox.at[lax.rem(step, 2)], dst_ref=chip_sum.at[off], send_sem=part_send.at[self.turn, step],
                recv_sem=part_recv.at[self.turn, off], device_id=(partner,), device_id_type=MESH)

        def from_partner(self, off):
            return pltpu.make_async_remote_copy(
                src_ref=outbox.at[0], dst_ref=chip_sum.at[off], send_sem=part_send.at[self.turn, 0],
                recv_sem=part_recv.at[self.turn, off], device_id=(partner,), device_id_type=MESH)

        def mail(self, kind):
            off = (3, off_first, off_second)[kind]
            dest = (first, first, second)[kind]
            return pltpu.make_async_remote_copy(
                src_ref=chip_sum.at[off], dst_ref=inbox.at[kind], send_sem=mail_send.at[self.turn, kind],
                recv_sem=mail_recv.at[self.turn, kind], device_id=(dest,), device_id_type=MESH)

        def step(self, step, prepare, partial):
            self.first_half(step, prepare, partial)
            self.second_half(step, prepare, partial)

        def first_half(self, step, prepare, partial):
            slot = lax.rem(step, 2)
            prepare(2 * step)

            def put_out(cols, value):
                outbox[slot, :, cols] = value
            partial(half_rows(2 * step), put_out)

        def second_half(self, step, prepare, partial):
            self.to_partner(step).start()
            prepare(2 * step + 1)
            off = step_off(step, 0)
            self.from_partner(off).wait_recv()

            def put_sum(cols, value):
                chip_sum[off, :, cols] += value
            partial(half_rows(2 * step + 1), put_sum)

        def pass_on(self):
            self.mail(0).wait_recv()

            def add_mail(k, _):
                part = pl.ds(pl.multiple_of(k * 16, 16), 16)
                chip_sum[off_second, part, :] += inbox[0, part, :]
                return 0
            lax.fori_loop(0, tokens // 16, add_mail, 0)

    out_round, grad_round = Scatter(0), Scatter(1)

    def prepare_out(half):
        @pl.when(half < 7)
        def _():
            fetch(half + 1).start()
        fetch(half).wait()
        activations(lax.rem(half, 2), half_rows(half))

    def weight_grads(begin, end):
        for copy in fetch_cols(begin):
            copy.start()

        def body(j, _):
            for copy in fetch_cols(j):
                copy.wait()

            def turn(k, _):
                part = pl.ds(pl.multiple_of(k * 256, 256), 256)
                mt_scr[:, part] = m_col[part, :].T
                dot_scr[:, part] = do_col[part, :].T
                return 0
            lax.fori_loop(0, m_col.shape[0] // 256, turn, 0)

            @pl.when(j + 1 < end)
            def _():
                for copy in fetch_cols(j + 1):
                    copy.start()
            rows = pl.ds(pl.multiple_of(j * 256, 256), 256)
            out = (pltpu.make_async_copy(st1, dw1_ref.at[rows, :], out_sem.at[0]),
                   pltpu.make_async_copy(st3, dw3_ref.at[rows, :], out_sem.at[1]),
                   pltpu.make_async_copy(st2, dw2_ref.at[:, rows], out_sem.at[2]))

            @pl.when(j > begin)
            def _():
                for copy in out:
                    copy.wait()

            def chunk(k, _):
                cols = pl.ds(pl.multiple_of(k * 512, 512), 512)
                st1[:, cols] = dot(mt_scr[...], gate_s[:, cols], 1, 0)
                st3[:, cols] = dot(mt_scr[...], up_s[:, cols], 1, 0)
                st2[cols, :] = dot(dot_scr[...], glu[:, cols], 1, 0).T
                return 0
            lax.fori_loop(0, hid // 512, chunk, 0)
            for copy in out:
                copy.start()
            return 0
        lax.fori_loop(begin, end, body, 0)
        rows = pl.ds((end - 1) * 256, 256)
        for copy in (pltpu.make_async_copy(st1, dw1_ref.at[rows, :], out_sem.at[0]),
                     pltpu.make_async_copy(st3, dw3_ref.at[rows, :], out_sem.at[1]),
                     pltpu.make_async_copy(st2, dw2_ref.at[:, rows], out_sem.at[2])):
            copy.wait()

    fetch(0).start()
    greet(other)
    do_gather = Gather(lambda d: dout_ref.at[tok_of(d), :], do_send, do_recv, where, dout_ref.at[pl.ds(0, 7 * tokens), :], own=dout_own)
    do_gather.start()
    own_in.wait()
    own_out = pltpu.make_async_copy(dh_own, dout_ref.at[tok_of(me), :], own_sem.at[1])
    own_out.start()
    for copy in loads:
        copy.wait()

    def out_step(step, _):
        @pl.when(step >= 2)
        def _():
            out_round.to_partner(step - 2).wait_send()
        out_round.step(step, prepare_out, add_mlp_out)

        @pl.when(step == 0)
        def _():
            out_round.mail(0).start()

        @pl.when(step == 2)
        def _():
            out_round.mail(1).start()
            do_gather.got_first()
            do_gather.got_second()
        return 0
    lax.fori_loop(0, 4, out_step, 0)
    out_round.pass_on()
    out_round.mail(2).start()
    for step in (2, 3):
        out_round.to_partner(step).wait_send()
    out_round.mail(0).wait_send()
    signal(0, partner)
    signal(1, first)
    do_gather.got_diag()
    for i in range(4):
        do_gather.got_partner(i)
    own_out.wait()
    fetch_dout(0).start()

    def grad_block(d, _):
        @pl.when(d < 7)
        def _():
            fetch_dout(d + 1).start()
        fetch_dout(d).wait()
        activation_grads(lax.rem(d, 2), tok_of(d))
        return 0
    lax.fori_loop(0, 8, grad_block, 0)

    as_is = lambda half: None
    grad_round.first_half(0, as_is, add_mlp_grad)
    pl.semaphore_wait(credit.at[0], 1)
    grad_round.second_half(0, as_is, add_mlp_grad)
    pl.semaphore_wait(credit.at[1], 1)
    grad_round.mail(0).start()
    weight_grads(0, 2)
    grad_round.first_half(1, as_is, add_mlp_grad)
    out_round.mail(1).wait_recv()
    out_round.mail(2).wait_recv()

    def layer_out(k, _):
        part = pl.ds(pl.multiple_of(k * 16, 16), 16)
        y_ref[part, :] = (h_ref[part, :].astype(F32) + (chip_sum[0, part, :] + inbox[1, part, :] + inbox[2, part, :])).astype(BF16)
        return 0
    lax.fori_loop(0, tokens // 16, layer_out, 0)
    y_store = pltpu.make_async_copy(y_ref, y_hbm, own_sem.at[2])
    y_store.start()
    out_round.mail(1).wait_send()
    out_round.mail(2).wait_send()
    signal(2, partner)
    signal(3, first)
    signal(4, second)
    pl.semaphore_wait(credit.at[2], 1)

    grad_round.second_half(1, as_is, add_mlp_grad)

    def grad_step(step, _):
        grad_round.to_partner(step - 2).wait_send()
        grad_round.step(step, as_is, add_mlp_grad)

        @pl.when(step == 2)
        def _():
            pl.semaphore_wait(credit.at[3], 1)
            grad_round.mail(1).start()
            grad_round.pass_on()
            pl.semaphore_wait(credit.at[4], 1)
            grad_round.mail(2).start()
        return 0
    lax.fori_loop(2, 4, grad_step, 0)
    weight_grads(2, 8)
    rows = early_ref.shape[0]
    for r in (2, 4, 6, 3, 5, 7, 1):
        dest = other(r & 1, (r >> 1) & 1, r >> 2)
        pltpu.make_async_remote_copy(
            src_ref=dw1_ref.at[pl.ds(pl.multiple_of(dest * 256, 256), rows), :],
            dst_ref=early_ref.at[:, pl.ds(pl.multiple_of(me * hid, hid), hid)], send_sem=early_sem.at[0],
            recv_sem=early_sem.at[1], device_id=(dest,), device_id_type=MESH).start()
    grad_round.mail(1).wait_recv()
    grad_round.mail(2).wait_recv()
    dg2_ref[...] = jnp.zeros_like(dg2_ref)

    def hidden_grad(k, _):
        part = pl.ds(pl.multiple_of(k * 16, 16), 16)
        d_mlp = (chip_sum[0, part, :] + inbox[1, part, :] + inbox[2, part, :]).astype(BF16).astype(F32)
        d_norm, d_gain = norm_backward(h_ref[part, :].astype(F32), g_ref[1:2, :], d_mlp)
        dh_own[part, :] = (dh_own[part, :].astype(F32) + d_norm).astype(BF16)
        dg2_ref[...] += d_gain
        return 0
    lax.fori_loop(0, tokens // 16, hidden_grad, 0, unroll=4)
    own_out = pltpu.make_async_copy(dh_own, dh_hbm, own_sem.at[3])
    own_out.start()
    dg2_store = pltpu.make_async_copy(dg2_ref, dg2_hbm, own_sem.at[4])
    dg2_store.start()
    for step in (2, 3):
        grad_round.to_partner(step).wait_send()
    for kind in range(3):
        grad_round.mail(kind).wait_send()
    seven = early_ref.at[:, pl.ds(0, 7 * hid)]
    for i in range(2):
        pltpu.make_async_copy(seven, seven, early_sem.at[i]).wait()
    do_gather.drain()
    own_out.wait()
    y_store.wait()
    dg2_store.wait()


def mlp_step(m_all, d_out, w1, w3, w2, hidden, gains):
    seq_len, model = m_all.shape
    hid, tokens = w1.shape[1], hidden.shape[0]
    shape = jax.ShapeDtypeStruct
    hbm = pl.BlockSpec(memory_space=pl.ANY)
    dma = pltpu.SemaphoreType.DMA
    vm = lambda *dims, dtype=BF16: pltpu.VMEM(dims, dtype)
    return pl.pallas_call(
        functools.partial(mlp_comm_kernel, 'sp'), name='mlp_comm',
        in_specs=[hbm] * 7, out_specs=[hbm] * 8,
        out_shape=[shape((model, hid), F32), shape((model, hid), F32), shape((hid, model), F32),
                   shape(hidden.shape, BF16), shape(hidden.shape, BF16), shape((1, model), F32), shape((EARLY_ROWS, 8 * hid), F32),
                   shape((seq_len, model), BF16)],
        scratch_shapes=[vm(*t.shape, dtype=t.dtype) for t in (w1, w3, w2, hidden, gains)] + [
            vm(tokens, model), vm(1, model, dtype=F32),
            vm(seq_len, hid), vm(seq_len, hid), vm(seq_len, hid),
            vm(2, tokens, model, dtype=F32), vm(4, tokens, model, dtype=F32), vm(3, tokens, model, dtype=F32),
            vm(2, tokens, model), vm(seq_len, 256), vm(seq_len, 256), vm(256, seq_len), vm(256, seq_len),
            vm(256, hid, dtype=F32), vm(256, hid, dtype=F32), vm(hid, 256, dtype=F32), vm(tokens, model),
            dma((2, 4)), dma((2, 4)), dma((2, 3)), dma((2, 3)), dma((1,)), dma((7,)),
            dma((2,)), dma((2,)), dma((3,)), dma((5,)), dma((5,)), dma((2,)), pltpu.SemaphoreType.REGULAR((5,))],
        compiler_params=pltpu.CompilerParams(collective_id=1, has_side_effects=True, vmem_limit_bytes=63 * 1024 * 1024),
    )(m_all, d_out, w1, w3, w2, hidden, gains)[:7]


def spread_tables(packed, upper):
    lanes = lax.broadcasted_iota(jnp.int32, packed.shape, 1)
    swapped = pltpu.roll(packed, 64, 1)
    both = jnp.where((lanes < 64) != upper, packed, swapped)
    low = lax.rem(lanes, 64) < 32
    return jnp.where(low, both, pltpu.roll(both, 32, 1)), jnp.where(low, -pltpu.roll(both, 96, 1), both)


def attention_comm_kernel(axis, heads, x_ref, pos_hbm, gain1_hbm, gain2_hbm, freq_hbm, wq_ref, wk_ref, wv_ref, wo_ref, wg_ref, wu_ref,
                          q_hbm, k_hbm, v_hbm, ot_hbm, ut_hbm, cos_hbm, sin_hbm, gfull_hbm, h_hbm, m_ref, w1_ref, w3_ref,
                          q_ref, k_ref, v_ref, ot_ref, ut_ref, cos_ref, sin_ref, gfull_ref, h_ref, pos_ref, gain1_ref, gain2_ref, freq_ref, gain_ref, x_all, gain_all, w_head, wo_all, o_all, u_blk, qkv_blk, o_scr, o_own, h_scr, m_out, stage,
                          g_send, g_recv, w_send, w_recv, x_send, x_recv, wo_send, wo_recv, bulk_send, bulk_recv,
                          o_send, o_recv, m_loc, m_send, m_recv, loc_sem, own_sem, st_sem):
    tiny = [pltpu.make_async_copy(src, dst, own_sem.at[8 + i]) for i, (src, dst) in enumerate((
        (gain1_hbm, gain1_ref), (gain2_hbm, gain2_ref), (pos_hbm, pos_ref), (freq_hbm, freq_ref)))]
    for copy in tiny:
        copy.start()
    where = place(axis)
    me, other, first, second = where
    core = lax.rem(me, 2)
    partner = other(1, 0, 0)
    greet(other)
    tokens, model = x_ref.shape
    seq_len, head_dim = k_ref.shape
    qw = heads * head_dim
    rows_own, hid = wg_ref.shape[0], w1_ref.shape[1]
    tok_of = lambda d: pl.ds(pl.multiple_of(d * tokens, tokens), tokens)
    cols_of = lambda d: pl.ds(pl.multiple_of(d * rows_own, rows_own), rows_own)
    hid_of = lambda d: pl.ds(pl.multiple_of(d * hid, hid), hid)
    peers = [other(r & 1, (r >> 1) & 1, r >> 2) for r in (6, 2, 4, 7, 3, 5, 1)]

    def to_all(src_of, dst, seven, sems):
        copies = [pltpu.make_async_remote_copy(
            src_ref=src_of(dest), dst_ref=dst, send_sem=sems[0], recv_sem=sems[1],
            device_id=(dest,), device_id_type=MESH) for dest in peers]
        for copy in copies:
            copy.start()
        return pltpu.make_async_remote_copy(src_ref=seven, dst_ref=seven, send_sem=sems[0], recv_sem=sems[1],
                                            device_id=(partner,), device_id_type=MESH)

    q_of = lambda d: pl.ds(pl.multiple_of(d * qw, qw), qw)
    kv_of = lambda d: pl.ds(pl.multiple_of(d * head_dim, head_dim), head_dim)
    seven_rows = pl.ds(0, 7 * rows_own)
    slices = []
    for i, (src, rows, low, high) in enumerate(((wq_ref, q_of, 0, qw), (wk_ref, kv_of, qw, qw + head_dim),
                                                (wv_ref, kv_of, qw + head_dim, qw + 2 * head_dim))):
        slices.append(to_all(lambda dest: src.at[rows(dest), :], w_head.at[low:high, cols_of(me)],
                             w_head.at[low:high, seven_rows], (w_send.at[i], w_recv.at[i])))
    x_gather = Gather(lambda d: x_all.at[tok_of(d), :], x_send, x_recv, where, x_all.at[pl.ds(0, 7 * tokens), :], own=x_ref)
    x_gather.start()
    for copy in tiny:
        copy.wait()
    gain_ref[...] = jnp.zeros_like(gain_ref)
    gain_ref[0:1, :] = gain1_ref[...].astype(F32).reshape(1, -1)
    gain_ref[1:2, :] = gain2_ref[...].astype(F32).reshape(1, -1)
    gain_ref[2:3, :] = pos_ref[...].astype(F32).reshape(1, -1)
    small = [to_all(lambda dest: gain_ref, gain_all.at[me], gain_all.at[pl.ds(0, 7)], (g_send.at[0], g_recv.at[0]))]
    wo_gather = Gather(lambda d: wo_all.at[cols_of(d), :], wo_send, wo_recv, where, wo_all.at[pl.ds(0, 7 * rows_own), :], own=wo_ref)
    bulk, parts = [], []
    quarter = rows_own // 4
    for mat, (src, dst) in enumerate(((wg_ref, w1_ref), (wu_ref, w3_ref))):
        for low, high in ((0, 16), (16, quarter), (quarter, 2 * quarter), (2 * quarter, 3 * quarter), (3 * quarter, rows_own)):
            parts.append(range(len(bulk), len(bulk) + len(peers)))
            for dest in peers:
                bulk.append(pltpu.make_async_remote_copy(
                    src_ref=src.at[pl.ds(low, high - low), hid_of(dest)],
                    dst_ref=dst.at[pl.ds(pl.multiple_of(me * rows_own + low, 16), high - low), :],
                    send_sem=bulk_send.at[mat], recv_sem=bulk_recv.at[mat], device_id=(dest,), device_id_type=MESH))

    def start_bulk(*which):
        for part in which:
            for i in parts[part]:
                bulk[i].start()
    start_bulk(0)

    stores = [pltpu.make_async_copy(src, dst, st_sem.at[i]) for i, (src, dst) in enumerate((
        (q_ref, q_hbm), (k_ref, k_hbm), (v_ref, v_hbm), (ot_ref, ot_hbm), (ut_ref, ut_hbm), (cos_ref, cos_hbm),
        (sin_ref, sin_hbm), (gfull_ref, gfull_hbm), (h_ref, h_hbm)))]
    own = [pltpu.make_async_copy(src, dst, own_sem.at[i]) for i, (src, dst) in enumerate((
        (gain_ref, gain_all.at[me]), (wq_ref.at[q_of(me), :], w_head.at[0:qw, cols_of(me)]),
        (wk_ref.at[kv_of(me), :], w_head.at[qw:qw + head_dim, cols_of(me)]),
        (wv_ref.at[kv_of(me), :], w_head.at[qw + head_dim:, cols_of(me)]),
        (x_ref, x_all.at[tok_of(me), :]), (wo_ref, wo_all.at[cols_of(me), :])))]
    for copy in own:
        copy.start()
    local = []
    for i, (src, dst) in enumerate(((wg_ref, w1_ref), (wu_ref, w3_ref))):
        local.append((pltpu.make_async_copy(src.at[:, hid_of(me)], stage.at[i], loc_sem.at[i]),
                      pltpu.make_async_copy(stage.at[i], dst.at[cols_of(me), :], loc_sem.at[2 + i])))
        local[-1][0].start()
    for load, store in local:
        load.wait()
        store.start()
    for copy in own:
        copy.wait()
    for copy in small:
        copy.wait_recv()
    for d in range(8):
        gfull_ref[:, d * rows_own:(d + 1) * rows_own] = gain_all[d]
    for copy in slices:
        copy.wait_recv()

    def use(d):
        base = pl.multiple_of(d * tokens, tokens)

        def norm(k, _):
            part = pl.ds(pl.multiple_of(k * 16, 16), 16)
            x_part = x_all[pl.ds(pl.multiple_of(base + k * 16, 16), 16), :].astype(F32)
            u_blk[part, :] = norm_forward(x_part, gfull_ref[0:1, :]).astype(BF16)
            return 0
        lax.fori_loop(0, tokens // 16, norm, 0)
        ut_ref[:, tok_of(d)] = u_blk[:, cols_of(me)].T
        qkv_blk[...] = dot(u_blk[...], w_head[...], 1, 1).astype(BF16)
        half = tokens // 2
        where_to = gain_all[d, 2:3, :]
        lanes = lax.broadcasted_iota(jnp.int32, (half, 2 * head_dim), 1)
        by_row = lambda lo: jnp.broadcast_to(where_to[:, lo:lo + half], (2 * head_dim, half)).T
        angles = jnp.where(lanes < head_dim, by_row(0), by_row(half)) * freq_ref[...]
        packed = jnp.where(lax.rem(lanes, head_dim) < head_dim // 2, jnp.cos(angles), jnp.sin(angles))
        for part in range(2):
            rows = pl.ds(pl.multiple_of(base + part * half, half), half)
            cos_blk, sin_blk = spread_tables(packed, part == 1)
            cos_ref[rows, :] = cos_blk
            sin_ref[rows, :] = sin_blk
            source = slice(part * half, (part + 1) * half)
            for pair in range(heads // 2):
                turned = turn_halves(qkv_blk[source, pair * 128:(pair + 1) * 128].astype(F32), cos_blk, sin_blk).astype(BF16)
                q_ref[2 * pair, rows, :] = turned[:, :head_dim]
                q_ref[2 * pair + 1, rows, :] = turned[:, head_dim:]
            turned = turn_halves(qkv_blk[source, qw:].astype(F32), cos_blk, sin_blk).astype(BF16)
            k_ref[rows, :] = turned[:, :head_dim]
            v_ref[rows, :] = qkv_blk[source, qw + head_dim:]

    x_gather.got_first()
    x_gather.got_second()
    wo_gather.start()
    start_bulk(1, 2, 3)
    x_gather.got_partner(0)

    def use_near(i, _):
        use(jnp.where(i == 0, me, jnp.where(i == 1, first, jnp.where(i == 2, second, partner))))
        return 0
    lax.fori_loop(0, 4, use_near, 0)
    x_gather.got_diag()
    for i in range(1, 4):
        x_gather.got_partner(i)

    def use_far(i, _):
        use(jnp.where(i == 0, other(0, 1, 1), jnp.where(i == 1, other(1, 1, 0), jnp.where(i == 2, other(1, 0, 1), other(1, 1, 1)))))
        return 0
    lax.fori_loop(0, 4, use_far, 0)

    def one_head(h, _):
        for start in range(0, seq_len, BLK):
            keys, rows = pl.ds(0, start + BLK), pl.ds(start, BLK)
            probs = probs_transposed(k_ref[keys, :], q_ref[h, rows, :], start)
            o_scr[h, rows, :] = dot(probs.astype(BF16), v_ref[keys, :], 0, 0).astype(BF16)
        return 0
    for i in (0, 1, 2, 4, 5, 6, 7):
        stores[i].start()
    lax.fori_loop(0, heads, one_head, 0)
    for h in range(heads):
        o_own[:, h * head_dim:(h + 1) * head_dim] = o_scr[h]
    o_gather = Gather(lambda d: o_all.at[:, cols_of(d)], o_send, o_recv, where, o_all.at[:, pl.ds(0, 7 * rows_own)], own=o_own)
    o_gather.start()
    wo_gather.got_first()
    wo_gather.got_second()
    start_bulk(4)
    o_all[:, cols_of(me)] = o_own[...]

    def turn_out(k, _):
        rows = tok_of(k)
        ot_ref[:, rows] = o_own[rows, :].T
        return 0
    lax.fori_loop(0, 8, turn_out, 0)
    stores[3].start()
    wo_gather.got_diag()
    for i in range(4):
        wo_gather.got_partner(i)
    o_gather.got_first()
    o_gather.got_second()
    start_bulk(5, 6)
    o_gather.got_partner(0)
    o_gather.got_diag()
    for i in range(1, 4):
        o_gather.got_partner(i)
    start_bulk(7, 8, 9)

    def rows_at(i):
        flips = lambda a, b: other(0, a, b)
        return tok_of(jnp.where(i == 0, me, jnp.where(i == 1, flips(1, 0), jnp.where(i == 2, flips(0, 1), flips(1, 1)))))

    def give(i):
        slot = lax.rem(i, 2)
        rows = rows_at(i)
        return (pltpu.make_async_copy(m_out.at[slot], m_ref.at[rows, :], m_loc.at[slot]),
                pltpu.make_async_remote_copy(src_ref=m_out.at[slot], dst_ref=m_ref.at[rows, :], send_sem=m_send.at[i],
                                             recv_sem=m_recv.at[i], device_id=(partner,), device_id_type=MESH))

    def hidden_block(i, _):
        rows = rows_at(i)
        base = rows.start
        slot = lax.rem(i, 2)

        @pl.when(i >= 2)
        def _():
            to_hbm, to_partner = give(i - 2)
            to_hbm.wait()
            to_partner.wait_send()

        def chunk(j, _):
            cols = pl.ds(pl.multiple_of(j * 256, 256), 256)
            h_scr[:, cols] = dot(o_all[rows, :], wo_all[:, cols], 1, 0)
            return 0
        lax.fori_loop(0, model // 256, chunk, 0)

        def norm(k, _):
            part = pl.ds(pl.multiple_of(k * 16, 16), 16)
            x_part = x_all[pl.ds(pl.multiple_of(base + k * 16, 16), 16), :].astype(F32)
            hidden = (x_part + h_scr[part, :]).astype(BF16)

            @pl.when(i == 0)
            def _():
                h_ref[part, :] = hidden
            m_out[slot, part, :] = norm_forward(hidden.astype(F32), gfull_ref[1:2, :]).astype(BF16)
            return 0
        lax.fori_loop(0, tokens // 16, norm, 0)
        for copy in give(i):
            copy.start()
        return 0
    lax.fori_loop(0, 4, hidden_block, 0)
    stores[8].start()
    for i in range(4):
        give(i)[1].wait_recv()
    for i in range(2, 4):
        give(i)[0].wait()
        give(i)[1].wait_send()
    for copy in small + slices:
        copy.wait_send()
    for gather in (x_gather, wo_gather, o_gather):
        gather.drain()
    for load, store in local:
        store.wait()
    for copy in stores:
        copy.wait()
    for mat, dst in enumerate((w1_ref, w3_ref)):
        seven = dst.at[pl.ds(0, 7 * rows_own), :]
        pltpu.make_async_remote_copy(src_ref=seven, dst_ref=seven, send_sem=bulk_send.at[mat], recv_sem=bulk_recv.at[mat],
                                     device_id=(partner,), device_id_type=MESH).wait()


def attention_step(heads, x_in, positions, gain1, gain2, w_q, w_k, w_v, wo_own, w_gate, w_up):
    tokens, model = x_in.shape
    seq_len = 8 * tokens
    head_dim = wo_own.shape[0] // heads
    rows_own, hid = w_gate.shape[0], w_gate.shape[1] // 8
    shape = jax.ShapeDtypeStruct
    hbm = pl.BlockSpec(memory_space=pl.ANY)
    dma = pltpu.SemaphoreType.DMA
    vm = lambda *dims, dtype=BF16: pltpu.VMEM(dims, dtype)
    steps = np.arange(head_dim // 2, dtype=np.float32) * np.float32(2.0 / head_dim)
    freq = np.tile(np.float32(1.0) / (np.float32(ROPE_BASE) ** steps), 4)[None]
    outs = (shape((heads, seq_len, head_dim), BF16), shape((seq_len, head_dim), BF16), shape((seq_len, head_dim), BF16),
            shape((heads * head_dim, seq_len), BF16), shape((rows_own, seq_len), BF16),
            shape((seq_len, 128), F32), shape((seq_len, 128), F32), shape((8, model), F32), shape((tokens, model), BF16))
    pairs = [dma((1,)), dma((1,)), dma((3,)), dma((3,)), dma((1,)), dma((7,)), dma((1,)), dma((7,)),
             dma((2,)), dma((2,)), dma((1,)), dma((7,))]
    return pl.pallas_call(
        functools.partial(attention_comm_kernel, 'sp', heads), name='attention_comm',
        in_specs=[hbm] * 11, out_specs=[hbm] * 12,
        out_shape=[*outs, shape((seq_len, model), BF16), shape((model, hid), BF16), shape((model, hid), BF16)],
        scratch_shapes=[vm(*t.shape, dtype=t.dtype) for t in outs] + [
            vm(tokens, dtype=jnp.int32), vm(rows_own), vm(rows_own), vm(1, 2 * head_dim, dtype=F32),
            vm(8, rows_own, dtype=F32), vm(seq_len, model), vm(8, 8, rows_own, dtype=F32),
            vm(384, model), vm(model, model), vm(seq_len, model), vm(tokens, model), vm(tokens, 384), vm(heads, seq_len, head_dim),
            vm(seq_len, heads * head_dim), vm(tokens, model, dtype=F32), vm(2, tokens, model), vm(2, rows_own, hid)] + pairs + [
            dma((2,)), dma((4,)), dma((4,)), dma((4,)), dma((12,)), dma((9,))],
        compiler_params=pltpu.CompilerParams(collective_id=0, has_side_effects=True, vmem_limit_bytes=63 * 1024 * 1024),
    )(x_in, positions, gain1, gain2, jnp.asarray(freq), w_q, w_k, w_v, wo_own, w_gate, w_up)


def hand_over_kernel(n_in, *refs):
    sources, gains, results = refs[:n_in], refs[n_in], refs[n_in + 1:2 * n_in + 1]
    gain_outs, lines, sem = refs[2 * n_in + 1:2 * n_in + 3], refs[2 * n_in + 3:2 * n_in + 5], refs[2 * n_in + 5]
    stores = [pltpu.make_async_copy(sources[i], results[i], sem.at[i]) for i in range(n_in)]
    for store in stores:
        store.start()
    for i in range(2):
        lines[i][...] = gains[i, :]
        stores.append(pltpu.make_async_copy(lines[i], gain_outs[i], sem.at[n_in + i]))
        stores[-1].start()
    for store in stores:
        store.wait()


def hand_over(arrays, gains):
    shape = jax.ShapeDtypeStruct
    hbm, vmem = pl.BlockSpec(memory_space=pltpu.HBM), pl.BlockSpec(memory_space=pltpu.VMEM)
    return pl.pallas_call(
        functools.partial(hand_over_kernel, len(arrays)), name='hand_over',
        in_specs=[vmem] * (len(arrays) + 1), out_specs=[hbm] * (len(arrays) + 2),
        out_shape=[shape(a.shape, a.dtype) for a in arrays] + [shape((gains.shape[1],), F32)] * 2,
        scratch_shapes=[pltpu.VMEM((gains.shape[1],), F32)] * 2 + [pltpu.SemaphoreType.DMA((len(arrays) + 2,))],
        compiler_params=pltpu.CompilerParams(vmem_limit_bytes=1024 * 1024),
    )(*[pltpu.with_memory_space_constraint(a, pltpu.VMEM) for a in arrays + (gains,)])


def solution(mesh):
    n_dev = mesh.shape['sp']

    def layer_step(x_in, positions, d_out, norm1_gain, norm2_gain, w_q, w_k, w_v, w_o, w_gate, w_up, w_down):
        tokens, model = x_in.shape
        head_dim = w_q.shape[2]
        heads = w_q.shape[1] // n_dev
        rows_own = w_q.shape[0]
        flat = lambda w: w.transpose(1, 2, 0).reshape(-1, rows_own)
        wo_own = w_o.reshape(-1, model)
        (q_rot, k_rot, v_lin, o_t, u_t, cos_tab, sin_tab, g_full, hidden,
         mlp_in, w1, w3) = attention_step(heads, x_in, positions, norm1_gain, norm2_gain, flat(w_q), flat(w_k), flat(w_v), wo_own, w_gate, w_up)
        d_w1s, d_w3s, d_down, y_out, dh_own, d_g2, early = mlp_step(mlp_in, d_out, w1, w3, w_down, hidden, g_full)
        d_wo, d_wq_t, d_wk_t, d_wv_t, d_w1, d_w3, d_x, d_gains, d_down, y_out = attention_backward_step(
            heads, dh_own, wo_own, o_t, q_rot, k_rot, v_lin, (cos_tab, sin_tab),
            d_w1s, d_w3s, flat(w_q), flat(w_k), flat(w_v), u_t, x_in, g_full, d_g2, d_down, y_out, early)
        from_cols = lambda d, w: d.reshape(w.shape[1], w.shape[2], rows_own).transpose(2, 0, 1)
        (d_down, y_out, d_w1, d_w3, d_wo, d_wq_t, d_wk_t, d_wv_t, d_x, d_g1, d_g2) = hand_over(
            (d_down, y_out, d_w1, d_w3, d_wo, d_wq_t, d_wk_t, d_wv_t, d_x), d_gains)
        return (y_out, d_x, d_g1, d_g2, from_cols(d_wq_t, w_q), from_cols(d_wk_t, w_k), from_cols(d_wv_t, w_v),
                d_wo.reshape(w_o.shape), d_w1, d_w3, d_down)

    all_rows = P('sp')
    return jax.shard_map(layer_step, mesh=mesh, in_specs=(all_rows,) * 12, out_specs=(all_rows,) * 11, check_vma=False)
```

```python
import functools
import jax
import jax.numpy as jnp
import numpy as np
from jax import lax
from jax.experimental import pallas as pl
from jax.experimental.pallas import tpu as pltpu
from jax.sharding import PartitionSpec as P

ROPE_BASE = 10000.0
NORM_EPS = 1e-5
NEG_LARGE = -1e30
F32 = jnp.float32
BF16 = jnp.bfloat16
BLK = 256
EARLY_ROWS = 8


def dot(lhs, rhs, lhs_dim, rhs_dim):
    return lax.dot_general(lhs, rhs, (((lhs_dim,), (rhs_dim,)), ((), ())), preferred_element_type=F32)


def norm_forward(hidden, gain_vec):
    inv_rms = lax.rsqrt(jnp.mean(hidden * hidden, axis=-1, keepdims=True) + NORM_EPS)
    return hidden * inv_rms * gain_vec


def probs_transposed(k_rows, q_blk, start):
    scores = dot(k_rows, q_blk, 1, 1)
    rows = lax.broadcasted_iota(jnp.int32, (BLK, BLK), 0)
    cols = lax.broadcasted_iota(jnp.int32, (BLK, BLK), 1)
    tail = jnp.where(rows <= cols, scores[start:], NEG_LARGE)
    scores = jnp.concatenate([scores[:start], tail], axis=0) if start else tail
    top = jnp.max(scores, axis=0, keepdims=True)
    weights = jnp.exp((scores - top) * (q_blk.shape[1] ** -0.5))
    return weights * (1.0 / jnp.sum(weights, axis=0, keepdims=True))


MESH = pl.DeviceIdType.MESH


def place(axis):
    me = lax.axis_index(axis)
    core = lax.rem(me, 2)
    col = lax.rem(lax.div(me, 2), 2)
    row = lax.div(me, 4)

    def other(flip_core, flip_col, flip_row):
        pick = lambda v, f: 1 - v if f else v
        return pick(row, flip_row) * 4 + pick(col, flip_col) * 2 + pick(core, flip_core)

    nbr_x, nbr_y = other(0, 1, 0), other(0, 0, 1)
    first = nbr_x * (1 - core) + nbr_y * core
    second = nbr_y * (1 - core) + nbr_x * core
    return me, other, first, second


def greet(where):
    _, other, first, second = where
    barrier = pltpu.get_barrier_semaphore()
    for device in (first, second, other(1, 0, 0)):
        pl.semaphore_signal(barrier, inc=1, device_id=(device,), device_id_type=MESH)
    pl.semaphore_wait(barrier, 3)


def relay(where, sem, base):
    _, other, first, second = where
    partner = other(1, 0, 0)
    for i, device in enumerate((first, second, partner)):
        pl.semaphore_signal(sem.at[base + i], inc=1, device_id=(device,), device_id_type=MESH)
    for i in range(3):
        pl.semaphore_wait(sem.at[base + i], 1)
    pl.semaphore_signal(sem.at[base + 3], inc=1, device_id=(partner,), device_id_type=MESH)
    pl.semaphore_wait(sem.at[base + 3], 1)


class Gather:
    def __init__(self, slot, send_sem, recv_sem, where, seven, own=None):
        me, other, first, second = where
        partner, diag = other(1, 0, 0), other(0, 1, 1)
        own = slot(me) if own is None else own
        self.copies = []
        plan = [(own, me, first), (own, me, second), (own, me, partner), (slot(first), first, second),
                (slot(first), first, partner), (slot(second), second, partner), (slot(diag), diag, partner)]
        for i, (src, what, dest) in enumerate(plan):
            self.copies.append(pltpu.make_async_remote_copy(
                src_ref=src, dst_ref=slot(what), send_sem=send_sem.at[0], recv_sem=recv_sem.at[i],
                device_id=(dest,), device_id_type=MESH))
        self.sent = pltpu.make_async_remote_copy(
            src_ref=seven, dst_ref=seven, send_sem=send_sem.at[0], recv_sem=recv_sem.at[0],
            device_id=(partner,), device_id_type=MESH)

    def start(self):
        for i in range(3):
            self.copies[i].start()

    def got_first(self):
        self.copies[0].wait_recv()
        self.copies[3].start()
        self.copies[4].start()

    def got_second(self):
        self.copies[1].wait_recv()
        self.copies[5].start()

    def got_diag(self):
        self.copies[3].wait_recv()
        self.copies[6].start()

    def got_partner(self, i):
        self.copies[(2, 4, 5, 6)[i]].wait_recv()

    def drain(self):
        self.sent.wait_send()


def turn_halves(values, cos_blk, sin_blk):
    width = values.shape[1]
    lanes = lax.broadcasted_iota(jnp.int32, values.shape, 1)
    partner = jnp.where(lax.rem(lanes, 64) < 32, pltpu.roll(values, width - 32, 1), pltpu.roll(values, 32, 1))
    return values * cos_blk + partner * sin_blk


def norm_backward(hidden, gain, d_out):
    inv = lax.rsqrt(jnp.mean(hidden * hidden, axis=-1, keepdims=True) + NORM_EPS)
    d_scaled = d_out * gain
    d_hidden = d_scaled * inv - hidden * (inv * inv * inv * jnp.mean(d_scaled * hidden, axis=-1, keepdims=True))
    return d_hidden, jnp.sum(d_out * (hidden * inv), axis=0, keepdims=True)


def attn_bwd_comm_kernel(axis, heads, dh_hbm, wo_hbm, ot_hbm, q_hbm, k_hbm, v_hbm, cos_hbm, sin_hbm,
                         dw1_ref, dw3_ref, wq_hbm, wk_hbm, wv_hbm, ut_hbm, x_hbm, g_hbm, dg2_hbm, ddown_hbm, y_hbm, early_hbm,
                         dwo_ref, dwq_ref, dwk_ref, dwv_ref, out1_ref, out3_ref, dx_ref, dg_ref, ddown_ref, y_ref,
                         dh_own, wo_ref, ot_ref, q_ref, k_ref, v_ref, cos_ref, sin_ref, wq_ref, wk_ref, wv_ref, ut_ref, g_ref, dg2_ref,
                         pool, do_scr, dg_own, dg_all, dk_acc, dv_acc, du_acc,
                         bulk_send, bulk_recv, hg_send, hg_recv, gat_send, gat_recv, du_send, du_rsem, dg_send, dg_recv, loc_sem, ld_sem, credit):
    loads = {}
    for i, (name, src, dst) in enumerate((
            ('wo', wo_hbm, wo_ref), ('ot', ot_hbm, ot_ref), ('q', q_hbm, q_ref), ('k', k_hbm, k_ref),
            ('v', v_hbm, v_ref), ('cos', cos_hbm, cos_ref), ('sin', sin_hbm, sin_ref), ('wq', wq_hbm, wq_ref), ('wk', wk_hbm, wk_ref),
            ('wv', wv_hbm, wv_ref), ('ut', ut_hbm, ut_ref), ('g', g_hbm, g_ref), ('dg2', dg2_hbm, dg2_ref),
            ('dh', dh_hbm, dh_own), ('ddown', ddown_hbm, ddown_ref), ('y', y_hbm, y_ref))):
        loads[name] = pltpu.make_async_copy(src, dst, ld_sem.at[i])
        loads[name].start()

    def need(*names):
        for name in names:
            loads[name].wait()

    where = place(axis)
    me, other, first, second = where
    greet(where)
    seq_len, head_dim = k_ref.shape
    rows_own, hid = out1_ref.shape[0], dw1_ref.shape[1]
    tokens, model = x_hbm.shape
    qw = heads * head_dim

    rows_of = lambda d: pl.ds(pl.multiple_of(d * rows_own, rows_own), rows_own)
    hid_of = lambda d: pl.ds(pl.multiple_of(d * hid, hid), hid)
    pairs = ((dw1_ref, out1_ref), (dw3_ref, out3_ref))
    peers = [other(r & 1, (r >> 1) & 1, r >> 2) for r in (2, 4, 6, 3, 5, 7, 1)]
    bulk, parts = [], []
    for mat, (src, dst) in enumerate(pairs):
        skip = (EARLY_ROWS, 0)[mat]
        for low, high in ((skip, skip + 16), (skip + 16, rows_own // 2), (rows_own // 2, rows_own)):
            parts.append(range(len(bulk), len(bulk) + len(peers)))
            for dest in peers:
                bulk.append(pltpu.make_async_remote_copy(
                    src_ref=src.at[pl.ds(pl.multiple_of(dest * rows_own + low, 8), high - low), :],
                    dst_ref=dst.at[pl.ds(low, high - low), hid_of(me)], send_sem=bulk_send.at[mat],
                    recv_sem=bulk_recv.at[mat], device_id=(dest,), device_id_type=MESH))

    def start_bulk(*which):
        for part in which:
            for i in parts[part]:
                bulk[i].start()
    tok_of = lambda d: pl.ds(pl.multiple_of(d * tokens, tokens), tokens)
    dh_ref = pool.at[:, 0:model]
    h_gather = Gather(lambda d: dh_ref.at[tok_of(d), :], hg_send, hg_recv, where, dh_ref.at[pl.ds(0, 7 * tokens), :], own=dh_hbm)
    h_gather.start()
    relay(where, credit, 3)
    start_bulk(0)
    local = [pltpu.make_async_copy(src.at[rows_of(me), :], dst.at[:, hid_of(me)], loc_sem.at[i]) for i, (src, dst) in enumerate(pairs)]
    for copy in local:
        copy.start()
    for dest in peers:
        pltpu.make_async_copy(early_hbm.at[:, hid_of(dest)], out1_ref.at[0:EARLY_ROWS, hid_of(dest)], loc_sem.at[2]).start()
    need('dh', 'wo', 'ot')
    pool[tok_of(me), 0:model] = dh_own[...]
    h_gather.got_first()
    h_gather.got_second()
    start_bulk(1, 2)
    h_gather.got_diag()
    for i in range(4):
        h_gather.got_partner(i)

    def split_out_grad(k, _):
        rows = pl.ds(pl.multiple_of(k * BLK, BLK), BLK)
        do_blk = dot(pool[rows, 0:model], wo_ref[...], 1, 1).astype(BF16)
        for h in range(heads):
            do_scr[h, rows, :] = do_blk[:, h * head_dim:(h + 1) * head_dim]
        cols = rows
        dwo_ref[:, cols] = dot(ot_ref[...], pool[:, cols], 1, 0)
        return 0
    lax.fori_loop(0, seq_len // BLK, split_out_grad, 0)
    h_gather.drain()
    for i, device in enumerate((first, second, other(1, 0, 0))):
        pl.semaphore_signal(credit.at[i], inc=1, device_id=(device,), device_id_type=MESH)
    x_ref = wo_ref
    x_load = pltpu.make_async_copy(x_hbm, x_ref, ld_sem.at[16])
    x_load.start()


    need('q', 'k', 'v')
    dk_acc[...] = jnp.zeros_like(dk_acc)
    dv_acc[...] = jnp.zeros_like(dv_acc)
    slot_cols = lambda d, off, width: pl.ds(pl.multiple_of(d * 384 + off, 128), width)

    def one_head(h, _):
        def one_block(start):
            keys = pl.ds(0, start + BLK)
            rows = pl.ds(start, BLK)
            q_blk, do_blk = q_ref[h, rows, :], do_scr[h, rows, :]
            probs = probs_transposed(k_ref[keys, :], q_blk, start)
            d_probs = dot(v_ref[keys, :], do_blk, 1, 1).astype(BF16).astype(F32)
            row_dot = jnp.sum(d_probs * probs, axis=0, keepdims=True)
            d_scores = (probs * (d_probs - row_dot) * (head_dim ** -0.5)).astype(BF16)
            do_scr[h, rows, :] = dot(d_scores, k_ref[keys, :], 0, 0).astype(BF16)
            dk_acc[keys, :] += dot(d_scores, q_blk, 1, 0)
            dv_acc[keys, :] += dot(probs.astype(BF16), do_blk, 1, 0)
        for start in range(0, seq_len, BLK):
            one_block(start)
        return 0
    lax.fori_loop(0, heads, one_head, 0)
    need('cos', 'sin')
    low = lax.broadcasted_iota(jnp.int32, (BLK, 128), 1) < head_dim

    def turn_back(k, _):
        rows = pl.ds(pl.multiple_of(k * BLK, BLK), BLK)
        cos_blk, sin_blk = cos_ref[rows, :], -sin_ref[rows, :]
        for pair in range(heads // 2):
            both = jnp.concatenate([do_scr[2 * pair, rows, :], do_scr[2 * pair + 1, rows, :]], axis=1)
            pool[rows, slot_cols(me, pair * 128, 128)] = turn_halves(both.astype(F32), cos_blk, sin_blk).astype(BF16)
        kv = jnp.concatenate([dk_acc[rows, :], dv_acc[rows, :]], axis=1).astype(BF16).astype(F32)
        pool[rows, slot_cols(me, qw, 128)] = jnp.where(low, turn_halves(kv, cos_blk, sin_blk), kv).astype(BF16)
        return 0
    lax.fori_loop(0, seq_len // BLK, turn_back, 0)

    gather = Gather(lambda d: pool.at[:, slot_cols(d, 0, 384)], gat_send, gat_recv, where, pool.at[:, pl.ds(0, 7 * 384)])
    for i in range(3):
        pl.semaphore_wait(credit.at[i], 1)
    gather.start()
    start_bulk(3)
    du_acc[...] = jnp.zeros_like(du_acc)
    need('wq', 'wk', 'wv', 'ut')

    def use(d):
        q_rows = pl.ds(pl.multiple_of(d * qw, qw), qw)
        kv_rows = pl.ds(pl.multiple_of(d * head_dim, head_dim), head_dim)
        w_all = jnp.concatenate([wq_ref[q_rows, :], wk_ref[kv_rows, :], wv_ref[kv_rows, :]], axis=0)

        def add_rows(k, _):
            rows = pl.ds(pl.multiple_of(k * 512, 512), 512)
            du_acc[rows, :] += dot(pool[rows, slot_cols(d, 0, 384)], w_all, 1, 0)
            return 0
        lax.fori_loop(0, seq_len // 512, add_rows, 0)
        d_w = dot(ut_ref[...], pool[:, slot_cols(d, 0, 384)], 1, 0).T
        dwq_ref[q_rows, :] = d_w[:qw]
        dwk_ref[kv_rows, :] = d_w[qw:qw + head_dim]
        dwv_ref[kv_rows, :] = d_w[qw + head_dim:]

    def use_many(*devices):
        def body(i, _):
            d = devices[0]
            for n in range(1, len(devices)):
                d = jnp.where(i == n, devices[n], d)
            use(d)
            return 0
        lax.fori_loop(0, len(devices), body, 0)

    use_many(me)
    gather.got_first()
    gather.got_second()
    start_bulk(4)
    gather.got_partner(0)
    use_many(first, second, other(1, 0, 0))
    gather.got_diag()
    for i in range(1, 4):
        gather.got_partner(i)
    use_many(other(0, 1, 1), other(1, 1, 0), other(1, 0, 1), other(1, 1, 1))
    gather.drain()
    du_scr = pool.at[:, 0:rows_own]

    def round_du(k, _):
        rows = pl.ds(pl.multiple_of(k * BLK, BLK), BLK)
        pool[rows, 0:rows_own] = du_acc[rows, :].astype(BF16)
        return 0
    lax.fori_loop(0, seq_len // BLK, round_du, 0)
    for dest in peers:
        pltpu.make_async_remote_copy(
            src_ref=du_scr.at[tok_of(dest), :], dst_ref=ot_ref.at[:, rows_of(me)], send_sem=du_send.at[0],
            recv_sem=du_rsem.at[0], device_id=(dest,), device_id_type=MESH).start()
    start_bulk(5)
    ot_ref[:, rows_of(me)] = pool[tok_of(me), 0:rows_own]
    need('g', 'dg2')
    x_load.wait()
    got = ot_ref.at[:, pl.ds(0, 7 * rows_own)]
    pltpu.make_async_copy(got, got, du_rsem.at[0]).wait()
    dg_own[...] = jnp.zeros_like(dg_own)
    dg_own[1:2, :] = dg2_ref[...]

    def input_grad(k, _):
        part = pl.ds(pl.multiple_of(k * 16, 16), 16)
        d_norm, d_gain = norm_backward(x_ref[part, :].astype(F32), g_ref[0:1, :], ot_ref[part, :].astype(F32))
        dh_part = dh_own[part, :]
        dx_ref[part, :] = (dh_part.astype(F32) + d_norm).astype(BF16)
        dg_own[0:1, :] += d_gain
        return 0
    lax.fori_loop(0, tokens // 16, input_grad, 0)
    for dest in peers:
        pltpu.make_async_remote_copy(
            src_ref=dg_own.at[:, rows_of(dest)], dst_ref=dg_all.at[me], send_sem=dg_send.at[0],
            recv_sem=dg_recv.at[0], device_id=(dest,), device_id_type=MESH).start()
    dg_all[me] = dg_own[:, rows_of(me)]
    got = dg_all.at[pl.ds(0, 7)]
    pltpu.make_async_copy(got, got, dg_recv.at[0]).wait()
    dg_ref[...] = jnp.sum(dg_all[...], axis=0)
    for sent, sem in ((du_scr.at[pl.ds(0, 7 * tokens), :], du_send), (dg_own.at[:, pl.ds(0, 7 * rows_own)], dg_send)):
        pltpu.make_async_copy(sent, sent, sem.at[0]).wait()
    need('ddown', 'y')
    for copy in local:
        copy.wait()
    seven = out1_ref.at[0:EARLY_ROWS, pl.ds(0, 7 * hid)]
    pltpu.make_async_copy(seven, seven, loc_sem.at[2]).wait()
    for mat, (src, dst) in enumerate(pairs):
        rows = rows_own - (EARLY_ROWS, 0)[mat]
        sent, got = src.at[pl.ds(0, 7 * rows), :], dst.at[0:rows, pl.ds(0, 7 * hid)]
        pltpu.make_async_copy(sent, sent, bulk_send.at[mat]).wait()
        pltpu.make_async_copy(got, got, bulk_recv.at[mat]).wait()


def attention_backward_step(heads, dh_own, wo_own, o_t, q_rot, k_rot, v_lin, tables, d_w1, d_w3, w_q, w_k, w_v, u_t, x_in, gains, d_g2, d_down, y_out, early_rows):
    seq_len, model = k_rot.shape[0], x_in.shape[1]
    head_dim = k_rot.shape[1]
    tokens = x_in.shape[0]
    rows_own, hid = model // 8, d_w1.shape[1]
    shape = jax.ShapeDtypeStruct
    hbm = pl.BlockSpec(memory_space=pl.ANY)
    dma = pltpu.SemaphoreType.DMA
    vm = lambda *dims, dtype=BF16: pltpu.VMEM(dims, dtype)
    early = (dh_own, wo_own, o_t, q_rot, k_rot, v_lin, *tables)
    late = (w_q, w_k, w_v, u_t, x_in, gains, d_g2)
    outs = [(wo_own.shape, F32), (w_q.shape, F32), (w_k.shape, F32), (w_v.shape, F32), ((rows_own, 8 * hid), F32),
            ((rows_own, 8 * hid), F32), (x_in.shape, BF16), ((8, rows_own), F32), (d_down.shape, F32), (y_out.shape, BF16)]
    vmem, far = pl.BlockSpec(memory_space=pltpu.VMEM), pl.BlockSpec(memory_space=pltpu.HBM)
    return pl.pallas_call(
        functools.partial(attn_bwd_comm_kernel, 'sp', heads), name='attn_bwd_comm',
        in_specs=[hbm] * 17 + [far] * 3, out_specs=[vmem] * 10,
        out_shape=[pltpu.VMEM(dims, dtype) for dims, dtype in outs],
        scratch_shapes=[vm(*t.shape, dtype=t.dtype) for t in early + late[:4] + late[5:]] + [
            vm(seq_len, 8 * 384), vm(heads, seq_len, head_dim),
            vm(8, model, dtype=F32), vm(8, 8, rows_own, dtype=F32),
            vm(seq_len, head_dim, dtype=F32), vm(seq_len, head_dim, dtype=F32),
            vm(seq_len, rows_own, dtype=F32),
            dma((2,)), dma((2,)), dma((1,)), dma((7,)), dma((1,)), dma((7,)), dma((1,)), dma((1,)), dma((1,)), dma((1,)), dma((3,)), dma((17,)), pltpu.SemaphoreType.REGULAR((7,))],
        compiler_params=pltpu.CompilerParams(collective_id=2, has_side_effects=True, vmem_limit_bytes=34340864),
    )(*early, d_w1, d_w3, *late, *[pltpu.with_memory_space_constraint(a, pltpu.HBM) for a in (d_down, y_out, early_rows)])


def mlp_comm_kernel(axis, m_ref, dout_own, w1_hbm, w3_hbm, w2_hbm, h_hbm, g_hbm,
                    dw1_ref, dw3_ref, dw2_ref, y_hbm, dh_hbm, dg2_hbm, early_ref, dout_ref,
                    w1_ref, w3_ref, w2_ref, h_ref, g_ref, y_ref, dg2_ref,
                    glu, gate_s, up_s, outbox, chip_sum, inbox, blk, m_col, do_col, mt_scr, dot_scr, st1, st3, st2, dh_own,
                    part_send, part_recv, mail_send, mail_recv, do_send, do_recv,
                    in_sem, col_sem, out_sem, own_sem, ld_sem, early_sem, credit):
    loads = [pltpu.make_async_copy(src, dst, ld_sem.at[i]) for i, (src, dst) in enumerate((
        (w1_hbm, w1_ref), (w3_hbm, w3_ref), (w2_hbm, w2_ref), (h_hbm, h_ref), (g_hbm, g_ref)))]
    own_in = pltpu.make_async_copy(dout_own, dh_own, own_sem.at[0])
    for copy in loads + [own_in]:
        copy.start()
    where = place(axis)
    me, other, first, second = where
    core = lax.rem(me, 2)
    partner = other(1, 0, 0)
    tokens, model = h_ref.shape
    hid = w1_ref.shape[1]
    tok_of = lambda d: pl.ds(pl.multiple_of(d * tokens, tokens), tokens)
    off_first, off_second = 1 + core, 2 - core

    def block_of(off, flip):
        d_col, d_row = lax.rem(off, 2), lax.div(off, 2)
        col, row = lax.rem(lax.div(me, 2), 2), lax.div(me, 4)
        mix = lambda v, f: v + f - 2 * v * f
        return mix(row, d_row) * 4 + mix(col, d_col) * 2 + mix(core, flip)

    def step_off(step, flip):
        mid_a = off_second * (1 - flip) + off_first * flip
        mid_b = off_first * (1 - flip) + off_second * flip
        return jnp.where(step == 0, 3, jnp.where(step == 1, mid_a, jnp.where(step == 2, mid_b, 0)))

    def half_rows(half):
        flip = 1 - lax.rem(half, 2)
        return tok_of(block_of(step_off(lax.div(half, 2), flip), flip))

    def fetch(half):
        slot = lax.rem(half, 2)
        return pltpu.make_async_copy(m_ref.at[half_rows(half), :], blk.at[slot], in_sem.at[slot])

    def fetch_dout(d):
        slot = lax.rem(d, 2)
        return pltpu.make_async_copy(dout_ref.at[tok_of(d), :], blk.at[slot], in_sem.at[slot])

    def fetch_cols(j):
        cols = pl.ds(pl.multiple_of(j * 256, 256), 256)
        return (pltpu.make_async_copy(m_ref.at[:, cols], m_col, col_sem.at[0]),
                pltpu.make_async_copy(dout_ref.at[:, cols], do_col, col_sem.at[1]))

    def sigmoid(value):
        return 1.0 / (1.0 + jnp.exp(-value))

    def activations(slot, rows):
        def chunk(j, _):
            cols = pl.ds(pl.multiple_of(j * 512, 512), 512)
            gate = dot(blk[slot], w1_ref[:, cols], 1, 0).astype(BF16)
            up = dot(blk[slot], w3_ref[:, cols], 1, 0).astype(BF16)
            gate_s[rows, cols] = gate
            up_s[rows, cols] = up
            gate = gate.astype(F32)
            glu[rows, cols] = (gate * sigmoid(gate) * up.astype(F32)).astype(BF16)
            return 0
        lax.fori_loop(0, hid // 512, chunk, 0)

    def activation_grads(slot, rows):
        def chunk(j, _):
            cols = pl.ds(pl.multiple_of(j * 512, 512), 512)
            d_act = dot(blk[slot], w2_ref[cols, :], 1, 1).astype(BF16).astype(F32)
            gate, up = gate_s[rows, cols].astype(F32), up_s[rows, cols].astype(F32)
            sig = sigmoid(gate)
            silu = gate * sig
            up_s[rows, cols] = (d_act * silu).astype(BF16)
            gate_s[rows, cols] = (d_act * up * (sig + silu * (1.0 - sig))).astype(BF16)
            return 0
        lax.fori_loop(0, hid // 512, chunk, 0)

    def add_mlp_grad(rows, put):
        def chunk(j, _):
            cols = pl.ds(pl.multiple_of(j * 512, 512), 512)
            put(cols, dot(gate_s[rows, :], w1_ref[cols, :], 1, 1) + dot(up_s[rows, :], w3_ref[cols, :], 1, 1))
            return 0
        lax.fori_loop(0, model // 512, chunk, 0)

    def add_mlp_out(rows, put):
        def chunk(j, _):
            cols = pl.ds(pl.multiple_of(j * 512, 512), 512)
            put(cols, dot(glu[rows, :], w2_ref[:, cols], 1, 0))
            return 0
        lax.fori_loop(0, model // 512, chunk, 0)

    def signal(index, device):
        pl.semaphore_signal(credit.at[index], inc=1, device_id=(device,), device_id_type=MESH)

    class Scatter:
        def __init__(self, turn):
            self.turn = turn

        def to_partner(self, step):
            off = step_off(step, 1)
            return pltpu.make_async_remote_copy(
                src_ref=outbox.at[lax.rem(step, 2)], dst_ref=chip_sum.at[off], send_sem=part_send.at[self.turn, step],
                recv_sem=part_recv.at[self.turn, off], device_id=(partner,), device_id_type=MESH)

        def from_partner(self, off):
            return pltpu.make_async_remote_copy(
                src_ref=outbox.at[0], dst_ref=chip_sum.at[off], send_sem=part_send.at[self.turn, 0],
                recv_sem=part_recv.at[self.turn, off], device_id=(partner,), device_id_type=MESH)

        def mail(self, kind):
            off = (3, off_first, off_second)[kind]
            dest = (first, first, second)[kind]
            return pltpu.make_async_remote_copy(
                src_ref=chip_sum.at[off], dst_ref=inbox.at[kind], send_sem=mail_send.at[self.turn, kind],
                recv_sem=mail_recv.at[self.turn, kind], device_id=(dest,), device_id_type=MESH)

        def step(self, step, prepare, partial):
            self.first_half(step, prepare, partial)
            self.second_half(step, prepare, partial)

        def first_half(self, step, prepare, partial):
            slot = lax.rem(step, 2)
            prepare(2 * step)

            def put_out(cols, value):
                outbox[slot, :, cols] = value
            partial(half_rows(2 * step), put_out)

        def second_half(self, step, prepare, partial):
            self.to_partner(step).start()
            prepare(2 * step + 1)
            off = step_off(step, 0)
            self.from_partner(off).wait_recv()

            def put_sum(cols, value):
                chip_sum[off, :, cols] += value
            partial(half_rows(2 * step + 1), put_sum)

        def pass_on(self):
            self.mail(0).wait_recv()

            def add_mail(k, _):
                part = pl.ds(pl.multiple_of(k * 16, 16), 16)
                chip_sum[off_second, part, :] += inbox[0, part, :]
                return 0
            lax.fori_loop(0, tokens // 16, add_mail, 0)

    out_round, grad_round = Scatter(0), Scatter(1)

    def prepare_out(half):
        @pl.when(half < 7)
        def _():
            fetch(half + 1).start()
        fetch(half).wait()
        activations(lax.rem(half, 2), half_rows(half))

    def weight_grads(begin, end):
        for copy in fetch_cols(begin):
            copy.start()

        def body(j, _):
            for copy in fetch_cols(j):
                copy.wait()

            def turn(k, _):
                part = pl.ds(pl.multiple_of(k * 256, 256), 256)
                mt_scr[:, part] = m_col[part, :].T
                dot_scr[:, part] = do_col[part, :].T
                return 0
            lax.fori_loop(0, m_col.shape[0] // 256, turn, 0)

            @pl.when(j + 1 < end)
            def _():
                for copy in fetch_cols(j + 1):
                    copy.start()
            rows = pl.ds(pl.multiple_of(j * 256, 256), 256)
            out = (pltpu.make_async_copy(st1, dw1_ref.at[rows, :], out_sem.at[0]),
                   pltpu.make_async_copy(st3, dw3_ref.at[rows, :], out_sem.at[1]),
                   pltpu.make_async_copy(st2, dw2_ref.at[:, rows], out_sem.at[2]))

            @pl.when(j > begin)
            def _():
                for copy in out:
                    copy.wait()

            def chunk(k, _):
                cols = pl.ds(pl.multiple_of(k * 512, 512), 512)
                st1[:, cols] = dot(mt_scr[...], gate_s[:, cols], 1, 0)
                st3[:, cols] = dot(mt_scr[...], up_s[:, cols], 1, 0)
                st2[cols, :] = dot(dot_scr[...], glu[:, cols], 1, 0).T
                return 0
            lax.fori_loop(0, hid // 512, chunk, 0)
            for copy in out:
                copy.start()
            return 0
        lax.fori_loop(begin, end, body, 0)
        rows = pl.ds((end - 1) * 256, 256)
        for copy in (pltpu.make_async_copy(st1, dw1_ref.at[rows, :], out_sem.at[0]),
                     pltpu.make_async_copy(st3, dw3_ref.at[rows, :], out_sem.at[1]),
                     pltpu.make_async_copy(st2, dw2_ref.at[:, rows], out_sem.at[2])):
            copy.wait()

    fetch(0).start()
    greet(where)
    do_gather = Gather(lambda d: dout_ref.at[tok_of(d), :], do_send, do_recv, where, dout_ref.at[pl.ds(0, 7 * tokens), :], own=dout_own)
    do_gather.start()
    own_in.wait()
    own_out = pltpu.make_async_copy(dh_own, dout_ref.at[tok_of(me), :], own_sem.at[1])
    own_out.start()
    for copy in loads:
        copy.wait()

    relay(where, credit, 5)
    def out_step(step, _):
        @pl.when(step >= 2)
        def _():
            out_round.to_partner(step - 2).wait_send()
        out_round.step(step, prepare_out, add_mlp_out)

        @pl.when(step == 0)
        def _():
            out_round.mail(0).start()

        @pl.when(step == 2)
        def _():
            out_round.mail(1).start()
            do_gather.got_first()
            do_gather.got_second()
        return 0
    lax.fori_loop(0, 4, out_step, 0)
    out_round.pass_on()
    out_round.mail(2).start()
    for step in (2, 3):
        out_round.to_partner(step).wait_send()
    out_round.mail(0).wait_send()
    signal(0, partner)
    signal(1, first)
    do_gather.got_diag()
    for i in range(4):
        do_gather.got_partner(i)
    own_out.wait()
    fetch_dout(0).start()

    def grad_block(d, _):
        @pl.when(d < 7)
        def _():
            fetch_dout(d + 1).start()
        fetch_dout(d).wait()
        activation_grads(lax.rem(d, 2), tok_of(d))
        return 0
    lax.fori_loop(0, 8, grad_block, 0)

    as_is = lambda half: None
    grad_round.first_half(0, as_is, add_mlp_grad)
    pl.semaphore_wait(credit.at[0], 1)
    grad_round.second_half(0, as_is, add_mlp_grad)
    pl.semaphore_wait(credit.at[1], 1)
    grad_round.mail(0).start()
    weight_grads(0, 2)
    grad_round.first_half(1, as_is, add_mlp_grad)
    out_round.mail(1).wait_recv()
    out_round.mail(2).wait_recv()

    def layer_out(k, _):
        part = pl.ds(pl.multiple_of(k * 16, 16), 16)
        y_ref[part, :] = (h_ref[part, :].astype(F32) + (chip_sum[0, part, :] + inbox[1, part, :] + inbox[2, part, :])).astype(BF16)
        return 0
    lax.fori_loop(0, tokens // 16, layer_out, 0)
    y_store = pltpu.make_async_copy(y_ref, y_hbm, own_sem.at[2])
    y_store.start()
    out_round.mail(1).wait_send()
    out_round.mail(2).wait_send()
    signal(2, partner)
    signal(3, first)
    signal(4, second)
    pl.semaphore_wait(credit.at[2], 1)

    grad_round.second_half(1, as_is, add_mlp_grad)

    def grad_step(step, _):
        grad_round.to_partner(step - 2).wait_send()
        grad_round.step(step, as_is, add_mlp_grad)

        @pl.when(step == 2)
        def _():
            pl.semaphore_wait(credit.at[3], 1)
            grad_round.mail(1).start()
            grad_round.pass_on()
            pl.semaphore_wait(credit.at[4], 1)
            grad_round.mail(2).start()
        return 0
    lax.fori_loop(2, 4, grad_step, 0)
    weight_grads(2, 8)
    rows = early_ref.shape[0]
    for r in (2, 4, 6, 3, 5, 7, 1):
        dest = other(r & 1, (r >> 1) & 1, r >> 2)
        pltpu.make_async_remote_copy(
            src_ref=dw1_ref.at[pl.ds(pl.multiple_of(dest * 256, 256), rows), :],
            dst_ref=early_ref.at[:, pl.ds(pl.multiple_of(me * hid, hid), hid)], send_sem=early_sem.at[0],
            recv_sem=early_sem.at[1], device_id=(dest,), device_id_type=MESH).start()
    grad_round.mail(1).wait_recv()
    grad_round.mail(2).wait_recv()
    dg2_ref[...] = jnp.zeros_like(dg2_ref)

    def hidden_grad(k, _):
        part = pl.ds(pl.multiple_of(k * 16, 16), 16)
        d_mlp = (chip_sum[0, part, :] + inbox[1, part, :] + inbox[2, part, :]).astype(BF16).astype(F32)
        d_norm, d_gain = norm_backward(h_ref[part, :].astype(F32), g_ref[1:2, :], d_mlp)
        dh_own[part, :] = (dh_own[part, :].astype(F32) + d_norm).astype(BF16)
        dg2_ref[...] += d_gain
        return 0
    lax.fori_loop(0, tokens // 16, hidden_grad, 0, unroll=4)
    own_out = pltpu.make_async_copy(dh_own, dh_hbm, own_sem.at[3])
    own_out.start()
    dg2_store = pltpu.make_async_copy(dg2_ref, dg2_hbm, own_sem.at[4])
    dg2_store.start()
    for step in (2, 3):
        grad_round.to_partner(step).wait_send()
    for kind in range(3):
        grad_round.mail(kind).wait_send()
    seven = early_ref.at[:, pl.ds(0, 7 * hid)]
    for i in range(2):
        pltpu.make_async_copy(seven, seven, early_sem.at[i]).wait()
    do_gather.drain()
    own_out.wait()
    y_store.wait()
    dg2_store.wait()


def mlp_step(m_all, d_out, w1, w3, w2, hidden, gains):
    seq_len, model = m_all.shape
    hid, tokens = w1.shape[1], hidden.shape[0]
    shape = jax.ShapeDtypeStruct
    hbm = pl.BlockSpec(memory_space=pl.ANY)
    dma = pltpu.SemaphoreType.DMA
    vm = lambda *dims, dtype=BF16: pltpu.VMEM(dims, dtype)
    return pl.pallas_call(
        functools.partial(mlp_comm_kernel, 'sp'), name='mlp_comm',
        in_specs=[hbm] * 7, out_specs=[hbm] * 8,
        out_shape=[shape((model, hid), F32), shape((model, hid), F32), shape((hid, model), F32),
                   shape(hidden.shape, BF16), shape(hidden.shape, BF16), shape((1, model), F32), shape((EARLY_ROWS, 8 * hid), F32),
                   shape((seq_len, model), BF16)],
        scratch_shapes=[vm(*t.shape, dtype=t.dtype) for t in (w1, w3, w2, hidden, gains)] + [
            vm(tokens, model), vm(1, model, dtype=F32),
            vm(seq_len, hid), vm(seq_len, hid), vm(seq_len, hid),
            vm(2, tokens, model, dtype=F32), vm(4, tokens, model, dtype=F32), vm(3, tokens, model, dtype=F32),
            vm(2, tokens, model), vm(seq_len, 256), vm(seq_len, 256), vm(256, seq_len), vm(256, seq_len),
            vm(256, hid, dtype=F32), vm(256, hid, dtype=F32), vm(hid, 256, dtype=F32), vm(tokens, model),
            dma((2, 4)), dma((2, 4)), dma((2, 3)), dma((2, 3)), dma((1,)), dma((7,)),
            dma((2,)), dma((2,)), dma((3,)), dma((5,)), dma((5,)), dma((2,)), pltpu.SemaphoreType.REGULAR((9,))],
        compiler_params=pltpu.CompilerParams(collective_id=1, has_side_effects=True, vmem_limit_bytes=63 * 1024 * 1024),
    )(m_all, d_out, w1, w3, w2, hidden, gains)[:7]


def spread_tables(packed, upper):
    lanes = lax.broadcasted_iota(jnp.int32, packed.shape, 1)
    swapped = pltpu.roll(packed, 64, 1)
    both = jnp.where((lanes < 64) != upper, packed, swapped)
    low = lax.rem(lanes, 64) < 32
    return jnp.where(low, both, pltpu.roll(both, 32, 1)), jnp.where(low, -pltpu.roll(both, 96, 1), both)


def attention_comm_kernel(axis, heads, x_ref, pos_hbm, gain1_hbm, gain2_hbm, freq_hbm, wq_ref, wk_ref, wv_ref, wo_ref, wg_ref, wu_ref,
                          q_hbm, k_hbm, v_hbm, ot_hbm, ut_hbm, cos_hbm, sin_hbm, gfull_hbm, h_hbm, m_ref, w1_ref, w3_ref,
                          q_ref, k_ref, v_ref, ot_ref, ut_ref, cos_ref, sin_ref, gfull_ref, h_ref, pos_ref, gain1_ref, gain2_ref, freq_ref, gain_ref, x_all, gain_all, w_head, wo_all, o_all, u_blk, qkv_blk, o_scr, o_own, h_scr, m_out, stage,
                          g_send, g_recv, w_send, w_recv, x_send, x_recv, wo_send, wo_recv, bulk_send, bulk_recv,
                          o_send, o_recv, m_loc, m_send, m_recv, loc_sem, own_sem, st_sem, entry):
    tiny = [pltpu.make_async_copy(src, dst, own_sem.at[8 + i]) for i, (src, dst) in enumerate((
        (gain1_hbm, gain1_ref), (gain2_hbm, gain2_ref), (pos_hbm, pos_ref), (freq_hbm, freq_ref)))]
    for copy in tiny:
        copy.start()
    where = place(axis)
    me, other, first, second = where
    core = lax.rem(me, 2)
    partner = other(1, 0, 0)
    greet(where)
    tokens, model = x_ref.shape
    seq_len, head_dim = k_ref.shape
    qw = heads * head_dim
    rows_own, hid = wg_ref.shape[0], w1_ref.shape[1]
    tok_of = lambda d: pl.ds(pl.multiple_of(d * tokens, tokens), tokens)
    cols_of = lambda d: pl.ds(pl.multiple_of(d * rows_own, rows_own), rows_own)
    hid_of = lambda d: pl.ds(pl.multiple_of(d * hid, hid), hid)
    peers = [other(r & 1, (r >> 1) & 1, r >> 2) for r in (6, 2, 4, 7, 3, 5, 1)]

    def to_all(src_of, dst, seven, sems):
        copies = [pltpu.make_async_remote_copy(
            src_ref=src_of(dest), dst_ref=dst, send_sem=sems[0], recv_sem=sems[1],
            device_id=(dest,), device_id_type=MESH) for dest in peers]
        for copy in copies:
            copy.start()
        return pltpu.make_async_remote_copy(src_ref=seven, dst_ref=seven, send_sem=sems[0], recv_sem=sems[1],
                                            device_id=(partner,), device_id_type=MESH)

    q_of = lambda d: pl.ds(pl.multiple_of(d * qw, qw), qw)
    kv_of = lambda d: pl.ds(pl.multiple_of(d * head_dim, head_dim), head_dim)
    seven_rows = pl.ds(0, 7 * rows_own)
    x_gather = Gather(lambda d: x_all.at[tok_of(d), :], x_send, x_recv, where, x_all.at[pl.ds(0, 7 * tokens), :], own=x_ref)
    x_gather.start()
    relay(where, entry, 0)
    slices = []
    for i, (src, rows, low, high) in enumerate(((wq_ref, q_of, 0, qw), (wk_ref, kv_of, qw, qw + head_dim),
                                                (wv_ref, kv_of, qw + head_dim, qw + 2 * head_dim))):
        slices.append(to_all(lambda dest: src.at[rows(dest), :], w_head.at[low:high, cols_of(me)],
                             w_head.at[low:high, seven_rows], (w_send.at[i], w_recv.at[i])))
    for copy in tiny:
        copy.wait()
    gain_ref[...] = jnp.zeros_like(gain_ref)
    gain_ref[0:1, :] = gain1_ref[...].astype(F32).reshape(1, -1)
    gain_ref[1:2, :] = gain2_ref[...].astype(F32).reshape(1, -1)
    gain_ref[2:3, :] = pos_ref[...].astype(F32).reshape(1, -1)
    small = [to_all(lambda dest: gain_ref, gain_all.at[me], gain_all.at[pl.ds(0, 7)], (g_send.at[0], g_recv.at[0]))]
    wo_gather = Gather(lambda d: wo_all.at[cols_of(d), :], wo_send, wo_recv, where, wo_all.at[pl.ds(0, 7 * rows_own), :], own=wo_ref)
    bulk, parts = [], []
    quarter = rows_own // 4
    for mat, (src, dst) in enumerate(((wg_ref, w1_ref), (wu_ref, w3_ref))):
        for low, high in ((0, 16), (16, quarter), (quarter, 2 * quarter), (2 * quarter, 3 * quarter), (3 * quarter, rows_own)):
            parts.append(range(len(bulk), len(bulk) + len(peers)))
            for dest in peers:
                bulk.append(pltpu.make_async_remote_copy(
                    src_ref=src.at[pl.ds(low, high - low), hid_of(dest)],
                    dst_ref=dst.at[pl.ds(pl.multiple_of(me * rows_own + low, 16), high - low), :],
                    send_sem=bulk_send.at[mat], recv_sem=bulk_recv.at[mat], device_id=(dest,), device_id_type=MESH))

    def start_bulk(*which):
        for part in which:
            for i in parts[part]:
                bulk[i].start()
    start_bulk(0)

    stores = [pltpu.make_async_copy(src, dst, st_sem.at[i]) for i, (src, dst) in enumerate((
        (q_ref, q_hbm), (k_ref, k_hbm), (v_ref, v_hbm), (ot_ref, ot_hbm), (ut_ref, ut_hbm), (cos_ref, cos_hbm),
        (sin_ref, sin_hbm), (gfull_ref, gfull_hbm), (h_ref, h_hbm)))]
    own = [pltpu.make_async_copy(src, dst, own_sem.at[i]) for i, (src, dst) in enumerate((
        (gain_ref, gain_all.at[me]), (wq_ref.at[q_of(me), :], w_head.at[0:qw, cols_of(me)]),
        (wk_ref.at[kv_of(me), :], w_head.at[qw:qw + head_dim, cols_of(me)]),
        (wv_ref.at[kv_of(me), :], w_head.at[qw + head_dim:, cols_of(me)]),
        (x_ref, x_all.at[tok_of(me), :]), (wo_ref, wo_all.at[cols_of(me), :])))]
    for copy in own:
        copy.start()
    local = []
    for i, (src, dst) in enumerate(((wg_ref, w1_ref), (wu_ref, w3_ref))):
        local.append((pltpu.make_async_copy(src.at[:, hid_of(me)], stage.at[i], loc_sem.at[i]),
                      pltpu.make_async_copy(stage.at[i], dst.at[cols_of(me), :], loc_sem.at[2 + i])))
        local[-1][0].start()
    for load, store in local:
        load.wait()
        store.start()
    for copy in own:
        copy.wait()
    for copy in small:
        copy.wait_recv()
    for d in range(8):
        gfull_ref[:, d * rows_own:(d + 1) * rows_own] = gain_all[d]
    for copy in slices:
        copy.wait_recv()

    def use(d):
        base = pl.multiple_of(d * tokens, tokens)

        def norm(k, _):
            part = pl.ds(pl.multiple_of(k * 16, 16), 16)
            x_part = x_all[pl.ds(pl.multiple_of(base + k * 16, 16), 16), :].astype(F32)
            u_blk[part, :] = norm_forward(x_part, gfull_ref[0:1, :]).astype(BF16)
            return 0
        lax.fori_loop(0, tokens // 16, norm, 0)
        ut_ref[:, tok_of(d)] = u_blk[:, cols_of(me)].T
        qkv_blk[...] = dot(u_blk[...], w_head[...], 1, 1).astype(BF16)
        half = tokens // 2
        where_to = gain_all[d, 2:3, :]
        lanes = lax.broadcasted_iota(jnp.int32, (half, 2 * head_dim), 1)
        by_row = lambda lo: jnp.broadcast_to(where_to[:, lo:lo + half], (2 * head_dim, half)).T
        angles = jnp.where(lanes < head_dim, by_row(0), by_row(half)) * freq_ref[...]
        packed = jnp.where(lax.rem(lanes, head_dim) < head_dim // 2, jnp.cos(angles), jnp.sin(angles))
        for part in range(2):
            rows = pl.ds(pl.multiple_of(base + part * half, half), half)
            cos_blk, sin_blk = spread_tables(packed, part == 1)
            cos_ref[rows, :] = cos_blk
            sin_ref[rows, :] = sin_blk
            source = slice(part * half, (part + 1) * half)
            for pair in range(heads // 2):
                turned = turn_halves(qkv_blk[source, pair * 128:(pair + 1) * 128].astype(F32), cos_blk, sin_blk).astype(BF16)
                q_ref[2 * pair, rows, :] = turned[:, :head_dim]
                q_ref[2 * pair + 1, rows, :] = turned[:, head_dim:]
            turned = turn_halves(qkv_blk[source, qw:].astype(F32), cos_blk, sin_blk).astype(BF16)
            k_ref[rows, :] = turned[:, :head_dim]
            v_ref[rows, :] = qkv_blk[source, qw + head_dim:]

    x_gather.got_first()
    x_gather.got_second()
    wo_gather.start()
    start_bulk(1, 2, 3)
    x_gather.got_partner(0)

    def use_near(i, _):
        use(jnp.where(i == 0, me, jnp.where(i == 1, first, jnp.where(i == 2, second, partner))))
        return 0
    lax.fori_loop(0, 4, use_near, 0)
    x_gather.got_diag()
    for i in range(1, 4):
        x_gather.got_partner(i)

    def use_far(i, _):
        use(jnp.where(i == 0, other(0, 1, 1), jnp.where(i == 1, other(1, 1, 0), jnp.where(i == 2, other(1, 0, 1), other(1, 1, 1)))))
        return 0
    lax.fori_loop(0, 4, use_far, 0)

    def one_head(h, _):
        for start in range(0, seq_len, BLK):
            keys, rows = pl.ds(0, start + BLK), pl.ds(start, BLK)
            probs = probs_transposed(k_ref[keys, :], q_ref[h, rows, :], start)
            o_scr[h, rows, :] = dot(probs.astype(BF16), v_ref[keys, :], 0, 0).astype(BF16)
        return 0
    for i in (0, 1, 2, 4, 5, 6, 7):
        stores[i].start()
    lax.fori_loop(0, heads, one_head, 0)
    for h in range(heads):
        o_own[:, h * head_dim:(h + 1) * head_dim] = o_scr[h]
    o_gather = Gather(lambda d: o_all.at[:, cols_of(d)], o_send, o_recv, where, o_all.at[:, pl.ds(0, 7 * rows_own)], own=o_own)
    o_gather.start()
    wo_gather.got_first()
    wo_gather.got_second()
    start_bulk(4)
    o_all[:, cols_of(me)] = o_own[...]

    def turn_out(k, _):
        rows = tok_of(k)
        ot_ref[:, rows] = o_own[rows, :].T
        return 0
    lax.fori_loop(0, 8, turn_out, 0)
    stores[3].start()
    wo_gather.got_diag()
    for i in range(4):
        wo_gather.got_partner(i)
    o_gather.got_first()
    o_gather.got_second()
    start_bulk(5, 6)
    o_gather.got_partner(0)
    o_gather.got_diag()
    for i in range(1, 4):
        o_gather.got_partner(i)
    start_bulk(7, 8, 9)

    def rows_at(i):
        flips = lambda a, b: other(0, a, b)
        return tok_of(jnp.where(i == 0, me, jnp.where(i == 1, flips(1, 0), jnp.where(i == 2, flips(0, 1), flips(1, 1)))))

    def give(i):
        slot = lax.rem(i, 2)
        rows = rows_at(i)
        return (pltpu.make_async_copy(m_out.at[slot], m_ref.at[rows, :], m_loc.at[slot]),
                pltpu.make_async_remote_copy(src_ref=m_out.at[slot], dst_ref=m_ref.at[rows, :], send_sem=m_send.at[i],
                                             recv_sem=m_recv.at[i], device_id=(partner,), device_id_type=MESH))

    def hidden_block(i, _):
        rows = rows_at(i)
        base = rows.start
        slot = lax.rem(i, 2)

        @pl.when(i >= 2)
        def _():
            to_hbm, to_partner = give(i - 2)
            to_hbm.wait()
            to_partner.wait_send()

        def chunk(j, _):
            cols = pl.ds(pl.multiple_of(j * 256, 256), 256)
            h_scr[:, cols] = dot(o_all[rows, :], wo_all[:, cols], 1, 0)
            return 0
        lax.fori_loop(0, model // 256, chunk, 0)

        def norm(k, _):
            part = pl.ds(pl.multiple_of(k * 16, 16), 16)
            x_part = x_all[pl.ds(pl.multiple_of(base + k * 16, 16), 16), :].astype(F32)
            hidden = (x_part + h_scr[part, :]).astype(BF16)

            @pl.when(i == 0)
            def _():
                h_ref[part, :] = hidden
            m_out[slot, part, :] = norm_forward(hidden.astype(F32), gfull_ref[1:2, :]).astype(BF16)
            return 0
        lax.fori_loop(0, tokens // 16, norm, 0)
        for copy in give(i):
            copy.start()
        return 0
    lax.fori_loop(0, 4, hidden_block, 0)
    stores[8].start()
    for i in range(4):
        give(i)[1].wait_recv()
    for i in range(2, 4):
        give(i)[0].wait()
        give(i)[1].wait_send()
    for copy in small + slices:
        copy.wait_send()
    for gather in (x_gather, wo_gather, o_gather):
        gather.drain()
    for load, store in local:
        store.wait()
    for copy in stores:
        copy.wait()
    for mat, dst in enumerate((w1_ref, w3_ref)):
        seven = dst.at[pl.ds(0, 7 * rows_own), :]
        pltpu.make_async_remote_copy(src_ref=seven, dst_ref=seven, send_sem=bulk_send.at[mat], recv_sem=bulk_recv.at[mat],
                                     device_id=(partner,), device_id_type=MESH).wait()


def attention_step(heads, x_in, positions, gain1, gain2, w_q, w_k, w_v, wo_own, w_gate, w_up):
    tokens, model = x_in.shape
    seq_len = 8 * tokens
    head_dim = wo_own.shape[0] // heads
    rows_own, hid = w_gate.shape[0], w_gate.shape[1] // 8
    shape = jax.ShapeDtypeStruct
    hbm = pl.BlockSpec(memory_space=pl.ANY)
    dma = pltpu.SemaphoreType.DMA
    vm = lambda *dims, dtype=BF16: pltpu.VMEM(dims, dtype)
    steps = np.arange(head_dim // 2, dtype=np.float32) * np.float32(2.0 / head_dim)
    freq = np.tile(np.float32(1.0) / (np.float32(ROPE_BASE) ** steps), 4)[None]
    outs = (shape((heads, seq_len, head_dim), BF16), shape((seq_len, head_dim), BF16), shape((seq_len, head_dim), BF16),
            shape((heads * head_dim, seq_len), BF16), shape((rows_own, seq_len), BF16),
            shape((seq_len, 128), F32), shape((seq_len, 128), F32), shape((8, model), F32), shape((tokens, model), BF16))
    pairs = [dma((1,)), dma((1,)), dma((3,)), dma((3,)), dma((1,)), dma((7,)), dma((1,)), dma((7,)),
             dma((2,)), dma((2,)), dma((1,)), dma((7,))]
    return pl.pallas_call(
        functools.partial(attention_comm_kernel, 'sp', heads), name='attention_comm',
        in_specs=[hbm] * 11, out_specs=[hbm] * 12,
        out_shape=[*outs, shape((seq_len, model), BF16), shape((model, hid), BF16), shape((model, hid), BF16)],
        scratch_shapes=[vm(*t.shape, dtype=t.dtype) for t in outs] + [
            vm(tokens, dtype=jnp.int32), vm(rows_own), vm(rows_own), vm(1, 2 * head_dim, dtype=F32),
            vm(8, rows_own, dtype=F32), vm(seq_len, model), vm(8, 8, rows_own, dtype=F32),
            vm(384, model), vm(model, model), vm(seq_len, model), vm(tokens, model), vm(tokens, 384), vm(heads, seq_len, head_dim),
            vm(seq_len, heads * head_dim), vm(tokens, model, dtype=F32), vm(2, tokens, model), vm(2, rows_own, hid)] + pairs + [
            dma((2,)), dma((4,)), dma((4,)), dma((4,)), dma((12,)), dma((9,)), pltpu.SemaphoreType.REGULAR((4,))],
        compiler_params=pltpu.CompilerParams(collective_id=0, has_side_effects=True, vmem_limit_bytes=63 * 1024 * 1024),
    )(x_in, positions, gain1, gain2, jnp.asarray(freq), w_q, w_k, w_v, wo_own, w_gate, w_up)


def hand_over_kernel(n_in, *refs):
    sources, gains, results = refs[:n_in], refs[n_in], refs[n_in + 1:2 * n_in + 1]
    gain_outs, lines, sem = refs[2 * n_in + 1:2 * n_in + 3], refs[2 * n_in + 3:2 * n_in + 5], refs[2 * n_in + 5]
    stores = [pltpu.make_async_copy(sources[i], results[i], sem.at[i]) for i in range(n_in)]
    for store in stores:
        store.start()
    for i in range(2):
        lines[i][...] = gains[i, :]
        stores.append(pltpu.make_async_copy(lines[i], gain_outs[i], sem.at[n_in + i]))
        stores[-1].start()
    for store in stores:
        store.wait()


def hand_over(arrays, gains):
    shape = jax.ShapeDtypeStruct
    hbm, vmem = pl.BlockSpec(memory_space=pltpu.HBM), pl.BlockSpec(memory_space=pltpu.VMEM)
    return pl.pallas_call(
        functools.partial(hand_over_kernel, len(arrays)), name='hand_over',
        in_specs=[vmem] * (len(arrays) + 1), out_specs=[hbm] * (len(arrays) + 2),
        out_shape=[shape(a.shape, a.dtype) for a in arrays] + [shape((gains.shape[1],), F32)] * 2,
        scratch_shapes=[pltpu.VMEM((gains.shape[1],), F32)] * 2 + [pltpu.SemaphoreType.DMA((len(arrays) + 2,))],
        compiler_params=pltpu.CompilerParams(vmem_limit_bytes=1024 * 1024),
    )(*[pltpu.with_memory_space_constraint(a, pltpu.VMEM) for a in arrays + (gains,)])


def solution(mesh):
    n_dev = mesh.shape['sp']

    def layer_step(x_in, positions, d_out, norm1_gain, norm2_gain, w_q, w_k, w_v, w_o, w_gate, w_up, w_down):
        tokens, model = x_in.shape
        head_dim = w_q.shape[2]
        heads = w_q.shape[1] // n_dev
        rows_own = w_q.shape[0]
        flat = lambda w: w.transpose(1, 2, 0).reshape(-1, rows_own)
        wo_own = w_o.reshape(-1, model)
        (q_rot, k_rot, v_lin, o_t, u_t, cos_tab, sin_tab, g_full, hidden,
         mlp_in, w1, w3) = attention_step(heads, x_in, positions, norm1_gain, norm2_gain, flat(w_q), flat(w_k), flat(w_v), wo_own, w_gate, w_up)
        d_w1s, d_w3s, d_down, y_out, dh_own, d_g2, early = mlp_step(mlp_in, d_out, w1, w3, w_down, hidden, g_full)
        d_wo, d_wq_t, d_wk_t, d_wv_t, d_w1, d_w3, d_x, d_gains, d_down, y_out = attention_backward_step(
            heads, dh_own, wo_own, o_t, q_rot, k_rot, v_lin, (cos_tab, sin_tab),
            d_w1s, d_w3s, flat(w_q), flat(w_k), flat(w_v), u_t, x_in, g_full, d_g2, d_down, y_out, early)
        from_cols = lambda d, w: d.reshape(w.shape[1], w.shape[2], rows_own).transpose(2, 0, 1)
        (d_down, y_out, d_w1, d_w3, d_wo, d_wq_t, d_wk_t, d_wv_t, d_x, d_g1, d_g2) = hand_over(
            (d_down, y_out, d_w1, d_w3, d_wo, d_wq_t, d_wk_t, d_wv_t, d_x), d_gains)
        return (y_out, d_x, d_g1, d_g2, from_cols(d_wq_t, w_q), from_cols(d_wk_t, w_k), from_cols(d_wv_t, w_v),
                d_wo.reshape(w_o.shape), d_w1, d_w3, d_down)

    all_rows = P('sp')
    return jax.shard_map(layer_step, mesh=mesh, in_specs=(all_rows,) * 12, out_specs=(all_rows,) * 11, check_vma=False)
```

```python
import functools
import jax
import jax.numpy as jnp
import numpy as np
from jax import lax
from jax.experimental import pallas as pl
from jax.experimental.pallas import tpu as pltpu
from jax.sharding import PartitionSpec as P

ROPE_BASE = 10000.0
NORM_EPS = 1e-5
NEG_LARGE = -1e30
F32 = jnp.float32
BF16 = jnp.bfloat16
BLK = 256
EARLY_ROWS = 8


def dot(lhs, rhs, lhs_dim, rhs_dim):
    return lax.dot_general(lhs, rhs, (((lhs_dim,), (rhs_dim,)), ((), ())), preferred_element_type=F32)


def norm_forward(hidden, gain_vec):
    inv_rms = lax.rsqrt(jnp.mean(hidden * hidden, axis=-1, keepdims=True) + NORM_EPS)
    return hidden * inv_rms * gain_vec


def probs_transposed(k_rows, q_blk, start):
    scores = dot(k_rows, q_blk, 1, 1)
    rows = lax.broadcasted_iota(jnp.int32, (BLK, BLK), 0)
    cols = lax.broadcasted_iota(jnp.int32, (BLK, BLK), 1)
    tail = jnp.where(rows <= cols, scores[start:], NEG_LARGE)
    scores = jnp.concatenate([scores[:start], tail], axis=0) if start else tail
    top = jnp.max(scores, axis=0, keepdims=True)
    weights = jnp.exp((scores - top) * (q_blk.shape[1] ** -0.5))
    return weights * (1.0 / jnp.sum(weights, axis=0, keepdims=True))


MESH = pl.DeviceIdType.MESH


def place(axis):
    me = lax.axis_index(axis)
    core = lax.rem(me, 2)
    col = lax.rem(lax.div(me, 2), 2)
    row = lax.div(me, 4)

    def other(flip_core, flip_col, flip_row):
        pick = lambda v, f: 1 - v if f else v
        return pick(row, flip_row) * 4 + pick(col, flip_col) * 2 + pick(core, flip_core)

    nbr_x, nbr_y = other(0, 1, 0), other(0, 0, 1)
    first = nbr_x * (1 - core) + nbr_y * core
    second = nbr_y * (1 - core) + nbr_x * core
    return me, other, first, second


def greet(where):
    _, other, first, second = where
    barrier = pltpu.get_barrier_semaphore()
    for device in (first, second, other(1, 0, 0)):
        pl.semaphore_signal(barrier, inc=1, device_id=(device,), device_id_type=MESH)
    pl.semaphore_wait(barrier, 3)


def relay(where, sem, base):
    _, other, first, second = where
    partner = other(1, 0, 0)
    for i, device in enumerate((first, second, partner)):
        pl.semaphore_signal(sem.at[base + i], inc=1, device_id=(device,), device_id_type=MESH)
    for i in range(3):
        pl.semaphore_wait(sem.at[base + i], 1)
    pl.semaphore_signal(sem.at[base + 3], inc=1, device_id=(partner,), device_id_type=MESH)
    pl.semaphore_wait(sem.at[base + 3], 1)


class Gather:
    def __init__(self, slot, send_sem, recv_sem, where, seven, own=None):
        me, other, first, second = where
        partner, diag = other(1, 0, 0), other(0, 1, 1)
        own = slot(me) if own is None else own
        self.copies = []
        plan = [(own, me, first), (own, me, second), (own, me, partner), (slot(first), first, second),
                (slot(first), first, partner), (slot(second), second, partner), (slot(diag), diag, partner)]
        for i, (src, what, dest) in enumerate(plan):
            self.copies.append(pltpu.make_async_remote_copy(
                src_ref=src, dst_ref=slot(what), send_sem=send_sem.at[0], recv_sem=recv_sem.at[i],
                device_id=(dest,), device_id_type=MESH))
        self.sent = pltpu.make_async_remote_copy(
            src_ref=seven, dst_ref=seven, send_sem=send_sem.at[0], recv_sem=recv_sem.at[0],
            device_id=(partner,), device_id_type=MESH)

    def start(self):
        for i in range(3):
            self.copies[i].start()

    def got_first(self):
        self.copies[0].wait_recv()
        self.copies[3].start()
        self.copies[4].start()

    def got_second(self):
        self.copies[1].wait_recv()
        self.copies[5].start()

    def got_diag(self):
        self.copies[3].wait_recv()
        self.copies[6].start()

    def got_partner(self, i):
        self.copies[(2, 4, 5, 6)[i]].wait_recv()

    def drain(self):
        self.sent.wait_send()


def turn_halves(values, cos_blk, sin_blk):
    width = values.shape[1]
    lanes = lax.broadcasted_iota(jnp.int32, values.shape, 1)
    partner = jnp.where(lax.rem(lanes, 64) < 32, pltpu.roll(values, width - 32, 1), pltpu.roll(values, 32, 1))
    return values * cos_blk + partner * sin_blk


def norm_backward(hidden, gain, d_out):
    inv = lax.rsqrt(jnp.mean(hidden * hidden, axis=-1, keepdims=True) + NORM_EPS)
    d_scaled = d_out * gain
    d_hidden = d_scaled * inv - hidden * (inv * inv * inv * jnp.mean(d_scaled * hidden, axis=-1, keepdims=True))
    return d_hidden, jnp.sum(d_out * (hidden * inv), axis=0, keepdims=True)


def attn_bwd_comm_kernel(axis, heads, dh_hbm, wo_hbm, ot_hbm, q_hbm, k_hbm, v_hbm, cos_hbm, sin_hbm,
                         dw1_ref, dw3_ref, wq_hbm, wk_hbm, wv_hbm, ut_hbm, x_hbm, g_hbm, dg2_hbm, ddown_hbm, y_hbm, early_hbm,
                         dwo_ref, dwq_ref, dwk_ref, dwv_ref, out1_ref, out3_ref, dx_ref, dg_ref, ddown_ref, y_ref,
                         dh_own, wo_ref, ot_ref, q_ref, k_ref, v_ref, cos_ref, sin_ref, wq_ref, wk_ref, wv_ref, ut_ref, g_ref, dg2_ref,
                         pool, do_scr, dg_own, dg_all, dk_acc, dv_acc, du_acc,
                         bulk_send, bulk_recv, hg_send, hg_recv, gat_send, gat_recv, du_send, du_rsem, dg_send, dg_recv, loc_sem, ld_sem, credit):
    loads = {}
    for i, (name, src, dst) in enumerate((
            ('wo', wo_hbm, wo_ref), ('ot', ot_hbm, ot_ref), ('q', q_hbm, q_ref), ('k', k_hbm, k_ref),
            ('v', v_hbm, v_ref), ('cos', cos_hbm, cos_ref), ('sin', sin_hbm, sin_ref), ('wq', wq_hbm, wq_ref), ('wk', wk_hbm, wk_ref),
            ('wv', wv_hbm, wv_ref), ('ut', ut_hbm, ut_ref), ('g', g_hbm, g_ref), ('dg2', dg2_hbm, dg2_ref),
            ('dh', dh_hbm, dh_own), ('ddown', ddown_hbm, ddown_ref), ('y', y_hbm, y_ref))):
        loads[name] = pltpu.make_async_copy(src, dst, ld_sem.at[i])
        loads[name].start()

    def need(*names):
        for name in names:
            loads[name].wait()

    where = place(axis)
    me, other, first, second = where
    greet(where)
    seq_len, head_dim = k_ref.shape
    rows_own, hid = out1_ref.shape[0], dw1_ref.shape[1]
    tokens, model = x_hbm.shape
    qw = heads * head_dim

    rows_of = lambda d: pl.ds(pl.multiple_of(d * rows_own, rows_own), rows_own)
    hid_of = lambda d: pl.ds(pl.multiple_of(d * hid, hid), hid)
    pairs = ((dw1_ref, out1_ref), (dw3_ref, out3_ref))
    peers = [other(r & 1, (r >> 1) & 1, r >> 2) for r in (2, 4, 6, 3, 5, 7, 1)]
    bulk, parts = [], []
    for mat, (src, dst) in enumerate(pairs):
        skip = (EARLY_ROWS, 0)[mat]
        for low, high in ((skip, skip + 16), (skip + 16, rows_own // 2), (rows_own // 2, rows_own)):
            parts.append(range(len(bulk), len(bulk) + len(peers)))
            for dest in peers:
                bulk.append(pltpu.make_async_remote_copy(
                    src_ref=src.at[pl.ds(pl.multiple_of(dest * rows_own + low, 8), high - low), :],
                    dst_ref=dst.at[pl.ds(low, high - low), hid_of(me)], send_sem=bulk_send.at[mat],
                    recv_sem=bulk_recv.at[mat], device_id=(dest,), device_id_type=MESH))

    def start_bulk(*which):
        for part in which:
            for i in parts[part]:
                bulk[i].start()
    tok_of = lambda d: pl.ds(pl.multiple_of(d * tokens, tokens), tokens)
    dh_ref = pool.at[:, 0:model]
    h_gather = Gather(lambda d: dh_ref.at[tok_of(d), :], hg_send, hg_recv, where, dh_ref.at[pl.ds(0, 7 * tokens), :], own=dh_hbm)
    h_gather.start()
    relay(where, credit, 3)
    start_bulk(0)
    local = [pltpu.make_async_copy(src.at[rows_of(me), :], dst.at[:, hid_of(me)], loc_sem.at[i]) for i, (src, dst) in enumerate(pairs)]
    for copy in local:
        copy.start()
    for dest in peers:
        pltpu.make_async_copy(early_hbm.at[:, hid_of(dest)], out1_ref.at[0:EARLY_ROWS, hid_of(dest)], loc_sem.at[2]).start()
    need('dh', 'wo', 'ot')
    pool[tok_of(me), 0:model] = dh_own[...]
    h_gather.got_first()
    h_gather.got_second()
    start_bulk(1, 2)
    h_gather.got_diag()
    for i in range(4):
        h_gather.got_partner(i)

    def split_out_grad(k, _):
        rows = pl.ds(pl.multiple_of(k * BLK, BLK), BLK)
        do_blk = dot(pool[rows, 0:model], wo_ref[...], 1, 1).astype(BF16)
        for h in range(heads):
            do_scr[h, rows, :] = do_blk[:, h * head_dim:(h + 1) * head_dim]
        cols = rows
        dwo_ref[:, cols] = dot(ot_ref[...], pool[:, cols], 1, 0)
        return 0
    lax.fori_loop(0, seq_len // BLK, split_out_grad, 0)
    h_gather.drain()
    for i, device in enumerate((first, second, other(1, 0, 0))):
        pl.semaphore_signal(credit.at[i], inc=1, device_id=(device,), device_id_type=MESH)
    x_ref = wo_ref
    x_load = pltpu.make_async_copy(x_hbm, x_ref, ld_sem.at[16])
    x_load.start()


    need('q', 'k', 'v')
    dk_acc[...] = jnp.zeros_like(dk_acc)
    dv_acc[...] = jnp.zeros_like(dv_acc)
    slot_cols = lambda d, off, width: pl.ds(pl.multiple_of(d * 384 + off, 128), width)

    def one_head(h, _):
        def one_block(start):
            keys = pl.ds(0, start + BLK)
            rows = pl.ds(start, BLK)
            q_blk, do_blk = q_ref[h, rows, :], do_scr[h, rows, :]
            probs = probs_transposed(k_ref[keys, :], q_blk, start)
            d_probs = dot(v_ref[keys, :], do_blk, 1, 1).astype(BF16).astype(F32)
            row_dot = jnp.sum(d_probs * probs, axis=0, keepdims=True)
            d_scores = (probs * (d_probs - row_dot) * (head_dim ** -0.5)).astype(BF16)
            do_scr[h, rows, :] = dot(d_scores, k_ref[keys, :], 0, 0).astype(BF16)
            dk_acc[keys, :] += dot(d_scores, q_blk, 1, 0)
            dv_acc[keys, :] += dot(probs.astype(BF16), do_blk, 1, 0)
        for start in range(0, seq_len, BLK):
            one_block(start)
        return 0
    lax.fori_loop(0, heads, one_head, 0)
    need('cos', 'sin')
    low = lax.broadcasted_iota(jnp.int32, (BLK, 128), 1) < head_dim

    def turn_back(k, _):
        rows = pl.ds(pl.multiple_of(k * BLK, BLK), BLK)
        cos_blk, sin_blk = cos_ref[rows, :], -sin_ref[rows, :]
        for pair in range(heads // 2):
            both = jnp.concatenate([do_scr[2 * pair, rows, :], do_scr[2 * pair + 1, rows, :]], axis=1)
            pool[rows, slot_cols(me, pair * 128, 128)] = turn_halves(both.astype(F32), cos_blk, sin_blk).astype(BF16)
        kv = jnp.concatenate([dk_acc[rows, :], dv_acc[rows, :]], axis=1).astype(BF16).astype(F32)
        pool[rows, slot_cols(me, qw, 128)] = jnp.where(low, turn_halves(kv, cos_blk, sin_blk), kv).astype(BF16)
        return 0
    lax.fori_loop(0, seq_len // BLK, turn_back, 0)

    gather = Gather(lambda d: pool.at[:, slot_cols(d, 0, 384)], gat_send, gat_recv, where, pool.at[:, pl.ds(0, 7 * 384)])
    for i in range(3):
        pl.semaphore_wait(credit.at[i], 1)
    gather.start()
    start_bulk(3)
    du_acc[...] = jnp.zeros_like(du_acc)
    need('wq', 'wk', 'wv', 'ut')

    def use(d):
        q_rows = pl.ds(pl.multiple_of(d * qw, qw), qw)
        kv_rows = pl.ds(pl.multiple_of(d * head_dim, head_dim), head_dim)
        w_all = jnp.concatenate([wq_ref[q_rows, :], wk_ref[kv_rows, :], wv_ref[kv_rows, :]], axis=0)

        def add_rows(k, _):
            rows = pl.ds(pl.multiple_of(k * 512, 512), 512)
            du_acc[rows, :] += dot(pool[rows, slot_cols(d, 0, 384)], w_all, 1, 0)
            return 0
        lax.fori_loop(0, seq_len // 512, add_rows, 0)
        d_w = dot(ut_ref[...], pool[:, slot_cols(d, 0, 384)], 1, 0).T
        dwq_ref[q_rows, :] = d_w[:qw]
        dwk_ref[kv_rows, :] = d_w[qw:qw + head_dim]
        dwv_ref[kv_rows, :] = d_w[qw + head_dim:]

    def use_many(*devices):
        def body(i, _):
            d = devices[0]
            for n in range(1, len(devices)):
                d = jnp.where(i == n, devices[n], d)
            use(d)
            return 0
        lax.fori_loop(0, len(devices), body, 0)

    use_many(me)
    gather.got_first()
    gather.got_second()
    start_bulk(4)
    gather.got_partner(0)
    use_many(first, second, other(1, 0, 0))
    gather.got_diag()
    for i in range(1, 4):
        gather.got_partner(i)
    use_many(other(0, 1, 1), other(1, 1, 0), other(1, 0, 1), other(1, 1, 1))
    gather.drain()
    du_scr = pool.at[:, 0:rows_own]

    def round_du(k, _):
        rows = pl.ds(pl.multiple_of(k * BLK, BLK), BLK)
        pool[rows, 0:rows_own] = du_acc[rows, :].astype(BF16)
        return 0
    lax.fori_loop(0, seq_len // BLK, round_du, 0)
    for dest in peers:
        pltpu.make_async_remote_copy(
            src_ref=du_scr.at[tok_of(dest), :], dst_ref=ot_ref.at[:, rows_of(me)], send_sem=du_send.at[0],
            recv_sem=du_rsem.at[0], device_id=(dest,), device_id_type=MESH).start()
    start_bulk(5)
    ot_ref[:, rows_of(me)] = pool[tok_of(me), 0:rows_own]
    need('g', 'dg2')
    x_load.wait()
    got = ot_ref.at[:, pl.ds(0, 7 * rows_own)]
    pltpu.make_async_copy(got, got, du_rsem.at[0]).wait()
    dg_own[...] = jnp.zeros_like(dg_own)
    dg_own[1:2, :] = dg2_ref[...]

    def input_grad(k, _):
        part = pl.ds(pl.multiple_of(k * 16, 16), 16)
        d_norm, d_gain = norm_backward(x_ref[part, :].astype(F32), g_ref[0:1, :], ot_ref[part, :].astype(F32))
        dh_part = dh_own[part, :]
        dx_ref[part, :] = (dh_part.astype(F32) + d_norm).astype(BF16)
        dg_own[0:1, :] += d_gain
        return 0
    lax.fori_loop(0, tokens // 16, input_grad, 0)
    for dest in peers:
        pltpu.make_async_remote_copy(
            src_ref=dg_own.at[:, rows_of(dest)], dst_ref=dg_all.at[me], send_sem=dg_send.at[0],
            recv_sem=dg_recv.at[0], device_id=(dest,), device_id_type=MESH).start()
    dg_all[me] = dg_own[:, rows_of(me)]
    got = dg_all.at[pl.ds(0, 7)]
    pltpu.make_async_copy(got, got, dg_recv.at[0]).wait()
    dg_ref[...] = jnp.sum(dg_all[...], axis=0)
    for sent, sem in ((du_scr.at[pl.ds(0, 7 * tokens), :], du_send), (dg_own.at[:, pl.ds(0, 7 * rows_own)], dg_send)):
        pltpu.make_async_copy(sent, sent, sem.at[0]).wait()
    need('ddown', 'y')
    for copy in local:
        copy.wait()
    seven = out1_ref.at[0:EARLY_ROWS, pl.ds(0, 7 * hid)]
    pltpu.make_async_copy(seven, seven, loc_sem.at[2]).wait()
    for mat, (src, dst) in enumerate(pairs):
        rows = rows_own - (EARLY_ROWS, 0)[mat]
        sent, got = src.at[pl.ds(0, 7 * rows), :], dst.at[0:rows, pl.ds(0, 7 * hid)]
        pltpu.make_async_copy(sent, sent, bulk_send.at[mat]).wait()
        pltpu.make_async_copy(got, got, bulk_recv.at[mat]).wait()


def attention_backward_step(heads, dh_own, wo_own, o_t, q_rot, k_rot, v_lin, tables, d_w1, d_w3, w_q, w_k, w_v, u_t, x_in, gains, d_g2, d_down, y_out, early_rows):
    seq_len, model = k_rot.shape[0], x_in.shape[1]
    head_dim = k_rot.shape[1]
    tokens = x_in.shape[0]
    rows_own, hid = model // 8, d_w1.shape[1]
    shape = jax.ShapeDtypeStruct
    hbm = pl.BlockSpec(memory_space=pl.ANY)
    dma = pltpu.SemaphoreType.DMA
    vm = lambda *dims, dtype=BF16: pltpu.VMEM(dims, dtype)
    early = (dh_own, wo_own, o_t, q_rot, k_rot, v_lin, *tables)
    late = (w_q, w_k, w_v, u_t, x_in, gains, d_g2)
    outs = [(wo_own.shape, F32), (w_q.shape, F32), (w_k.shape, F32), (w_v.shape, F32), ((rows_own, 8 * hid), F32),
            ((rows_own, 8 * hid), F32), (x_in.shape, BF16), ((8, rows_own), F32), (d_down.shape, F32), (y_out.shape, BF16)]
    vmem, far = pl.BlockSpec(memory_space=pltpu.VMEM), pl.BlockSpec(memory_space=pltpu.HBM)
    return pl.pallas_call(
        functools.partial(attn_bwd_comm_kernel, 'sp', heads), name='attn_bwd_comm',
        in_specs=[hbm] * 17 + [far] * 3, out_specs=[vmem] * 10,
        out_shape=[pltpu.VMEM(dims, dtype) for dims, dtype in outs],
        scratch_shapes=[vm(*t.shape, dtype=t.dtype) for t in early + late[:4] + late[5:]] + [
            vm(seq_len, 8 * 384), vm(heads, seq_len, head_dim),
            vm(8, model, dtype=F32), vm(8, 8, rows_own, dtype=F32),
            vm(seq_len, head_dim, dtype=F32), vm(seq_len, head_dim, dtype=F32),
            vm(seq_len, rows_own, dtype=F32),
            dma((2,)), dma((2,)), dma((1,)), dma((7,)), dma((1,)), dma((7,)), dma((1,)), dma((1,)), dma((1,)), dma((1,)), dma((3,)), dma((17,)), pltpu.SemaphoreType.REGULAR((7,))],
        compiler_params=pltpu.CompilerParams(collective_id=2, has_side_effects=True, vmem_limit_bytes=34340864),
    )(*early, d_w1, d_w3, *late, *[pltpu.with_memory_space_constraint(a, pltpu.HBM) for a in (d_down, y_out, early_rows)])


def mlp_comm_kernel(axis, m_ref, dout_own, w1_hbm, w3_hbm, w2_hbm, h_hbm, g_hbm,
                    dw1_ref, dw3_ref, dw2_ref, y_hbm, dh_hbm, dg2_hbm, early_ref, dout_ref,
                    w1_ref, w3_ref, w2_ref, h_ref, g_ref, y_ref, dg2_ref,
                    glu, gate_s, up_s, outbox, chip_sum, inbox, blk, m_col, do_col, mt_scr, dot_scr, st1, st3, st2, dh_own,
                    part_send, part_recv, mail_send, mail_recv, do_send, do_recv,
                    in_sem, col_sem, out_sem, own_sem, ld_sem, early_sem, credit):
    loads = [pltpu.make_async_copy(src, dst, ld_sem.at[i]) for i, (src, dst) in enumerate((
        (w1_hbm, w1_ref), (w3_hbm, w3_ref), (w2_hbm, w2_ref), (h_hbm, h_ref), (g_hbm, g_ref)))]
    own_in = pltpu.make_async_copy(dout_own, dh_own, own_sem.at[0])
    for copy in loads + [own_in]:
        copy.start()
    where = place(axis)
    me, other, first, second = where
    core = lax.rem(me, 2)
    partner = other(1, 0, 0)
    tokens, model = h_ref.shape
    hid = w1_ref.shape[1]
    tok_of = lambda d: pl.ds(pl.multiple_of(d * tokens, tokens), tokens)
    off_first, off_second = 1 + core, 2 - core

    def block_of(off, flip):
        d_col, d_row = lax.rem(off, 2), lax.div(off, 2)
        col, row = lax.rem(lax.div(me, 2), 2), lax.div(me, 4)
        mix = lambda v, f: v + f - 2 * v * f
        return mix(row, d_row) * 4 + mix(col, d_col) * 2 + mix(core, flip)

    def step_off(step, flip):
        mid_a = off_second * (1 - flip) + off_first * flip
        mid_b = off_first * (1 - flip) + off_second * flip
        return jnp.where(step == 0, 3, jnp.where(step == 1, mid_a, jnp.where(step == 2, mid_b, 0)))

    def half_rows(half):
        flip = 1 - lax.rem(half, 2)
        return tok_of(block_of(step_off(lax.div(half, 2), flip), flip))

    def fetch(half):
        slot = lax.rem(half, 2)
        return pltpu.make_async_copy(m_ref.at[half_rows(half), :], blk.at[slot], in_sem.at[slot])

    def fetch_dout(d):
        slot = lax.rem(d, 2)
        return pltpu.make_async_copy(dout_ref.at[tok_of(d), :], blk.at[slot], in_sem.at[slot])

    def fetch_cols(j):
        cols = pl.ds(pl.multiple_of(j * 256, 256), 256)
        return (pltpu.make_async_copy(m_ref.at[:, cols], m_col, col_sem.at[0]),
                pltpu.make_async_copy(dout_ref.at[:, cols], do_col, col_sem.at[1]))

    def sigmoid(value):
        return 1.0 / (1.0 + jnp.exp(-value))

    def activations(slot, rows):
        def chunk(j, _):
            cols = pl.ds(pl.multiple_of(j * 512, 512), 512)
            gate = dot(blk[slot], w1_ref[:, cols], 1, 0).astype(BF16)
            up = dot(blk[slot], w3_ref[:, cols], 1, 0).astype(BF16)
            gate_s[rows, cols] = gate
            up_s[rows, cols] = up
            gate = gate.astype(F32)
            glu[rows, cols] = (gate * sigmoid(gate) * up.astype(F32)).astype(BF16)
            return 0
        lax.fori_loop(0, hid // 512, chunk, 0)

    def activation_grads(slot, rows):
        def chunk(j, _):
            cols = pl.ds(pl.multiple_of(j * 512, 512), 512)
            d_act = dot(blk[slot], w2_ref[cols, :], 1, 1).astype(BF16).astype(F32)
            gate, up = gate_s[rows, cols].astype(F32), up_s[rows, cols].astype(F32)
            sig = sigmoid(gate)
            silu = gate * sig
            up_s[rows, cols] = (d_act * silu).astype(BF16)
            gate_s[rows, cols] = (d_act * up * (sig + silu * (1.0 - sig))).astype(BF16)
            return 0
        lax.fori_loop(0, hid // 512, chunk, 0)

    def add_mlp_grad(rows, put):
        def chunk(j, _):
            cols = pl.ds(pl.multiple_of(j * 512, 512), 512)
            put(cols, dot(gate_s[rows, :], w1_ref[cols, :], 1, 1) + dot(up_s[rows, :], w3_ref[cols, :], 1, 1))
            return 0
        lax.fori_loop(0, model // 512, chunk, 0)

    def add_mlp_out(rows, put):
        def chunk(j, _):
            cols = pl.ds(pl.multiple_of(j * 512, 512), 512)
            put(cols, dot(glu[rows, :], w2_ref[:, cols], 1, 0))
            return 0
        lax.fori_loop(0, model // 512, chunk, 0)

    def signal(index, device):
        pl.semaphore_signal(credit.at[index], inc=1, device_id=(device,), device_id_type=MESH)

    class Scatter:
        def __init__(self, turn):
            self.turn = turn

        def to_partner(self, step):
            off = step_off(step, 1)
            return pltpu.make_async_remote_copy(
                src_ref=outbox.at[lax.rem(step, 2)], dst_ref=chip_sum.at[off], send_sem=part_send.at[self.turn, step],
                recv_sem=part_recv.at[self.turn, off], device_id=(partner,), device_id_type=MESH)

        def from_partner(self, off):
            return pltpu.make_async_remote_copy(
                src_ref=outbox.at[0], dst_ref=chip_sum.at[off], send_sem=part_send.at[self.turn, 0],
                recv_sem=part_recv.at[self.turn, off], device_id=(partner,), device_id_type=MESH)

        def mail(self, kind):
            off = (3, off_first, off_second)[kind]
            dest = (first, first, second)[kind]
            return pltpu.make_async_remote_copy(
                src_ref=chip_sum.at[off], dst_ref=inbox.at[kind], send_sem=mail_send.at[self.turn, kind],
                recv_sem=mail_recv.at[self.turn, kind], device_id=(dest,), device_id_type=MESH)

        def step(self, step, prepare, partial):
            self.first_half(step, prepare, partial)
            self.second_half(step, prepare, partial)

        def first_half(self, step, prepare, partial):
            slot = lax.rem(step, 2)
            prepare(2 * step)

            def put_out(cols, value):
                outbox[slot, :, cols] = value
            partial(half_rows(2 * step), put_out)

        def second_half(self, step, prepare, partial):
            self.to_partner(step).start()
            prepare(2 * step + 1)
            off = step_off(step, 0)
            self.from_partner(off).wait_recv()

            def put_sum(cols, value):
                chip_sum[off, :, cols] += value
            partial(half_rows(2 * step + 1), put_sum)

        def pass_on(self):
            self.mail(0).wait_recv()

            def add_mail(k, _):
                part = pl.ds(pl.multiple_of(k * 16, 16), 16)
                chip_sum[off_second, part, :] += inbox[0, part, :]
                return 0
            lax.fori_loop(0, tokens // 16, add_mail, 0)

    out_round, grad_round = Scatter(0), Scatter(1)

    def prepare_out(half):
        @pl.when(half < 7)
        def _():
            fetch(half + 1).start()
        fetch(half).wait()
        activations(lax.rem(half, 2), half_rows(half))

    def weight_grads(begin, end):
        for copy in fetch_cols(begin):
            copy.start()

        def body(j, _):
            for copy in fetch_cols(j):
                copy.wait()

            def turn(k, _):
                part = pl.ds(pl.multiple_of(k * 256, 256), 256)
                mt_scr[:, part] = m_col[part, :].T
                dot_scr[:, part] = do_col[part, :].T
                return 0
            lax.fori_loop(0, m_col.shape[0] // 256, turn, 0)

            @pl.when(j + 1 < end)
            def _():
                for copy in fetch_cols(j + 1):
                    copy.start()
            rows = pl.ds(pl.multiple_of(j * 256, 256), 256)
            out = (pltpu.make_async_copy(st1, dw1_ref.at[rows, :], out_sem.at[0]),
                   pltpu.make_async_copy(st3, dw3_ref.at[rows, :], out_sem.at[1]),
                   pltpu.make_async_copy(st2, dw2_ref.at[:, rows], out_sem.at[2]))

            @pl.when(j > begin)
            def _():
                for copy in out:
                    copy.wait()

            def chunk(k, _):
                cols = pl.ds(pl.multiple_of(k * 512, 512), 512)
                st1[:, cols] = dot(mt_scr[...], gate_s[:, cols], 1, 0)
                st3[:, cols] = dot(mt_scr[...], up_s[:, cols], 1, 0)
                st2[cols, :] = dot(dot_scr[...], glu[:, cols], 1, 0).T
                return 0
            lax.fori_loop(0, hid // 512, chunk, 0)
            for copy in out:
                copy.start()
            return 0
        lax.fori_loop(begin, end, body, 0)
        rows = pl.ds((end - 1) * 256, 256)
        for copy in (pltpu.make_async_copy(st1, dw1_ref.at[rows, :], out_sem.at[0]),
                     pltpu.make_async_copy(st3, dw3_ref.at[rows, :], out_sem.at[1]),
                     pltpu.make_async_copy(st2, dw2_ref.at[:, rows], out_sem.at[2])):
            copy.wait()

    fetch(0).start()
    greet(where)
    do_gather = Gather(lambda d: dout_ref.at[tok_of(d), :], do_send, do_recv, where, dout_ref.at[pl.ds(0, 7 * tokens), :], own=dout_own)
    do_gather.start()
    own_in.wait()
    own_out = pltpu.make_async_copy(dh_own, dout_ref.at[tok_of(me), :], own_sem.at[1])
    own_out.start()
    for copy in loads:
        copy.wait()

    relay(where, credit, 5)
    def out_step(step, _):
        @pl.when(step >= 2)
        def _():
            out_round.to_partner(step - 2).wait_send()
        out_round.step(step, prepare_out, add_mlp_out)

        @pl.when(step == 0)
        def _():
            out_round.mail(0).start()

        @pl.when(step == 2)
        def _():
            out_round.mail(1).start()
            do_gather.got_first()
            do_gather.got_second()
        return 0
    lax.fori_loop(0, 4, out_step, 0)
    out_round.pass_on()
    out_round.mail(2).start()
    for step in (2, 3):
        out_round.to_partner(step).wait_send()
    out_round.mail(0).wait_send()
    signal(0, partner)
    signal(1, first)
    do_gather.got_diag()
    for i in range(4):
        do_gather.got_partner(i)
    own_out.wait()
    fetch_dout(0).start()

    def grad_block(d, _):
        @pl.when(d < 7)
        def _():
            fetch_dout(d + 1).start()
        fetch_dout(d).wait()
        activation_grads(lax.rem(d, 2), tok_of(d))
        return 0
    lax.fori_loop(0, 8, grad_block, 0)

    as_is = lambda half: None
    grad_round.first_half(0, as_is, add_mlp_grad)
    pl.semaphore_wait(credit.at[0], 1)
    grad_round.second_half(0, as_is, add_mlp_grad)
    pl.semaphore_wait(credit.at[1], 1)
    grad_round.mail(0).start()
    weight_grads(0, 2)
    grad_round.first_half(1, as_is, add_mlp_grad)
    out_round.mail(1).wait_recv()
    out_round.mail(2).wait_recv()

    def layer_out(k, _):
        part = pl.ds(pl.multiple_of(k * 16, 16), 16)
        y_ref[part, :] = (h_ref[part, :].astype(F32) + (chip_sum[0, part, :] + inbox[1, part, :] + inbox[2, part, :])).astype(BF16)
        return 0
    lax.fori_loop(0, tokens // 16, layer_out, 0)
    y_store = pltpu.make_async_copy(y_ref, y_hbm, own_sem.at[2])
    y_store.start()
    out_round.mail(1).wait_send()
    out_round.mail(2).wait_send()
    signal(2, partner)
    signal(3, first)
    signal(4, second)
    pl.semaphore_wait(credit.at[2], 1)

    grad_round.second_half(1, as_is, add_mlp_grad)

    def grad_step(step, _):
        grad_round.to_partner(step - 2).wait_send()
        grad_round.step(step, as_is, add_mlp_grad)

        @pl.when(step == 2)
        def _():
            pl.semaphore_wait(credit.at[3], 1)
            grad_round.mail(1).start()
            grad_round.pass_on()
            pl.semaphore_wait(credit.at[4], 1)
            grad_round.mail(2).start()
        return 0
    lax.fori_loop(2, 4, grad_step, 0)
    weight_grads(2, 8)
    rows = early_ref.shape[0]
    for r in (2, 4, 6, 3, 5, 7, 1):
        dest = other(r & 1, (r >> 1) & 1, r >> 2)
        pltpu.make_async_remote_copy(
            src_ref=dw1_ref.at[pl.ds(pl.multiple_of(dest * 256, 256), rows), :],
            dst_ref=early_ref.at[:, pl.ds(pl.multiple_of(me * hid, hid), hid)], send_sem=early_sem.at[0],
            recv_sem=early_sem.at[1], device_id=(dest,), device_id_type=MESH).start()
    grad_round.mail(1).wait_recv()
    grad_round.mail(2).wait_recv()
    dg2_ref[...] = jnp.zeros_like(dg2_ref)

    def hidden_grad(k, _):
        part = pl.ds(pl.multiple_of(k * 16, 16), 16)
        d_mlp = (chip_sum[0, part, :] + inbox[1, part, :] + inbox[2, part, :]).astype(BF16).astype(F32)
        d_norm, d_gain = norm_backward(h_ref[part, :].astype(F32), g_ref[1:2, :], d_mlp)
        dh_own[part, :] = (dh_own[part, :].astype(F32) + d_norm).astype(BF16)
        dg2_ref[...] += d_gain
        return 0
    lax.fori_loop(0, tokens // 16, hidden_grad, 0, unroll=4)
    own_out = pltpu.make_async_copy(dh_own, dh_hbm, own_sem.at[3])
    own_out.start()
    dg2_store = pltpu.make_async_copy(dg2_ref, dg2_hbm, own_sem.at[4])
    dg2_store.start()
    for step in (2, 3):
        grad_round.to_partner(step).wait_send()
    for kind in range(3):
        grad_round.mail(kind).wait_send()
    seven = early_ref.at[:, pl.ds(0, 7 * hid)]
    for i in range(2):
        pltpu.make_async_copy(seven, seven, early_sem.at[i]).wait()
    do_gather.drain()
    own_out.wait()
    y_store.wait()
    dg2_store.wait()


def mlp_step(m_all, d_out, w1, w3, w2, hidden, gains):
    seq_len, model = m_all.shape
    hid, tokens = w1.shape[1], hidden.shape[0]
    shape = jax.ShapeDtypeStruct
    hbm = pl.BlockSpec(memory_space=pl.ANY)
    dma = pltpu.SemaphoreType.DMA
    vm = lambda *dims, dtype=BF16: pltpu.VMEM(dims, dtype)
    return pl.pallas_call(
        functools.partial(mlp_comm_kernel, 'sp'), name='mlp_comm',
        in_specs=[hbm] * 7, out_specs=[hbm] * 8,
        out_shape=[shape((model, hid), F32), shape((model, hid), F32), shape((hid, model), F32),
                   shape(hidden.shape, BF16), shape(hidden.shape, BF16), shape((1, model), F32), shape((EARLY_ROWS, 8 * hid), F32),
                   shape((seq_len, model), BF16)],
        scratch_shapes=[vm(*t.shape, dtype=t.dtype) for t in (w1, w3, w2, hidden, gains)] + [
            vm(tokens, model), vm(1, model, dtype=F32),
            vm(seq_len, hid), vm(seq_len, hid), vm(seq_len, hid),
            vm(2, tokens, model, dtype=F32), vm(4, tokens, model, dtype=F32), vm(3, tokens, model, dtype=F32),
            vm(2, tokens, model), vm(seq_len, 256), vm(seq_len, 256), vm(256, seq_len), vm(256, seq_len),
            vm(256, hid, dtype=F32), vm(256, hid, dtype=F32), vm(hid, 256, dtype=F32), vm(tokens, model),
            dma((2, 4)), dma((2, 4)), dma((2, 3)), dma((2, 3)), dma((1,)), dma((7,)),
            dma((2,)), dma((2,)), dma((3,)), dma((5,)), dma((5,)), dma((2,)), pltpu.SemaphoreType.REGULAR((9,))],
        compiler_params=pltpu.CompilerParams(collective_id=1, has_side_effects=True, vmem_limit_bytes=63 * 1024 * 1024),
    )(m_all, d_out, w1, w3, w2, hidden, gains)[:7]


def spread_tables(packed, upper):
    lanes = lax.broadcasted_iota(jnp.int32, packed.shape, 1)
    swapped = pltpu.roll(packed, 64, 1)
    both = jnp.where((lanes < 64) != upper, packed, swapped)
    low = lax.rem(lanes, 64) < 32
    return jnp.where(low, both, pltpu.roll(both, 32, 1)), jnp.where(low, -pltpu.roll(both, 96, 1), both)


def attention_comm_kernel(axis, heads, x_ref, pos_hbm, gain1_hbm, gain2_hbm, freq_hbm, wq_ref, wk_ref, wv_ref, wo_ref, wg_ref, wu_ref,
                          q_hbm, k_hbm, v_hbm, ot_hbm, ut_hbm, cos_hbm, sin_hbm, gfull_hbm, h_hbm, m_ref, w1_ref, w3_ref,
                          q_ref, k_ref, v_ref, ot_ref, ut_ref, cos_ref, sin_ref, gfull_ref, h_ref, pos_ref, gain1_ref, gain2_ref, freq_ref, gain_ref, x_all, gain_all, w_head, wo_all, o_all, u_blk, qkv_blk, o_scr, o_own, h_scr, m_out, stage,
                          g_send, g_recv, w_send, w_recv, x_send, x_recv, wo_send, wo_recv, bulk_send, bulk_recv,
                          o_send, o_recv, m_loc, m_send, m_recv, loc_sem, own_sem, st_sem, entry):
    tiny = [pltpu.make_async_copy(src, dst, own_sem.at[8 + i]) for i, (src, dst) in enumerate((
        (gain1_hbm, gain1_ref), (gain2_hbm, gain2_ref), (pos_hbm, pos_ref), (freq_hbm, freq_ref)))]
    for copy in tiny:
        copy.start()
    where = place(axis)
    me, other, first, second = where
    core = lax.rem(me, 2)
    partner = other(1, 0, 0)
    greet(where)
    tokens, model = x_ref.shape
    seq_len, head_dim = k_ref.shape
    qw = heads * head_dim
    rows_own, hid = wg_ref.shape[0], w1_ref.shape[1]
    tok_of = lambda d: pl.ds(pl.multiple_of(d * tokens, tokens), tokens)
    cols_of = lambda d: pl.ds(pl.multiple_of(d * rows_own, rows_own), rows_own)
    hid_of = lambda d: pl.ds(pl.multiple_of(d * hid, hid), hid)
    peers = [other(r & 1, (r >> 1) & 1, r >> 2) for r in (6, 2, 4, 7, 3, 5, 1)]

    def to_all(src_of, dst, seven, sems):
        copies = [pltpu.make_async_remote_copy(
            src_ref=src_of(dest), dst_ref=dst, send_sem=sems[0], recv_sem=sems[1],
            device_id=(dest,), device_id_type=MESH) for dest in peers]
        for copy in copies:
            copy.start()
        return pltpu.make_async_remote_copy(src_ref=seven, dst_ref=seven, send_sem=sems[0], recv_sem=sems[1],
                                            device_id=(partner,), device_id_type=MESH)

    q_of = lambda d: pl.ds(pl.multiple_of(d * qw, qw), qw)
    kv_of = lambda d: pl.ds(pl.multiple_of(d * head_dim, head_dim), head_dim)
    seven_rows = pl.ds(0, 7 * rows_own)
    x_gather = Gather(lambda d: x_all.at[tok_of(d), :], x_send, x_recv, where, x_all.at[pl.ds(0, 7 * tokens), :], own=x_ref)
    x_gather.start()
    relay(where, entry, 0)
    slices = []
    for i, (src, rows, low, high) in enumerate(((wq_ref, q_of, 0, qw), (wk_ref, kv_of, qw, qw + head_dim),
                                                (wv_ref, kv_of, qw + head_dim, qw + 2 * head_dim))):
        slices.append(to_all(lambda dest: src.at[rows(dest), :], w_head.at[low:high, cols_of(me)],
                             w_head.at[low:high, seven_rows], (w_send.at[i], w_recv.at[i])))
    for copy in tiny:
        copy.wait()
    gain_ref[...] = jnp.zeros_like(gain_ref)
    gain_ref[0:1, :] = gain1_ref[...].astype(F32).reshape(1, -1)
    gain_ref[1:2, :] = gain2_ref[...].astype(F32).reshape(1, -1)
    gain_ref[2:3, :] = pos_ref[...].astype(F32).reshape(1, -1)
    small = [to_all(lambda dest: gain_ref, gain_all.at[me], gain_all.at[pl.ds(0, 7)], (g_send.at[0], g_recv.at[0]))]
    wo_gather = Gather(lambda d: wo_all.at[cols_of(d), :], wo_send, wo_recv, where, wo_all.at[pl.ds(0, 7 * rows_own), :], own=wo_ref)
    bulk, parts = [], []
    quarter = rows_own // 4
    for mat, (src, dst) in enumerate(((wg_ref, w1_ref), (wu_ref, w3_ref))):
        for low, high in ((0, 16), (16, quarter), (quarter, 2 * quarter), (2 * quarter, 3 * quarter), (3 * quarter, rows_own)):
            parts.append(range(len(bulk), len(bulk) + len(peers)))
            for dest in peers:
                bulk.append(pltpu.make_async_remote_copy(
                    src_ref=src.at[pl.ds(low, high - low), hid_of(dest)],
                    dst_ref=dst.at[pl.ds(pl.multiple_of(me * rows_own + low, 16), high - low), :],
                    send_sem=bulk_send.at[mat], recv_sem=bulk_recv.at[mat], device_id=(dest,), device_id_type=MESH))

    def start_bulk(*which):
        for part in which:
            for i in parts[part]:
                bulk[i].start()
    start_bulk(0)

    stores = [pltpu.make_async_copy(src, dst, st_sem.at[i]) for i, (src, dst) in enumerate((
        (q_ref, q_hbm), (k_ref, k_hbm), (v_ref, v_hbm), (ot_ref, ot_hbm), (ut_ref, ut_hbm), (cos_ref, cos_hbm),
        (sin_ref, sin_hbm), (gfull_ref, gfull_hbm), (h_ref, h_hbm)))]
    own = [pltpu.make_async_copy(src, dst, own_sem.at[i]) for i, (src, dst) in enumerate((
        (gain_ref, gain_all.at[me]), (wq_ref.at[q_of(me), :], w_head.at[0:qw, cols_of(me)]),
        (wk_ref.at[kv_of(me), :], w_head.at[qw:qw + head_dim, cols_of(me)]),
        (wv_ref.at[kv_of(me), :], w_head.at[qw + head_dim:, cols_of(me)]),
        (x_ref, x_all.at[tok_of(me), :]), (wo_ref, wo_all.at[cols_of(me), :])))]
    for copy in own:
        copy.start()
    local = []
    for i, (src, dst) in enumerate(((wg_ref, w1_ref), (wu_ref, w3_ref))):
        local.append((pltpu.make_async_copy(src.at[:, hid_of(me)], stage.at[i], loc_sem.at[i]),
                      pltpu.make_async_copy(stage.at[i], dst.at[cols_of(me), :], loc_sem.at[2 + i])))
        local[-1][0].start()
    for load, store in local:
        load.wait()
        store.start()
    for copy in own:
        copy.wait()
    for copy in small:
        copy.wait_recv()
    for d in range(8):
        gfull_ref[:, d * rows_own:(d + 1) * rows_own] = gain_all[d]
    for copy in slices:
        copy.wait_recv()

    def use(d):
        base = pl.multiple_of(d * tokens, tokens)

        def norm(k, _):
            part = pl.ds(pl.multiple_of(k * 16, 16), 16)
            x_part = x_all[pl.ds(pl.multiple_of(base + k * 16, 16), 16), :].astype(F32)
            u_blk[part, :] = norm_forward(x_part, gfull_ref[0:1, :]).astype(BF16)
            return 0
        lax.fori_loop(0, tokens // 16, norm, 0)
        ut_ref[:, tok_of(d)] = u_blk[:, cols_of(me)].T
        qkv_blk[...] = dot(u_blk[...], w_head[...], 1, 1).astype(BF16)
        half = tokens // 2
        where_to = gain_all[d, 2:3, :]
        lanes = lax.broadcasted_iota(jnp.int32, (half, 2 * head_dim), 1)
        by_row = lambda lo: jnp.broadcast_to(where_to[:, lo:lo + half], (2 * head_dim, half)).T
        angles = jnp.where(lanes < head_dim, by_row(0), by_row(half)) * freq_ref[...]
        packed = jnp.where(lax.rem(lanes, head_dim) < head_dim // 2, jnp.cos(angles), jnp.sin(angles))
        for part in range(2):
            rows = pl.ds(pl.multiple_of(base + part * half, half), half)
            cos_blk, sin_blk = spread_tables(packed, part == 1)
            cos_ref[rows, :] = cos_blk
            sin_ref[rows, :] = sin_blk
            source = slice(part * half, (part + 1) * half)
            for pair in range(heads // 2):
                turned = turn_halves(qkv_blk[source, pair * 128:(pair + 1) * 128].astype(F32), cos_blk, sin_blk).astype(BF16)
                q_ref[2 * pair, rows, :] = turned[:, :head_dim]
                q_ref[2 * pair + 1, rows, :] = turned[:, head_dim:]
            turned = turn_halves(qkv_blk[source, qw:].astype(F32), cos_blk, sin_blk).astype(BF16)
            k_ref[rows, :] = turned[:, :head_dim]
            v_ref[rows, :] = qkv_blk[source, qw + head_dim:]

    x_gather.got_first()
    x_gather.got_second()
    wo_gather.start()
    start_bulk(1, 2, 3)
    x_gather.got_partner(0)

    def use_near(i, _):
        use(jnp.where(i == 0, me, jnp.where(i == 1, first, jnp.where(i == 2, second, partner))))
        return 0
    lax.fori_loop(0, 4, use_near, 0)
    x_gather.got_diag()
    for i in range(1, 4):
        x_gather.got_partner(i)

    def use_far(i, _):
        use(jnp.where(i == 0, other(0, 1, 1), jnp.where(i == 1, other(1, 1, 0), jnp.where(i == 2, other(1, 0, 1), other(1, 1, 1)))))
        return 0
    lax.fori_loop(0, 4, use_far, 0)

    def one_head(h, _):
        for start in range(0, seq_len, BLK):
            keys, rows = pl.ds(0, start + BLK), pl.ds(start, BLK)
            probs = probs_transposed(k_ref[keys, :], q_ref[h, rows, :], start)
            o_scr[h, rows, :] = dot(probs.astype(BF16), v_ref[keys, :], 0, 0).astype(BF16)
        return 0
    for i in (0, 1, 2, 4, 5, 6, 7):
        stores[i].start()
    lax.fori_loop(0, heads, one_head, 0)
    for h in range(heads):
        o_own[:, h * head_dim:(h + 1) * head_dim] = o_scr[h]
    o_gather = Gather(lambda d: o_all.at[:, cols_of(d)], o_send, o_recv, where, o_all.at[:, pl.ds(0, 7 * rows_own)], own=o_own)
    o_gather.start()
    wo_gather.got_first()
    wo_gather.got_second()
    start_bulk(4)
    o_all[:, cols_of(me)] = o_own[...]

    def turn_out(k, _):
        rows = tok_of(k)
        ot_ref[:, rows] = o_own[rows, :].T
        return 0
    lax.fori_loop(0, 8, turn_out, 0)
    stores[3].start()
    wo_gather.got_diag()
    for i in range(4):
        wo_gather.got_partner(i)
    o_gather.got_first()
    o_gather.got_second()
    start_bulk(5, 6)
    o_gather.got_partner(0)
    o_gather.got_diag()
    for i in range(1, 4):
        o_gather.got_partner(i)
    start_bulk(7, 8, 9)

    def rows_at(i):
        flips = lambda a, b: other(0, a, b)
        return tok_of(jnp.where(i == 0, me, jnp.where(i == 1, flips(1, 0), jnp.where(i == 2, flips(0, 1), flips(1, 1)))))

    def give(i):
        slot = lax.rem(i, 2)
        rows = rows_at(i)
        return (pltpu.make_async_copy(m_out.at[slot], m_ref.at[rows, :], m_loc.at[slot]),
                pltpu.make_async_remote_copy(src_ref=m_out.at[slot], dst_ref=m_ref.at[rows, :], send_sem=m_send.at[i],
                                             recv_sem=m_recv.at[i], device_id=(partner,), device_id_type=MESH))

    def hidden_block(i, _):
        rows = rows_at(i)
        base = rows.start
        slot = lax.rem(i, 2)

        @pl.when(i >= 2)
        def _():
            to_hbm, to_partner = give(i - 2)
            to_hbm.wait()
            to_partner.wait_send()

        def chunk(j, _):
            cols = pl.ds(pl.multiple_of(j * 256, 256), 256)
            h_scr[:, cols] = dot(o_all[rows, :], wo_all[:, cols], 1, 0)
            return 0
        lax.fori_loop(0, model // 256, chunk, 0)

        def norm(k, _):
            part = pl.ds(pl.multiple_of(k * 16, 16), 16)
            x_part = x_all[pl.ds(pl.multiple_of(base + k * 16, 16), 16), :].astype(F32)
            hidden = (x_part + h_scr[part, :]).astype(BF16)

            @pl.when(i == 0)
            def _():
                h_ref[part, :] = hidden
            m_out[slot, part, :] = norm_forward(hidden.astype(F32), gfull_ref[1:2, :]).astype(BF16)
            return 0
        lax.fori_loop(0, tokens // 16, norm, 0)
        for copy in give(i):
            copy.start()
        return 0
    lax.fori_loop(0, 4, hidden_block, 0)
    stores[8].start()
    for i in range(4):
        give(i)[1].wait_recv()
    for i in range(2, 4):
        give(i)[0].wait()
        give(i)[1].wait_send()
    for copy in small + slices:
        copy.wait_send()
    for gather in (x_gather, wo_gather, o_gather):
        gather.drain()
    for load, store in local:
        store.wait()
    for copy in stores:
        copy.wait()
    for mat, dst in enumerate((w1_ref, w3_ref)):
        seven = dst.at[pl.ds(0, 7 * rows_own), :]
        pltpu.make_async_remote_copy(src_ref=seven, dst_ref=seven, send_sem=bulk_send.at[mat], recv_sem=bulk_recv.at[mat],
                                     device_id=(partner,), device_id_type=MESH).wait()


def attention_step(heads, x_in, positions, gain1, gain2, w_q, w_k, w_v, wo_own, w_gate, w_up):
    tokens, model = x_in.shape
    seq_len = 8 * tokens
    head_dim = wo_own.shape[0] // heads
    rows_own, hid = w_gate.shape[0], w_gate.shape[1] // 8
    shape = jax.ShapeDtypeStruct
    hbm = pl.BlockSpec(memory_space=pl.ANY)
    dma = pltpu.SemaphoreType.DMA
    vm = lambda *dims, dtype=BF16: pltpu.VMEM(dims, dtype)
    steps = np.arange(head_dim // 2, dtype=np.float32) * np.float32(2.0 / head_dim)
    freq = np.tile(np.float32(1.0) / (np.float32(ROPE_BASE) ** steps), 4)[None]
    outs = (shape((heads, seq_len, head_dim), BF16), shape((seq_len, head_dim), BF16), shape((seq_len, head_dim), BF16),
            shape((heads * head_dim, seq_len), BF16), shape((rows_own, seq_len), BF16),
            shape((seq_len, 128), F32), shape((seq_len, 128), F32), shape((8, model), F32), shape((tokens, model), BF16))
    pairs = [dma((1,)), dma((1,)), dma((3,)), dma((3,)), dma((1,)), dma((7,)), dma((1,)), dma((7,)),
             dma((2,)), dma((2,)), dma((1,)), dma((7,))]
    return pl.pallas_call(
        functools.partial(attention_comm_kernel, 'sp', heads), name='attention_comm',
        in_specs=[hbm] * 11, out_specs=[hbm] * 12,
        out_shape=[*outs, shape((seq_len, model), BF16), shape((model, hid), BF16), shape((model, hid), BF16)],
        scratch_shapes=[vm(*t.shape, dtype=t.dtype) for t in outs] + [
            vm(tokens, dtype=jnp.int32), vm(rows_own), vm(rows_own), vm(1, 2 * head_dim, dtype=F32),
            vm(8, rows_own, dtype=F32), vm(seq_len, model), vm(8, 8, rows_own, dtype=F32),
            vm(384, model), vm(model, model), vm(seq_len, model), vm(tokens, model), vm(tokens, 384), vm(heads, seq_len, head_dim),
            vm(seq_len, heads * head_dim), vm(tokens, model, dtype=F32), vm(2, tokens, model), vm(2, rows_own, hid)] + pairs + [
            dma((2,)), dma((4,)), dma((4,)), dma((4,)), dma((12,)), dma((9,)), pltpu.SemaphoreType.REGULAR((4,))],
        compiler_params=pltpu.CompilerParams(collective_id=0, has_side_effects=True, vmem_limit_bytes=63 * 1024 * 1024),
    )(x_in, positions, gain1, gain2, jnp.asarray(freq), w_q, w_k, w_v, wo_own, w_gate, w_up)


def hand_over_kernel(n_in, *refs):
    sources, gains, results = refs[:n_in], refs[n_in], refs[n_in + 1:2 * n_in + 1]
    gain_outs, lines, sem = refs[2 * n_in + 1:2 * n_in + 3], refs[2 * n_in + 3:2 * n_in + 5], refs[2 * n_in + 5]
    stores = []
    for i, (src, dst) in enumerate(zip(sources, results)):
        rows = max(16, min(src.shape[0], (1 << 21) // (src.shape[1] * src.dtype.itemsize)))
        for low in range(0, src.shape[0], rows):
            pltpu.make_async_copy(src.at[pl.ds(low, rows)], dst.at[pl.ds(low, rows)], sem.at[i]).start()
        stores.append(pltpu.make_async_copy(src, dst, sem.at[i]))
    for i in range(2):
        lines[i][...] = gains[i, :]
        stores.append(pltpu.make_async_copy(lines[i], gain_outs[i], sem.at[n_in + i]))
        stores[-1].start()
    for store in stores:
        store.wait()


def hand_over(arrays, gains):
    shape = jax.ShapeDtypeStruct
    hbm, vmem = pl.BlockSpec(memory_space=pltpu.HBM), pl.BlockSpec(memory_space=pltpu.VMEM)
    return pl.pallas_call(
        functools.partial(hand_over_kernel, len(arrays)), name='hand_over',
        in_specs=[vmem] * (len(arrays) + 1), out_specs=[hbm] * (len(arrays) + 2),
        out_shape=[shape(a.shape, a.dtype) for a in arrays] + [shape((gains.shape[1],), F32)] * 2,
        scratch_shapes=[pltpu.VMEM((gains.shape[1],), F32)] * 2 + [pltpu.SemaphoreType.DMA((len(arrays) + 2,))],
        compiler_params=pltpu.CompilerParams(vmem_limit_bytes=1024 * 1024),
    )(*[pltpu.with_memory_space_constraint(a, pltpu.VMEM) for a in arrays + (gains,)])


def solution(mesh):
    n_dev = mesh.shape['sp']

    def layer_step(x_in, positions, d_out, norm1_gain, norm2_gain, w_q, w_k, w_v, w_o, w_gate, w_up, w_down):
        tokens, model = x_in.shape
        head_dim = w_q.shape[2]
        heads = w_q.shape[1] // n_dev
        rows_own = w_q.shape[0]
        flat = lambda w: w.transpose(1, 2, 0).reshape(-1, rows_own)
        wo_own = w_o.reshape(-1, model)
        (q_rot, k_rot, v_lin, o_t, u_t, cos_tab, sin_tab, g_full, hidden,
         mlp_in, w1, w3) = attention_step(heads, x_in, positions, norm1_gain, norm2_gain, flat(w_q), flat(w_k), flat(w_v), wo_own, w_gate, w_up)
        d_w1s, d_w3s, d_down, y_out, dh_own, d_g2, early = mlp_step(mlp_in, d_out, w1, w3, w_down, hidden, g_full)
        d_wo, d_wq_t, d_wk_t, d_wv_t, d_w1, d_w3, d_x, d_gains, d_down, y_out = attention_backward_step(
            heads, dh_own, wo_own, o_t, q_rot, k_rot, v_lin, (cos_tab, sin_tab),
            d_w1s, d_w3s, flat(w_q), flat(w_k), flat(w_v), u_t, x_in, g_full, d_g2, d_down, y_out, early)
        from_cols = lambda d, w: d.reshape(w.shape[1], w.shape[2], rows_own).transpose(2, 0, 1)
        (d_down, y_out, d_w1, d_w3, d_wo, d_wq_t, d_wk_t, d_wv_t, d_x, d_g1, d_g2) = hand_over(
            (d_down, y_out, d_w1, d_w3, d_wo, d_wq_t, d_wk_t, d_wv_t, d_x), d_gains)
        return (y_out, d_x, d_g1, d_g2, from_cols(d_wq_t, w_q), from_cols(d_wk_t, w_k), from_cols(d_wv_t, w_v),
                d_wo.reshape(w_o.shape), d_w1, d_w3, d_down)

    all_rows = P('sp')
    return jax.shard_map(layer_step, mesh=mesh, in_specs=(all_rows,) * 12, out_specs=(all_rows,) * 11, check_vma=False)
```
